8 devices in a mesh: dp: 2 (over z, y), tp: 4 (over x, core).
Axes of the slice: x: 2, y: 2, z: 1, core: 2. Of those that a mesh axis runs over, the one named last changes fastest.
Arguments:
- hidden: bfloat16 [16384, 4096], P(('dp', 'tp')), parts along dimension 0
- ln_gain: float32 [4096], replicated
- ln_bias: float32 [4096], replicated
- embed: bfloat16 [8192, 4096], P('tp')
- targets: int32 [16384], P(('dp', 'tp')), parts along dimension 0
- loss_mask: int32 [16384], P(('dp', 'tp')), parts along dimension 0
Outputs:
- output 1: float32 [16384], P(('dp', 'tp')), parts along dimension 0
- output 2: float32 [2], P('dp'), parts along dimension 0
- output 3: bfloat16 [16384, 4096], P(('dp', 'tp')), parts along dimension 0
- output 4: float32 [16384, 4096], P(('dp', 'tp')), parts along dimension 0
- output 5: float32 [8192], P('dp'), parts along dimension 0
- output 6: float32 [8192], P('dp'), parts along dimension 0
There are 2 independent parts. The reference program is written for one: setup_inputs(seed, part) draws one part's arguments, and reference() takes and returns one part's arrays. A program takes and returns all parts, laid end to end along the dimension named above; an argument that names none is the same for every part.
All inputs are finite; a program needn't handle non-finite values.
Results may differ from the reference program's by a relative error of at most 0.001.
Values are sent between devices in bfloat16 or wider.
A program may use at most 1 GiB of HBM per device.

```python
import jax
import jax.numpy as jnp
from jax import lax

TOKENS_DEV = 2048
GROUP_SIZE = 4
MODEL_DIM = 4096
VOCAB_SIZE = 8192
LN_EPS = 1e-5


def setup_inputs(seed: int = 0, part: int = 0) -> dict:
    seq_len = GROUP_SIZE * TOKENS_DEV
    part_keys = jax.random.split(jax.random.fold_in(jax.random.key(seed), part), 4)
    shared_keys = jax.random.split(jax.random.key(seed + 1), 3)
    embed_scale = 2.5 * MODEL_DIM ** -0.5
    hidden = jax.random.normal(part_keys[0], (seq_len, MODEL_DIM), jnp.float32).astype(jnp.bfloat16)
    ln_gain = 1.0 + 0.3 * jax.random.normal(shared_keys[0], (MODEL_DIM,), jnp.float32)
    ln_bias = 0.3 * jax.random.normal(shared_keys[1], (MODEL_DIM,), jnp.float32)
    embed = (embed_scale * jax.random.normal(shared_keys[2], (VOCAB_SIZE, MODEL_DIM), jnp.float32)).astype(jnp.bfloat16)
    targets = jax.random.randint(part_keys[1], (seq_len,), 0, VOCAB_SIZE, dtype=jnp.int32)
    shard_rate = jax.random.randint(part_keys[2], (GROUP_SIZE, 1), 40, 96, dtype=jnp.int32)
    draws = jax.random.randint(part_keys[3], (GROUP_SIZE, TOKENS_DEV), 0, 100, dtype=jnp.int32)
    loss_mask = (draws < shard_rate).astype(jnp.int32).reshape(seq_len)
    return {'hidden': hidden, 'ln_gain': ln_gain, 'ln_bias': ln_bias, 'embed': embed, 'targets': targets, 'loss_mask': loss_mask}


def normalize(hidden):
    h_f32 = hidden.astype(jnp.float32)
    centred = h_f32 - jnp.mean(h_f32, axis=-1, keepdims=True)
    inv_std = lax.rsqrt(jnp.mean(centred * centred, axis=-1, keepdims=True) + LN_EPS)
    return centred * inv_std, inv_std


def reference(hidden, ln_gain, ln_bias, embed, targets, loss_mask):
    seq_len = GROUP_SIZE * TOKENS_DEV
    x_hat, inv_std = normalize(hidden)
    normed = (x_hat * ln_gain + ln_bias).astype(jnp.bfloat16)
    weights = loss_mask.astype(jnp.float32)
    count = jnp.sum(weights)
    vocab_ids = jnp.arange(VOCAB_SIZE, dtype=jnp.int32)

    def block_step(embed_acc, block):
        x_blk, t_blk, w_blk = block
        logits = jnp.dot(x_blk, embed.T, preferred_element_type=jnp.float32)
        row_max = jnp.max(logits, axis=-1, keepdims=True)
        log_norm = row_max[:, 0] + jnp.log(jnp.sum(jnp.exp(logits - row_max), axis=-1))
        onehot = (vocab_ids[None, :] == t_blk[:, None]).astype(jnp.float32)
        t_logit = jnp.sum(logits * onehot, axis=-1)
        loss_blk = (log_norm - t_logit) * w_blk
        d_logits = ((jnp.exp(logits - log_norm[:, None]) - onehot) * (w_blk / count)[:, None]).astype(jnp.bfloat16)
        embed_acc = embed_acc + jnp.dot(d_logits.T, x_blk, preferred_element_type=jnp.float32)
        d_x = jnp.dot(d_logits, embed, preferred_element_type=jnp.float32)
        return embed_acc, (loss_blk, d_x)

    blocks = (normed.reshape(GROUP_SIZE, TOKENS_DEV, MODEL_DIM), targets.reshape(GROUP_SIZE, TOKENS_DEV), weights.reshape(GROUP_SIZE, TOKENS_DEV))
    d_embed, outs = lax.scan(block_step, jnp.zeros((VOCAB_SIZE, MODEL_DIM), jnp.float32), blocks)
    loss = outs[0].reshape(seq_len)
    d_normed = outs[1].reshape(seq_len, MODEL_DIM)
    mean_loss = jnp.sum(loss) / count
    d_gain = jnp.sum(d_normed * x_hat, axis=0)
    d_bias = jnp.sum(d_normed, axis=0)
    d_xhat = d_normed * ln_gain
    centre_term = jnp.mean(d_xhat, axis=-1, keepdims=True)
    proj_term = jnp.mean(d_xhat * x_hat, axis=-1, keepdims=True)
    d_hidden = (inv_std * (d_xhat - centre_term - x_hat * proj_term)).astype(jnp.bfloat16)
    return loss, mean_loss.reshape(1), d_hidden, d_embed, d_gain, d_bias
```

```python
import jax
import jax.numpy as jnp
from jax import lax
from jax.sharding import PartitionSpec as P

LN_EPS = 1e-5
E_CHUNKS = 4
X_CHUNKS = 2


def layer_norm(hidden, ln_gain, ln_bias):
    h_f32 = hidden.astype(jnp.float32)
    centred = h_f32 - jnp.mean(h_f32, axis=-1, keepdims=True)
    inv_std = lax.rsqrt(jnp.mean(centred * centred, axis=-1, keepdims=True) + LN_EPS)
    x_hat = centred * inv_std
    return x_hat, inv_std, (x_hat * ln_gain + ln_bias).astype(jnp.bfloat16)


def norm_backward(d_normed, x_hat, inv_std, ln_gain):
    value_a6 = d_normed * ln_gain
    centre_term = jnp.mean(value_a6, axis=-1, keepdims=True)
    proj_term = jnp.mean(value_a6 * x_hat, axis=-1, keepdims=True)
    return (inv_std * (value_a6 - centre_term - x_hat * proj_term)).astype(jnp.bfloat16)


def solution(mesh):
    n_dev = mesh.size

    def send(x, bit):
        return lax.ppermute(x, ('dp', 'tp'), [(i, i ^ bit) for i in range(n_dev)])

    def body(hidden, ln_gain, ln_bias, embed, targets, loss_mask):
        tokens = hidden.shape[0]
        rows = embed.shape[0]
        half = rows // 2
        chunk = half // E_CHUNKS
        grp = lax.axis_index('dp')
        rank = lax.axis_index('tp')
        core = rank % 2
        other = 2 - (rank - core)
        weights = loss_mask.astype(jnp.float32)
        count = lax.psum(jnp.sum(weights), 'tp')

        pieces = []
        for j in range(E_CHUNKS):
            mine = lax.dynamic_slice_in_dim(embed, grp * half + j * chunk, chunk)
            a = send(mine, 2)
            b = send(a, 4)
            base_a = (other + core) * rows + grp * half + j * chunk
            base_b = (other + core) * rows + (1 - grp) * half + j * chunk
            shift = (1 - 2 * core) * rows
            pieces += [(a, base_a), (b, base_b), (send(a, 1), base_a + shift), (send(b, 1), base_b + shift)]
        part_embed = send(embed, 1)

        x_hat, inv_std, normed = layer_norm(hidden, ln_gain, ln_bias)

        def grad_block(z, lse, tgt, w, base):
            ids = base + lax.broadcasted_iota(jnp.int32, (1, z.shape[1]), 1)
            onehot = (ids == tgt[:, None]).astype(jnp.float32)
            return ((jnp.exp(z - lse[:, None]) - onehot) * (w / count)[:, None]).astype(jnp.bfloat16)

        own_base = rank * rows
        part_base = own_base + (1 - 2 * core) * rows
        blocks = [(embed, own_base), (part_embed, part_base)]
        for j in range(E_CHUNKS):
            grp_pieces = pieces[4 * j:4 * j + 4]
            blocks += grp_pieces
        zs = []
        stats = []
        for e, base in blocks:
            z = jnp.einsum('sd,vd->sv', normed, e, preferred_element_type=jnp.float32)
            m = jnp.max(z, axis=-1)
            s = jnp.sum(jnp.exp(z - m[:, None]), axis=-1)
            ids = base + lax.broadcasted_iota(jnp.int32, (1, z.shape[1]), 1)
            t = jnp.sum(jnp.where(ids == targets[:, None], z, 0.0), axis=-1)
            zs.append(z)
            stats.append((m, s, t))
        gmax = jnp.max(jnp.stack([m for m, _, _ in stats]), axis=0)
        total = sum(s * jnp.exp(m - gmax) for m, s, _ in stats)
        t_logit = sum(t for _, _, t in stats)
        lse = gmax + jnp.log(total)
        loss = (lse - t_logit) * weights
        mean_loss = lax.psum(jnp.sum(loss), 'tp') / count

        def hop(bit):
            return tuple(send(v, bit) for v in (lse, targets, weights))
        part_info = hop(1)
        rem_info = hop(2)
        remp_info = tuple(send(v, 1) for v in rem_info)

        xc = tokens // X_CHUNKS
        rem_x = [send(normed[k * xc:(k + 1) * xc], 2) for k in range(X_CHUNKS)]
        remp_x = [send(v, 1) for v in rem_x]
        part_x = send(normed, 1)

        dzs = [grad_block(z, lse, targets, weights, base) for z, (_, base) in zip(zs, blocks)]
        dz_from_part = send(dzs[1], 1)
        d_normed = sum(jnp.einsum('sv,vd->sd', dz, e, preferred_element_type=jnp.float32) for dz, (e, _) in zip(dzs, blocks))
        d_embed = jnp.einsum('sv,sd->vd', dzs[0], normed, preferred_element_type=jnp.float32)
        d_embed += jnp.einsum('sv,sd->vd', dz_from_part, part_x, preferred_element_type=jnp.float32)
        for k in range(X_CHUNKS):
            for x, info in ((rem_x[k], rem_info), (remp_x[k], remp_info)):
                l, t, w = (v[k * xc:(k + 1) * xc] for v in info)
                z = jnp.einsum('sd,vd->sv', x, embed, preferred_element_type=jnp.float32)
                dz = grad_block(z, l, t, w, own_base)
                d_embed += jnp.einsum('sv,sd->vd', dz, x, preferred_element_type=jnp.float32)
        norm_grads = lax.psum(jnp.stack([jnp.sum(d_normed * x_hat, axis=0), jnp.sum(d_normed, axis=0)]), 'tp')
        d_hidden = norm_backward(d_normed, x_hat, inv_std, ln_gain)
        return loss, mean_loss.reshape(1), d_hidden, d_embed, norm_grads[0], norm_grads[1]

    token_rows = P(('dp', 'tp'))
    token_mat = P(('dp', 'tp'), None)
    return jax.shard_map(body, mesh=mesh, in_specs=(token_mat, P(), P(), P('tp', None), token_rows, token_rows), out_specs=(token_rows, P('dp'), token_mat, token_mat, P('dp'), P('dp')), check_vma=False)
```

```python
import functools

import jax
import jax.numpy as jnp
from jax import lax
from jax.experimental import pallas as pl
from jax.experimental.pallas import tpu as pltpu
from jax.sharding import PartitionSpec as P

LN_EPS = 1e-5
LOWEST = float(jnp.finfo(jnp.float32).min)

TOK = 2048
ROWS = 2048
DIM = 4096
VOCAB = 8192
TILE = 512
TILES = VOCAB // TILE
HB = 1024
HBS = TOK // HB
CHUNK = 64
CHUNKS = ROWS // 2 // CHUNK
LN_ROWS = 256
STAT_ROWS = 16
NT = (((1,), (1,)), ((), ()))


def peers():
    dp, tp = lax.axis_index('dp'), lax.axis_index('tp')
    core = lax.rem(tp, 2)
    pair = tp - core
    other = 2 - pair
    part = pair + 1 - core
    return dp, tp, (dp, part), (dp, other + core), (dp, other + 1 - core), (1 - dp, tp)


def remote(src, dst, ssem, rsem, dev):
    return pltpu.make_async_remote_copy(
        src_ref=src, dst_ref=dst, send_sem=ssem, recv_sem=rsem, device_id=dev, device_id_type=pl.DeviceIdType.MESH)


def gather_logits_kernel(hid, gain, bias, emb, tcol, info, e_all, x_out, z_out, stat_all, info_all,
                         xs, hbuf, ebuf, z0, z1, tc_v, m_s, s_s, t_s, info_v, stat_v,
                         h_sem, xo_sem, e_sem, eo_sem, z_sem, small_sem,
                         xs_send, ys_send, ds_send, pe_send, sm_send,
                         x_recv, y_recv, d_recv, pe_recv, info_recv, stat_recv):
    dp, tp, part, xp, xq, yp = peers()
    barrier = pltpu.get_barrier_semaphore()
    for dev in (part, xp, xq, yp):
        pl.semaphore_signal(barrier, inc=1, device_id=dev, device_id_type=pl.DeviceIdType.MESH)
    pl.semaphore_wait(barrier, 4)

    def tile_row(j):
        return ROWS * 2 + (j // 2) * TILE + lax.rem(j, 2) * CHUNK

    def x_copy(j):
        src = emb.at[pl.ds(pl.multiple_of(dp * (ROWS // 2) + j * CHUNK, CHUNK), CHUNK)]
        return remote(src, e_all.at[pl.ds(pl.multiple_of(tile_row(j), CHUNK), CHUNK)], xs_send, x_recv.at[j], xp)

    def piece(j, p):
        return e_all.at[pl.ds(pl.multiple_of(tile_row(j) + p * 2 * CHUNK, CHUNK), CHUNK)]

    def y_copy(j):
        return remote(piece(j, 0), piece(j, 1), ys_send, y_recv.at[j], yp)

    def d_copy(j, p):
        return remote(piece(j, p), piece(j, p + 2), ds_send, d_recv.at[j // 2], part)

    def pe_copy(i):
        return remote(emb.at[pl.ds(pl.multiple_of(i * TILE, TILE), TILE)],
                      e_all.at[pl.ds(pl.multiple_of(ROWS + i * TILE, TILE), TILE)], pe_send, pe_recv.at[i], part)

    cp = pltpu.make_async_copy(info, info_v, small_sem.at[0])
    cp.start()
    tcp = pltpu.make_async_copy(tcol, tc_v, small_sem.at[1])
    tcp.start()

    def h_copy(i):
        return pltpu.make_async_copy(hid.at[pl.ds(pl.multiple_of(i * LN_ROWS, LN_ROWS), LN_ROWS)], hbuf.at[lax.rem(i, 2)], h_sem.at[lax.rem(i, 2)])
    h_copy(0).start()

    for p, dev in ((1, part), (2, xp), (3, xq)):
        remote(info, info_all.at[p], sm_send, info_recv.at[p], dev).start()

    def start_x(j, c):
        x_copy(j).start()
        return c
    lax.fori_loop(0, CHUNKS, start_x, 0)

    def start_pe(i, c):
        pe_copy(i).start()
        return c
    lax.fori_loop(0, ROWS // TILE, start_pe, 0)

    def e_load(t):
        slot = lax.rem(t, 2)
        return pltpu.make_async_copy(e_all.at[pl.ds(pl.multiple_of(t * TILE, TILE), TILE)], ebuf.at[slot], e_sem.at[slot])

    def e_load_own(t):
        slot = lax.rem(t, 2)
        return pltpu.make_async_copy(emb.at[pl.ds(pl.multiple_of(t * TILE, TILE), TILE)], ebuf.at[slot], e_sem.at[slot])
    e_load_own(0).start()

    cp.wait()
    pltpu.make_async_copy(info_v, info_all.at[0], small_sem.at[0]).start()
    g_row = gain[...]
    b_row = bias[...]

    def ln_tile(i, c):
        @pl.when(i + 1 < TOK // LN_ROWS)
        def _():
            h_copy(i + 1).start()
        h_copy(i).wait()

        def ln_rows(r, c2):
            h = hbuf[lax.rem(i, 2), pl.ds(pl.multiple_of(r * 32, 32), 32), :].astype(jnp.float32)
            mean = jnp.mean(h, axis=-1, keepdims=True)
            centred = h - mean
            rstd = lax.rsqrt(jnp.mean(centred * centred, axis=-1, keepdims=True) + LN_EPS)
            row = pl.multiple_of(i * LN_ROWS + r * 32, 32)
            xs[pl.ds(row, 32), :] = (centred * rstd * g_row + b_row).astype(jnp.bfloat16)
            return c2
        lax.fori_loop(0, LN_ROWS // 32, ln_rows, 0)
        rows = pl.ds(pl.multiple_of(i * LN_ROWS, LN_ROWS), LN_ROWS)
        pltpu.make_async_copy(xs.at[rows], x_out.at[rows], xo_sem).start()
        return c
    lax.fori_loop(0, TOK // LN_ROWS, ln_tile, 0)

    m_s[...] = jnp.full((TOK, 128), LOWEST, jnp.float32)
    s_s[...] = jnp.zeros((TOK, 128), jnp.float32)
    t_s[...] = jnp.zeros((TOK, 128), jnp.float32)
    tcp.wait()

    zs = (z0, z1)

    def product(t, h):
        zs[h][...] = lax.dot_general(xs[h * HB:(h + 1) * HB, :], ebuf[lax.rem(t, 2)], NT, preferred_element_type=jnp.float32)

    def statistics(t, h):
        z = zs[h]
        lane = lax.broadcasted_iota(jnp.int32, (STAT_ROWS, 128), 1)
        for r in range(0, HB, STAT_ROWS):
            rows = slice(h * HB + r, h * HB + r + STAT_ROWS)
            zk = [z[r:r + STAT_ROWS, k * 128:(k + 1) * 128] for k in range(TILE // 128)]
            old = m_s[rows, :]
            new = jnp.maximum(jnp.maximum(jnp.maximum(zk[0], zk[1]), jnp.maximum(zk[2], zk[3])), old)
            tot = s_s[rows, :] * jnp.exp(old - new)
            tgt = t_s[rows, :]
            diff = tc_v[rows, :] - t * TILE
            for k in range(TILE // 128):
                tot = tot + jnp.exp(zk[k] - new)
                tgt = tgt + jnp.where(diff == lane + k * 128, zk[k], 0.0)
            m_s[rows, :] = new
            s_s[rows, :] = tot
            t_s[rows, :] = tgt

    def z_copy(t, h):
        return pltpu.make_async_copy(
            zs[h], z_out.at[pl.ds(h * HB, HB), pl.ds(pl.multiple_of(t * TILE, TILE), TILE)], z_sem.at[h])

    def x_event(j):
        x_copy(j).wait_recv()
        y_copy(j).start()
        d_copy(j, 0).start()

    def y_event(j):
        y_copy(j).wait_recv()
        d_copy(j, 1).start()

    def p_event(k):
        rows = e_all.at[pl.ds(pl.multiple_of(2 * ROWS + k * TILE + TILE // 2, TILE // 2), TILE // 2)]
        pltpu.make_async_copy(rows, rows, d_recv.at[k]).wait()
        e_load(8 + k).start()

    half_tiles = TILES // 2

    def start_events(t):
        @pl.when(t < TILES - 1)
        def _():
            x_event(t)

        @pl.when(t == TILES - 2)
        def _():
            y_event(TILES - 3)
            p_event(6)

        @pl.when(t == TILES - 1)
        def _():
            y_event(TILES - 2)
            y_event(TILES - 1)
            p_event(7)
        e_load(t).wait()

        @pl.when(t < 4)
        def _():
            slot = lax.rem(t, 2)
            pltpu.make_async_copy(ebuf.at[slot], e_all.at[pl.ds(pl.multiple_of(t * TILE, TILE), TILE)], eo_sem.at[slot]).start()

    def middle_events(t):
        @pl.when((t >= 1) & (t < TILES - 2))
        def _():
            y_event(t - 1)

        @pl.when((t >= 1) & (t < 5))
        def _():
            slot = lax.rem(t - 1, 2)
            pltpu.make_async_copy(ebuf.at[slot], e_all.at[pl.ds(0, TILE)], eo_sem.at[slot]).wait()

        @pl.when(t < 3)
        def _():
            e_load_own(t + 1).start()

        @pl.when((t >= 3) & (t < 7))
        def _():
            pe_copy(t - 3).wait_recv()
            e_load(t + 1).start()

        @pl.when((t >= half_tiles - 1) & (t < TILES - 3))
        def _():
            p_event(t - (half_tiles - 1))

        @pl.when(t == TILES - 2)
        def _():
            x_event(TILES - 1)

    start_events(0)
    product(0, 0)

    def step(t, c):
        z_copy(t, 0).start()
        middle_events(t)

        @pl.when(t > 0)
        def _():
            z_copy(t - 1, 1).wait()
        product(t, 1)
        statistics(t, 0)
        start_events(t + 1)
        z_copy(t, 1).start()
        z_copy(t, 0).wait()
        product(t + 1, 0)
        statistics(t, 1)
        return c
    last = TILES - 1
    lax.fori_loop(0, last, step, 0)
    z_copy(last, 0).start()
    z_copy(last - 1, 1).wait()
    statistics(last, 0)
    product(last, 1)
    z_copy(last, 1).start()
    statistics(last, 1)

    def finish(i, c):
        for u in range(4):
            r = i * 4 + u
            rows = pl.ds(pl.multiple_of(r * 128, 128), 128)
            m = m_s[rows, :]
            top = jnp.max(m, axis=-1, keepdims=True)
            tot = jnp.sum(s_s[rows, :] * jnp.exp(m - top), axis=-1, keepdims=True)
            lse = jnp.broadcast_to(top + jnp.log(tot), (128, 128))
            tgt = jnp.broadcast_to(jnp.sum(t_s[rows, :], axis=-1, keepdims=True), (128, 128))
            stat_v[0, pl.ds(r, 1), :] = jnp.transpose(lse)[0:1, :]
            stat_v[1, pl.ds(r, 1), :] = jnp.transpose(tgt)[0:1, :]
        return c
    lax.fori_loop(0, TOK // 512, finish, 0)
    own = pltpu.make_async_copy(stat_v, stat_all.at[0], small_sem.at[1])
    own.start()
    for p, dev in ((1, part), (2, xp), (3, xq)):
        remote(stat_v, stat_all.at[p], sm_send, stat_recv.at[p], dev).start()

    own.wait()
    pltpu.make_async_copy(info_v, info_all.at[0], small_sem.at[0]).wait()
    for h in range(2):
        z_copy(last, h).wait()
    pltpu.make_async_copy(xs, x_out, xo_sem).wait()
    half = e_all.at[pl.ds(0, ROWS // 2)]
    pltpu.make_async_copy(half, half, xs_send).wait()
    pltpu.make_async_copy(half, half, ys_send).wait()
    full = e_all.at[pl.ds(0, ROWS)]
    pltpu.make_async_copy(full, full, ds_send).wait()
    pltpu.make_async_copy(full, full, pe_send).wait()
    for p, dev in ((1, part), (2, xp), (3, xq)):
        remote(info, info_all.at[p], sm_send, info_recv.at[p], dev).wait()
        remote(stat_v, stat_all.at[p], sm_send, stat_recv.at[p], dev).wait()


def gather_logits(hidden, gain, bias, embed, tcol, info):
    any_spec = pl.BlockSpec(memory_space=pl.ANY)
    vmem_spec = pl.BlockSpec(memory_space=pltpu.VMEM)
    f32, bf16, i32 = jnp.float32, jnp.bfloat16, jnp.int32
    dma = pltpu.SemaphoreType.DMA
    groups = TOK // 128
    return pl.pallas_call(
        gather_logits_kernel,
        name="gather_logits",
        out_shape=(
            jax.ShapeDtypeStruct((VOCAB, DIM), bf16),
            jax.ShapeDtypeStruct((TOK, DIM), bf16),
            jax.ShapeDtypeStruct((TOK, VOCAB), f32),
            jax.ShapeDtypeStruct((4, 2, groups, 128), f32),
            jax.ShapeDtypeStruct((4, 2, groups, 128), i32),
        ),
        in_specs=[any_spec, vmem_spec, vmem_spec, any_spec, any_spec, any_spec],
        out_specs=[any_spec] * 5,
        scratch_shapes=[
            pltpu.VMEM((TOK, DIM), bf16),
            pltpu.VMEM((2, LN_ROWS, DIM), bf16),
            pltpu.VMEM((2, TILE, DIM), bf16),
            pltpu.VMEM((HB, TILE), f32),
            pltpu.VMEM((HB, TILE), f32),
            pltpu.VMEM((TOK, 128), i32),
            pltpu.VMEM((TOK, 128), f32),
            pltpu.VMEM((TOK, 128), f32),
            pltpu.VMEM((TOK, 128), f32),
            pltpu.VMEM((2, groups, 128), i32),
            pltpu.VMEM((2, groups, 128), f32),
            dma((2,)), dma, dma((2,)), dma((2,)), dma((2,)), dma((2,)),
            dma, dma, dma, dma, dma,
            dma((CHUNKS,)), dma((CHUNKS,)), dma((TILES // 2,)), dma((4,)), dma((4,)), dma((4,)),
        ],
        compiler_params=pltpu.CompilerParams(collective_id=0, has_side_effects=True, vmem_limit_bytes=60 * 1024 * 1024),
        cost_estimate=pl.CostEstimate(flops=2 * TOK * VOCAB * DIM, bytes_accessed=300 * 2 ** 20, transcendentals=TOK * VOCAB),
    )(hidden, gain, bias, embed, tcol, info)


def layer_norm_parts(hidden):
    h_f32 = hidden.astype(jnp.float32)
    centred = h_f32 - jnp.mean(h_f32, axis=-1, keepdims=True)
    inv_std = lax.rsqrt(jnp.mean(centred * centred, axis=-1, keepdims=True) + LN_EPS)
    return centred * inv_std, inv_std


def norm_backward(d_normed, x_hat, inv_std, ln_gain):
    value_a6 = d_normed * ln_gain
    centre_term = jnp.mean(value_a6, axis=-1, keepdims=True)
    proj_term = jnp.mean(value_a6 * x_hat, axis=-1, keepdims=True)
    return (inv_std * (value_a6 - centre_term - x_hat * proj_term)).astype(jnp.bfloat16)


def solution(mesh):
    def body(hidden, ln_gain, ln_bias, embed, targets, loss_mask):
        dp, rank = lax.axis_index('dp'), lax.axis_index('tp')
        shard = targets // ROWS
        block = jnp.bitwise_xor(shard, rank)
        row = targets % ROWS
        half = row // (ROWS // 2)
        sub = row % (ROWS // 2)
        piece = (block - 2) * 2 + jnp.bitwise_xor(half, dp)
        far = 2 * ROWS + (sub // 128) * TILE + piece * 128 + sub % 128
        tcol = jnp.where(block < 2, block * ROWS + row, far)
        info = jnp.stack([targets, loss_mask]).reshape(2, TOK // 128, 128)
        e_all, normed, logits, stat_all, info_all = gather_logits(
            hidden, ln_gain.reshape(1, DIM), ln_bias.reshape(1, DIM), embed, jnp.broadcast_to(tcol[:, None], (TOK, 128)), info)
        stat_all = stat_all.reshape(4, 2, TOK)
        info_all = info_all.reshape(4, 2, TOK)
        weights = info_all[:, 1].astype(jnp.float32)
        count = jnp.sum(weights)
        scale = weights / count
        all_loss = (stat_all[:, 0] - stat_all[:, 1]) * weights
        loss = all_loss[0]
        mean_loss = jnp.sum(all_loss) / count
        lse = stat_all[:, 0]
        tgt = info_all[:, 0]

        x_all = lax.all_gather(normed, 'tp', tiled=True)
        cols = lax.broadcasted_iota(jnp.int32, (1, VOCAB), 1)
        onehot = (cols == tcol[:, None]).astype(jnp.float32)
        d_logits = ((jnp.exp(logits - lse[0][:, None]) - onehot) * scale[0][:, None]).astype(jnp.bfloat16)
        d_normed = jnp.einsum('sv,vd->sd', d_logits, e_all, preferred_element_type=jnp.float32)
        dz_part = lax.ppermute(d_logits[:, ROWS:2 * ROWS], ('dp', 'tp'), [(i, i ^ 1) for i in range(mesh.size)])
        core = rank % 2
        pair = rank - core

        def pick(k):
            return lax.dynamic_slice_in_dim(x_all, jnp.bitwise_xor(rank, k) * TOK, TOK)
        d_embed = jnp.einsum('sv,sd->vd', d_logits[:, :ROWS], normed, preferred_element_type=jnp.float32)
        d_embed += jnp.einsum('sv,sd->vd', dz_part, pick(1), preferred_element_type=jnp.float32)
        ids = rank * ROWS + lax.broadcasted_iota(jnp.int32, (1, ROWS), 1)
        for k in (2, 3):
            x = pick(k)
            z = jnp.einsum('sd,vd->sv', x, embed, preferred_element_type=jnp.float32)
            hot = (ids == tgt[k][:, None]).astype(jnp.float32)
            dz = ((jnp.exp(z - lse[k][:, None]) - hot) * scale[k][:, None]).astype(jnp.bfloat16)
            d_embed += jnp.einsum('sv,sd->vd', dz, x, preferred_element_type=jnp.float32)
        x_hat, inv_std = layer_norm_parts(hidden)
        norm_grads = lax.psum(jnp.stack([jnp.sum(d_normed * x_hat, axis=0), jnp.sum(d_normed, axis=0)]), 'tp')
        d_hidden = norm_backward(d_normed, x_hat, inv_std, ln_gain)
        return loss, mean_loss.reshape(1), d_hidden, d_embed, norm_grads[0], norm_grads[1]

    token_rows = P(('dp', 'tp'))
    token_mat = P(('dp', 'tp'), None)
    return jax.shard_map(body, mesh=mesh, in_specs=(token_mat, P(), P(), P('tp', None), token_rows, token_rows), out_specs=(token_rows, P('dp'), token_mat, token_mat, P('dp'), P('dp')), check_vma=False)
```

```python
import functools

import jax
import jax.numpy as jnp
from jax import lax
from jax.experimental import pallas as pl
from jax.experimental.pallas import tpu as pltpu
from jax.sharding import PartitionSpec as P

LN_EPS = 1e-5
LOWEST = float(jnp.finfo(jnp.float32).min)

TOK = 2048
ROWS = 2048
DIM = 4096
VOCAB = 8192
TILE = 512
TILES = VOCAB // TILE
HB = 1024
HBS = TOK // HB
CHUNK = 64
CHUNKS = ROWS // 2 // CHUNK
LN_ROWS = 256
STAT_ROWS = 16
LN_UNROLL = 4
NT = (((1,), (1,)), ((), ()))


def peers():
    dp, tp = lax.axis_index('dp'), lax.axis_index('tp')
    core = lax.rem(tp, 2)
    pair = tp - core
    other = 2 - pair
    part = pair + 1 - core
    return dp, tp, (dp, part), (dp, other + core), (dp, other + 1 - core), (1 - dp, tp)


def remote(src, dst, ssem, rsem, dev):
    return pltpu.make_async_remote_copy(
        src_ref=src, dst_ref=dst, send_sem=ssem, recv_sem=rsem, device_id=dev, device_id_type=pl.DeviceIdType.MESH)


def gather_logits_kernel(hid, gain, bias, emb, tcol, info, e_all, x_out, z_out, stat_all, info_all, lse_b, mean_b, rstd_b,
                         xs, hbuf, ebuf, z0, z1, tc_v, m_s, s_s, t_s, info_v, stat_v, mr_v, gb8,
                         h_sem, xo_sem, e_sem, eo_sem, z_sem, small_sem, wide_sem,
                         xs_send, ys_send, ds_send, pe_send, sm_send,
                         x_recv, y_recv, d_recv, pe_recv, info_recv, stat_recv):
    dp, tp, part, xp, xq, yp = peers()
    barrier = pltpu.get_barrier_semaphore()
    for dev in (part, xp, xq, yp):
        pl.semaphore_signal(barrier, inc=1, device_id=dev, device_id_type=pl.DeviceIdType.MESH)
    pl.semaphore_wait(barrier, 4)

    def tile_row(j):
        return ROWS * 2 + (j // 2) * TILE + lax.rem(j, 2) * CHUNK

    def x_copy(j):
        src = emb.at[pl.ds(pl.multiple_of(dp * (ROWS // 2) + j * CHUNK, CHUNK), CHUNK)]
        return remote(src, e_all.at[pl.ds(pl.multiple_of(tile_row(j), CHUNK), CHUNK)], xs_send, x_recv.at[j], xp)

    def piece(j, p):
        return e_all.at[pl.ds(pl.multiple_of(tile_row(j) + p * 2 * CHUNK, CHUNK), CHUNK)]

    def y_copy(j):
        return remote(piece(j, 0), piece(j, 1), ys_send, y_recv.at[j], yp)

    def d_copy(j, p):
        return remote(piece(j, p), piece(j, p + 2), ds_send, d_recv.at[j // 2], part)

    def pe_copy(i):
        return remote(emb.at[pl.ds(pl.multiple_of(i * TILE, TILE), TILE)],
                      e_all.at[pl.ds(pl.multiple_of(ROWS + i * TILE, TILE), TILE)], pe_send, pe_recv.at[i], part)

    cp = pltpu.make_async_copy(info, info_v, small_sem.at[0])
    cp.start()
    tcp = pltpu.make_async_copy(tcol, tc_v, small_sem.at[1])
    tcp.start()

    def h_copy(i):
        return pltpu.make_async_copy(hid.at[pl.ds(pl.multiple_of(i * LN_ROWS, LN_ROWS), LN_ROWS)], hbuf.at[lax.rem(i, 2)], h_sem.at[lax.rem(i, 2)])
    h_copy(0).start()

    group = ((1, part), (2, xp), (3, xq))
    for p, dev in group:
        remote(info, info_all.at[tp], sm_send, info_recv.at[p], dev).start()

    def start_x(j, c):
        x_copy(j).start()
        return c
    lax.fori_loop(0, CHUNKS, start_x, 0)

    def start_pe(i, c):
        pe_copy(i).start()
        return c
    lax.fori_loop(0, ROWS // TILE, start_pe, 0)

    def e_load(t):
        slot = lax.rem(t, 2)
        return pltpu.make_async_copy(e_all.at[pl.ds(pl.multiple_of(t * TILE, TILE), TILE)], ebuf.at[slot], e_sem.at[slot])

    def e_load_own(t):
        slot = lax.rem(t, 2)
        return pltpu.make_async_copy(emb.at[pl.ds(pl.multiple_of(t * TILE, TILE), TILE)], ebuf.at[slot], e_sem.at[slot])
    e_load_own(0).start()

    cp.wait()
    pltpu.make_async_copy(info_v, info_all.at[tp], small_sem.at[0]).start()
    gb8[0] = jnp.broadcast_to(gain[...], (8, DIM))
    gb8[1] = jnp.broadcast_to(bias[...], (8, DIM))

    def ln_tile(i, c):
        slot = lax.rem(i, 2)

        @pl.when(i + 1 < TOK // LN_ROWS)
        def _():
            h_copy(i + 1).start()
        h_copy(i).wait()

        def ln_rows(r, c2):
            base = r * LN_UNROLL * 16

            def at(u):
                return pl.ds(pl.multiple_of(base + u * 16, 16), 16)

            def part_of(u, k):
                return hbuf[slot, at(u), k * 128:(k + 1) * 128].astype(jnp.float32)
            means, rstds = [], []
            for u in range(LN_UNROLL):
                tot = part_of(u, 0)
                for k in range(1, DIM // 128):
                    tot = tot + part_of(u, k)
                means.append(jnp.broadcast_to(jnp.sum(tot, axis=-1, keepdims=True) * (1.0 / DIM), (16, 128)))
            for u in range(LN_UNROLL):
                tot = jnp.zeros((16, 128), jnp.float32)
                for k in range(DIM // 128):
                    diff = part_of(u, k) - means[u]
                    tot = tot + diff * diff
                var = jnp.sum(tot, axis=-1, keepdims=True) * (1.0 / DIM)
                rstds.append(jnp.broadcast_to(lax.rsqrt(var + LN_EPS), (16, 128)))
            for u in range(LN_UNROLL):
                row = pl.ds(pl.multiple_of(i * LN_ROWS + base + u * 16, 16), 16)
                mr_v[0, row, :] = means[u]
                mr_v[1, row, :] = rstds[u]
                for k in range(DIM // 128):
                    cols = slice(k * 128, (k + 1) * 128)
                    g2 = jnp.concatenate([gb8[0, :, cols]] * 2, axis=0)
                    b2 = jnp.concatenate([gb8[1, :, cols]] * 2, axis=0)
                    xs[row, cols] = ((part_of(u, k) - means[u]) * rstds[u] * g2 + b2).astype(jnp.bfloat16)
            return c2
        lax.fori_loop(0, LN_ROWS // (16 * LN_UNROLL), ln_rows, 0)
        rows = pl.ds(pl.multiple_of(i * LN_ROWS, LN_ROWS), LN_ROWS)
        pltpu.make_async_copy(xs.at[rows], x_out.at[rows], xo_sem).start()
        return c
    lax.fori_loop(0, TOK // LN_ROWS, ln_tile, 0)

    for i, dst in enumerate((mean_b, rstd_b)):
        pltpu.make_async_copy(mr_v.at[i], dst, wide_sem.at[i + 1]).start()
    m_s[...] = jnp.full((TOK, 128), LOWEST, jnp.float32)
    s_s[...] = jnp.zeros((TOK, 128), jnp.float32)
    t_s[...] = jnp.zeros((TOK, 128), jnp.float32)
    tcp.wait()

    zs = (z0, z1)

    def product(t, h):
        zs[h][...] = lax.dot_general(xs[h * HB:(h + 1) * HB, :], ebuf[lax.rem(t, 2)], NT, preferred_element_type=jnp.float32)

    def statistics(t, h):
        z = zs[h]
        lane = lax.broadcasted_iota(jnp.int32, (STAT_ROWS, 128), 1)
        for r in range(0, HB, STAT_ROWS):
            rows = slice(h * HB + r, h * HB + r + STAT_ROWS)
            zk = [z[r:r + STAT_ROWS, k * 128:(k + 1) * 128] for k in range(TILE // 128)]
            old = m_s[rows, :]
            new = jnp.maximum(jnp.maximum(jnp.maximum(zk[0], zk[1]), jnp.maximum(zk[2], zk[3])), old)
            tot = s_s[rows, :] * jnp.exp(old - new)
            tgt = t_s[rows, :]
            diff = tc_v[rows, :] - t * TILE
            for k in range(TILE // 128):
                tot = tot + jnp.exp(zk[k] - new)
                tgt = tgt + jnp.where(diff == lane + k * 128, zk[k], 0.0)
            m_s[rows, :] = new
            s_s[rows, :] = tot
            t_s[rows, :] = tgt

    def z_copy(t, h):
        return pltpu.make_async_copy(
            zs[h], z_out.at[pl.ds(h * HB, HB), pl.ds(pl.multiple_of(t * TILE, TILE), TILE)], z_sem.at[h])

    def x_event(j):
        x_copy(j).wait_recv()
        y_copy(j).start()
        d_copy(j, 0).start()

    def y_event(j):
        y_copy(j).wait_recv()
        d_copy(j, 1).start()

    def p_event(k):
        rows = e_all.at[pl.ds(pl.multiple_of(2 * ROWS + k * TILE + TILE // 2, TILE // 2), TILE // 2)]
        pltpu.make_async_copy(rows, rows, d_recv.at[k]).wait()
        e_load(8 + k).start()

    half_tiles = TILES // 2

    def start_events(t):
        @pl.when(t < TILES - 1)
        def _():
            x_event(t)

        @pl.when(t == TILES - 2)
        def _():
            y_event(TILES - 3)
            p_event(6)

        @pl.when(t == TILES - 1)
        def _():
            y_event(TILES - 2)
            y_event(TILES - 1)
            p_event(7)
        e_load(t).wait()

        @pl.when(t < 4)
        def _():
            slot = lax.rem(t, 2)
            pltpu.make_async_copy(ebuf.at[slot], e_all.at[pl.ds(pl.multiple_of(t * TILE, TILE), TILE)], eo_sem.at[slot]).start()

    def middle_events(t):
        @pl.when((t >= 1) & (t < TILES - 2))
        def _():
            y_event(t - 1)

        @pl.when((t >= 1) & (t < 5))
        def _():
            slot = lax.rem(t - 1, 2)
            pltpu.make_async_copy(ebuf.at[slot], e_all.at[pl.ds(0, TILE)], eo_sem.at[slot]).wait()

        @pl.when(t < 3)
        def _():
            e_load_own(t + 1).start()

        @pl.when((t >= 3) & (t < 7))
        def _():
            pe_copy(t - 3).wait_recv()
            e_load(t + 1).start()

        @pl.when((t >= half_tiles - 1) & (t < TILES - 3))
        def _():
            p_event(t - (half_tiles - 1))

        @pl.when(t == TILES - 2)
        def _():
            x_event(TILES - 1)

    start_events(0)
    product(0, 0)

    def step(t, c):
        z_copy(t, 0).start()
        middle_events(t)

        @pl.when(t > 0)
        def _():
            z_copy(t - 1, 1).wait()
        product(t, 1)
        statistics(t, 0)
        start_events(t + 1)
        z_copy(t, 1).start()
        z_copy(t, 0).wait()
        product(t + 1, 0)
        statistics(t, 1)
        return c
    last = TILES - 1
    lax.fori_loop(0, last, step, 0)
    z_copy(last, 0).start()
    z_copy(last - 1, 1).wait()
    statistics(last, 0)
    product(last, 1)
    z_copy(last, 1).start()
    statistics(last, 1)

    def finish(i, c):
        for u in range(4):
            r = i * 4 + u
            rows = pl.ds(pl.multiple_of(r * 128, 128), 128)
            m = m_s[rows, :]
            top = jnp.max(m, axis=-1, keepdims=True)
            tot = jnp.sum(s_s[rows, :] * jnp.exp(m - top), axis=-1, keepdims=True)
            lse = jnp.broadcast_to(top + jnp.log(tot), (128, 128))
            tgt = jnp.broadcast_to(jnp.sum(t_s[rows, :], axis=-1, keepdims=True), (128, 128))
            m_s[rows, :] = lse
            stat_v[0, pl.ds(r, 1), :] = jnp.transpose(lse)[0:1, :]
            stat_v[1, pl.ds(r, 1), :] = jnp.transpose(tgt)[0:1, :]
        return c
    lax.fori_loop(0, TOK // 512, finish, 0)
    pltpu.make_async_copy(m_s, lse_b, wide_sem.at[0]).start()
    pltpu.make_async_copy(info_v, info_all.at[tp], small_sem.at[0]).wait()
    for h in range(2):
        z_copy(last, h).wait()
    pltpu.make_async_copy(xs, x_out, xo_sem).wait()
    half = e_all.at[pl.ds(0, ROWS // 2)]
    pltpu.make_async_copy(half, half, xs_send).wait()
    pltpu.make_async_copy(half, half, ys_send).wait()
    full = e_all.at[pl.ds(0, ROWS)]
    pltpu.make_async_copy(full, full, ds_send).wait()
    pltpu.make_async_copy(full, full, pe_send).wait()
    own = pltpu.make_async_copy(stat_v, stat_all.at[tp], small_sem.at[1])
    own.start()
    for p, dev in group:
        remote(stat_v, stat_all.at[tp], sm_send, stat_recv.at[p], dev).start()

    own.wait()
    for p, dev in group:
        remote(info, info_all.at[tp], sm_send, info_recv.at[p], dev).wait()
        remote(stat_v, stat_all.at[tp], sm_send, stat_recv.at[p], dev).wait()
    for i, (src, dst) in enumerate(((m_s, lse_b), (mr_v.at[0], mean_b), (mr_v.at[1], rstd_b))):
        pltpu.make_async_copy(src, dst, wide_sem.at[i]).wait()


def gather_logits(hidden, gain, bias, embed, tcol, info):
    any_spec = pl.BlockSpec(memory_space=pl.ANY)
    vmem_spec = pl.BlockSpec(memory_space=pltpu.VMEM)
    f32, bf16, i32 = jnp.float32, jnp.bfloat16, jnp.int32
    dma = pltpu.SemaphoreType.DMA
    groups = TOK // 128
    return pl.pallas_call(
        gather_logits_kernel,
        name="gather_logits",
        out_shape=(
            jax.ShapeDtypeStruct((VOCAB, DIM), bf16),
            jax.ShapeDtypeStruct((TOK, DIM), bf16),
            jax.ShapeDtypeStruct((TOK, VOCAB), f32),
            jax.ShapeDtypeStruct((4, 2, groups, 128), f32),
            jax.ShapeDtypeStruct((4, 2, groups, 128), i32),
            jax.ShapeDtypeStruct((TOK, 128), f32),
            jax.ShapeDtypeStruct((TOK, 128), f32),
            jax.ShapeDtypeStruct((TOK, 128), f32),
        ),
        in_specs=[any_spec, vmem_spec, vmem_spec, any_spec, any_spec, any_spec],
        out_specs=[any_spec] * 8,
        scratch_shapes=[
            pltpu.VMEM((TOK, DIM), bf16),
            pltpu.VMEM((2, LN_ROWS, DIM), bf16),
            pltpu.VMEM((2, TILE, DIM), bf16),
            pltpu.VMEM((HB, TILE), f32),
            pltpu.VMEM((HB, TILE), f32),
            pltpu.VMEM((TOK, 128), i32),
            pltpu.VMEM((TOK, 128), f32),
            pltpu.VMEM((TOK, 128), f32),
            pltpu.VMEM((TOK, 128), f32),
            pltpu.VMEM((2, groups, 128), i32),
            pltpu.VMEM((2, groups, 128), f32),
            pltpu.VMEM((2, TOK, 128), f32),
            pltpu.VMEM((2, 8, DIM), f32),
            dma((2,)), dma, dma((2,)), dma((2,)), dma((2,)), dma((2,)), dma((3,)),
            dma, dma, dma, dma, dma,
            dma((CHUNKS,)), dma((CHUNKS,)), dma((TILES // 2,)), dma((4,)), dma((4,)), dma((4,)),
        ],
        compiler_params=pltpu.CompilerParams(collective_id=0, has_side_effects=True, vmem_limit_bytes=60 * 1024 * 1024),
        cost_estimate=pl.CostEstimate(flops=2 * TOK * VOCAB * DIM, bytes_accessed=300 * 2 ** 20, transcendentals=TOK * VOCAB),
    )(hidden, gain, bias, embed, tcol, info)


XCH = 256
XCHS = TOK // XCH
KT = 512
DEFER = 4
WAIT_STEP = {6: 0, 10: 1, 15: 2}


def backward_kernel(z, e_all, emb, xo, hid, gain, lse_b, scale_b, tcol_b, mean_b, rstd_b, lse_r, scale_r, trel_r,
                    dhid, x_part, x_xp, x_xq, dzt_own, dzt_out, dzt_part, dzt_last, de_part, gsum_all,
                    acc, gb_v, gs_v, g8, ld_sem, z_sem, e_sem, dzo_sem, big_sem, g_sem,
                    xs_send, xd_send, xp_send, dz_send, g_send, x_recv, d_recv, xp_recv, dz_recv, g_recv):
    dp, tp, part, xp, xq, yp = peers()
    barrier = pltpu.get_barrier_semaphore()
    group = ((1, part), (2, xp), (3, xq))
    for _, dev in group:
        pl.semaphore_signal(barrier, inc=1, device_id=dev, device_id_type=pl.DeviceIdType.MESH)
    pl.semaphore_wait(barrier, 3)

    def xrows(ref, j):
        return ref.at[pl.ds(pl.multiple_of(j * XCH, XCH), XCH)]

    def x_copy(j):
        return remote(xrows(xo, j), xrows(x_xp, j), xs_send, x_recv.at[j], xp)

    def xd_copy(j):
        return remote(xrows(x_xp, j), xrows(x_xq, j), xd_send, d_recv.at[j], part)

    def x_event(j):
        x_copy(j).wait_recv()
        xd_copy(j).start()

    def start_x(j, c):
        x_copy(j).start()
        return c
    lax.fori_loop(0, XCHS, start_x, 0)
    xp_copy = remote(xo, x_part, xp_send, xp_recv, part)
    xp_copy.start()

    def dzt_copy(k):
        rows = pl.ds(pl.multiple_of(lax.rem(k, 4) * KT, KT), KT)
        return remote(dzt_out.at[rows], dzt_part.at[rows], dz_send, dz_recv.at[lax.rem(k, 4)], part)

    def d_phase(zt, et, dz, dzt, lse_v, scale_v, tcol_v):
        loads = [pltpu.make_async_copy(src, dst, ld_sem.at[i]) for i, (src, dst) in enumerate(((lse_b, lse_v), (scale_b, scale_v), (tcol_b, tcol_v)))]
        for cp in loads:
            cp.start()
        def z_load(k):
            slot = lax.rem(k, 2)
            return pltpu.make_async_copy(z.at[:, pl.ds(pl.multiple_of(k * KT, KT), KT)], zt.at[slot], z_sem.at[slot])

        def e_load(k):
            slot = lax.rem(k, 2)
            return pltpu.make_async_copy(e_all.at[pl.ds(pl.multiple_of(k * KT, KT), KT)], et.at[slot], e_sem.at[slot])

        def dzt_store(k, ref):
            return pltpu.make_async_copy(dzt, ref.at[pl.ds(pl.multiple_of(lax.rem(k, 4) * KT, KT), KT)], dzo_sem)
        z_load(0).start()
        e_load(0).start()
        acc[...] = jnp.zeros(acc.shape, jnp.float32)
        for cp in loads:
            cp.wait()

        def step(k, c):
            slot = lax.rem(k, 2)

            @pl.when(k + 1 < VOCAB // KT)
            def _():
                z_load(k + 1).start()
                e_load(k + 1).start()
            for at, j in WAIT_STEP.items():
                @pl.when(k == at)
                def _(j=j):
                    x_event(j)

            @pl.when((k >= 1) & (k <= 8))
            def _():
                dzt_store(0, dzt_own).wait()

            @pl.when((k >= 5) & (k <= 8))
            def _():
                dzt_copy(k - 1).start()
            z_load(k).wait()

            def block(r, c2):
                rows = pl.ds(pl.multiple_of(r * 256, 256), 256)
                lane = lax.broadcasted_iota(jnp.int32, (32, 128), 1)
                for q in range(8):
                    sub = pl.ds(pl.multiple_of(r * 256 + q * 32, 32), 32)
                    lse = lse_v[sub, :]
                    scale = scale_v[sub, :]
                    diff = tcol_v[sub, :] - k * KT
                    for g in range(KT // 128):
                        hot = (diff == lane + g * 128).astype(jnp.float32)
                        val = (jnp.exp(zt[slot, sub, g * 128:(g + 1) * 128] - lse) - hot) * scale
                        dz[sub, g * 128:(g + 1) * 128] = val.astype(jnp.bfloat16)
                return c2
            lax.fori_loop(0, TOK // 256, block, 0)

            @pl.when(k < 8)
            def _():
                def flip(r, c2):
                    rows = pl.ds(pl.multiple_of(r * 256, 256), 256)
                    dzt[:, rows] = jnp.transpose(dz[rows, :])
                    return c2
                lax.fori_loop(0, TOK // 256, flip, 0)

            @pl.when(k < 4)
            def _():
                dzt_store(k, dzt_own).start()

            @pl.when((k >= 4) & (k < 8))
            def _():
                dzt_store(k, dzt_out).start()
            e_load(k).wait()

            def mul(h, c2):
                rows = pl.ds(pl.multiple_of(h * HB, HB), HB)
                for n in range(0, DIM, NCOL):
                    acc[rows, n:n + NCOL] += jnp.dot(dz[rows, :], et[slot, :, n:n + NCOL], preferred_element_type=jnp.float32)
                return c2
            lax.fori_loop(0, HBS, mul, 0)
            return c
        lax.fori_loop(0, VOCAB // KT, step, 0)
    pl.run_scoped(d_phase, pltpu.VMEM((2, TOK, KT), jnp.float32), pltpu.VMEM((2, KT, DIM), jnp.bfloat16),
                  pltpu.VMEM((TOK, KT), jnp.bfloat16), pltpu.VMEM((KT, TOK), jnp.bfloat16),
                  pltpu.VMEM((TOK, 128), jnp.float32), pltpu.VMEM((TOK, 128), jnp.float32), pltpu.VMEM((TOK, 128), jnp.int32))

    def n_phase(hb, ob, mr):
        def h_load(i):
            slot = lax.rem(i, 2)
            return pltpu.make_async_copy(hid.at[pl.ds(pl.multiple_of(i * LN_ROWS, LN_ROWS), LN_ROWS)], hb.at[slot], z_sem.at[slot])

        def o_store(i):
            slot = lax.rem(i, 2)
            return pltpu.make_async_copy(ob.at[slot], dhid.at[pl.ds(pl.multiple_of(i * LN_ROWS, LN_ROWS), LN_ROWS)], e_sem.at[slot])
        mr_loads = [pltpu.make_async_copy(src, mr.at[i], ld_sem.at[i]) for i, src in enumerate((mean_b, rstd_b))]
        for cp in mr_loads:
            cp.start()
        h_load(0).start()
        gb_v[...] = jnp.zeros(gb_v.shape, jnp.float32)
        g8[...] = jnp.broadcast_to(gain[...], (8, DIM))
        for cp in mr_loads:
            cp.wait()

        def tile(i, c):
            slot = lax.rem(i, 2)

            @pl.when(i + 1 < TOK // LN_ROWS)
            def _():
                h_load(i + 1).start()

            @pl.when(i >= 2)
            def _():
                o_store(i - 2).wait()
            h_load(i).wait()

            def rows_body(r, c2):
                units = range(NB_UNROLL)
                base = r * 16 * NB_UNROLL
                low = [pl.ds(pl.multiple_of(base + u * 16, 16), 16) for u in units]
                row = [pl.ds(pl.multiple_of(i * LN_ROWS + base + u * 16, 16), 16) for u in units]
                zero = jnp.zeros((16, 128), jnp.float32)
                sum1, sum3 = [zero] * NB_UNROLL, [zero] * NB_UNROLL

                def load(u, cols):
                    dx = acc[row[u], cols]
                    xhat = (hb[slot, low[u], cols].astype(jnp.float32) - mr[0, row[u], :]) * mr[1, row[u], :]
                    return dx, xhat, dx * jnp.concatenate([g8[:, cols]] * 2, axis=0)
                for k in range(DIM // 128):
                    cols = slice(k * 128, (k + 1) * 128)
                    d_gain, d_bias = gb_v[0, :, cols], gb_v[1, :, cols]
                    for u in units:
                        dx, xhat, gx = load(u, cols)
                        sum1[u] = sum1[u] + gx
                        sum3[u] = sum3[u] + gx * xhat
                        dgx = dx * xhat
                        d_gain = d_gain + (dgx[0:8] + dgx[8:16])
                        d_bias = d_bias + (dx[0:8] + dx[8:16])
                    gb_v[0, :, cols] = d_gain
                    gb_v[1, :, cols] = d_bias
                c1 = [jnp.broadcast_to(jnp.sum(v, axis=-1, keepdims=True) * (1.0 / DIM), (16, 128)) for v in sum1]
                c3 = [jnp.broadcast_to(jnp.sum(v, axis=-1, keepdims=True) * (1.0 / DIM), (16, 128)) for v in sum3]
                for u in units:
                    for k in range(DIM // 128):
                        cols = slice(k * 128, (k + 1) * 128)
                        _, xhat, gx = load(u, cols)
                        ob[slot, low[u], cols] = (mr[1, row[u], :] * (gx - c1[u] - xhat * c3[u])).astype(jnp.bfloat16)
                        acc[row[u], cols] = zero
                return c2
            lax.fori_loop(0, LN_ROWS // (16 * NB_UNROLL), rows_body, 0)
            o_store(i).start()
            return c
        lax.fori_loop(0, TOK // LN_ROWS, tile, 0)
        for i in range(2):
            o_store(TOK // LN_ROWS - 2 + i).wait()
        gs_v[0:1, :] = jnp.sum(gb_v[0], axis=0, keepdims=True)
        gs_v[1:2, :] = jnp.sum(gb_v[1], axis=0, keepdims=True)
    pl.run_scoped(n_phase, pltpu.VMEM((2, LN_ROWS, DIM), jnp.bfloat16), pltpu.VMEM((2, LN_ROWS, DIM), jnp.bfloat16),
                  pltpu.VMEM((2, TOK, 128), jnp.float32))
    x_event(3)
    own = pltpu.make_async_copy(gs_v, gsum_all.at[tp], g_sem)

    def e_phase(eo, xt, dzb, zs):
        eo_load = pltpu.make_async_copy(emb, eo, big_sem)

        def x_load(ref, row, slot):
            return pltpu.make_async_copy(ref.at[pl.ds(pl.multiple_of(row, KT), KT)], xt.at[slot], z_sem.at[slot])

        def dz_load(ref, col, slot):
            return pltpu.make_async_copy(ref.at[:, pl.ds(pl.multiple_of(col, KT), KT)], dzb.at[slot], e_sem.at[slot])

        def start_local(i):
            slot = lax.rem(i, 2)

            @pl.when(i < 4)
            def _():
                x_load(xo, i * KT, slot).start()
                dz_load(dzt_own, i * KT, slot).start()

            @pl.when(i >= 4)
            def _():
                x_load(x_part, (i - 4) * KT, slot).start()
                dz_load(dzt_part, (i - 4) * KT, slot).start()

        def add(slot):
            def mul(h, c2):
                rows = pl.ds(pl.multiple_of(h * HB, HB), HB)
                for n in range(0, DIM, NCOL):
                    acc[rows, n:n + NCOL] += jnp.dot(dzb[slot, rows, :], xt[slot, :, n:n + NCOL], preferred_element_type=jnp.float32)
                return c2
            lax.fori_loop(0, HBS, mul, 0)

        start_local(0)

        def rem_load(r):
            slot = lax.rem(r, 2)
            return [pltpu.make_async_copy(xrows(ref, r), xt.at[slot, pl.ds(i * XCH, XCH)], z_sem.at[slot])
                    for i, ref in enumerate((x_xp, x_xq))]

        def local(i, c):
            slot = lax.rem(i, 2)

            @pl.when(i == 0)
            def _():
                eo_load.start()

            @pl.when(i == 2)
            def _():
                xp_copy.wait_recv()

                def wait_dz(q, c2):
                    dzt_copy(q).wait_recv()
                    return c2
                lax.fori_loop(0, 4, wait_dz, 0)

            @pl.when(i == 1)
            def _():
                own.start()
                for p, dev in group:
                    remote(gs_v, gsum_all.at[tp], g_send, g_recv.at[p], dev).start()

            @pl.when(i == 5)
            def _():
                x_event(4)

            @pl.when(i < 7)
            def _():
                start_local(i + 1)

            @pl.when(i == 7)
            def _():
                xd_copy(0).wait_recv()
                for cp in rem_load(0):
                    cp.start()
            x_load(xo, 0, slot).wait()
            dz_load(dzt_own, 0, slot).wait()
            add(slot)
            return c
        lax.fori_loop(0, 8, local, 0)
        eo_load.wait()

        def far(r, c):
            slot = lax.rem(r, 2)

            @pl.when(r == 1)
            def _():
                x_event(5)

            @pl.when(r == 3)
            def _():
                x_event(6)

            @pl.when(r == 6)
            def _():
                x_event(7)

            @pl.when(r + 1 < XCHS)
            def _():
                xd_copy(r + 1).wait_recv()
                for cp in rem_load(r + 1):
                    cp.start()
            x_load(xo, 0, slot).wait()

            @pl.when(r == XCHS - DEFER)
            def _():
                pltpu.make_async_copy(acc, de_part, big_sem).start()

            @pl.when(r > XCHS - DEFER)
            def _():
                dz_out(0, 0, slot).wait()
                dz_out(0, 1, slot).wait()

            lse = lse_r[pl.ds(r, 1), :]
            scale = scale_r[pl.ds(r, 1), :]
            trel = trel_r[pl.ds(r, 1), :]

            def logits(h, c2):
                for k in range(0, DIM, KCOL):
                    prod = lax.dot_general(eo[pl.ds(pl.multiple_of(h * ZB, ZB), ZB), k:k + KCOL], xt[slot, :, k:k + KCOL], NT, preferred_element_type=jnp.float32)
                    zs[...] = prod if k == 0 else zs[...] + prod
                for q in range(ZB // 32):
                    row = h * ZB + q * 32
                    hot = ((trel - row) == lax.broadcasted_iota(jnp.int32, (32, KT), 0)).astype(jnp.float32)
                    val = (jnp.exp(zs[q * 32:(q + 1) * 32, :] - lse) - hot) * scale
                    dzb[0, pl.ds(pl.multiple_of(row, 32), 32), :] = val.astype(jnp.bfloat16)
                return c2
            lax.fori_loop(0, ROWS // ZB, logits, 0)

            @pl.when(r < XCHS - DEFER)
            def _():
                def mul(h, c2):
                    rows = pl.ds(pl.multiple_of(h * HB, HB), HB)
                    for n in range(0, DIM, NCOL):
                        acc[rows, n:n + NCOL] += jnp.dot(dzb[0, rows, :], xt[slot, :, n:n + NCOL], preferred_element_type=jnp.float32)
                    return c2
                lax.fori_loop(0, HBS, mul, 0)

            @pl.when(r >= XCHS - DEFER)
            def _():
                for i in range(2):
                    dz_out(r - (XCHS - DEFER), i, 0).start()
            return c

        def dz_out(q, i, slot):
            return pltpu.make_async_copy(
                dzb.at[0, :, pl.ds(i * XCH, XCH)], dzt_last.at[i, :, pl.ds(pl.multiple_of(q * XCH, XCH), XCH)], dzo_sem)
        lax.fori_loop(0, XCHS, far, 0)
        dz_out(0, 0, 0).wait()
        dz_out(0, 1, 0).wait()
        pltpu.make_async_copy(acc, de_part, big_sem).wait()
    pl.run_scoped(e_phase, pltpu.VMEM((ROWS, DIM), jnp.bfloat16), pltpu.VMEM((2, KT, DIM), jnp.bfloat16),
                  pltpu.VMEM((2, ROWS, KT), jnp.bfloat16), pltpu.VMEM((ZB, KT), jnp.float32))

    own.wait()
    pltpu.make_async_copy(xo, xo, xs_send).wait()
    pltpu.make_async_copy(xo, xo, xd_send).wait()
    xp_copy.wait_send()
    pltpu.make_async_copy(dzt_out, dzt_out, dz_send).wait()
    for p, dev in group:
        remote(gs_v, gsum_all.at[tp], g_send, g_recv.at[p], dev).wait()


ZB = 512
KCOL = 1024
NCOL = 512
NB_UNROLL = 8


def backward(z, e_all, embed, normed, hidden, gain, lse_b, scale_b, tcol_b, mean_b, rstd_b, lse_r, scale_r, trel_r):
    any_spec = pl.BlockSpec(memory_space=pl.ANY)
    vmem_spec = pl.BlockSpec(memory_space=pltpu.VMEM)
    f32, bf16, i32 = jnp.float32, jnp.bfloat16, jnp.int32
    dma = pltpu.SemaphoreType.DMA
    shapes = [((TOK, DIM), bf16), ((TOK, DIM), bf16), ((TOK, DIM), bf16), ((TOK, DIM), bf16), ((ROWS, TOK), bf16),
              ((ROWS, TOK), bf16), ((ROWS, TOK), bf16), ((2, ROWS, DEFER * XCH), bf16), ((ROWS, DIM), f32), ((4, 2, DIM), f32)]
    return pl.pallas_call(
        backward_kernel,
        name="backward",
        out_shape=[jax.ShapeDtypeStruct(s, d) for s, d in shapes],
        in_specs=[any_spec] * 5 + [vmem_spec] + [any_spec] * 5 + [vmem_spec] * 3,
        out_specs=[any_spec] * len(shapes),
        scratch_shapes=[
            pltpu.VMEM((TOK, DIM), f32),
            pltpu.VMEM((2, 8, DIM), f32), pltpu.VMEM((2, DIM), f32), pltpu.VMEM((8, DIM), f32),
            dma((3,)), dma((2,)), dma((2,)), dma, dma, dma,
            dma, dma, dma, dma, dma, dma((XCHS,)), dma((XCHS,)), dma, dma((4,)), dma((4,)),
        ],
        compiler_params=pltpu.CompilerParams(collective_id=1, has_side_effects=True, vmem_limit_bytes=67043328),
        cost_estimate=pl.CostEstimate(flops=5 * TOK * VOCAB * DIM, bytes_accessed=400 * 2 ** 20, transcendentals=2 * TOK * VOCAB),
    )(z, e_all, embed, normed, hidden, gain, lse_b, scale_b, tcol_b, mean_b, rstd_b, lse_r, scale_r, trel_r)


def finish_kernel(de_in, dz0, dz1, xa, xb, dh_in, de_out, dh_out):
    prod = jnp.dot(dz0[0], xa[...], preferred_element_type=jnp.float32) + jnp.dot(dz1[0], xb[...], preferred_element_type=jnp.float32)
    de_out[...] = de_in[...] + prod
    dh_out[...] = dh_in[...]


def finish(de_part, dzt_last, x_xp, x_xq, dhid):
    cols = 512
    steps = DIM // cols
    depth = DEFER * XCH
    row_block = (TOK - depth) // depth
    rows = TOK // steps
    return pl.pallas_call(
        finish_kernel,
        name="finish",
        grid=(steps,),
        out_shape=[jax.ShapeDtypeStruct((ROWS, DIM), jnp.float32), jax.ShapeDtypeStruct((TOK, DIM), jnp.bfloat16)],
        in_specs=[
            pl.BlockSpec((ROWS, cols), lambda i: (0, i)),
            pl.BlockSpec((1, ROWS, depth), lambda i: (0, 0, 0)),
            pl.BlockSpec((1, ROWS, depth), lambda i: (1, 0, 0)),
            pl.BlockSpec((depth, cols), lambda i: (row_block, i)),
            pl.BlockSpec((depth, cols), lambda i: (row_block, i)),
            pl.BlockSpec((rows, DIM), lambda i: (i, 0)),
        ],
        out_specs=[pl.BlockSpec((ROWS, cols), lambda i: (0, i)), pl.BlockSpec((rows, DIM), lambda i: (i, 0))],
        compiler_params=pltpu.CompilerParams(vmem_limit_bytes=60 * 1024 * 1024),
        cost_estimate=pl.CostEstimate(flops=4 * ROWS * DIM * depth, bytes_accessed=120 * 2 ** 20, transcendentals=0),
    )(de_part, dzt_last, dzt_last, x_xp, x_xq, dhid)


def solution(mesh):
    def body(hidden, ln_gain, ln_bias, embed, targets, loss_mask):
        dp, rank = lax.axis_index('dp'), lax.axis_index('tp')
        shard = targets // ROWS
        block = jnp.bitwise_xor(shard, rank)
        row = targets % ROWS
        half = row // (ROWS // 2)
        sub = row % (ROWS // 2)
        piece = (block - 2) * 2 + jnp.bitwise_xor(half, dp)
        far = 2 * ROWS + (sub // 128) * TILE + piece * 128 + sub % 128
        tcol = jnp.where(block < 2, block * ROWS + row, far)
        tcol_b = jnp.broadcast_to(tcol[:, None], (TOK, 128))
        info = jnp.stack([targets, loss_mask]).reshape(2, TOK // 128, 128)
        gain = ln_gain.reshape(1, DIM)
        e_all, normed, logits, stat_all, info_all, lse_b, mean_b, rstd_b = gather_logits(
            hidden, gain, ln_bias.reshape(1, DIM), embed, tcol_b, info)
        stat_all = stat_all.reshape(4, 2, TOK)
        info_all = info_all.reshape(4, 2, TOK)
        weights = info_all[:, 1].astype(jnp.float32)
        count = jnp.sum(weights)
        scale = weights / count
        all_loss = (stat_all[:, 0] - stat_all[:, 1]) * weights
        loss = all_loss[rank]
        mean_loss = jnp.sum(all_loss) / count
        trel = info_all[:, 0] - rank * ROWS

        def far_rows(v):
            both = jnp.stack([v[jnp.bitwise_xor(rank, 2)], v[jnp.bitwise_xor(rank, 3)]])
            return both.reshape(2, XCHS, XCH).transpose(1, 0, 2).reshape(XCHS, 2 * XCH)
        own_scale = loss_mask.astype(jnp.float32) / count
        outs = backward(logits, e_all, embed, normed, hidden, gain, lse_b, jnp.broadcast_to(own_scale[:, None], (TOK, 128)), tcol_b,
                        mean_b, rstd_b, far_rows(stat_all[:, 0]), far_rows(scale), far_rows(trel))
        dhid, x_xp, x_xq, dzt_last, de_part, gsum_all = outs[0], outs[2], outs[3], outs[7], outs[8], outs[9]
        d_embed, d_hidden = finish(de_part, dzt_last, x_xp, x_xq, dhid)
        sums = jnp.sum(gsum_all, axis=0)
        return loss, mean_loss.reshape(1), d_hidden, d_embed, sums[0], sums[1]

    token_rows = P(('dp', 'tp'))
    token_mat = P(('dp', 'tp'), None)
    return jax.shard_map(body, mesh=mesh, in_specs=(token_mat, P(), P(), P('tp', None), token_rows, token_rows), out_specs=(token_rows, P('dp'), token_mat, token_mat, P('dp'), P('dp')), check_vma=False)
```

```python
import functools

import jax
import jax.numpy as jnp
from jax import lax
from jax.experimental import pallas as pl
from jax.experimental.pallas import tpu as pltpu
from jax.sharding import PartitionSpec as P

LN_EPS = 1e-5
LOWEST = float(jnp.finfo(jnp.float32).min)

TOK = 2048
ROWS = 2048
DIM = 4096
VOCAB = 8192
TILE = 512
TILES = VOCAB // TILE
HB = 1024
HBS = TOK // HB
CHUNK = 64
CHUNKS = ROWS // 2 // CHUNK
LN_ROWS = 256
STAT_ROWS = 16
LN_UNROLL = 4
XCH = 256
XCHS = TOK // XCH
KT = 512
DEFER = 6
WAIT_STEP = {2: 0, 6: 1, 10: 2, 15: 3}
ZB = 512
NCOL = 512
KCOL = 1024
NB_UNROLL = 8
GROUPS = TOK // 128
NT = (((1,), (1,)), ((), ()))


def peers():
    dp, tp = lax.axis_index('dp'), lax.axis_index('tp')
    core = lax.rem(tp, 2)
    pair = tp - core
    other = 2 - pair
    part = pair + 1 - core
    return dp, tp, (dp, part), (dp, other + core), (dp, other + 1 - core), (1 - dp, tp)


def remote(src, dst, ssem, rsem, dev):
    return pltpu.make_async_remote_copy(
        src_ref=src, dst_ref=dst, send_sem=ssem, recv_sem=rsem, device_id=dev, device_id_type=pl.DeviceIdType.MESH)


def spread(row, rows, dst):
    dst[rows, :] = jnp.transpose(jnp.broadcast_to(row, (128, 128)))


def step_kernel(hid, gain, bias, emb, tcol, info,
                e_all, x_out, z_out, stat_all, info_all, lse_b, mean_b, rstd_b,
                dhid, x_part, x_xp, x_xq, dzt_own, dzt_out, dzt_part, dzt_last, de_part, gsum_all,
                info_v, stat_v, stats, infos, gb_v, gs_v, g8,
                h_sem, xo_sem, e_sem, eo_sem, z_sem, small_sem, wide_sem, dzo_sem, big_sem, g_sem,
                xs_send, ys_send, ds_send, pe_send, sm_send, xt_send, xd_send, xp_send, dz_send, g_send,
                x_recv, y_recv, d_recv, pe_recv, info_recv, stat_recv, xt_recv, xd_recv, xp_recv, dz_recv, g_recv):
    dp, tp, part, xp, xq, yp = peers()
    core = lax.rem(tp, 2)
    xp_rank = 2 - (tp - core) + core
    xq_rank = 2 - (tp - core) + 1 - core
    group = ((1, part), (2, xp), (3, xq))
    barrier = pltpu.get_barrier_semaphore()
    for dev in (part, xp, xq, yp):
        pl.semaphore_signal(barrier, inc=1, device_id=dev, device_id_type=pl.DeviceIdType.MESH)
    pl.semaphore_wait(barrier, 4)

    def xrows(ref, j):
        return ref.at[pl.ds(pl.multiple_of(j * XCH, XCH), XCH)]

    def xt_copy(j):
        return remote(xrows(x_out, j), xrows(x_xp, j), xt_send, xt_recv.at[j], xp)

    def xd_copy(j):
        return remote(xrows(x_xp, j), xrows(x_xq, j), xd_send, xd_recv.at[j], part)

    def xt_event(j):
        xt_copy(j).wait_recv()
        xd_copy(j).start()
    xp_copy = remote(x_out, x_part, xp_send, xp_recv, part)

    def forward(xs, hbuf, ebuf, z0, z1, tc_v, m_s, s_s, t_s, mr_v, gb8):
        def tile_row(j):
            return ROWS * 2 + (j // 2) * TILE + lax.rem(j, 2) * CHUNK

        def x_copy(j):
            src = emb.at[pl.ds(pl.multiple_of(dp * (ROWS // 2) + j * CHUNK, CHUNK), CHUNK)]
            return remote(src, e_all.at[pl.ds(pl.multiple_of(tile_row(j), CHUNK), CHUNK)], xs_send, x_recv.at[j], xp)

        def piece(j, p):
            return e_all.at[pl.ds(pl.multiple_of(tile_row(j) + p * 2 * CHUNK, CHUNK), CHUNK)]

        def y_copy(j):
            return remote(piece(j, 0), piece(j, 1), ys_send, y_recv.at[j], yp)

        def d_copy(j, p):
            return remote(piece(j, p), piece(j, p + 2), ds_send, d_recv.at[j // 2], part)

        def pe_copy(i):
            return remote(emb.at[pl.ds(pl.multiple_of(i * TILE, TILE), TILE)],
                          e_all.at[pl.ds(pl.multiple_of(ROWS + i * TILE, TILE), TILE)], pe_send, pe_recv.at[i], part)

        cp = pltpu.make_async_copy(info, info_v, small_sem.at[0])
        cp.start()

        def h_copy(i):
            return pltpu.make_async_copy(hid.at[pl.ds(pl.multiple_of(i * LN_ROWS, LN_ROWS), LN_ROWS)], hbuf.at[lax.rem(i, 2)], h_sem.at[lax.rem(i, 2)])
        h_copy(0).start()

        for p, dev in group:
            remote(info, info_all.at[tp], sm_send, info_recv.at[p], dev).start()

        def start_x(j, c):
            x_copy(j).start()
            return c
        lax.fori_loop(0, CHUNKS, start_x, 0)

        def start_pe(i, c):
            pe_copy(i).start()
            return c
        lax.fori_loop(0, ROWS // TILE, start_pe, 0)

        def e_load(t):
            slot = lax.rem(t, 2)
            return pltpu.make_async_copy(e_all.at[pl.ds(pl.multiple_of(t * TILE, TILE), TILE)], ebuf.at[slot], e_sem.at[slot])

        def e_load_own(t):
            slot = lax.rem(t, 2)
            return pltpu.make_async_copy(emb.at[pl.ds(pl.multiple_of(t * TILE, TILE), TILE)], ebuf.at[slot], e_sem.at[slot])
        e_load_own(0).start()

        cp.wait()
        pltpu.make_async_copy(info_v, info_all.at[tp], small_sem.at[0]).start()
        gb8[0] = jnp.broadcast_to(gain[...], (8, DIM))
        gb8[1] = jnp.broadcast_to(bias[...], (8, DIM))

        def ln_tile(i, c):
            slot = lax.rem(i, 2)

            @pl.when(i + 1 < TOK // LN_ROWS)
            def _():
                h_copy(i + 1).start()
            h_copy(i).wait()

            def ln_rows(r, c2):
                base = r * LN_UNROLL * 16

                def at(u):
                    return pl.ds(pl.multiple_of(base + u * 16, 16), 16)

                def part_of(u, k):
                    return hbuf[slot, at(u), k * 128:(k + 1) * 128].astype(jnp.float32)
                means, rstds = [], []
                for u in range(LN_UNROLL):
                    tot = part_of(u, 0)
                    for k in range(1, DIM // 128):
                        tot = tot + part_of(u, k)
                    means.append(jnp.broadcast_to(jnp.sum(tot, axis=-1, keepdims=True) * (1.0 / DIM), (16, 128)))
                for u in range(LN_UNROLL):
                    tot = jnp.zeros((16, 128), jnp.float32)
                    for k in range(DIM // 128):
                        diff = part_of(u, k) - means[u]
                        tot = tot + diff * diff
                    var = jnp.sum(tot, axis=-1, keepdims=True) * (1.0 / DIM)
                    rstds.append(jnp.broadcast_to(lax.rsqrt(var + LN_EPS), (16, 128)))
                for u in range(LN_UNROLL):
                    row = pl.ds(pl.multiple_of(i * LN_ROWS + base + u * 16, 16), 16)
                    mr_v[0, row, :] = means[u]
                    mr_v[1, row, :] = rstds[u]
                    for k in range(DIM // 128):
                        cols = slice(k * 128, (k + 1) * 128)
                        g2 = jnp.concatenate([gb8[0, :, cols]] * 2, axis=0)
                        b2 = jnp.concatenate([gb8[1, :, cols]] * 2, axis=0)
                        xs[row, cols] = ((part_of(u, k) - means[u]) * rstds[u] * g2 + b2).astype(jnp.bfloat16)
                return c2
            lax.fori_loop(0, LN_ROWS // (16 * LN_UNROLL), ln_rows, 0)
            rows = pl.ds(pl.multiple_of(i * LN_ROWS, LN_ROWS), LN_ROWS)
            pltpu.make_async_copy(xs.at[rows], x_out.at[rows], xo_sem).start()
            return c
        lax.fori_loop(0, TOK // LN_ROWS, ln_tile, 0)

        for i, dst in enumerate((mean_b, rstd_b)):
            pltpu.make_async_copy(mr_v.at[i], dst, wide_sem.at[i + 1]).start()
        m_s[...] = jnp.full((TOK, 128), LOWEST, jnp.float32)
        s_s[...] = jnp.zeros((TOK, 128), jnp.float32)
        t_s[...] = jnp.zeros((TOK, 128), jnp.float32)
        for r in range(GROUPS):
            spread(tcol[r:r + 1, :], slice(r * 128, (r + 1) * 128), tc_v)
        z1[...] = jnp.full((HB, TILE), LOWEST, jnp.float32)

        zs = (z0, z1)

        def product(t, h):
            zs[h][...] = lax.dot_general(xs[h * HB:(h + 1) * HB, :], ebuf[lax.rem(t, 2)], NT, preferred_element_type=jnp.float32)

        def statistics(t, h):
            z = zs[h]
            lane = lax.broadcasted_iota(jnp.int32, (STAT_ROWS, 128), 1)
            for r in range(0, HB, STAT_ROWS):
                rows = slice(h * HB + r, h * HB + r + STAT_ROWS)
                zk = [z[r:r + STAT_ROWS, k * 128:(k + 1) * 128] for k in range(TILE // 128)]
                old = m_s[rows, :]
                new = jnp.maximum(jnp.maximum(jnp.maximum(zk[0], zk[1]), jnp.maximum(zk[2], zk[3])), old)
                tot = s_s[rows, :] * jnp.exp(old - new)
                tgt = t_s[rows, :]
                diff = tc_v[rows, :] - t * TILE
                for k in range(TILE // 128):
                    tot = tot + jnp.exp(zk[k] - new)
                    tgt = tgt + jnp.where(diff == lane + k * 128, zk[k], 0.0)
                m_s[rows, :] = new
                s_s[rows, :] = tot
                t_s[rows, :] = tgt

        def z_copy(t, h):
            return pltpu.make_async_copy(
                zs[h], z_out.at[pl.ds(h * HB, HB), pl.ds(pl.multiple_of(t * TILE, TILE), TILE)], z_sem.at[h])

        def x_event(j):
            x_copy(j).wait_recv()
            y_copy(j).start()
            d_copy(j, 0).start()

        def y_event(j):
            y_copy(j).wait_recv()
            d_copy(j, 1).start()

        def p_event(k):
            rows = e_all.at[pl.ds(pl.multiple_of(2 * ROWS + k * TILE + TILE // 2, TILE // 2), TILE // 2)]
            pltpu.make_async_copy(rows, rows, d_recv.at[k]).wait()
            e_load(8 + k).start()

        half_tiles = TILES // 2

        def start_events(t):
            @pl.when(t < TILES - 1)
            def _():
                x_event(t)

            @pl.when(t == TILES - 2)
            def _():
                xt_copy(0).start()
                y_event(TILES - 3)
                p_event(6)

            @pl.when(t == TILES - 1)
            def _():
                y_event(TILES - 2)
                y_event(TILES - 1)
                p_event(7)
            e_load(t).wait()

            @pl.when(t < 4)
            def _():
                slot = lax.rem(t, 2)
                pltpu.make_async_copy(ebuf.at[slot], e_all.at[pl.ds(pl.multiple_of(t * TILE, TILE), TILE)], eo_sem.at[slot]).start()

        def middle_events(t):
            @pl.when((t >= 1) & (t < TILES - 2))
            def _():
                y_event(t - 1)

            @pl.when((t >= 1) & (t < 5))
            def _():
                slot = lax.rem(t - 1, 2)
                pltpu.make_async_copy(ebuf.at[slot], e_all.at[pl.ds(0, TILE)], eo_sem.at[slot]).wait()

            @pl.when(t == 8)
            def _():
                pltpu.make_async_copy(xs, x_out, xo_sem).wait()

            @pl.when(t < 3)
            def _():
                e_load_own(t + 1).start()

            @pl.when((t >= 3) & (t < 7))
            def _():
                pe_copy(t - 3).wait_recv()
                e_load(t + 1).start()

            @pl.when((t >= half_tiles - 1) & (t < TILES - 3))
            def _():
                p_event(t - (half_tiles - 1))

            @pl.when(t == TILES - 2)
            def _():
                x_event(TILES - 1)

        def step(t, c):
            @pl.when(t > 0)
            def _():
                z_copy(t - 1, 1).start()
            start_events(t)

            @pl.when(t > 0)
            def _():
                z_copy(t - 1, 0).wait()
            statistics(t - 1, 1)
            product(t, 0)
            z_copy(t, 0).start()
            middle_events(t)

            @pl.when(t > 0)
            def _():
                z_copy(t - 1, 1).wait()
            statistics(t, 0)
            product(t, 1)
            return c
        last = TILES - 1
        lax.fori_loop(0, TILES, step, 0)
        z_copy(last, 1).start()
        statistics(last, 1)

        def finish(i, c):
            for u in range(4):
                r = i * 4 + u
                rows = pl.ds(pl.multiple_of(r * 128, 128), 128)
                m = m_s[rows, :]
                top = jnp.max(m, axis=-1, keepdims=True)
                tot = jnp.sum(s_s[rows, :] * jnp.exp(m - top), axis=-1, keepdims=True)
                lse = jnp.broadcast_to(top + jnp.log(tot), (128, 128))
                tgt = jnp.broadcast_to(jnp.sum(t_s[rows, :], axis=-1, keepdims=True), (128, 128))
                m_s[rows, :] = lse
                stat_v[0, pl.ds(r, 1), :] = jnp.transpose(lse)[0:1, :]
                stat_v[1, pl.ds(r, 1), :] = jnp.transpose(tgt)[0:1, :]
            return c
        lax.fori_loop(0, TOK // 512, finish, 0)
        pltpu.make_async_copy(m_s, lse_b, wide_sem.at[0]).start()
        pltpu.make_async_copy(info_v, info_all.at[tp], small_sem.at[0]).wait()
        for h in range(2):
            z_copy(last, h).wait()
        half = e_all.at[pl.ds(0, ROWS // 2)]
        pltpu.make_async_copy(half, half, xs_send).wait()
        pltpu.make_async_copy(half, half, ys_send).wait()
        full = e_all.at[pl.ds(0, ROWS)]
        pltpu.make_async_copy(full, full, ds_send).wait()
        pltpu.make_async_copy(full, full, pe_send).wait()
        own = pltpu.make_async_copy(stat_v, stat_all.at[tp], small_sem.at[1])
        own.start()
        for p, dev in group:
            remote(stat_v, stat_all.at[tp], sm_send, stat_recv.at[p], dev).start()

        def start_xt(j, c):
            xt_copy(j).start()
            return c
        lax.fori_loop(1, XCHS, start_xt, 0)
        xp_copy.start()
        own.wait()
        for i, (src, dst) in enumerate(((m_s, lse_b), (mr_v.at[0], mean_b), (mr_v.at[1], rstd_b))):
            pltpu.make_async_copy(src, dst, wide_sem.at[i]).wait()
    bf16, f32 = jnp.bfloat16, jnp.float32
    wide = pltpu.VMEM((TOK, 128), f32)
    pl.run_scoped(forward, pltpu.VMEM((TOK, DIM), bf16), pltpu.VMEM((2, LN_ROWS, DIM), bf16), pltpu.VMEM((2, TILE, DIM), bf16),
                  pltpu.VMEM((HB, TILE), f32), pltpu.VMEM((HB, TILE), f32), pltpu.VMEM((TOK, 128), jnp.int32), wide, wide, wide,
                  pltpu.VMEM((2, TOK, 128), f32), pltpu.VMEM((2, 8, DIM), f32))

    def dzt_copy(k):
        rows = pl.ds(pl.multiple_of(lax.rem(k, 4) * KT, KT), KT)
        return remote(dzt_out.at[rows], dzt_part.at[rows], dz_send, dz_recv.at[lax.rem(k, 4)], part)

    def token_count():
        return jnp.sum(infos[:, 1].astype(f32))

    def backward(acc):
        def d_phase(zt, et, dz, dzt, lse_v, scale_v, tcol_v):
            lse_load = pltpu.make_async_copy(lse_b, lse_v, wide_sem.at[0])
            lse_load.start()
            for p, dev in group:
                remote(info, info_all.at[tp], sm_send, info_recv.at[p], dev).wait_recv()
            info_load = pltpu.make_async_copy(info_all, infos, small_sem.at[0])
            info_load.start()

            def z_load(k):
                slot = lax.rem(k, 2)
                return pltpu.make_async_copy(z_out.at[:, pl.ds(pl.multiple_of(k * KT, KT), KT)], zt.at[slot], z_sem.at[slot])

            def e_load(k):
                slot = lax.rem(k, 2)
                return pltpu.make_async_copy(e_all.at[pl.ds(pl.multiple_of(k * KT, KT), KT)], et.at[slot], e_sem.at[slot])

            def dzt_store(k, ref):
                return pltpu.make_async_copy(dzt, ref.at[pl.ds(pl.multiple_of(lax.rem(k, 4) * KT, KT), KT)], dzo_sem)
            z_load(0).start()
            e_load(0).start()
            acc[...] = jnp.zeros(acc.shape, jnp.float32)
            info_load.wait()
            lse_load.wait()
            count = jnp.broadcast_to(token_count(), (1, 128))
            for r in range(GROUPS):
                rows = slice(r * 128, (r + 1) * 128)
                spread(info_v[1, r:r + 1, :].astype(f32) / count, rows, scale_v)
                spread(tcol[r:r + 1, :], rows, tcol_v)

            def step(k, c):
                slot = lax.rem(k, 2)

                @pl.when(k + 1 < VOCAB // KT)
                def _():
                    z_load(k + 1).start()
                    e_load(k + 1).start()
                for at, j in WAIT_STEP.items():
                    @pl.when(k == at)
                    def _(j=j):
                        xt_event(j)

                @pl.when((k >= 1) & (k <= 8))
                def _():
                    dzt_store(0, dzt_own).wait()

                @pl.when((k >= 5) & (k <= 8))
                def _():
                    dzt_copy(k - 1).start()
                z_load(k).wait()

                def block(r, c2):
                    rows = pl.ds(pl.multiple_of(r * 256, 256), 256)
                    lane = lax.broadcasted_iota(jnp.int32, (32, 128), 1)
                    for q in range(8):
                        sub = pl.ds(pl.multiple_of(r * 256 + q * 32, 32), 32)
                        lse = lse_v[sub, :]
                        scale = scale_v[sub, :]
                        diff = tcol_v[sub, :] - k * KT
                        for g in range(KT // 128):
                            hot = (diff == lane + g * 128).astype(jnp.float32)
                            val = (jnp.exp(zt[slot, sub, g * 128:(g + 1) * 128] - lse) - hot) * scale
                            dz[sub, g * 128:(g + 1) * 128] = val.astype(jnp.bfloat16)
                    return c2
                lax.fori_loop(0, TOK // 256, block, 0)

                @pl.when(k < 8)
                def _():
                    def flip(r, c2):
                        rows = pl.ds(pl.multiple_of(r * 256, 256), 256)
                        dzt[:, rows] = jnp.transpose(dz[rows, :])
                        return c2
                    lax.fori_loop(0, TOK // 256, flip, 0)

                @pl.when(k < 4)
                def _():
                    dzt_store(k, dzt_own).start()

                @pl.when((k >= 4) & (k < 8))
                def _():
                    dzt_store(k, dzt_out).start()
                e_load(k).wait()

                def mul(h, c2):
                    rows = pl.ds(pl.multiple_of(h * HB, HB), HB)
                    for n in range(0, DIM, NCOL):
                        acc[rows, n:n + NCOL] += jnp.dot(dz[rows, :], et[slot, :, n:n + NCOL], preferred_element_type=jnp.float32)
                    return c2
                lax.fori_loop(0, HBS, mul, 0)
                return c
            lax.fori_loop(0, VOCAB // KT, step, 0)
        pl.run_scoped(d_phase, pltpu.VMEM((2, TOK, KT), jnp.float32), pltpu.VMEM((2, KT, DIM), jnp.bfloat16),
                      pltpu.VMEM((TOK, KT), jnp.bfloat16), pltpu.VMEM((KT, TOK), jnp.bfloat16),
                      pltpu.VMEM((TOK, 128), jnp.float32), pltpu.VMEM((TOK, 128), jnp.float32), pltpu.VMEM((TOK, 128), jnp.int32))

        def n_phase(hb, ob, mr):
            def h_load(i):
                slot = lax.rem(i, 2)
                return pltpu.make_async_copy(hid.at[pl.ds(pl.multiple_of(i * LN_ROWS, LN_ROWS), LN_ROWS)], hb.at[slot], z_sem.at[slot])

            def o_store(i):
                slot = lax.rem(i, 2)
                return pltpu.make_async_copy(ob.at[slot], dhid.at[pl.ds(pl.multiple_of(i * LN_ROWS, LN_ROWS), LN_ROWS)], e_sem.at[slot])
            mr_loads = [pltpu.make_async_copy(src, mr.at[i], wide_sem.at[i]) for i, src in enumerate((mean_b, rstd_b))]
            for cp in mr_loads:
                cp.start()
            h_load(0).start()
            gb_v[...] = jnp.zeros(gb_v.shape, jnp.float32)
            g8[...] = jnp.broadcast_to(gain[...], (8, DIM))
            for cp in mr_loads:
                cp.wait()

            def tile(i, c):
                slot = lax.rem(i, 2)

                @pl.when(i + 1 < TOK // LN_ROWS)
                def _():
                    h_load(i + 1).start()

                @pl.when(i >= 2)
                def _():
                    o_store(i - 2).wait()
                h_load(i).wait()

                def rows_body(r, c2):
                    units = range(NB_UNROLL)
                    base = r * 16 * NB_UNROLL
                    low = [pl.ds(pl.multiple_of(base + u * 16, 16), 16) for u in units]
                    row = [pl.ds(pl.multiple_of(i * LN_ROWS + base + u * 16, 16), 16) for u in units]
                    zero = jnp.zeros((16, 128), jnp.float32)
                    sum1, sum3 = [zero] * NB_UNROLL, [zero] * NB_UNROLL

                    def load(u, cols):
                        dx = acc[row[u], cols]
                        xhat = (hb[slot, low[u], cols].astype(jnp.float32) - mr[0, row[u], :]) * mr[1, row[u], :]
                        return dx, xhat, dx * jnp.concatenate([g8[:, cols]] * 2, axis=0)
                    for k in range(DIM // 128):
                        cols = slice(k * 128, (k + 1) * 128)
                        d_gain, d_bias = gb_v[0, :, cols], gb_v[1, :, cols]
                        for u in units:
                            dx, xhat, gx = load(u, cols)
                            sum1[u] = sum1[u] + gx
                            sum3[u] = sum3[u] + gx * xhat
                            dgx = dx * xhat
                            d_gain = d_gain + (dgx[0:8] + dgx[8:16])
                            d_bias = d_bias + (dx[0:8] + dx[8:16])
                        gb_v[0, :, cols] = d_gain
                        gb_v[1, :, cols] = d_bias
                    c1 = [jnp.broadcast_to(jnp.sum(v, axis=-1, keepdims=True) * (1.0 / DIM), (16, 128)) for v in sum1]
                    c3 = [jnp.broadcast_to(jnp.sum(v, axis=-1, keepdims=True) * (1.0 / DIM), (16, 128)) for v in sum3]
                    for u in units:
                        for k in range(DIM // 128):
                            cols = slice(k * 128, (k + 1) * 128)
                            _, xhat, gx = load(u, cols)
                            ob[slot, low[u], cols] = (mr[1, row[u], :] * (gx - c1[u] - xhat * c3[u])).astype(jnp.bfloat16)
                            acc[row[u], cols] = zero
                    return c2
                lax.fori_loop(0, LN_ROWS // (16 * NB_UNROLL), rows_body, 0)
                o_store(i).start()
                return c
            lax.fori_loop(0, TOK // LN_ROWS, tile, 0)
            for i in range(2):
                o_store(TOK // LN_ROWS - 2 + i).wait()
            gs_v[0:1, :] = jnp.sum(gb_v[0], axis=0, keepdims=True)
            gs_v[1:2, :] = jnp.sum(gb_v[1], axis=0, keepdims=True)
        pl.run_scoped(n_phase, pltpu.VMEM((2, LN_ROWS, DIM), jnp.bfloat16), pltpu.VMEM((2, LN_ROWS, DIM), jnp.bfloat16),
                      pltpu.VMEM((2, TOK, 128), jnp.float32))
        own = pltpu.make_async_copy(gs_v, gsum_all.at[tp], g_sem)

        def e_phase(eo, xt, dzb, zs):
            eo_load = pltpu.make_async_copy(emb, eo, big_sem)

            def x_load(ref, row, slot):
                return pltpu.make_async_copy(ref.at[pl.ds(pl.multiple_of(row, KT), KT)], xt.at[slot], z_sem.at[slot])

            def dz_load(ref, col, slot):
                return pltpu.make_async_copy(ref.at[:, pl.ds(pl.multiple_of(col, KT), KT)], dzb.at[slot], e_sem.at[slot])

            def start_local(i):
                slot = lax.rem(i, 2)

                @pl.when(i < 4)
                def _():
                    x_load(x_out, i * KT, slot).start()
                    dz_load(dzt_own, i * KT, slot).start()

                @pl.when(i >= 4)
                def _():
                    x_load(x_part, (i - 4) * KT, slot).start()
                    dz_load(dzt_part, (i - 4) * KT, slot).start()

            def add(slot):
                def mul(h, c2):
                    rows = pl.ds(pl.multiple_of(h * HB, HB), HB)
                    for n in range(0, DIM, NCOL):
                        acc[rows, n:n + NCOL] += jnp.dot(dzb[slot, rows, :], xt[slot, :, n:n + NCOL], preferred_element_type=jnp.float32)
                    return c2
                lax.fori_loop(0, HBS, mul, 0)

            start_local(0)

            def rem_load(r):
                slot = lax.rem(r, 2)
                return [pltpu.make_async_copy(xrows(ref, r), xt.at[slot, pl.ds(i * XCH, XCH)], z_sem.at[slot])
                        for i, ref in enumerate((x_xp, x_xq))]

            def local(i, c):
                slot = lax.rem(i, 2)

                @pl.when(i == 0)
                def _():
                    eo_load.start()

                @pl.when(i == 2)
                def _():
                    xp_copy.wait_recv()

                    def wait_dz(q, c2):
                        dzt_copy(q).wait_recv()
                        return c2
                    lax.fori_loop(0, 4, wait_dz, 0)

                @pl.when(i == 1)
                def _():
                    own.start()
                    for p, dev in group:
                        remote(gs_v, gsum_all.at[tp], g_send, g_recv.at[p], dev).start()

                @pl.when(i == 1)
                def _():
                    xt_event(4)

                @pl.when(i == 6)
                def _():
                    xt_event(5)

                @pl.when(i < 7)
                def _():
                    start_local(i + 1)

                @pl.when(i == 7)
                def _():
                    xd_copy(0).wait_recv()
                    for cp in rem_load(0):
                        cp.start()
                x_load(x_out, 0, slot).wait()
                dz_load(dzt_own, 0, slot).wait()
                add(slot)
                return c
            lax.fori_loop(0, 8, local, 0)
            eo_load.wait()
            for p, dev in group:
                remote(stat_v, stat_all.at[tp], sm_send, stat_recv.at[p], dev).wait_recv()
            stat_load = pltpu.make_async_copy(stat_all, stats, small_sem.at[1])
            stat_load.start()
            stat_load.wait()
            count = jnp.broadcast_to(token_count(), (1, 128))

            def far(r, c):
                slot = lax.rem(r, 2)

                @pl.when(r == 2)
                def _():
                    xt_event(6)

                @pl.when(r == 6)
                def _():
                    xt_event(7)

                @pl.when(r + 1 < XCHS)
                def _():
                    xd_copy(r + 1).wait_recv()
                    for cp in rem_load(r + 1):
                        cp.start()
                x_load(x_out, 0, slot).wait()

                @pl.when(r == XCHS - DEFER)
                def _():
                    pltpu.make_async_copy(acc, de_part, big_sem).start()

                @pl.when(r > XCHS - DEFER)
                def _():
                    dz_out(0, 0, slot).wait()
                    dz_out(0, 1, slot).wait()

                far_rows = []
                for g in range(4):
                    who = xp_rank if g < 2 else xq_rank
                    at = pl.ds(2 * r + g % 2, 1)
                    far_rows.append((stats[who, 0, at, :], infos[who, 1, at, :].astype(f32) / count, infos[who, 0, at, :] - tp * ROWS))

                def logits(h, c2):
                    for k in range(0, DIM, KCOL):
                        prod = lax.dot_general(eo[pl.ds(pl.multiple_of(h * ZB, ZB), ZB), k:k + KCOL], xt[slot, :, k:k + KCOL], NT, preferred_element_type=jnp.float32)
                        zs[...] = prod if k == 0 else zs[...] + prod
                    for q in range(ZB // 32):
                        row = h * ZB + q * 32
                        line = lax.broadcasted_iota(jnp.int32, (32, 128), 0)
                        for g, (lse, scale, trel) in enumerate(far_rows):
                            cols = slice(g * 128, (g + 1) * 128)
                            hot = ((trel - row) == line).astype(f32)
                            val = (jnp.exp(zs[q * 32:(q + 1) * 32, cols] - lse) - hot) * scale
                            dzb[0, pl.ds(pl.multiple_of(row, 32), 32), cols] = val.astype(bf16)
                    return c2
                lax.fori_loop(0, ROWS // ZB, logits, 0)

                @pl.when(r < XCHS - DEFER)
                def _():
                    def mul(h, c2):
                        rows = pl.ds(pl.multiple_of(h * HB, HB), HB)
                        for n in range(0, DIM, NCOL):
                            acc[rows, n:n + NCOL] += jnp.dot(dzb[0, rows, :], xt[slot, :, n:n + NCOL], preferred_element_type=jnp.float32)
                        return c2
                    lax.fori_loop(0, HBS, mul, 0)

                @pl.when(r >= XCHS - DEFER)
                def _():
                    for i in range(2):
                        dz_out(r - (XCHS - DEFER), i, 0).start()
                return c

            def dz_out(q, i, slot):
                return pltpu.make_async_copy(
                    dzb.at[0, :, pl.ds(i * XCH, XCH)], dzt_last.at[i, :, pl.ds(pl.multiple_of(q * XCH, XCH), XCH)], dzo_sem)
            lax.fori_loop(0, XCHS, far, 0)
            dz_out(0, 0, 0).wait()
            dz_out(0, 1, 0).wait()
            pltpu.make_async_copy(acc, de_part, big_sem).wait()
        pl.run_scoped(e_phase, pltpu.VMEM((ROWS, DIM), jnp.bfloat16), pltpu.VMEM((2, KT, DIM), jnp.bfloat16),
                      pltpu.VMEM((2, ROWS, KT), jnp.bfloat16), pltpu.VMEM((ZB, KT), jnp.float32))

        own.wait()
    pl.run_scoped(backward, pltpu.VMEM((TOK, DIM), f32))

    pltpu.make_async_copy(x_out, x_out, xt_send).wait()
    pltpu.make_async_copy(x_out, x_out, xd_send).wait()
    xp_copy.wait_send()
    pltpu.make_async_copy(dzt_out, dzt_out, dz_send).wait()
    for p, dev in group:
        remote(info, info_all.at[tp], sm_send, info_recv.at[p], dev).wait_send()
        remote(stat_v, stat_all.at[tp], sm_send, stat_recv.at[p], dev).wait_send()
        remote(gs_v, gsum_all.at[tp], g_send, g_recv.at[p], dev).wait()


def run_step(hidden, gain, bias, embed, tcol, info):
    any_spec = pl.BlockSpec(memory_space=pl.ANY)
    vmem_spec = pl.BlockSpec(memory_space=pltpu.VMEM)
    f32, bf16, i32 = jnp.float32, jnp.bfloat16, jnp.int32
    dma = pltpu.SemaphoreType.DMA
    small = (4, 2, GROUPS, 128)
    wide = ((TOK, 128), f32)
    mat, square = ((TOK, DIM), bf16), ((ROWS, TOK), bf16)
    shapes = [((VOCAB, DIM), bf16), mat, ((TOK, VOCAB), f32), (small, f32), (small, i32), wide, wide, wide,
              mat, mat, mat, mat, square, square, square, ((2, ROWS, DEFER * XCH), bf16), ((ROWS, DIM), f32), ((4, 2, DIM), f32)]
    return pl.pallas_call(
        step_kernel,
        name="step",
        out_shape=[jax.ShapeDtypeStruct(s, d) for s, d in shapes],
        in_specs=[any_spec, vmem_spec, vmem_spec, any_spec, vmem_spec, any_spec],
        out_specs=[any_spec] * len(shapes),
        scratch_shapes=[
            pltpu.VMEM((2, GROUPS, 128), i32), pltpu.VMEM((2, GROUPS, 128), f32), pltpu.VMEM(small, f32), pltpu.VMEM(small, i32),
            pltpu.VMEM((2, 8, DIM), f32), pltpu.VMEM((2, DIM), f32), pltpu.VMEM((8, DIM), f32),
            dma((2,)), dma, dma((2,)), dma((2,)), dma((2,)), dma((2,)), dma((3,)), dma, dma, dma,
            dma, dma, dma, dma, dma, dma, dma, dma, dma, dma,
            dma((CHUNKS,)), dma((CHUNKS,)), dma((TILES // 2,)), dma((4,)), dma((4,)), dma((4,)),
            dma((XCHS,)), dma((XCHS,)), dma, dma((4,)), dma((4,)),
        ],
        compiler_params=pltpu.CompilerParams(collective_id=0, has_side_effects=True, vmem_limit_bytes=67043328),
        cost_estimate=pl.CostEstimate(flops=12 * TOK * VOCAB * DIM, bytes_accessed=700 * 2 ** 20, transcendentals=3 * TOK * VOCAB),
    )(hidden, gain, bias, embed, tcol, info)


def finish_kernel(*refs):
    nb = DEFER * XCH // KT
    de_in, dz0, dz1 = refs[:3]
    xs = refs[3:3 + 2 * nb]
    dh_in, stat_all, info_all, gsum_all, de_out, dh_out, loss, mean, sums = refs[3 + 2 * nb:]
    prod = de_in[...]
    for b in range(nb):
        prod = prod + jnp.dot(dz0[0, :, b * KT:(b + 1) * KT], xs[b][...], preferred_element_type=jnp.float32)
        prod = prod + jnp.dot(dz1[0, :, b * KT:(b + 1) * KT], xs[nb + b][...], preferred_element_type=jnp.float32)
    de_out[...] = prod
    dh_out[...] = dh_in[...]

    @pl.when(pl.program_id(0) == 0)
    def _():
        weights = info_all[:, 1].astype(jnp.float32)
        all_loss = (stat_all[:, 0] - stat_all[:, 1]) * weights
        tp = lax.axis_index('tp')
        loss[...] = (stat_all[tp, 0] - stat_all[tp, 1]) * info_all[tp, 1].astype(jnp.float32)
        mean[...] = jnp.broadcast_to(jnp.sum(all_loss), (1, 128)) / jnp.broadcast_to(jnp.sum(weights), (1, 128))
        sums[...] = ((gsum_all[0] + gsum_all[1]) + gsum_all[2]) + gsum_all[3]


def finish(de_part, dzt_last, x_xp, x_xq, dhid, stat_all, info_all, gsum_all):
    cols = 512
    steps = DIM // cols
    depth = DEFER * XCH
    rows = TOK // steps
    first = (TOK - depth) // KT
    once = pl.Buffered(1)
    x_specs = [pl.BlockSpec((KT, cols), lambda i, b=b: (b, i)) for b in range(first, TOK // KT)]

    def whole(shape):
        return pl.BlockSpec(shape, lambda i: (0,) * len(shape))
    nb = len(x_specs)
    outs = [((ROWS, DIM), jnp.float32), ((TOK, DIM), jnp.bfloat16), ((GROUPS, 128), jnp.float32), ((1, 128), jnp.float32), ((2, DIM), jnp.float32)]
    return pl.pallas_call(
        finish_kernel,
        name="finish",
        grid=(steps,),
        out_shape=[jax.ShapeDtypeStruct(s, d) for s, d in outs],
        in_specs=[
            pl.BlockSpec((ROWS, cols), lambda i: (0, i)),
            pl.BlockSpec((1, ROWS, depth), lambda i: (0, 0, 0), pipeline_mode=once),
            pl.BlockSpec((1, ROWS, depth), lambda i: (1, 0, 0), pipeline_mode=once),
            *x_specs, *x_specs,
            pl.BlockSpec((rows, DIM), lambda i: (i, 0)),
            whole(stat_all.shape), whole(info_all.shape), whole(gsum_all.shape),
        ],
        out_specs=[pl.BlockSpec((ROWS, cols), lambda i: (0, i)), pl.BlockSpec((rows, DIM), lambda i: (i, 0)),
                   whole((GROUPS, 128)), whole((1, 128)), whole((2, DIM))],
        compiler_params=pltpu.CompilerParams(vmem_limit_bytes=60 * 1024 * 1024),
        cost_estimate=pl.CostEstimate(flops=4 * ROWS * DIM * depth, bytes_accessed=120 * 2 ** 20, transcendentals=0),
    )(de_part, dzt_last, dzt_last, *[x_xp] * nb, *[x_xq] * nb, dhid, stat_all, info_all, gsum_all)


def solution(mesh):
    def body(hidden, ln_gain, ln_bias, embed, targets, loss_mask):
        dp, rank = lax.axis_index('dp'), lax.axis_index('tp')
        info = jnp.stack([targets, loss_mask]).reshape(2, GROUPS, 128)
        shard = targets // ROWS
        block = jnp.bitwise_xor(shard, rank)
        row = targets % ROWS
        half = row // (ROWS // 2)
        sub = row % (ROWS // 2)
        piece = (block - 2) * 2 + jnp.bitwise_xor(half, dp)
        far = 2 * ROWS + (sub // 128) * TILE + piece * 128 + sub % 128
        tcol = jnp.where(block < 2, block * ROWS + row, far).reshape(GROUPS, 128)
        outs = run_step(hidden, ln_gain.reshape(1, DIM), ln_bias.reshape(1, DIM), embed, tcol, info)
        stat_all, info_all, dhid, x_xp, x_xq, dzt_last, de_part, gsum_all = (outs[i] for i in (3, 4, 8, 10, 11, 15, 16, 17))
        d_embed, d_hidden, loss, mean, sums = finish(de_part, dzt_last, x_xp, x_xq, dhid, stat_all, info_all, gsum_all)
        return loss.reshape(TOK), mean[0, :1], d_hidden, d_embed, sums[0], sums[1]

    token_rows = P(('dp', 'tp'))
    token_mat = P(('dp', 'tp'), None)
    return jax.shard_map(body, mesh=mesh, in_specs=(token_mat, P(), P(), P('tp', None), token_rows, token_rows), out_specs=(token_rows, P('dp'), token_mat, token_mat, P('dp'), P('dp')), check_vma=False)
```

```python
import functools

import jax
import jax.numpy as jnp
from jax import lax
from jax.experimental import pallas as pl
from jax.experimental.pallas import tpu as pltpu
from jax.sharding import PartitionSpec as P

LN_EPS = 1e-5
LOWEST = float(jnp.finfo(jnp.float32).min)

TOK = 2048
ROWS = 2048
DIM = 4096
VOCAB = 8192
TILE = 512
TILES = VOCAB // TILE
HB = 1024
HBS = TOK // HB
CHUNK = 64
CHUNKS = ROWS // 2 // CHUNK
LN_ROWS = 256
STAT_ROWS = 32
PIECE = 32
LN_UNROLL = 4
XCH = 256
XCHS = TOK // XCH
KT = 512
DEFER = 4
WAIT_STEP = {2: 0, 7: 1, 13: 2}
ZB = 512
NCOL = 512
KCOL = 1024
NB_UNROLL = 8
GROUPS = TOK // 128
NT = (((1,), (1,)), ((), ()))


def peers():
    dp, tp = lax.axis_index('dp'), lax.axis_index('tp')
    core = lax.rem(tp, 2)
    pair = tp - core
    other = 2 - pair
    part = pair + 1 - core
    return dp, tp, (dp, part), (dp, other + core), (dp, other + 1 - core), (1 - dp, tp)


def remote(src, dst, ssem, rsem, dev):
    return pltpu.make_async_remote_copy(
        src_ref=src, dst_ref=dst, send_sem=ssem, recv_sem=rsem, device_id=dev, device_id_type=pl.DeviceIdType.MESH)


def spread(row, rows, dst):
    dst[rows, :] = jnp.transpose(jnp.broadcast_to(row, (128, 128)))


def step_kernel(hid, gain, bias, emb, tcol, info,
                e_all, x_out, z_out, stat_all, info_all, lse_b, mean_b, rstd_b,
                dhid, x_part, x_xp, x_xq, dzt_own, dzt_out, dzt_part, dzt_last, de_part, gsum_all,
                info_v, stat_v, stats, infos, gb_v, gs_v, g8,
                h_sem, xo_sem, e_sem, eo_sem, z_sem, small_sem, wide_sem, dzo_sem, big_sem, g_sem,
                xs_send, ys_send, ds_send, pe_send, sm_send, xt_send, xd_send, xp_send, dz_send, g_send,
                x_recv, y_recv, d_recv, pe_recv, info_recv, stat_recv, xt_recv, xd_recv, xp_recv, dz_recv, g_recv):
    dp, tp, part, xp, xq, yp = peers()
    core = lax.rem(tp, 2)
    xp_rank = 2 - (tp - core) + core
    xq_rank = 2 - (tp - core) + 1 - core
    group = ((1, part), (2, xp), (3, xq))
    barrier = pltpu.get_barrier_semaphore()
    for dev in (part, xp, xq, yp):
        pl.semaphore_signal(barrier, inc=1, device_id=dev, device_id_type=pl.DeviceIdType.MESH)
    pl.semaphore_wait(barrier, 4)

    def xrows(ref, j):
        return ref.at[pl.ds(pl.multiple_of(j * XCH, XCH), XCH)]

    def xt_copy(j):
        return remote(xrows(x_out, j), xrows(x_xp, j), xt_send, xt_recv.at[j], xp)

    def xd_copy(j):
        return remote(xrows(x_xp, j), xrows(x_xq, j), xd_send, xd_recv.at[j], part)

    def xt_event(j):
        xt_copy(j).wait_recv()
        xd_copy(j).start()
    xp_copy = remote(x_out, x_part, xp_send, xp_recv, part)

    def forward(xs, hbuf, ebuf, z0, z1, tc_v, m_s, s_s, t_s, mr_v, gb8):
        def tile_row(j):
            return ROWS * 2 + (j // 2) * TILE + lax.rem(j, 2) * CHUNK

        def x_copy(j):
            src = emb.at[pl.ds(pl.multiple_of(dp * (ROWS // 2) + j * CHUNK, CHUNK), CHUNK)]
            return remote(src, e_all.at[pl.ds(pl.multiple_of(tile_row(j), CHUNK), CHUNK)], xs_send, x_recv.at[j], xp)

        def piece(j, p):
            return e_all.at[pl.ds(pl.multiple_of(tile_row(j) + p * 2 * CHUNK, CHUNK), CHUNK)]

        def y_copy(j):
            return remote(piece(j, 0), piece(j, 1), ys_send, y_recv.at[j], yp)

        def d_copy(j, p):
            return remote(piece(j, p), piece(j, p + 2), ds_send, d_recv.at[j // 2], part)

        def pe_copy(i):
            return remote(emb.at[pl.ds(pl.multiple_of(i * TILE, TILE), TILE)],
                          e_all.at[pl.ds(pl.multiple_of(ROWS + i * TILE, TILE), TILE)], pe_send, pe_recv.at[i], part)

        cp = pltpu.make_async_copy(info, info_v, small_sem.at[0])
        cp.start()

        def h_copy(i):
            return pltpu.make_async_copy(hid.at[pl.ds(pl.multiple_of(i * LN_ROWS, LN_ROWS), LN_ROWS)], hbuf.at[lax.rem(i, 2)], h_sem.at[lax.rem(i, 2)])
        h_copy(0).start()

        for p, dev in group:
            remote(info, info_all.at[tp], sm_send, info_recv.at[p], dev).start()

        def start_x(j, c):
            x_copy(j).start()
            return c
        lax.fori_loop(0, CHUNKS, start_x, 0)

        def start_pe(i, c):
            pe_copy(i).start()
            return c
        lax.fori_loop(0, ROWS // TILE, start_pe, 0)

        def e_load(t):
            slot = lax.rem(t, 2)
            return pltpu.make_async_copy(e_all.at[pl.ds(pl.multiple_of(t * TILE, TILE), TILE)], ebuf.at[slot], e_sem.at[slot])

        def e_load_own(t):
            slot = lax.rem(t, 2)
            return pltpu.make_async_copy(emb.at[pl.ds(pl.multiple_of(t * TILE, TILE), TILE)], ebuf.at[slot], e_sem.at[slot])
        e_load_own(0).start()

        cp.wait()
        pltpu.make_async_copy(info_v, info_all.at[tp], small_sem.at[0]).start()
        gb8[0] = jnp.broadcast_to(gain[...], (8, DIM))
        gb8[1] = jnp.broadcast_to(bias[...], (8, DIM))

        def ln_tile(i, c):
            slot = lax.rem(i, 2)

            @pl.when(i + 1 < TOK // LN_ROWS)
            def _():
                h_copy(i + 1).start()
            h_copy(i).wait()

            def ln_rows(r, c2):
                base = r * LN_UNROLL * 16

                def at(u):
                    return pl.ds(pl.multiple_of(base + u * 16, 16), 16)

                def part_of(u, k):
                    return hbuf[slot, at(u), k * 128:(k + 1) * 128].astype(jnp.float32)
                means, rstds = [], []
                for u in range(LN_UNROLL):
                    tot = part_of(u, 0)
                    for k in range(1, DIM // 128):
                        tot = tot + part_of(u, k)
                    means.append(jnp.broadcast_to(jnp.sum(tot, axis=-1, keepdims=True) * (1.0 / DIM), (16, 128)))
                for u in range(LN_UNROLL):
                    tot = jnp.zeros((16, 128), jnp.float32)
                    for k in range(DIM // 128):
                        diff = part_of(u, k) - means[u]
                        tot = tot + diff * diff
                    var = jnp.sum(tot, axis=-1, keepdims=True) * (1.0 / DIM)
                    rstds.append(jnp.broadcast_to(lax.rsqrt(var + LN_EPS), (16, 128)))
                for u in range(LN_UNROLL):
                    row = pl.ds(pl.multiple_of(i * LN_ROWS + base + u * 16, 16), 16)
                    mr_v[0, row, :] = means[u]
                    mr_v[1, row, :] = rstds[u]
                    for k in range(DIM // 128):
                        cols = slice(k * 128, (k + 1) * 128)
                        g2 = jnp.concatenate([gb8[0, :, cols]] * 2, axis=0)
                        b2 = jnp.concatenate([gb8[1, :, cols]] * 2, axis=0)
                        xs[row, cols] = ((part_of(u, k) - means[u]) * rstds[u] * g2 + b2).astype(jnp.bfloat16)
                return c2
            lax.fori_loop(0, LN_ROWS // (16 * LN_UNROLL), ln_rows, 0)
            rows = pl.ds(pl.multiple_of(i * LN_ROWS, LN_ROWS), LN_ROWS)
            pltpu.make_async_copy(xs.at[rows], x_out.at[rows], xo_sem).start()
            return c
        lax.fori_loop(0, TOK // LN_ROWS, ln_tile, 0)

        for i, dst in enumerate((mean_b, rstd_b)):
            pltpu.make_async_copy(mr_v.at[i], dst, wide_sem.at[i + 1]).start()
        m_s[...] = jnp.full((TOK, 128), LOWEST, jnp.float32)
        s_s[...] = jnp.zeros((TOK, 128), jnp.float32)
        t_s[...] = jnp.zeros((TOK, 128), jnp.float32)
        for r in range(GROUPS):
            spread(tcol[r:r + 1, :], slice(r * 128, (r + 1) * 128), tc_v)
        z1[...] = jnp.full((HB, TILE), LOWEST, jnp.float32)

        zs = (z0, z1)

        def product(t, h):
            zs[h][...] = lax.dot_general(xs[h * HB:(h + 1) * HB, :], ebuf[lax.rem(t, 2)], NT, preferred_element_type=jnp.float32)

        def statistics(t, h):
            z = zs[h]
            lane = lax.broadcasted_iota(jnp.int32, (STAT_ROWS, 128), 1)
            for r in range(0, HB, STAT_ROWS):
                rows = slice(h * HB + r, h * HB + r + STAT_ROWS)
                zk = [z[r:r + STAT_ROWS, k * 128:(k + 1) * 128] for k in range(TILE // 128)]
                old = m_s[rows, :]
                new = jnp.maximum(jnp.maximum(jnp.maximum(zk[0], zk[1]), jnp.maximum(zk[2], zk[3])), old)
                tot = s_s[rows, :] * jnp.exp(old - new)
                tgt = t_s[rows, :]
                diff = tc_v[rows, :] - t * TILE
                for k in range(TILE // 128):
                    tot = tot + jnp.exp(zk[k] - new)
                    tgt = tgt + jnp.where(diff == lane + k * 128, zk[k], 0.0)
                m_s[rows, :] = new
                s_s[rows, :] = tot
                t_s[rows, :] = tgt

        def z_copy(t, h):
            return pltpu.make_async_copy(
                zs[h], z_out.at[pl.ds(h * HB, HB), pl.ds(pl.multiple_of(t * TILE, TILE), TILE)], z_sem.at[h])

        def x_event(j):
            x_copy(j).wait_recv()
            y_copy(j).start()
            d_copy(j, 0).start()

        def y_event(j):
            y_copy(j).wait_recv()
            d_copy(j, 1).start()

        def p_event(k):
            rows = e_all.at[pl.ds(pl.multiple_of(2 * ROWS + k * TILE + TILE // 2, TILE // 2), TILE // 2)]
            pltpu.make_async_copy(rows, rows, d_recv.at[k]).wait()
            e_load(8 + k).start()

        half_tiles = TILES // 2

        def start_events(t):
            @pl.when(t < TILES - 1)
            def _():
                x_event(t)

            @pl.when(t == TILES - 2)
            def _():
                xt_copy(0).start()
                y_event(TILES - 3)
                p_event(6)

            @pl.when(t == TILES - 1)
            def _():
                y_event(TILES - 2)
                y_event(TILES - 1)
                p_event(7)
            e_load(t).wait()

            @pl.when(t < 4)
            def _():
                slot = lax.rem(t, 2)
                pltpu.make_async_copy(ebuf.at[slot], e_all.at[pl.ds(pl.multiple_of(t * TILE, TILE), TILE)], eo_sem.at[slot]).start()

        def middle_events(t):
            @pl.when((t >= 1) & (t < TILES - 2))
            def _():
                y_event(t - 1)

            @pl.when((t >= 1) & (t < 5))
            def _():
                slot = lax.rem(t - 1, 2)
                pltpu.make_async_copy(ebuf.at[slot], e_all.at[pl.ds(0, TILE)], eo_sem.at[slot]).wait()

            @pl.when(t == 8)
            def _():
                pltpu.make_async_copy(xs, x_out, xo_sem).wait()

            @pl.when(t < 3)
            def _():
                e_load_own(t + 1).start()

            @pl.when((t >= 3) & (t < 7))
            def _():
                pe_copy(t - 3).wait_recv()
                e_load(t + 1).start()

            @pl.when((t >= half_tiles - 1) & (t < TILES - 3))
            def _():
                p_event(t - (half_tiles - 1))

            @pl.when(t == TILES - 2)
            def _():
                x_event(TILES - 1)

        def step(t, c):
            @pl.when(t > 0)
            def _():
                z_copy(t - 1, 1).start()
            start_events(t)

            @pl.when(t > 0)
            def _():
                z_copy(t - 1, 0).wait()
            statistics(t - 1, 1)
            product(t, 0)
            z_copy(t, 0).start()
            middle_events(t)

            @pl.when(t > 0)
            def _():
                z_copy(t - 1, 1).wait()
            statistics(t, 0)
            product(t, 1)
            return c
        last = TILES - 1
        lax.fori_loop(0, TILES, step, 0)
        z_copy(last, 1).start()
        statistics(last, 1)

        def finish(i, c):
            for u in range(4):
                r = i * 4 + u
                rows = pl.ds(pl.multiple_of(r * 128, 128), 128)
                m = m_s[rows, :]
                top = jnp.max(m, axis=-1, keepdims=True)
                tot = jnp.sum(s_s[rows, :] * jnp.exp(m - top), axis=-1, keepdims=True)
                lse = jnp.broadcast_to(top + jnp.log(tot), (128, 128))
                tgt = jnp.broadcast_to(jnp.sum(t_s[rows, :], axis=-1, keepdims=True), (128, 128))
                m_s[rows, :] = lse
                stat_v[0, pl.ds(r, 1), :] = jnp.transpose(lse)[0:1, :]
                stat_v[1, pl.ds(r, 1), :] = jnp.transpose(tgt)[0:1, :]
            return c
        lax.fori_loop(0, TOK // 512, finish, 0)
        pltpu.make_async_copy(m_s, lse_b, wide_sem.at[0]).start()
        pltpu.make_async_copy(info_v, info_all.at[tp], small_sem.at[0]).wait()
        for h in range(2):
            z_copy(last, h).wait()
        half = e_all.at[pl.ds(0, ROWS // 2)]
        pltpu.make_async_copy(half, half, xs_send).wait()
        pltpu.make_async_copy(half, half, ys_send).wait()
        full = e_all.at[pl.ds(0, ROWS)]
        pltpu.make_async_copy(full, full, ds_send).wait()
        pltpu.make_async_copy(full, full, pe_send).wait()
        own = pltpu.make_async_copy(stat_v, stat_all.at[tp], small_sem.at[1])
        own.start()
        for p, dev in group:
            remote(stat_v, stat_all.at[tp], sm_send, stat_recv.at[p], dev).start()

        def start_xt(j, c):
            xt_copy(j).start()
            return c
        lax.fori_loop(1, XCHS, start_xt, 0)
        xp_copy.start()
        own.wait()
        for i, (src, dst) in enumerate(((m_s, lse_b), (mr_v.at[0], mean_b), (mr_v.at[1], rstd_b))):
            pltpu.make_async_copy(src, dst, wide_sem.at[i]).wait()
    bf16, f32 = jnp.bfloat16, jnp.float32
    wide = pltpu.VMEM((TOK, 128), f32)
    pl.run_scoped(forward, pltpu.VMEM((TOK, DIM), bf16), pltpu.VMEM((2, LN_ROWS, DIM), bf16), pltpu.VMEM((2, TILE, DIM), bf16),
                  pltpu.VMEM((HB, TILE), f32), pltpu.VMEM((HB, TILE), f32), pltpu.VMEM((TOK, 128), jnp.int32), wide, wide, wide,
                  pltpu.VMEM((2, TOK, 128), f32), pltpu.VMEM((2, 8, DIM), f32))

    def dzt_copy(k):
        rows = pl.ds(pl.multiple_of(lax.rem(k, 4) * KT, KT), KT)
        return remote(dzt_out.at[rows], dzt_part.at[rows], dz_send, dz_recv.at[lax.rem(k, 4)], part)

    def token_count():
        return jnp.sum(infos[:, 1].astype(f32))

    def backward(acc):
        def d_phase(zt, et, da, db, dzt, lse_v, scale_v, tcol_v):
            lse_load = pltpu.make_async_copy(lse_b, lse_v, wide_sem.at[0])
            lse_load.start()
            for p, dev in group:
                remote(info, info_all.at[tp], sm_send, info_recv.at[p], dev).wait_recv()
            info_load = pltpu.make_async_copy(info_all, infos, small_sem.at[0])
            info_load.start()

            def z_load(k):
                slot = lax.rem(k, 2)
                return pltpu.make_async_copy(z_out.at[:, pl.ds(pl.multiple_of(k * KT, KT), KT)], zt.at[slot], z_sem.at[slot])

            def e_load(k):
                slot = lax.rem(k, 2)
                return pltpu.make_async_copy(e_all.at[pl.ds(pl.multiple_of(k * KT, KT), KT)], et.at[slot], e_sem.at[slot])

            def dzt_store(k, ref):
                slot = lax.rem(k, 2)
                return pltpu.make_async_copy(dzt.at[slot], ref.at[pl.ds(pl.multiple_of(lax.rem(k, 4) * KT, KT), KT)], eo_sem.at[slot])
            z_load(0).start()
            e_load(0).start()
            acc[...] = jnp.zeros(acc.shape, jnp.float32)
            info_load.wait()
            lse_load.wait()
            count = jnp.broadcast_to(token_count(), (1, 128))
            for r in range(GROUPS):
                rows = slice(r * 128, (r + 1) * 128)
                spread(info_v[1, r:r + 1, :].astype(f32) / count, rows, scale_v)
                spread(tcol[r:r + 1, :], rows, tcol_v)

            lane = lax.broadcasted_iota(jnp.int32, (PIECE, 128), 1)

            def piece(dst, rows, low, k, tie):
                slot = lax.rem(k, 2)
                lse = lse_v[rows, :]
                if tie is not None:
                    floor = 0.0 - jnp.maximum(0.0 - tie, -LOWEST)
                    lse = jnp.maximum(lse, jnp.concatenate([floor] * (PIECE // 8), axis=0))
                scale = scale_v[rows, :]
                diff = tcol_v[rows, :] - k * KT
                for g in range(KT // 128):
                    cols = slice(g * 128, (g + 1) * 128)
                    hot = (diff == lane + g * 128).astype(f32)
                    val = (jnp.exp(zt[slot, rows, cols] - lse) - hot) * scale
                    dst[low, cols] = val.astype(bf16)

            def half_step(k, src, dst, base, dst_base, dst_k):
                slot = lax.rem(k, 2)
                per = HB // (DIM // NCOL)
                for n in range(DIM // NCOL):
                    cols = slice(n * NCOL, (n + 1) * NCOL)
                    prod = jnp.dot(src[...], et[slot, :, cols], preferred_element_type=f32)
                    acc[base:base + HB, cols] += prod
                    for q in range(0, per, PIECE):
                        at = q * HB // per
                        low = n * per + q
                        piece(dst, slice(dst_base + low, dst_base + low + PIECE), slice(low, low + PIECE), dst_k, prod[at:at + 8, 0:128])
                    if n * per % 256 == 0:
                        low = n * per
                        dzt[slot, :, base + low:base + low + 256] = jnp.transpose(src[low:low + 256, :])

            z_load(0).wait()

            def first(i, c):
                rows = pl.ds(pl.multiple_of(i * PIECE, PIECE), PIECE)
                piece(da, rows, rows, 0, None)
                return c
            lax.fori_loop(0, HB // PIECE, first, 0)

            def step(k, c):
                @pl.when(k + 1 < VOCAB // KT)
                def _():
                    z_load(k + 1).start()
                    e_load(k + 1).start()
                for at, j in WAIT_STEP.items():
                    @pl.when(k == at)
                    def _(j=j):
                        xt_event(j)

                @pl.when((k >= 2) & (k < 10))
                def _():
                    dzt_store(k, dzt_own).wait()

                @pl.when((k >= 6) & (k < 10))
                def _():
                    dzt_copy(k - 2).start()
                e_load(k).wait()
                half_step(k, da, db, 0, HB, k)

                @pl.when(k + 1 < VOCAB // KT)
                def _():
                    z_load(k + 1).wait()
                half_step(k, db, da, HB, 0, k + 1)

                @pl.when(k < 4)
                def _():
                    dzt_store(k, dzt_own).start()

                @pl.when((k >= 4) & (k < 8))
                def _():
                    dzt_store(k, dzt_out).start()
                return c
            lax.fori_loop(0, VOCAB // KT, step, 0)
        half = pltpu.VMEM((HB, KT), bf16)
        pl.run_scoped(d_phase, pltpu.VMEM((2, TOK, KT), f32), pltpu.VMEM((2, KT, DIM), bf16), half, half, pltpu.VMEM((2, KT, TOK), bf16),
                      pltpu.VMEM((TOK, 128), f32), pltpu.VMEM((TOK, 128), f32), pltpu.VMEM((TOK, 128), jnp.int32))

        def n_phase(hb, ob, mr):
            def h_load(i):
                slot = lax.rem(i, 2)
                return pltpu.make_async_copy(hid.at[pl.ds(pl.multiple_of(i * LN_ROWS, LN_ROWS), LN_ROWS)], hb.at[slot], z_sem.at[slot])

            def o_store(i):
                slot = lax.rem(i, 2)
                return pltpu.make_async_copy(ob.at[slot], dhid.at[pl.ds(pl.multiple_of(i * LN_ROWS, LN_ROWS), LN_ROWS)], e_sem.at[slot])
            mr_loads = [pltpu.make_async_copy(src, mr.at[i], wide_sem.at[i]) for i, src in enumerate((mean_b, rstd_b))]
            for cp in mr_loads:
                cp.start()
            h_load(0).start()
            gb_v[...] = jnp.zeros(gb_v.shape, jnp.float32)
            g8[...] = jnp.broadcast_to(gain[...], (8, DIM))
            for cp in mr_loads:
                cp.wait()

            def tile(i, c):
                slot = lax.rem(i, 2)

                @pl.when(i + 1 < TOK // LN_ROWS)
                def _():
                    h_load(i + 1).start()

                @pl.when(i >= 2)
                def _():
                    o_store(i - 2).wait()
                h_load(i).wait()

                def rows_body(r, c2):
                    units = range(NB_UNROLL)
                    base = r * 16 * NB_UNROLL
                    low = [pl.ds(pl.multiple_of(base + u * 16, 16), 16) for u in units]
                    row = [pl.ds(pl.multiple_of(i * LN_ROWS + base + u * 16, 16), 16) for u in units]
                    zero = jnp.zeros((16, 128), jnp.float32)
                    sum1, sum3 = [zero] * NB_UNROLL, [zero] * NB_UNROLL

                    def load(u, cols):
                        dx = acc[row[u], cols]
                        xhat = (hb[slot, low[u], cols].astype(jnp.float32) - mr[0, row[u], :]) * mr[1, row[u], :]
                        return dx, xhat, dx * jnp.concatenate([g8[:, cols]] * 2, axis=0)
                    for k in range(DIM // 128):
                        cols = slice(k * 128, (k + 1) * 128)
                        d_gain, d_bias = gb_v[0, :, cols], gb_v[1, :, cols]
                        for u in units:
                            dx, xhat, gx = load(u, cols)
                            sum1[u] = sum1[u] + gx
                            sum3[u] = sum3[u] + gx * xhat
                            dgx = dx * xhat
                            d_gain = d_gain + (dgx[0:8] + dgx[8:16])
                            d_bias = d_bias + (dx[0:8] + dx[8:16])
                        gb_v[0, :, cols] = d_gain
                        gb_v[1, :, cols] = d_bias
                    c1 = [jnp.broadcast_to(jnp.sum(v, axis=-1, keepdims=True) * (1.0 / DIM), (16, 128)) for v in sum1]
                    c3 = [jnp.broadcast_to(jnp.sum(v, axis=-1, keepdims=True) * (1.0 / DIM), (16, 128)) for v in sum3]
                    for u in units:
                        for k in range(DIM // 128):
                            cols = slice(k * 128, (k + 1) * 128)
                            _, xhat, gx = load(u, cols)
                            ob[slot, low[u], cols] = (mr[1, row[u], :] * (gx - c1[u] - xhat * c3[u])).astype(jnp.bfloat16)
                            acc[row[u], cols] = zero
                    return c2
                lax.fori_loop(0, LN_ROWS // (16 * NB_UNROLL), rows_body, 0)
                o_store(i).start()
                return c
            lax.fori_loop(0, TOK // LN_ROWS, tile, 0)
            for i in range(2):
                o_store(TOK // LN_ROWS - 2 + i).wait()
            gs_v[0:1, :] = jnp.sum(gb_v[0], axis=0, keepdims=True)
            gs_v[1:2, :] = jnp.sum(gb_v[1], axis=0, keepdims=True)
        pl.run_scoped(n_phase, pltpu.VMEM((2, LN_ROWS, DIM), jnp.bfloat16), pltpu.VMEM((2, LN_ROWS, DIM), jnp.bfloat16),
                      pltpu.VMEM((2, TOK, 128), jnp.float32))
        own = pltpu.make_async_copy(gs_v, gsum_all.at[tp], g_sem)
        xt_event(3)

        def e_phase(eo, xt, dzb, zs):
            eo_load = pltpu.make_async_copy(emb, eo, big_sem)

            def x_load(ref, row, slot):
                return pltpu.make_async_copy(ref.at[pl.ds(pl.multiple_of(row, KT), KT)], xt.at[slot], z_sem.at[slot])

            def dz_load(ref, col, slot):
                return pltpu.make_async_copy(ref.at[:, pl.ds(pl.multiple_of(col, KT), KT)], dzb.at[slot], e_sem.at[slot])

            def start_local(i):
                slot = lax.rem(i, 2)

                @pl.when(i < 4)
                def _():
                    x_load(x_out, i * KT, slot).start()
                    dz_load(dzt_own, i * KT, slot).start()

                @pl.when(i >= 4)
                def _():
                    x_load(x_part, (i - 4) * KT, slot).start()
                    dz_load(dzt_part, (i - 4) * KT, slot).start()

            def add(slot):
                def mul(h, c2):
                    rows = pl.ds(pl.multiple_of(h * HB, HB), HB)
                    for n in range(0, DIM, NCOL):
                        acc[rows, n:n + NCOL] += jnp.dot(dzb[slot, rows, :], xt[slot, :, n:n + NCOL], preferred_element_type=jnp.float32)
                    return c2
                lax.fori_loop(0, HBS, mul, 0)

            start_local(0)

            def rem_load(r):
                slot = lax.rem(r, 2)
                return [pltpu.make_async_copy(xrows(ref, r), xt.at[slot, pl.ds(i * XCH, XCH)], z_sem.at[slot])
                        for i, ref in enumerate((x_xp, x_xq))]

            def local(i, c):
                slot = lax.rem(i, 2)

                @pl.when(i == 0)
                def _():
                    eo_load.start()

                @pl.when(i == 2)
                def _():
                    xp_copy.wait_recv()

                    def wait_dz(q, c2):
                        dzt_copy(q).wait_recv()
                        return c2
                    lax.fori_loop(0, 4, wait_dz, 0)

                @pl.when(i == 1)
                def _():
                    own.start()
                    for p, dev in group:
                        remote(gs_v, gsum_all.at[tp], g_send, g_recv.at[p], dev).start()

                @pl.when(i == 4)
                def _():
                    xt_event(4)

                @pl.when(i < 7)
                def _():
                    start_local(i + 1)

                @pl.when(i == 7)
                def _():
                    xd_copy(0).wait_recv()
                    for cp in rem_load(0):
                        cp.start()
                x_load(x_out, 0, slot).wait()
                dz_load(dzt_own, 0, slot).wait()
                add(slot)
                return c
            lax.fori_loop(0, 8, local, 0)
            eo_load.wait()
            for p, dev in group:
                remote(stat_v, stat_all.at[tp], sm_send, stat_recv.at[p], dev).wait_recv()
            stat_load = pltpu.make_async_copy(stat_all, stats, small_sem.at[1])
            stat_load.start()
            stat_load.wait()
            count = jnp.broadcast_to(token_count(), (1, 128))

            def far(r, c):
                slot = lax.rem(r, 2)

                @pl.when(r == 1)
                def _():
                    xt_event(5)

                @pl.when(r == 3)
                def _():
                    xt_event(6)

                @pl.when(r == 6)
                def _():
                    xt_event(7)

                @pl.when(r + 1 < XCHS)
                def _():
                    xd_copy(r + 1).wait_recv()
                    for cp in rem_load(r + 1):
                        cp.start()
                x_load(x_out, 0, slot).wait()

                @pl.when(r == XCHS - DEFER)
                def _():
                    pltpu.make_async_copy(acc, de_part, big_sem).start()

                @pl.when(r > XCHS - DEFER + 1)
                def _():
                    dz_out(0, 0, slot).wait()
                    dz_out(0, 1, slot).wait()

                far_rows = []
                for g in range(4):
                    who = xp_rank if g < 2 else xq_rank
                    at = pl.ds(2 * r + g % 2, 1)
                    far_rows.append((stats[who, 0, at, :], infos[who, 1, at, :].astype(f32) / count, infos[who, 0, at, :] - tp * ROWS))

                def logits(h, c2):
                    for k in range(0, DIM, KCOL):
                        prod = lax.dot_general(eo[pl.ds(pl.multiple_of(h * ZB, ZB), ZB), k:k + KCOL], xt[slot, :, k:k + KCOL], NT, preferred_element_type=jnp.float32)
                        zs[...] = prod if k == 0 else zs[...] + prod
                    for q in range(ZB // 32):
                        row = h * ZB + q * 32
                        line = lax.broadcasted_iota(jnp.int32, (32, 128), 0)
                        for g, (lse, scale, trel) in enumerate(far_rows):
                            cols = slice(g * 128, (g + 1) * 128)
                            hot = ((trel - row) == line).astype(f32)
                            val = (jnp.exp(zs[q * 32:(q + 1) * 32, cols] - lse) - hot) * scale
                            dzb[slot, pl.ds(pl.multiple_of(row, 32), 32), cols] = val.astype(bf16)
                    return c2
                lax.fori_loop(0, ROWS // ZB, logits, 0)

                @pl.when(r < XCHS - DEFER)
                def _():
                    def mul(h, c2):
                        rows = pl.ds(pl.multiple_of(h * HB, HB), HB)
                        for n in range(0, DIM, NCOL):
                            acc[rows, n:n + NCOL] += jnp.dot(dzb[slot, rows, :], xt[slot, :, n:n + NCOL], preferred_element_type=jnp.float32)
                        return c2
                    lax.fori_loop(0, HBS, mul, 0)

                @pl.when(r >= XCHS - DEFER)
                def _():
                    for i in range(2):
                        dz_out(r - (XCHS - DEFER), i, slot).start()
                return c

            def dz_out(q, i, slot):
                return pltpu.make_async_copy(
                    dzb.at[slot, :, pl.ds(i * XCH, XCH)], dzt_last.at[i, :, pl.ds(pl.multiple_of(q * XCH, XCH), XCH)], dzo_sem.at[slot])
            lax.fori_loop(0, XCHS, far, 0)
            for slot in range(2):
                dz_out(0, 0, slot).wait()
                dz_out(0, 1, slot).wait()
            pltpu.make_async_copy(acc, de_part, big_sem).wait()
        pl.run_scoped(e_phase, pltpu.VMEM((ROWS, DIM), jnp.bfloat16), pltpu.VMEM((2, KT, DIM), jnp.bfloat16),
                      pltpu.VMEM((2, ROWS, KT), jnp.bfloat16), pltpu.VMEM((ZB, KT), jnp.float32))

        own.wait()
    pl.run_scoped(backward, pltpu.VMEM((TOK, DIM), f32))

    pltpu.make_async_copy(x_out, x_out, xt_send).wait()
    pltpu.make_async_copy(x_out, x_out, xd_send).wait()
    xp_copy.wait_send()
    pltpu.make_async_copy(dzt_out, dzt_out, dz_send).wait()
    for p, dev in group:
        remote(info, info_all.at[tp], sm_send, info_recv.at[p], dev).wait_send()
        remote(stat_v, stat_all.at[tp], sm_send, stat_recv.at[p], dev).wait_send()
        remote(gs_v, gsum_all.at[tp], g_send, g_recv.at[p], dev).wait()


def run_step(hidden, gain, bias, embed, tcol, info):
    any_spec = pl.BlockSpec(memory_space=pl.ANY)
    vmem_spec = pl.BlockSpec(memory_space=pltpu.VMEM)
    f32, bf16, i32 = jnp.float32, jnp.bfloat16, jnp.int32
    dma = pltpu.SemaphoreType.DMA
    small = (4, 2, GROUPS, 128)
    wide = ((TOK, 128), f32)
    mat, square = ((TOK, DIM), bf16), ((ROWS, TOK), bf16)
    shapes = [((VOCAB, DIM), bf16), mat, ((TOK, VOCAB), f32), (small, f32), (small, i32), wide, wide, wide,
              mat, mat, mat, mat, square, square, square, ((2, ROWS, DEFER * XCH), bf16), ((ROWS, DIM), f32), ((4, 2, DIM), f32)]
    return pl.pallas_call(
        step_kernel,
        name="step",
        out_shape=[jax.ShapeDtypeStruct(s, d) for s, d in shapes],
        in_specs=[any_spec, vmem_spec, vmem_spec, any_spec, vmem_spec, any_spec],
        out_specs=[any_spec] * len(shapes),
        scratch_shapes=[
            pltpu.VMEM((2, GROUPS, 128), i32), pltpu.VMEM((2, GROUPS, 128), f32), pltpu.VMEM(small, f32), pltpu.VMEM(small, i32),
            pltpu.VMEM((2, 8, DIM), f32), pltpu.VMEM((2, DIM), f32), pltpu.VMEM((8, DIM), f32),
            dma((2,)), dma, dma((2,)), dma((2,)), dma((2,)), dma((2,)), dma((3,)), dma((2,)), dma, dma,
            dma, dma, dma, dma, dma, dma, dma, dma, dma, dma,
            dma((CHUNKS,)), dma((CHUNKS,)), dma((TILES // 2,)), dma((4,)), dma((4,)), dma((4,)),
            dma((XCHS,)), dma((XCHS,)), dma, dma((4,)), dma((4,)),
        ],
        compiler_params=pltpu.CompilerParams(collective_id=0, has_side_effects=True, vmem_limit_bytes=67043328),
        cost_estimate=pl.CostEstimate(flops=12 * TOK * VOCAB * DIM, bytes_accessed=700 * 2 ** 20, transcendentals=3 * TOK * VOCAB),
    )(hidden, gain, bias, embed, tcol, info)


def finish_kernel(*refs):
    nb = DEFER * XCH // KT
    de_in, dz0, dz1 = refs[:3]
    xs = refs[3:3 + 2 * nb]
    dh_in, stat_all, info_all, gsum_all, de_out, dh_out, loss, mean, sums = refs[3 + 2 * nb:]
    prod = de_in[...]
    for b in range(nb):
        prod = prod + jnp.dot(dz0[0, :, b * KT:(b + 1) * KT], xs[b][...], preferred_element_type=jnp.float32)
        prod = prod + jnp.dot(dz1[0, :, b * KT:(b + 1) * KT], xs[nb + b][...], preferred_element_type=jnp.float32)
    de_out[...] = prod
    dh_out[...] = dh_in[...]

    @pl.when(pl.program_id(0) == 0)
    def _():
        weights = info_all[:, 1].astype(jnp.float32)
        all_loss = (stat_all[:, 0] - stat_all[:, 1]) * weights
        tp = lax.axis_index('tp')
        loss[...] = (stat_all[tp, 0] - stat_all[tp, 1]) * info_all[tp, 1].astype(jnp.float32)
        mean[...] = jnp.broadcast_to(jnp.sum(all_loss), (1, 128)) / jnp.broadcast_to(jnp.sum(weights), (1, 128))
        sums[...] = ((gsum_all[0] + gsum_all[1]) + gsum_all[2]) + gsum_all[3]


def finish(de_part, dzt_last, x_xp, x_xq, dhid, stat_all, info_all, gsum_all):
    cols = 512
    steps = DIM // cols
    depth = DEFER * XCH
    rows = TOK // steps
    first = (TOK - depth) // KT
    once = pl.Buffered(1)
    x_specs = [pl.BlockSpec((KT, cols), lambda i, b=b: (b, i)) for b in range(first, TOK // KT)]

    def whole(shape):
        return pl.BlockSpec(shape, lambda i: (0,) * len(shape))
    nb = len(x_specs)
    outs = [((ROWS, DIM), jnp.float32), ((TOK, DIM), jnp.bfloat16), ((GROUPS, 128), jnp.float32), ((1, 128), jnp.float32), ((2, DIM), jnp.float32)]
    return pl.pallas_call(
        finish_kernel,
        name="finish",
        grid=(steps,),
        out_shape=[jax.ShapeDtypeStruct(s, d) for s, d in outs],
        in_specs=[
            pl.BlockSpec((ROWS, cols), lambda i: (0, i)),
            pl.BlockSpec((1, ROWS, depth), lambda i: (0, 0, 0), pipeline_mode=once),
            pl.BlockSpec((1, ROWS, depth), lambda i: (1, 0, 0), pipeline_mode=once),
            *x_specs, *x_specs,
            pl.BlockSpec((rows, DIM), lambda i: (i, 0)),
            whole(stat_all.shape), whole(info_all.shape), whole(gsum_all.shape),
        ],
        out_specs=[pl.BlockSpec((ROWS, cols), lambda i: (0, i)), pl.BlockSpec((rows, DIM), lambda i: (i, 0)),
                   whole((GROUPS, 128)), whole((1, 128)), whole((2, DIM))],
        compiler_params=pltpu.CompilerParams(vmem_limit_bytes=60 * 1024 * 1024),
        cost_estimate=pl.CostEstimate(flops=4 * ROWS * DIM * depth, bytes_accessed=120 * 2 ** 20, transcendentals=0),
    )(de_part, dzt_last, dzt_last, *[x_xp] * nb, *[x_xq] * nb, dhid, stat_all, info_all, gsum_all)


def solution(mesh):
    def body(hidden, ln_gain, ln_bias, embed, targets, loss_mask):
        dp, rank = lax.axis_index('dp'), lax.axis_index('tp')
        info = jnp.stack([targets, loss_mask]).reshape(2, GROUPS, 128)
        shard = targets // ROWS
        block = jnp.bitwise_xor(shard, rank)
        row = targets % ROWS
        half = row // (ROWS // 2)
        sub = row % (ROWS // 2)
        piece = (block - 2) * 2 + jnp.bitwise_xor(half, dp)
        far = 2 * ROWS + (sub // 128) * TILE + piece * 128 + sub % 128
        tcol = jnp.where(block < 2, block * ROWS + row, far).reshape(GROUPS, 128)
        outs = run_step(hidden, ln_gain.reshape(1, DIM), ln_bias.reshape(1, DIM), embed, tcol, info)
        stat_all, info_all, dhid, x_xp, x_xq, dzt_last, de_part, gsum_all = (outs[i] for i in (3, 4, 8, 10, 11, 15, 16, 17))
        d_embed, d_hidden, loss, mean, sums = finish(de_part, dzt_last, x_xp, x_xq, dhid, stat_all, info_all, gsum_all)
        return loss.reshape(TOK), mean[0, :1], d_hidden, d_embed, sums[0], sums[1]

    token_rows = P(('dp', 'tp'))
    token_mat = P(('dp', 'tp'), None)
    return jax.shard_map(body, mesh=mesh, in_specs=(token_mat, P(), P(), P('tp', None), token_rows, token_rows), out_specs=(token_rows, P('dp'), token_mat, token_mat, P('dp'), P('dp')), check_vma=False)
```

```python
import functools

import jax
import jax.numpy as jnp
from jax import lax
from jax.experimental import pallas as pl
from jax.experimental.pallas import tpu as pltpu
from jax.sharding import PartitionSpec as P

LN_EPS = 1e-5
LOWEST = float(jnp.finfo(jnp.float32).min)

TOK = 2048
ROWS = 2048
DIM = 4096
VOCAB = 8192
TILE = 256
TILES = VOCAB // TILE
HB = 1024
HBS = TOK // HB
CHUNK = 32
PIECE_ROWS = 2 * CHUNK
NEAR = 2 * ROWS // TILE
PE_ROWS = 512
CHUNKS = ROWS // 2 // CHUNK
LN_ROWS = 256
STAT_ROWS = 32
PIECE = 32
LN_UNROLL = 4
XCH = 256
XCHS = TOK // XCH
KT = 512
DEFER = 4
WAIT_STEP = {4: 0, 9: 1, 14: 2}
ZB = 512
NCOL = 512
KCOL = 1024
NB_UNROLL = 8
NB_ROWS = 128
GROUPS = TOK // 128
NT = (((1,), (1,)), ((), ()))


def peers():
    dp, tp = lax.axis_index('dp'), lax.axis_index('tp')
    core = lax.rem(tp, 2)
    pair = tp - core
    other = 2 - pair
    part = pair + 1 - core
    return dp, tp, (dp, part), (dp, other + core), (dp, other + 1 - core), (1 - dp, tp)


def remote(src, dst, ssem, rsem, dev):
    return pltpu.make_async_remote_copy(
        src_ref=src, dst_ref=dst, send_sem=ssem, recv_sem=rsem, device_id=dev, device_id_type=pl.DeviceIdType.MESH)


def spread(row, rows, dst):
    dst[rows, :] = jnp.transpose(jnp.broadcast_to(row, (128, 128)))


def step_kernel(hid, gain, bias, emb, info,
                e_all, x_out, z_out, stat_all, info_all,
                dhid, x_part, x_xp, x_xq, dzt_own, dzt_out, dzt_part, dzt_last, de_part, gsum_all,
                info_v, stat_v, stats, infos, gb_v, gs_v, g8,
                h_sem, xo_sem, e_sem, eo_sem, z_sem, zt_sem, et_sem, small_sem, dzo_sem, big_sem, g_sem,
                xs_send, ys_send, ds_send, pe_send, sm_send, xt_send, xd_send, xp_send, dz_send, g_send,
                x_recv, y_recv, d_recv, pe_recv, info_recv, stat_recv, xt_recv, xd_recv, xp_recv, dz_recv, g_recv):
    bf16, f32 = jnp.bfloat16, jnp.float32
    dp, tp, part, xp, xq, yp = peers()
    core = lax.rem(tp, 2)
    xp_rank = 2 - (tp - core) + core
    xq_rank = 2 - (tp - core) + 1 - core
    group = ((1, part), (2, xp), (3, xq))
    barrier = pltpu.get_barrier_semaphore()
    for dev in (part, xp, xq, yp):
        pl.semaphore_signal(barrier, inc=1, device_id=dev, device_id_type=pl.DeviceIdType.MESH)
    pl.semaphore_wait(barrier, 4)

    def xrows(ref, j):
        return ref.at[pl.ds(pl.multiple_of(j * XCH, XCH), XCH)]

    def xt_copy(j):
        return remote(xrows(x_out, j), xrows(x_xp, j), xt_send, xt_recv.at[j], xp)

    def xd_copy(j):
        return remote(xrows(x_xp, j), xrows(x_xq, j), xd_send, xd_recv.at[j], part)

    def xt_event(j):
        xt_copy(j).wait_recv()
        xd_copy(j).start()
    xp_copy = remote(x_out, x_part, xp_send, xp_recv, part)

    def forward(m_s, scale_v, tc_v, mr_v, zt, et, xs, hbuf, ebuf, z0, z1, s_s, t_s, gb8):
        def tile_row(j):
            return ROWS * 2 + (j // 2) * TILE + lax.rem(j, 2) * CHUNK

        def x_copy(j):
            src = emb.at[pl.ds(pl.multiple_of(dp * (ROWS // 2) + j * CHUNK, CHUNK), CHUNK)]
            return remote(src, e_all.at[pl.ds(pl.multiple_of(tile_row(j), CHUNK), CHUNK)], xs_send, x_recv.at[j], xp)

        def piece(j, p):
            return e_all.at[pl.ds(pl.multiple_of(tile_row(j) + p * PIECE_ROWS, CHUNK), CHUNK)]

        def y_copy(j):
            return remote(piece(j, 0), piece(j, 1), ys_send, y_recv.at[j], yp)

        def d_copy(j, p):
            return remote(piece(j, p), piece(j, p + 2), ds_send, d_recv.at[j // 2], part)

        def pe_copy(i):
            return remote(emb.at[pl.ds(pl.multiple_of(i * PE_ROWS, PE_ROWS), PE_ROWS)],
                          e_all.at[pl.ds(pl.multiple_of(ROWS + i * PE_ROWS, PE_ROWS), PE_ROWS)], pe_send, pe_recv.at[i], part)

        cp = pltpu.make_async_copy(info, info_v, small_sem.at[0])
        cp.start()

        def h_copy(i):
            return pltpu.make_async_copy(hid.at[pl.ds(pl.multiple_of(i * LN_ROWS, LN_ROWS), LN_ROWS)], hbuf.at[lax.rem(i, 2)], h_sem.at[lax.rem(i, 2)])
        h_copy(0).start()

        for p, dev in group:
            remote(info, info_all.at[tp], sm_send, info_recv.at[p], dev).start()

        def start_x(j, c):
            x_copy(j).start()
            return c
        lax.fori_loop(0, CHUNKS, start_x, 0)

        def start_pe(i, c):
            pe_copy(i).start()
            return c
        lax.fori_loop(0, ROWS // PE_ROWS, start_pe, 0)

        def e_load(t):
            slot = lax.rem(t, 2)
            return pltpu.make_async_copy(e_all.at[pl.ds(pl.multiple_of(t * TILE, TILE), TILE)], ebuf.at[slot], e_sem.at[slot])

        def e_load_own(t):
            slot = lax.rem(t, 2)
            return pltpu.make_async_copy(emb.at[pl.ds(pl.multiple_of(t * TILE, TILE), TILE)], ebuf.at[slot], e_sem.at[slot])
        e_load_own(0).start()

        def x_event(j):
            x_copy(j).wait_recv()
            y_copy(j).start()
            d_copy(j, 0).start()

        def y_event(j):
            y_copy(j).wait_recv()
            d_copy(j, 1).start()

        def p_event(k):
            rows = e_all.at[pl.ds(pl.multiple_of(2 * ROWS + k * TILE + TILE // 2, TILE // 2), TILE // 2)]
            pltpu.make_async_copy(rows, rows, d_recv.at[k]).wait()
            e_load(NEAR + k).start()

        cp.wait()
        pltpu.make_async_copy(info_v, info_all.at[tp], small_sem.at[0]).start()
        gb8[0] = jnp.broadcast_to(gain[...], (8, DIM))
        gb8[1] = jnp.broadcast_to(bias[...], (8, DIM))

        def ln_tile(i, c):
            slot = lax.rem(i, 2)

            @pl.when(i + 1 < TOK // LN_ROWS)
            def _():
                h_copy(i + 1).start()
            h_copy(i).wait()

            @pl.when(i == 6)
            def _():
                x_event(0)

            def ln_rows(r, c2):
                base = r * LN_UNROLL * 16

                def at(u):
                    return pl.ds(pl.multiple_of(base + u * 16, 16), 16)

                def part_of(u, k):
                    return hbuf[slot, at(u), k * 128:(k + 1) * 128].astype(jnp.float32)
                means, rstds = [], []
                for u in range(LN_UNROLL):
                    tot = part_of(u, 0)
                    for k in range(1, DIM // 128):
                        tot = tot + part_of(u, k)
                    means.append(jnp.broadcast_to(jnp.sum(tot, axis=-1, keepdims=True) * (1.0 / DIM), (16, 128)))
                for u in range(LN_UNROLL):
                    tot = jnp.zeros((16, 128), jnp.float32)
                    for k in range(DIM // 128):
                        diff = part_of(u, k) - means[u]
                        tot = tot + diff * diff
                    var = jnp.sum(tot, axis=-1, keepdims=True) * (1.0 / DIM)
                    rstds.append(jnp.broadcast_to(lax.rsqrt(var + LN_EPS), (16, 128)))
                for u in range(LN_UNROLL):
                    row = pl.ds(pl.multiple_of(i * LN_ROWS + base + u * 16, 16), 16)
                    mr_v[0, row, :] = means[u]
                    mr_v[1, row, :] = rstds[u]
                    for k in range(DIM // 128):
                        cols = slice(k * 128, (k + 1) * 128)
                        g2 = jnp.concatenate([gb8[0, :, cols]] * 2, axis=0)
                        b2 = jnp.concatenate([gb8[1, :, cols]] * 2, axis=0)
                        xs[row, cols] = ((part_of(u, k) - means[u]) * rstds[u] * g2 + b2).astype(jnp.bfloat16)
                return c2
            lax.fori_loop(0, LN_ROWS // (16 * LN_UNROLL), ln_rows, 0)
            rows = pl.ds(pl.multiple_of(i * LN_ROWS, LN_ROWS), LN_ROWS)
            pltpu.make_async_copy(xs.at[rows], x_out.at[rows], xo_sem).start()
            return c
        lax.fori_loop(0, TOK // LN_ROWS, ln_tile, 0)

        m_s[...] = jnp.full((TOK, 128), LOWEST, jnp.float32)
        s_s[...] = jnp.zeros((TOK, 128), jnp.float32)
        t_s[...] = jnp.zeros((TOK, 128), jnp.float32)
        for r in range(GROUPS):
            spread(info_v[2, r:r + 1, :], slice(r * 128, (r + 1) * 128), tc_v)
        z1[...] = jnp.full((HB, TILE), LOWEST, jnp.float32)

        zs = (z0, z1)

        def product(t, h):
            for r in range(0, HB, 512):
                zs[h][r:r + 512, :] = lax.dot_general(
                    xs[h * HB + r:h * HB + r + 512, :], ebuf[lax.rem(t, 2)], NT, preferred_element_type=jnp.float32)

        def statistics(t, h):
            z = zs[h]
            lane = lax.broadcasted_iota(jnp.int32, (STAT_ROWS, 128), 1)
            for r in range(0, HB, STAT_ROWS):
                rows = slice(h * HB + r, h * HB + r + STAT_ROWS)
                zk = [z[r:r + STAT_ROWS, k * 128:(k + 1) * 128] for k in range(TILE // 128)]
                old = m_s[rows, :]
                new = jnp.maximum(jnp.maximum(zk[0], zk[1]), old)
                tot = s_s[rows, :] * jnp.exp(old - new)
                tgt = t_s[rows, :]
                diff = tc_v[rows, :] - t * TILE
                for k in range(TILE // 128):
                    tot = tot + jnp.exp(zk[k] - new)
                    tgt = tgt + jnp.where(diff == lane + k * 128, zk[k], 0.0)
                m_s[rows, :] = new
                s_s[rows, :] = tot
                t_s[rows, :] = tgt

        def z_copy(t, h):
            return pltpu.make_async_copy(
                zs[h], z_out.at[pl.ds(h * HB, HB), pl.ds(pl.multiple_of(t * TILE, TILE), TILE)], z_sem.at[h])

        def start_events(t):
            @pl.when(t < TILES - 1)
            def _():
                x_event(t + 1)

            @pl.when(t == TILES - 2)
            def _():
                xt_copy(0).start()

            @pl.when(t == TILES - 1)
            def _():
                y_event(TILES - 1)
                p_event(TILES - 1 - NEAR)
            e_load(t).wait()

            @pl.when(t < ROWS // TILE)
            def _():
                slot = lax.rem(t, 2)
                pltpu.make_async_copy(ebuf.at[slot], e_all.at[pl.ds(pl.multiple_of(t * TILE, TILE), TILE)], eo_sem.at[slot]).start()

        def middle_events(t):
            @pl.when(t < TILES - 1)
            def _():
                y_event(t)

            @pl.when((t >= 1) & (t < ROWS // TILE + 1))
            def _():
                slot = lax.rem(t - 1, 2)
                pltpu.make_async_copy(ebuf.at[slot], e_all.at[pl.ds(0, TILE)], eo_sem.at[slot]).wait()

            @pl.when(t == NEAR)
            def _():
                pltpu.make_async_copy(xs, x_out, xo_sem).wait()

            @pl.when(t < ROWS // TILE - 1)
            def _():
                e_load_own(t + 1).start()

            @pl.when((t >= ROWS // TILE - 1) & (t < NEAR - 1))
            def _():
                @pl.when(lax.rem(t + 1, PE_ROWS // TILE) == 0)
                def _():
                    pe_copy((t + 1 - ROWS // TILE) // (PE_ROWS // TILE)).wait_recv()
                e_load(t + 1).start()

            @pl.when((t >= NEAR - 1) & (t < TILES - 2))
            def _():
                p_event(t - (NEAR - 1))

            @pl.when(t == NEAR + 1)
            def _():
                for p, dev in group:
                    remote(info, info_all.at[tp], sm_send, info_recv.at[p], dev).wait_recv()
                pltpu.make_async_copy(info_v, info_all.at[tp], small_sem.at[0]).wait()
                load = pltpu.make_async_copy(info_all, infos, small_sem.at[0])
                load.start()
                load.wait()
                count = jnp.broadcast_to(token_count(), (1, 128))
                for r in range(GROUPS):
                    spread(info_v[1, r:r + 1, :].astype(f32) / count, slice(r * 128, (r + 1) * 128), scale_v)

        def step(t, c):
            @pl.when(t > 0)
            def _():
                z_copy(t - 1, 1).start()
            start_events(t)

            @pl.when(t > 0)
            def _():
                z_copy(t - 1, 0).wait()
            statistics(t - 1, 1)
            product(t, 0)
            z_copy(t, 0).start()
            middle_events(t)

            @pl.when(t > 0)
            def _():
                z_copy(t - 1, 1).wait()
            statistics(t, 0)
            product(t, 1)
            return c
        last = TILES - 1
        lax.fori_loop(0, TILES, step, 0)
        z_copy(last, 1).start()
        statistics(last, 1)

        def finish(i, c):
            for u in range(4):
                r = i * 4 + u
                rows = pl.ds(pl.multiple_of(r * 128, 128), 128)
                m = m_s[rows, :]
                top = jnp.max(m, axis=-1, keepdims=True)
                tot = jnp.sum(s_s[rows, :] * jnp.exp(m - top), axis=-1, keepdims=True)
                lse = jnp.broadcast_to(top + jnp.log(tot), (128, 128))
                tgt = jnp.broadcast_to(jnp.sum(t_s[rows, :], axis=-1, keepdims=True), (128, 128))
                m_s[rows, :] = lse
                stat_v[0, pl.ds(r, 1), :] = jnp.transpose(lse)[0:1, :]
                stat_v[1, pl.ds(r, 1), :] = jnp.transpose(tgt)[0:1, :]
            return c
        lax.fori_loop(0, TOK // 512, finish, 0)
        for h in range(2):
            z_copy(last, h).wait()
        z_load(zt, 0).start()
        et_load(et, 0).start()
        half = e_all.at[pl.ds(0, ROWS // 2)]
        pltpu.make_async_copy(half, half, xs_send).wait()
        pltpu.make_async_copy(half, half, ys_send).wait()
        full = e_all.at[pl.ds(0, ROWS)]
        pltpu.make_async_copy(full, full, ds_send).wait()
        pltpu.make_async_copy(full, full, pe_send).wait()
        pltpu.make_async_copy(stat_v, stat_all.at[tp], small_sem.at[1]).start()
        for p, dev in group:
            remote(stat_v, stat_all.at[tp], sm_send, stat_recv.at[p], dev).start()

        def start_xt(j, c):
            xt_copy(j).start()
            return c
        lax.fori_loop(1, XCHS, start_xt, 0)
        xp_copy.start()

    def z_load(zt, k):
        slot = lax.rem(k, 2)
        return pltpu.make_async_copy(z_out.at[:, pl.ds(pl.multiple_of(k * KT, KT), KT)], zt.at[slot], zt_sem.at[slot])

    def et_load(et, k):
        slot = lax.rem(k, 2)
        return pltpu.make_async_copy(e_all.at[pl.ds(pl.multiple_of(k * KT, KT), KT)], et.at[slot], et_sem.at[slot])

    def dzt_copy(k):
        rows = pl.ds(pl.multiple_of(lax.rem(k, 4) * KT, KT), KT)
        return remote(dzt_out.at[rows], dzt_part.at[rows], dz_send, dz_recv.at[lax.rem(k, 4)], part)

    def token_count():
        return jnp.sum(infos[:, 1].astype(f32))

    def token_grads(lse_v, scale_v, tcol_v, mr, zt, et, acc):
        def d_phase(da, db, dzt):
            def dzt_store(k, ref):
                slot = lax.rem(k, 2)
                return pltpu.make_async_copy(dzt.at[slot], ref.at[pl.ds(pl.multiple_of(lax.rem(k, 4) * KT, KT), KT)], eo_sem.at[slot])
            acc[...] = jnp.zeros(acc.shape, f32)
            lane = lax.broadcasted_iota(jnp.int32, (PIECE, 128), 1)

            def piece(dst, rows, low, k, tie):
                slot = lax.rem(k, 2)
                lse = lse_v[rows, :]
                if tie is not None:
                    floor = 0.0 - jnp.maximum(0.0 - tie, -LOWEST)
                    lse = jnp.maximum(lse, jnp.concatenate([floor] * (PIECE // 8), axis=0))
                scale = scale_v[rows, :]
                diff = tcol_v[rows, :] - k * KT
                for g in range(KT // 128):
                    cols = slice(g * 128, (g + 1) * 128)
                    hot = (diff == lane + g * 128).astype(f32)
                    val = (jnp.exp(zt[slot, rows, cols] - lse) - hot) * scale
                    dst[low, cols] = val.astype(bf16)

            def half_step(k, src, dst, base, dst_base, dst_k):
                slot = lax.rem(k, 2)
                per = HB // (DIM // NCOL)
                for n in range(DIM // NCOL):
                    cols = slice(n * NCOL, (n + 1) * NCOL)
                    prod = jnp.dot(src[...], et[slot, :, cols], preferred_element_type=f32)
                    acc[base:base + HB, cols] += prod
                    for q in range(0, per, PIECE):
                        at = q * HB // per
                        low = n * per + q
                        piece(dst, slice(dst_base + low, dst_base + low + PIECE), slice(low, low + PIECE), dst_k, prod[at:at + 8, 0:128])
                    if n * per % 256 == 0:
                        low = n * per
                        dzt[slot, :, base + low:base + low + 256] = jnp.transpose(src[low:low + 256, :])

            z_load(zt, 0).wait()

            def first(i, c):
                rows = pl.ds(pl.multiple_of(i * PIECE, PIECE), PIECE)
                piece(da, rows, rows, 0, None)
                return c
            lax.fori_loop(0, HB // PIECE, first, 0)

            def step(k, c):
                @pl.when(k + 1 < VOCAB // KT)
                def _():
                    z_load(zt, k + 1).start()
                    et_load(et, k + 1).start()
                for at, j in WAIT_STEP.items():
                    @pl.when(k == at)
                    def _(j=j):
                        xt_event(j)

                @pl.when((k >= 2) & (k < 10))
                def _():
                    dzt_store(k, dzt_own).wait()

                @pl.when((k >= 6) & (k < 10))
                def _():
                    dzt_copy(k - 2).start()
                et_load(et, k).wait()
                half_step(k, da, db, 0, HB, k)

                @pl.when(k + 1 < VOCAB // KT)
                def _():
                    z_load(zt, k + 1).wait()
                half_step(k, db, da, HB, 0, k + 1)

                @pl.when(k < 4)
                def _():
                    dzt_store(k, dzt_own).start()

                @pl.when((k >= 4) & (k < 8))
                def _():
                    dzt_store(k, dzt_out).start()
                return c
            lax.fori_loop(0, VOCAB // KT, step, 0)
        half = pltpu.VMEM((HB, KT), bf16)
        pl.run_scoped(d_phase, half, half, pltpu.VMEM((2, KT, TOK), bf16))

        def n_phase(hb, ob):
            def h_load(i):
                slot = lax.rem(i, 2)
                return pltpu.make_async_copy(hid.at[pl.ds(pl.multiple_of(i * NB_ROWS, NB_ROWS), NB_ROWS)], hb.at[slot], z_sem.at[slot])

            def o_store(i):
                slot = lax.rem(i, 2)
                return pltpu.make_async_copy(ob.at[slot], dhid.at[pl.ds(pl.multiple_of(i * NB_ROWS, NB_ROWS), NB_ROWS)], e_sem.at[slot])
            h_load(0).start()
            gb_v[...] = jnp.zeros(gb_v.shape, jnp.float32)
            g8[...] = jnp.broadcast_to(gain[...], (8, DIM))

            def tile(i, c):
                slot = lax.rem(i, 2)

                @pl.when(i + 1 < TOK // NB_ROWS)
                def _():
                    h_load(i + 1).start()

                @pl.when(i >= 2)
                def _():
                    o_store(i - 2).wait()
                h_load(i).wait()

                def rows_body(r, c2):
                    units = range(NB_UNROLL)
                    base = r * 16 * NB_UNROLL
                    low = [pl.ds(pl.multiple_of(base + u * 16, 16), 16) for u in units]
                    row = [pl.ds(pl.multiple_of(i * NB_ROWS + base + u * 16, 16), 16) for u in units]
                    zero = jnp.zeros((16, 128), jnp.float32)
                    sum1, sum3 = [zero] * NB_UNROLL, [zero] * NB_UNROLL

                    def load(u, cols):
                        dx = acc[row[u], cols]
                        xhat = (hb[slot, low[u], cols].astype(jnp.float32) - mr[0, row[u], :]) * mr[1, row[u], :]
                        return dx, xhat, dx * jnp.concatenate([g8[:, cols]] * 2, axis=0)
                    for k in range(DIM // 128):
                        cols = slice(k * 128, (k + 1) * 128)
                        d_gain, d_bias = gb_v[0, :, cols], gb_v[1, :, cols]
                        for u in units:
                            dx, xhat, gx = load(u, cols)
                            sum1[u] = sum1[u] + gx
                            sum3[u] = sum3[u] + gx * xhat
                            dgx = dx * xhat
                            d_gain = d_gain + (dgx[0:8] + dgx[8:16])
                            d_bias = d_bias + (dx[0:8] + dx[8:16])
                        gb_v[0, :, cols] = d_gain
                        gb_v[1, :, cols] = d_bias
                    c1 = [jnp.broadcast_to(jnp.sum(v, axis=-1, keepdims=True) * (1.0 / DIM), (16, 128)) for v in sum1]
                    c3 = [jnp.broadcast_to(jnp.sum(v, axis=-1, keepdims=True) * (1.0 / DIM), (16, 128)) for v in sum3]
                    for u in units:
                        for k in range(DIM // 128):
                            cols = slice(k * 128, (k + 1) * 128)
                            _, xhat, gx = load(u, cols)
                            ob[slot, low[u], cols] = (mr[1, row[u], :] * (gx - c1[u] - xhat * c3[u])).astype(jnp.bfloat16)
                    return c2
                lax.fori_loop(0, NB_ROWS // (16 * NB_UNROLL), rows_body, 0)
                o_store(i).start()
                return c
            lax.fori_loop(0, TOK // NB_ROWS, tile, 0)
            for i in range(2):
                o_store(TOK // NB_ROWS - 2 + i).wait()
            gs_v[0:1, :] = jnp.sum(gb_v[0], axis=0, keepdims=True)
            gs_v[1:2, :] = jnp.sum(gb_v[1], axis=0, keepdims=True)
        pl.run_scoped(n_phase, pltpu.VMEM((2, NB_ROWS, DIM), bf16), pltpu.VMEM((2, NB_ROWS, DIM), bf16))

    def weight_grads(acc):
        own = pltpu.make_async_copy(gs_v, gsum_all.at[tp], g_sem)
        xt_event(3)

        def e_phase(eo, xt, dzb, zs):
            eo_load = pltpu.make_async_copy(emb, eo, big_sem)

            def x_load(ref, row, slot):
                return pltpu.make_async_copy(ref.at[pl.ds(pl.multiple_of(row, KT), KT)], xt.at[slot], z_sem.at[slot])

            def dz_load(ref, col, slot):
                return pltpu.make_async_copy(ref.at[:, pl.ds(pl.multiple_of(col, KT), KT)], dzb.at[slot], e_sem.at[slot])

            def start_local(i):
                slot = lax.rem(i, 2)

                @pl.when(i < 4)
                def _():
                    x_load(x_out, i * KT, slot).start()
                    dz_load(dzt_own, i * KT, slot).start()

                @pl.when(i >= 4)
                def _():
                    x_load(x_part, (i - 4) * KT, slot).start()
                    dz_load(dzt_part, (i - 4) * KT, slot).start()

            def add(slot):
                def mul(h, c2):
                    rows = pl.ds(pl.multiple_of(h * HB, HB), HB)
                    for n in range(0, DIM, NCOL):
                        acc[rows, n:n + NCOL] += jnp.dot(dzb[slot, rows, :], xt[slot, :, n:n + NCOL], preferred_element_type=jnp.float32)
                    return c2
                lax.fori_loop(0, HBS, mul, 0)

            start_local(0)
            acc[...] = jnp.zeros(acc.shape, f32)

            def rem_load(r):
                slot = lax.rem(r, 2)
                return [pltpu.make_async_copy(xrows(ref, r), xt.at[slot, pl.ds(i * XCH, XCH)], z_sem.at[slot])
                        for i, ref in enumerate((x_xp, x_xq))]

            def local(i, c):
                slot = lax.rem(i, 2)

                @pl.when(i == 0)
                def _():
                    eo_load.start()

                @pl.when(i == 2)
                def _():
                    xp_copy.wait_recv()

                    def wait_dz(q, c2):
                        dzt_copy(q).wait_recv()
                        return c2
                    lax.fori_loop(0, 4, wait_dz, 0)

                @pl.when(i == 1)
                def _():
                    own.start()
                    for p, dev in group:
                        remote(gs_v, gsum_all.at[tp], g_send, g_recv.at[p], dev).start()

                @pl.when(i == 5)
                def _():
                    xt_event(4)

                @pl.when(i < 7)
                def _():
                    start_local(i + 1)

                @pl.when(i == 7)
                def _():
                    xd_copy(0).wait_recv()
                    for cp in rem_load(0):
                        cp.start()
                x_load(x_out, 0, slot).wait()
                dz_load(dzt_own, 0, slot).wait()
                add(slot)
                return c
            lax.fori_loop(0, 8, local, 0)
            eo_load.wait()
            for p, dev in group:
                remote(stat_v, stat_all.at[tp], sm_send, stat_recv.at[p], dev).wait_recv()
            pltpu.make_async_copy(stat_v, stat_all.at[tp], small_sem.at[1]).wait()
            stat_load = pltpu.make_async_copy(stat_all, stats, small_sem.at[1])
            stat_load.start()
            stat_load.wait()
            count = jnp.broadcast_to(token_count(), (1, 128))

            def far(r, c):
                slot = lax.rem(r, 2)

                @pl.when(r == 1)
                def _():
                    xt_event(5)

                @pl.when(r == 4)
                def _():
                    xt_event(6)

                def fetch():
                    xd_copy(r + 1).wait_recv()
                    for cp in rem_load(r + 1):
                        cp.start()
                pl.when(r < XCHS - 2)(fetch)
                x_load(x_out, 0, slot).wait()

                @pl.when(r == XCHS - DEFER)
                def _():
                    pltpu.make_async_copy(acc, de_part, big_sem).start()

                @pl.when(r > XCHS - DEFER + 1)
                def _():
                    dz_out(0, 0, slot).wait()
                    dz_out(0, 1, slot).wait()

                far_rows = []
                for g in range(4):
                    who = xp_rank if g < 2 else xq_rank
                    at = pl.ds(2 * r + g % 2, 1)
                    far_rows.append((stats[who, 0, at, :], infos[who, 1, at, :].astype(f32) / count, infos[who, 0, at, :] - tp * ROWS))

                def logits(h, c2):
                    for k in range(0, DIM, KCOL):
                        prod = lax.dot_general(eo[pl.ds(pl.multiple_of(h * ZB, ZB), ZB), k:k + KCOL], xt[slot, :, k:k + KCOL], NT, preferred_element_type=jnp.float32)
                        zs[...] = prod if k == 0 else zs[...] + prod
                    for q in range(ZB // 32):
                        row = h * ZB + q * 32
                        line = lax.broadcasted_iota(jnp.int32, (32, 128), 0)
                        for g, (lse, scale, trel) in enumerate(far_rows):
                            cols = slice(g * 128, (g + 1) * 128)
                            hot = ((trel - row) == line).astype(f32)
                            val = (jnp.exp(zs[q * 32:(q + 1) * 32, cols] - lse) - hot) * scale
                            dzb[slot, pl.ds(pl.multiple_of(row, 32), 32), cols] = val.astype(bf16)
                    return c2
                lax.fori_loop(0, ROWS // ZB, logits, 0)

                @pl.when(r == XCHS - 2)
                def _():
                    xt_event(XCHS - 1)
                    fetch()

                @pl.when(r < XCHS - DEFER)
                def _():
                    def mul(h, c2):
                        rows = pl.ds(pl.multiple_of(h * HB, HB), HB)
                        for n in range(0, DIM, NCOL):
                            acc[rows, n:n + NCOL] += jnp.dot(dzb[slot, rows, :], xt[slot, :, n:n + NCOL], preferred_element_type=jnp.float32)
                        return c2
                    lax.fori_loop(0, HBS, mul, 0)

                @pl.when(r >= XCHS - DEFER)
                def _():
                    for i in range(2):
                        dz_out(r - (XCHS - DEFER), i, slot).start()
                return c

            def dz_out(q, i, slot):
                return pltpu.make_async_copy(
                    dzb.at[slot, :, pl.ds(i * XCH, XCH)], dzt_last.at[i, :, pl.ds(pl.multiple_of(q * XCH, XCH), XCH)], dzo_sem.at[slot])
            lax.fori_loop(0, XCHS, far, 0)
            for slot in range(2):
                dz_out(0, 0, slot).wait()
                dz_out(0, 1, slot).wait()
            pltpu.make_async_copy(acc, de_part, big_sem).wait()
        pl.run_scoped(e_phase, pltpu.VMEM((ROWS, DIM), jnp.bfloat16), pltpu.VMEM((2, KT, DIM), jnp.bfloat16),
                      pltpu.VMEM((2, ROWS, KT), jnp.bfloat16), pltpu.VMEM((ZB, KT), jnp.float32))

        own.wait()

    wide = pltpu.VMEM((TOK, 128), f32)
    big = pltpu.VMEM((TOK, DIM), f32)

    def tokens(m_s, scale_v, tc_v, mr_v, zt, et):
        kept = (m_s, scale_v, tc_v, mr_v, zt, et)
        pl.run_scoped(functools.partial(forward, *kept), pltpu.VMEM((TOK, DIM), bf16), pltpu.VMEM((2, LN_ROWS, DIM), bf16),
                      pltpu.VMEM((2, TILE, DIM), bf16), pltpu.VMEM((HB, TILE), f32), pltpu.VMEM((HB, TILE), f32), wide, wide,
                      pltpu.VMEM((2, 8, DIM), f32))
        pl.run_scoped(functools.partial(token_grads, *kept), big)
    pl.run_scoped(tokens, wide, wide, pltpu.VMEM((TOK, 128), jnp.int32), pltpu.VMEM((2, TOK, 128), f32),
                  pltpu.VMEM((2, TOK, KT), f32), pltpu.VMEM((2, KT, DIM), bf16))
    pl.run_scoped(weight_grads, big)

    pltpu.make_async_copy(x_out, x_out, xt_send).wait()
    pltpu.make_async_copy(x_out, x_out, xd_send).wait()
    xp_copy.wait_send()
    pltpu.make_async_copy(dzt_out, dzt_out, dz_send).wait()
    for p, dev in group:
        remote(info, info_all.at[tp], sm_send, info_recv.at[p], dev).wait_send()
        remote(stat_v, stat_all.at[tp], sm_send, stat_recv.at[p], dev).wait_send()
        remote(gs_v, gsum_all.at[tp], g_send, g_recv.at[p], dev).wait()


def run_step(hidden, gain, bias, embed, info):
    any_spec = pl.BlockSpec(memory_space=pl.ANY)
    vmem_spec = pl.BlockSpec(memory_space=pltpu.VMEM)
    f32, bf16, i32 = jnp.float32, jnp.bfloat16, jnp.int32
    dma = pltpu.SemaphoreType.DMA
    small, ints = (4, 2, GROUPS, 128), (4, 3, GROUPS, 128)
    mat, square = ((TOK, DIM), bf16), ((ROWS, TOK), bf16)
    shapes = [((VOCAB, DIM), bf16), mat, ((TOK, VOCAB), f32), (small, f32), (ints, i32),
              mat, mat, mat, mat, square, square, square, ((2, ROWS, DEFER * XCH), bf16), ((ROWS, DIM), f32), ((4, 2, DIM), f32)]
    return pl.pallas_call(
        step_kernel,
        name="step",
        out_shape=[jax.ShapeDtypeStruct(s, d) for s, d in shapes],
        in_specs=[any_spec, vmem_spec, vmem_spec, any_spec, any_spec],
        out_specs=[any_spec] * len(shapes),
        scratch_shapes=[
            pltpu.VMEM((3, GROUPS, 128), i32), pltpu.VMEM((2, GROUPS, 128), f32), pltpu.VMEM(small, f32), pltpu.VMEM(ints, i32),
            pltpu.VMEM((2, 8, DIM), f32), pltpu.VMEM((2, DIM), f32), pltpu.VMEM((8, DIM), f32),
            dma((2,)), dma, dma((2,)), dma((2,)), dma((2,)), dma((2,)), dma((2,)), dma((2,)), dma((2,)), dma, dma,
            dma, dma, dma, dma, dma, dma, dma, dma, dma, dma,
            dma((CHUNKS,)), dma((CHUNKS,)), dma((TILES - NEAR,)), dma((ROWS // PE_ROWS,)), dma((4,)), dma((4,)),
            dma((XCHS,)), dma((XCHS,)), dma, dma((4,)), dma((4,)),
        ],
        compiler_params=pltpu.CompilerParams(collective_id=0, has_side_effects=True, vmem_limit_bytes=67043328),
        cost_estimate=pl.CostEstimate(flops=12 * TOK * VOCAB * DIM, bytes_accessed=700 * 2 ** 20, transcendentals=3 * TOK * VOCAB),
    )(hidden, gain, bias, embed, info)


def finish_kernel(*refs):
    nb = DEFER * XCH // KT
    de_in, dz0, dz1 = refs[:3]
    xs = refs[3:3 + 2 * nb]
    dh_in, stat_all, info_all, gsum_all, de_out, dh_out, loss, mean, d_gain, d_bias = refs[3 + 2 * nb:]
    for h in range(HBS):
        rows = slice(h * HB, (h + 1) * HB)
        prod = None
        for b in range(nb):
            for dz, x in ((dz0, xs[b]), (dz1, xs[nb + b])):
                part = jnp.dot(dz[0, rows, b * KT:(b + 1) * KT], x[...], preferred_element_type=jnp.float32)
                prod = part if prod is None else prod + part
        de_out[rows, :] = de_in[rows, :] + prod
    dh_out[...] = dh_in[...]

    @pl.when(pl.program_id(0) == 0)
    def _():
        weights = info_all[:, 1].astype(jnp.float32)
        all_loss = (stat_all[:, 0] - stat_all[:, 1]) * weights
        tp = lax.axis_index('tp')
        loss[...] = (stat_all[tp, 0] - stat_all[tp, 1]) * info_all[tp, 1].astype(jnp.float32)
        mean[...] = jnp.broadcast_to(jnp.sum(all_loss), (1, 1)) / jnp.broadcast_to(jnp.sum(weights), (1, 1))
        sums = ((gsum_all[0] + gsum_all[1]) + gsum_all[2]) + gsum_all[3]
        d_gain[...] = sums[0:1]
        d_bias[...] = sums[1:2]


def finish(de_part, dzt_last, x_xp, x_xq, dhid, stat_all, info_all, gsum_all):
    cols = 512
    steps = DIM // cols
    depth = DEFER * XCH
    rows = TOK // steps
    first = (TOK - depth) // KT
    once = pl.Buffered(1)
    x_specs = [pl.BlockSpec((KT, cols), lambda i, b=b: (b, i)) for b in range(first, TOK // KT)]

    def whole(shape):
        return pl.BlockSpec(shape, lambda i: (0,) * len(shape))
    nb = len(x_specs)
    outs = [((ROWS, DIM), jnp.float32), ((TOK, DIM), jnp.bfloat16), ((GROUPS, 128), jnp.float32), ((1, 1), jnp.float32), ((1, DIM), jnp.float32), ((1, DIM), jnp.float32)]
    return pl.pallas_call(
        finish_kernel,
        name="finish",
        grid=(steps,),
        out_shape=[jax.ShapeDtypeStruct(s, d) for s, d in outs],
        in_specs=[
            pl.BlockSpec((ROWS, cols), lambda i: (0, i)),
            pl.BlockSpec((1, ROWS, depth), lambda i: (0, 0, 0), pipeline_mode=once),
            pl.BlockSpec((1, ROWS, depth), lambda i: (1, 0, 0), pipeline_mode=once),
            *x_specs, *x_specs,
            pl.BlockSpec((rows, DIM), lambda i: (i, 0)),
            whole(stat_all.shape), whole(info_all.shape), whole(gsum_all.shape),
        ],
        out_specs=[pl.BlockSpec((ROWS, cols), lambda i: (0, i)), pl.BlockSpec((rows, DIM), lambda i: (i, 0)),
                   whole((GROUPS, 128)), whole((1, 1)), whole((1, DIM)), whole((1, DIM))],
        compiler_params=pltpu.CompilerParams(vmem_limit_bytes=60 * 1024 * 1024),
        cost_estimate=pl.CostEstimate(flops=4 * ROWS * DIM * depth, bytes_accessed=120 * 2 ** 20, transcendentals=0),
    )(de_part, dzt_last, dzt_last, *[x_xp] * nb, *[x_xq] * nb, dhid, stat_all, info_all, gsum_all)


def solution(mesh):
    def body(hidden, ln_gain, ln_bias, embed, targets, loss_mask):
        dp, rank = lax.axis_index('dp'), lax.axis_index('tp')
        shard = targets // ROWS
        block = jnp.bitwise_xor(shard, rank)
        row = targets % ROWS
        half = row // (ROWS // 2)
        sub = row % (ROWS // 2)
        piece = (block - 2) * 2 + jnp.bitwise_xor(half, dp)
        far = 2 * ROWS + (sub // PIECE_ROWS) * TILE + piece * PIECE_ROWS + sub % PIECE_ROWS
        tcol = jnp.where(block < 2, block * ROWS + row, far)
        info = jnp.stack([targets, loss_mask, tcol]).reshape(3, GROUPS, 128)
        outs = run_step(hidden, ln_gain.reshape(1, DIM), ln_bias.reshape(1, DIM), embed, info)
        stat_all, info_all, dhid, x_xp, x_xq, dzt_last, de_part, gsum_all = (outs[i] for i in (3, 4, 5, 7, 8, 12, 13, 14))
        d_embed, d_hidden, loss, mean, d_gain, d_bias = finish(de_part, dzt_last, x_xp, x_xq, dhid, stat_all, info_all, gsum_all)
        return loss.reshape(TOK), mean.reshape(1), d_hidden, d_embed, d_gain.reshape(DIM), d_bias.reshape(DIM)

    token_rows = P(('dp', 'tp'))
    token_mat = P(('dp', 'tp'), None)
    return jax.shard_map(body, mesh=mesh, in_specs=(token_mat, P(), P(), P('tp', None), token_rows, token_rows), out_specs=(token_rows, P('dp'), token_mat, token_mat, P('dp'), P('dp')), check_vma=False)
```

```python
import functools

import jax
import jax.numpy as jnp
from jax import lax
from jax.experimental import pallas as pl
from jax.experimental.pallas import tpu as pltpu
from jax.sharding import PartitionSpec as P

LN_EPS = 1e-5
LOWEST = float(jnp.finfo(jnp.float32).min)

TOK = 2048
ROWS = 2048
DIM = 4096
VOCAB = 8192
TILE = 256
TILES = VOCAB // TILE
HB = 1024
HBS = TOK // HB
CHUNK = 32
PIECE_ROWS = 2 * CHUNK
NEAR = 2 * ROWS // TILE
PE_ROWS = 512
CHUNKS = ROWS // 2 // CHUNK
LN_ROWS = 256
STAT_ROWS = 32
PIECE = 32
LN_UNROLL = 4
XCH = 256
XCHS = TOK // XCH
KT = 512
DEFER = 6
WAIT_STEP = {4: 0, 9: 1, 14: 2}
ZB = 512
NCOL = 512
KCOL = 1024
NB_UNROLL = 8
NB_ROWS = 128
GROUPS = TOK // 128
NT = (((1,), (1,)), ((), ()))


def peers():
    dp, tp = lax.axis_index('dp'), lax.axis_index('tp')
    core = lax.rem(tp, 2)
    pair = tp - core
    other = 2 - pair
    part = pair + 1 - core
    return dp, tp, (dp, part), (dp, other + core), (dp, other + 1 - core), (1 - dp, tp)


def remote(src, dst, ssem, rsem, dev):
    return pltpu.make_async_remote_copy(
        src_ref=src, dst_ref=dst, send_sem=ssem, recv_sem=rsem, device_id=dev, device_id_type=pl.DeviceIdType.MESH)


def spread(row, rows, dst):
    dst[rows, :] = jnp.transpose(jnp.broadcast_to(row, (128, 128)))


def step_kernel(hid, gain, bias, emb, info,
                e_all, x_out, z_out, stat_all, info_all,
                dhid, x_part, x_xp, x_xq, dzt_own, dzt_out, dzt_part, dzt_last, de_part, gsum_all,
                info_v, stat_v, stats, infos, gb_v, gs_v, g8,
                h_sem, xo_sem, e_sem, eo_sem, z_sem, zt_sem, et_sem, small_sem, dzo_sem, big_sem, g_sem,
                xs_send, ys_send, ds_send, pe_send, sm_send, xt_send, xd_send, xp_send, dz_send, g_send,
                x_recv, y_recv, d_recv, pe_recv, info_recv, stat_recv, xt_recv, xd_recv, xp_recv, dz_recv, g_recv):
    bf16, f32 = jnp.bfloat16, jnp.float32
    dp, tp, part, xp, xq, yp = peers()
    core = lax.rem(tp, 2)
    xp_rank = 2 - (tp - core) + core
    xq_rank = 2 - (tp - core) + 1 - core
    group = ((1, part), (2, xp), (3, xq))
    barrier = pltpu.get_barrier_semaphore()
    for dev in (part, xp, xq, yp):
        pl.semaphore_signal(barrier, inc=1, device_id=dev, device_id_type=pl.DeviceIdType.MESH)
    pl.semaphore_wait(barrier, 4)

    def xrows(ref, j):
        return ref.at[pl.ds(pl.multiple_of(j * XCH, XCH), XCH)]

    def xt_copy(j):
        return remote(xrows(x_out, j), xrows(x_xp, j), xt_send, xt_recv.at[j], xp)

    def xd_copy(j):
        return remote(xrows(x_xp, j), xrows(x_xq, j), xd_send, xd_recv.at[j], part)

    def xt_event(j):
        xt_copy(j).wait_recv()
        xd_copy(j).start()
    xp_copy = remote(x_out, x_part, xp_send, xp_recv, part)

    def forward(m_s, scale_v, tc_v, mr_v, zt, et, xs, hbuf, ebuf, z0, z1, s_s, t_s, gb8):
        def tile_row(j):
            return ROWS * 2 + (j // 2) * TILE + lax.rem(j, 2) * CHUNK

        def x_copy(j):
            src = emb.at[pl.ds(pl.multiple_of(dp * (ROWS // 2) + j * CHUNK, CHUNK), CHUNK)]
            return remote(src, e_all.at[pl.ds(pl.multiple_of(tile_row(j), CHUNK), CHUNK)], xs_send, x_recv.at[j], xp)

        def piece(j, p):
            return e_all.at[pl.ds(pl.multiple_of(tile_row(j) + p * PIECE_ROWS, CHUNK), CHUNK)]

        def y_copy(j):
            return remote(piece(j, 0), piece(j, 1), ys_send, y_recv.at[j], yp)

        def d_copy(j, p):
            return remote(piece(j, p), piece(j, p + 2), ds_send, d_recv.at[j // 2], part)

        def pe_copy(i):
            return remote(emb.at[pl.ds(pl.multiple_of(i * PE_ROWS, PE_ROWS), PE_ROWS)],
                          e_all.at[pl.ds(pl.multiple_of(ROWS + i * PE_ROWS, PE_ROWS), PE_ROWS)], pe_send, pe_recv.at[i], part)

        cp = pltpu.make_async_copy(info, info_v, small_sem.at[0])
        cp.start()

        def h_copy(i):
            return pltpu.make_async_copy(hid.at[pl.ds(pl.multiple_of(i * LN_ROWS, LN_ROWS), LN_ROWS)], hbuf.at[lax.rem(i, 2)], h_sem.at[lax.rem(i, 2)])
        h_copy(0).start()

        for p, dev in group:
            remote(info, info_all.at[tp], sm_send, info_recv.at[p], dev).start()

        def start_x(j, c):
            x_copy(j).start()
            return c
        lax.fori_loop(0, CHUNKS, start_x, 0)

        def start_pe(i, c):
            pe_copy(i).start()
            return c
        lax.fori_loop(0, ROWS // PE_ROWS, start_pe, 0)

        def e_load(t):
            slot = lax.rem(t, 2)
            return pltpu.make_async_copy(e_all.at[pl.ds(pl.multiple_of(t * TILE, TILE), TILE)], ebuf.at[slot], e_sem.at[slot])

        def e_load_own(t):
            slot = lax.rem(t, 2)
            return pltpu.make_async_copy(emb.at[pl.ds(pl.multiple_of(t * TILE, TILE), TILE)], ebuf.at[slot], e_sem.at[slot])
        e_load_own(0).start()

        def x_event(j):
            x_copy(j).wait_recv()
            y_copy(j).start()
            d_copy(j, 0).start()

        def y_event(j):
            y_copy(j).wait_recv()
            d_copy(j, 1).start()

        def p_event(k):
            rows = e_all.at[pl.ds(pl.multiple_of(2 * ROWS + k * TILE + TILE // 2, TILE // 2), TILE // 2)]
            pltpu.make_async_copy(rows, rows, d_recv.at[k]).wait()
            e_load(NEAR + k).start()

        cp.wait()
        pltpu.make_async_copy(info_v, info_all.at[tp], small_sem.at[0]).start()
        gb8[0] = jnp.broadcast_to(gain[...], (8, DIM))
        gb8[1] = jnp.broadcast_to(bias[...], (8, DIM))

        def ln_tile(i, c):
            slot = lax.rem(i, 2)

            @pl.when(i + 1 < TOK // LN_ROWS)
            def _():
                h_copy(i + 1).start()
            h_copy(i).wait()

            @pl.when(i == 6)
            def _():
                x_event(0)

            def ln_rows(r, c2):
                base = r * LN_UNROLL * 16

                def at(u):
                    return pl.ds(pl.multiple_of(base + u * 16, 16), 16)

                def part_of(u, k):
                    return hbuf[slot, at(u), k * 128:(k + 1) * 128].astype(jnp.float32)
                means, rstds = [], []
                for u in range(LN_UNROLL):
                    tot = part_of(u, 0)
                    for k in range(1, DIM // 128):
                        tot = tot + part_of(u, k)
                    means.append(jnp.broadcast_to(jnp.sum(tot, axis=-1, keepdims=True) * (1.0 / DIM), (16, 128)))
                for u in range(LN_UNROLL):
                    tot = jnp.zeros((16, 128), jnp.float32)
                    for k in range(DIM // 128):
                        diff = part_of(u, k) - means[u]
                        tot = tot + diff * diff
                    var = jnp.sum(tot, axis=-1, keepdims=True) * (1.0 / DIM)
                    rstds.append(jnp.broadcast_to(lax.rsqrt(var + LN_EPS), (16, 128)))
                for u in range(LN_UNROLL):
                    row = pl.ds(pl.multiple_of(i * LN_ROWS + base + u * 16, 16), 16)
                    mr_v[0, row, :] = means[u]
                    mr_v[1, row, :] = rstds[u]
                    for k in range(DIM // 128):
                        cols = slice(k * 128, (k + 1) * 128)
                        g2 = jnp.concatenate([gb8[0, :, cols]] * 2, axis=0)
                        b2 = jnp.concatenate([gb8[1, :, cols]] * 2, axis=0)
                        xs[row, cols] = ((part_of(u, k) - means[u]) * rstds[u] * g2 + b2).astype(jnp.bfloat16)
                return c2
            lax.fori_loop(0, LN_ROWS // (16 * LN_UNROLL), ln_rows, 0)
            rows = pl.ds(pl.multiple_of(i * LN_ROWS, LN_ROWS), LN_ROWS)
            pltpu.make_async_copy(xs.at[rows], x_out.at[rows], xo_sem).start()
            return c
        lax.fori_loop(0, TOK // LN_ROWS, ln_tile, 0)

        m_s[...] = jnp.full((TOK, 128), LOWEST, jnp.float32)
        s_s[...] = jnp.zeros((TOK, 128), jnp.float32)
        t_s[...] = jnp.zeros((TOK, 128), jnp.float32)
        for r in range(GROUPS):
            spread(info_v[2, r:r + 1, :], slice(r * 128, (r + 1) * 128), tc_v)
        z1[...] = jnp.full((HB, TILE), LOWEST, jnp.float32)

        zs = (z0, z1)

        def product(t, h):
            for r in range(0, HB, 512):
                zs[h][r:r + 512, :] = lax.dot_general(
                    xs[h * HB + r:h * HB + r + 512, :], ebuf[lax.rem(t, 2)], NT, preferred_element_type=jnp.float32)

        def statistics(t, h):
            z = zs[h]
            lane = lax.broadcasted_iota(jnp.int32, (STAT_ROWS, 128), 1)
            for r in range(0, HB, STAT_ROWS):
                rows = slice(h * HB + r, h * HB + r + STAT_ROWS)
                zk = [z[r:r + STAT_ROWS, k * 128:(k + 1) * 128] for k in range(TILE // 128)]
                old = m_s[rows, :]
                new = jnp.maximum(jnp.maximum(zk[0], zk[1]), old)
                tot = s_s[rows, :] * jnp.exp(old - new)
                tgt = t_s[rows, :]
                diff = tc_v[rows, :] - t * TILE
                for k in range(TILE // 128):
                    tot = tot + jnp.exp(zk[k] - new)
                    tgt = tgt + jnp.where(diff == lane + k * 128, zk[k], 0.0)
                m_s[rows, :] = new
                s_s[rows, :] = tot
                t_s[rows, :] = tgt

        def z_copy(t, h):
            return pltpu.make_async_copy(
                zs[h], z_out.at[pl.ds(h * HB, HB), pl.ds(pl.multiple_of(t * TILE, TILE), TILE)], z_sem.at[h])

        def start_events(t):
            @pl.when(t < TILES - 1)
            def _():
                x_event(t + 1)

            @pl.when(t == TILES - 2)
            def _():
                xt_copy(0).start()

            @pl.when(t == TILES - 1)
            def _():
                y_event(TILES - 1)
                p_event(TILES - 1 - NEAR)
            e_load(t).wait()

            @pl.when(t < ROWS // TILE)
            def _():
                slot = lax.rem(t, 2)
                pltpu.make_async_copy(ebuf.at[slot], e_all.at[pl.ds(pl.multiple_of(t * TILE, TILE), TILE)], eo_sem.at[slot]).start()

        def middle_events(t):
            @pl.when(t < TILES - 1)
            def _():
                y_event(t)

            @pl.when((t >= 1) & (t < ROWS // TILE + 1))
            def _():
                slot = lax.rem(t - 1, 2)
                pltpu.make_async_copy(ebuf.at[slot], e_all.at[pl.ds(0, TILE)], eo_sem.at[slot]).wait()

            @pl.when(t == NEAR)
            def _():
                pltpu.make_async_copy(xs, x_out, xo_sem).wait()

            @pl.when(t < ROWS // TILE - 1)
            def _():
                e_load_own(t + 1).start()

            @pl.when((t >= ROWS // TILE - 1) & (t < NEAR - 1))
            def _():
                @pl.when(lax.rem(t + 1, PE_ROWS // TILE) == 0)
                def _():
                    pe_copy((t + 1 - ROWS // TILE) // (PE_ROWS // TILE)).wait_recv()
                e_load(t + 1).start()

            @pl.when((t >= NEAR - 1) & (t < TILES - 2))
            def _():
                p_event(t - (NEAR - 1))

            @pl.when(t == NEAR + 1)
            def _():
                for p, dev in group:
                    remote(info, info_all.at[tp], sm_send, info_recv.at[p], dev).wait_recv()
                pltpu.make_async_copy(info_v, info_all.at[tp], small_sem.at[0]).wait()
                load = pltpu.make_async_copy(info_all, infos, small_sem.at[0])
                load.start()
                load.wait()
                count = jnp.broadcast_to(token_count(), (1, 128))
                for r in range(GROUPS):
                    spread(info_v[1, r:r + 1, :].astype(f32) / count, slice(r * 128, (r + 1) * 128), scale_v)

        def step(t, c):
            @pl.when(t > 0)
            def _():
                z_copy(t - 1, 1).start()
            start_events(t)

            @pl.when(t > 0)
            def _():
                z_copy(t - 1, 0).wait()
            statistics(t - 1, 1)
            product(t, 0)
            z_copy(t, 0).start()
            middle_events(t)

            @pl.when(t > 0)
            def _():
                z_copy(t - 1, 1).wait()
            statistics(t, 0)
            product(t, 1)
            return c
        last = TILES - 1
        lax.fori_loop(0, TILES, step, 0)
        z_copy(last, 1).start()
        statistics(last, 1)

        def finish(i, c):
            for u in range(4):
                r = i * 4 + u
                rows = pl.ds(pl.multiple_of(r * 128, 128), 128)
                m = m_s[rows, :]
                top = jnp.max(m, axis=-1, keepdims=True)
                tot = jnp.sum(s_s[rows, :] * jnp.exp(m - top), axis=-1, keepdims=True)
                lse = jnp.broadcast_to(top + jnp.log(tot), (128, 128))
                tgt = jnp.broadcast_to(jnp.sum(t_s[rows, :], axis=-1, keepdims=True), (128, 128))
                m_s[rows, :] = lse
                stat_v[0, pl.ds(r, 1), :] = jnp.transpose(lse)[0:1, :]
                stat_v[1, pl.ds(r, 1), :] = jnp.transpose(tgt)[0:1, :]
            return c
        lax.fori_loop(0, TOK // 512, finish, 0)
        for h in range(2):
            z_copy(last, h).wait()
        z_load(zt, 0).start()
        et_load(et, 0).start()
        half = e_all.at[pl.ds(0, ROWS // 2)]
        pltpu.make_async_copy(half, half, xs_send).wait()
        pltpu.make_async_copy(half, half, ys_send).wait()
        full = e_all.at[pl.ds(0, ROWS)]
        pltpu.make_async_copy(full, full, ds_send).wait()
        pltpu.make_async_copy(full, full, pe_send).wait()
        pltpu.make_async_copy(stat_v, stat_all.at[tp], small_sem.at[1]).start()
        for p, dev in group:
            remote(stat_v, stat_all.at[tp], sm_send, stat_recv.at[p], dev).start()

        def start_xt(j, c):
            xt_copy(j).start()
            return c
        lax.fori_loop(1, XCHS, start_xt, 0)
        xp_copy.start()

    def z_load(zt, k):
        slot = lax.rem(k, 2)
        return pltpu.make_async_copy(z_out.at[:, pl.ds(pl.multiple_of(k * KT, KT), KT)], zt.at[slot], zt_sem.at[slot])

    def et_load(et, k):
        slot = lax.rem(k, 2)
        return pltpu.make_async_copy(e_all.at[pl.ds(pl.multiple_of(k * KT, KT), KT)], et.at[slot], et_sem.at[slot])

    def dzt_copy(k):
        rows = pl.ds(pl.multiple_of(lax.rem(k, 4) * KT, KT), KT)
        return remote(dzt_out.at[rows], dzt_part.at[rows], dz_send, dz_recv.at[lax.rem(k, 4)], part)

    def token_count():
        return jnp.sum(infos[:, 1].astype(f32))

    def token_grads(lse_v, scale_v, tcol_v, mr, zt, et, acc):
        def d_phase(da, db, dzt):
            def dzt_store(k, ref):
                slot = lax.rem(k, 2)
                return pltpu.make_async_copy(dzt.at[slot], ref.at[pl.ds(pl.multiple_of(lax.rem(k, 4) * KT, KT), KT)], eo_sem.at[slot])
            acc[...] = jnp.zeros(acc.shape, f32)
            lane = lax.broadcasted_iota(jnp.int32, (PIECE, 128), 1)

            def piece(dst, rows, low, k, tie):
                slot = lax.rem(k, 2)
                lse = lse_v[rows, :]
                if tie is not None:
                    floor = 0.0 - jnp.maximum(0.0 - tie, -LOWEST)
                    lse = jnp.maximum(lse, jnp.concatenate([floor] * (PIECE // 8), axis=0))
                scale = scale_v[rows, :]
                diff = tcol_v[rows, :] - k * KT
                for g in range(KT // 128):
                    cols = slice(g * 128, (g + 1) * 128)
                    hot = (diff == lane + g * 128).astype(f32)
                    val = (jnp.exp(zt[slot, rows, cols] - lse) - hot) * scale
                    dst[low, cols] = val.astype(bf16)

            def half_step(k, src, dst, base, dst_base, dst_k):
                slot = lax.rem(k, 2)
                per = HB // (DIM // NCOL)
                for n in range(DIM // NCOL):
                    cols = slice(n * NCOL, (n + 1) * NCOL)
                    prod = jnp.dot(src[...], et[slot, :, cols], preferred_element_type=f32)
                    acc[base:base + HB, cols] += prod
                    for q in range(0, per, PIECE):
                        at = q * HB // per
                        low = n * per + q
                        piece(dst, slice(dst_base + low, dst_base + low + PIECE), slice(low, low + PIECE), dst_k, prod[at:at + 8, 0:128])
                    if n * per % 256 == 0:
                        low = n * per
                        dzt[slot, :, base + low:base + low + 256] = jnp.transpose(src[low:low + 256, :])

            z_load(zt, 0).wait()

            def first(i, c):
                rows = pl.ds(pl.multiple_of(i * PIECE, PIECE), PIECE)
                piece(da, rows, rows, 0, None)
                return c
            lax.fori_loop(0, HB // PIECE, first, 0)

            def step(k, c):
                @pl.when(k + 1 < VOCAB // KT)
                def _():
                    z_load(zt, k + 1).start()
                    et_load(et, k + 1).start()
                for at, j in WAIT_STEP.items():
                    @pl.when(k == at)
                    def _(j=j):
                        xt_event(j)

                @pl.when((k >= 2) & (k < 10))
                def _():
                    dzt_store(k, dzt_own).wait()

                @pl.when((k >= 6) & (k < 10))
                def _():
                    dzt_copy(k - 2).start()
                et_load(et, k).wait()
                half_step(k, da, db, 0, HB, k)

                @pl.when(k + 1 < VOCAB // KT)
                def _():
                    z_load(zt, k + 1).wait()
                half_step(k, db, da, HB, 0, k + 1)

                @pl.when(k < 4)
                def _():
                    dzt_store(k, dzt_own).start()

                @pl.when((k >= 4) & (k < 8))
                def _():
                    dzt_store(k, dzt_out).start()
                return c
            lax.fori_loop(0, VOCAB // KT, step, 0)
        half = pltpu.VMEM((HB, KT), bf16)
        pl.run_scoped(d_phase, half, half, pltpu.VMEM((2, KT, TOK), bf16))

        def n_phase(hb, ob):
            def h_load(i):
                slot = lax.rem(i, 2)
                return pltpu.make_async_copy(hid.at[pl.ds(pl.multiple_of(i * NB_ROWS, NB_ROWS), NB_ROWS)], hb.at[slot], z_sem.at[slot])

            def o_store(i):
                slot = lax.rem(i, 2)
                return pltpu.make_async_copy(ob.at[slot], dhid.at[pl.ds(pl.multiple_of(i * NB_ROWS, NB_ROWS), NB_ROWS)], e_sem.at[slot])
            h_load(0).start()
            gb_v[...] = jnp.zeros(gb_v.shape, jnp.float32)
            g8[...] = jnp.broadcast_to(gain[...], (8, DIM))

            def tile(i, c):
                slot = lax.rem(i, 2)

                @pl.when(i + 1 < TOK // NB_ROWS)
                def _():
                    h_load(i + 1).start()

                @pl.when(i >= 2)
                def _():
                    o_store(i - 2).wait()
                h_load(i).wait()

                def rows_body(r, c2):
                    units = range(NB_UNROLL)
                    base = r * 16 * NB_UNROLL
                    low = [pl.ds(pl.multiple_of(base + u * 16, 16), 16) for u in units]
                    row = [pl.ds(pl.multiple_of(i * NB_ROWS + base + u * 16, 16), 16) for u in units]
                    zero = jnp.zeros((16, 128), jnp.float32)
                    sum1, sum3 = [zero] * NB_UNROLL, [zero] * NB_UNROLL

                    def load(u, cols):
                        dx = acc[row[u], cols]
                        xhat = (hb[slot, low[u], cols].astype(jnp.float32) - mr[0, row[u], :]) * mr[1, row[u], :]
                        return dx, xhat, dx * jnp.concatenate([g8[:, cols]] * 2, axis=0)
                    for k in range(DIM // 128):
                        cols = slice(k * 128, (k + 1) * 128)
                        d_gain, d_bias = gb_v[0, :, cols], gb_v[1, :, cols]
                        for u in units:
                            dx, xhat, gx = load(u, cols)
                            sum1[u] = sum1[u] + gx
                            sum3[u] = sum3[u] + gx * xhat
                            dgx = dx * xhat
                            d_gain = d_gain + (dgx[0:8] + dgx[8:16])
                            d_bias = d_bias + (dx[0:8] + dx[8:16])
                        gb_v[0, :, cols] = d_gain
                        gb_v[1, :, cols] = d_bias
                    c1 = [jnp.broadcast_to(jnp.sum(v, axis=-1, keepdims=True) * (1.0 / DIM), (16, 128)) for v in sum1]
                    c3 = [jnp.broadcast_to(jnp.sum(v, axis=-1, keepdims=True) * (1.0 / DIM), (16, 128)) for v in sum3]
                    for u in units:
                        for k in range(DIM // 128):
                            cols = slice(k * 128, (k + 1) * 128)
                            _, xhat, gx = load(u, cols)
                            ob[slot, low[u], cols] = (mr[1, row[u], :] * (gx - c1[u] - xhat * c3[u])).astype(jnp.bfloat16)
                    return c2
                lax.fori_loop(0, NB_ROWS // (16 * NB_UNROLL), rows_body, 0)
                o_store(i).start()
                return c
            lax.fori_loop(0, TOK // NB_ROWS, tile, 0)
            for i in range(2):
                o_store(TOK // NB_ROWS - 2 + i).wait()
            gs_v[0:1, :] = jnp.sum(gb_v[0], axis=0, keepdims=True)
            gs_v[1:2, :] = jnp.sum(gb_v[1], axis=0, keepdims=True)
        pl.run_scoped(n_phase, pltpu.VMEM((2, NB_ROWS, DIM), bf16), pltpu.VMEM((2, NB_ROWS, DIM), bf16))

    def weight_grads(acc):
        own = pltpu.make_async_copy(gs_v, gsum_all.at[tp], g_sem)
        xt_event(3)

        def e_phase(eo, xt, dzb, zs):
            eo_load = pltpu.make_async_copy(emb, eo, big_sem)

            def x_load(ref, row, slot):
                return pltpu.make_async_copy(ref.at[pl.ds(pl.multiple_of(row, KT), KT)], xt.at[slot], z_sem.at[slot])

            def dz_load(ref, col, slot):
                return pltpu.make_async_copy(ref.at[:, pl.ds(pl.multiple_of(col, KT), KT)], dzb.at[slot], e_sem.at[slot])

            def start_local(i):
                slot = lax.rem(i, 2)

                @pl.when(i < 4)
                def _():
                    x_load(x_out, i * KT, slot).start()
                    dz_load(dzt_own, i * KT, slot).start()

                @pl.when(i >= 4)
                def _():
                    x_load(x_part, (i - 4) * KT, slot).start()
                    dz_load(dzt_part, (i - 4) * KT, slot).start()

            def add(slot):
                def mul(h, c2):
                    rows = pl.ds(pl.multiple_of(h * HB, HB), HB)
                    for n in range(0, DIM, NCOL):
                        acc[rows, n:n + NCOL] += jnp.dot(dzb[slot, rows, :], xt[slot, :, n:n + NCOL], preferred_element_type=jnp.float32)
                    return c2
                lax.fori_loop(0, HBS, mul, 0)

            start_local(0)
            acc[...] = jnp.zeros(acc.shape, f32)

            def rem_load(r):
                slot = lax.rem(r, 2)
                return [pltpu.make_async_copy(xrows(ref, r), xt.at[slot, pl.ds(i * XCH, XCH)], z_sem.at[slot])
                        for i, ref in enumerate((x_xp, x_xq))]

            def local(i, c):
                slot = lax.rem(i, 2)

                @pl.when(i == 0)
                def _():
                    eo_load.start()

                @pl.when(i == 2)
                def _():
                    xp_copy.wait_recv()

                    def wait_dz(q, c2):
                        dzt_copy(q).wait_recv()
                        return c2
                    lax.fori_loop(0, 4, wait_dz, 0)

                @pl.when(i == 1)
                def _():
                    own.start()
                    for p, dev in group:
                        remote(gs_v, gsum_all.at[tp], g_send, g_recv.at[p], dev).start()

                @pl.when(i == 5)
                def _():
                    xt_event(4)

                @pl.when(i < 7)
                def _():
                    start_local(i + 1)

                @pl.when(i == 7)
                def _():
                    xd_copy(0).wait_recv()
                    for cp in rem_load(0):
                        cp.start()
                x_load(x_out, 0, slot).wait()
                dz_load(dzt_own, 0, slot).wait()
                add(slot)
                return c
            lax.fori_loop(0, 8, local, 0)
            eo_load.wait()
            for p, dev in group:
                remote(stat_v, stat_all.at[tp], sm_send, stat_recv.at[p], dev).wait_recv()
            pltpu.make_async_copy(stat_v, stat_all.at[tp], small_sem.at[1]).wait()
            stat_load = pltpu.make_async_copy(stat_all, stats, small_sem.at[1])
            stat_load.start()
            stat_load.wait()
            count = jnp.broadcast_to(token_count(), (1, 128))

            def far(r, c):
                slot = lax.rem(r, 2)

                @pl.when(r == 1)
                def _():
                    xt_event(5)

                @pl.when(r == 5)
                def _():
                    xt_event(6)

                def fetch():
                    xd_copy(r + 1).wait_recv()
                    for cp in rem_load(r + 1):
                        cp.start()
                pl.when(r < XCHS - 2)(fetch)
                x_load(x_out, 0, slot).wait()

                @pl.when(r == XCHS - DEFER)
                def _():
                    pltpu.make_async_copy(acc, de_part, big_sem).start()

                @pl.when(r > XCHS - DEFER + 1)
                def _():
                    dz_out(0, 0, slot).wait()
                    dz_out(0, 1, slot).wait()

                far_rows = []
                for g in range(4):
                    who = xp_rank if g < 2 else xq_rank
                    at = pl.ds(2 * r + g % 2, 1)
                    far_rows.append((stats[who, 0, at, :], infos[who, 1, at, :].astype(f32) / count, infos[who, 0, at, :] - tp * ROWS))

                def logits(h, c2):
                    for k in range(0, DIM, KCOL):
                        prod = lax.dot_general(eo[pl.ds(pl.multiple_of(h * ZB, ZB), ZB), k:k + KCOL], xt[slot, :, k:k + KCOL], NT, preferred_element_type=jnp.float32)
                        zs[...] = prod if k == 0 else zs[...] + prod
                    for q in range(ZB // 32):
                        row = h * ZB + q * 32
                        line = lax.broadcasted_iota(jnp.int32, (32, 128), 0)
                        for g, (lse, scale, trel) in enumerate(far_rows):
                            cols = slice(g * 128, (g + 1) * 128)
                            hot = ((trel - row) == line).astype(f32)
                            val = (jnp.exp(zs[q * 32:(q + 1) * 32, cols] - lse) - hot) * scale
                            dzb[slot, pl.ds(pl.multiple_of(row, 32), 32), cols] = val.astype(bf16)
                    return c2
                lax.fori_loop(0, ROWS // ZB, logits, 0)

                @pl.when(r == XCHS - 2)
                def _():
                    xt_event(XCHS - 1)
                    fetch()

                @pl.when(r < XCHS - DEFER)
                def _():
                    def mul(h, c2):
                        rows = pl.ds(pl.multiple_of(h * HB, HB), HB)
                        for n in range(0, DIM, NCOL):
                            acc[rows, n:n + NCOL] += jnp.dot(dzb[slot, rows, :], xt[slot, :, n:n + NCOL], preferred_element_type=jnp.float32)
                        return c2
                    lax.fori_loop(0, HBS, mul, 0)

                @pl.when(r >= XCHS - DEFER)
                def _():
                    for i in range(2):
                        dz_out(r - (XCHS - DEFER), i, slot).start()
                return c

            def dz_out(q, i, slot):
                return pltpu.make_async_copy(
                    dzb.at[slot, :, pl.ds(i * XCH, XCH)], dzt_last.at[i, :, pl.ds(pl.multiple_of(q * XCH, XCH), XCH)], dzo_sem.at[slot])
            lax.fori_loop(0, XCHS, far, 0)
            for slot in range(2):
                dz_out(0, 0, slot).wait()
                dz_out(0, 1, slot).wait()
            pltpu.make_async_copy(acc, de_part, big_sem).wait()
        pl.run_scoped(e_phase, pltpu.VMEM((ROWS, DIM), jnp.bfloat16), pltpu.VMEM((2, KT, DIM), jnp.bfloat16),
                      pltpu.VMEM((2, ROWS, KT), jnp.bfloat16), pltpu.VMEM((ZB, KT), jnp.float32))

        own.wait()

    wide = pltpu.VMEM((TOK, 128), f32)
    big = pltpu.VMEM((TOK, DIM), f32)

    def tokens(m_s, scale_v, tc_v, mr_v, zt, et):
        kept = (m_s, scale_v, tc_v, mr_v, zt, et)
        pl.run_scoped(functools.partial(forward, *kept), pltpu.VMEM((TOK, DIM), bf16), pltpu.VMEM((2, LN_ROWS, DIM), bf16),
                      pltpu.VMEM((2, TILE, DIM), bf16), pltpu.VMEM((HB, TILE), f32), pltpu.VMEM((HB, TILE), f32), wide, wide,
                      pltpu.VMEM((2, 8, DIM), f32))
        pl.run_scoped(functools.partial(token_grads, *kept), big)
    pl.run_scoped(tokens, wide, wide, pltpu.VMEM((TOK, 128), jnp.int32), pltpu.VMEM((2, TOK, 128), f32),
                  pltpu.VMEM((2, TOK, KT), f32), pltpu.VMEM((2, KT, DIM), bf16))
    pl.run_scoped(weight_grads, big)

    pltpu.make_async_copy(x_out, x_out, xt_send).wait()
    pltpu.make_async_copy(x_out, x_out, xd_send).wait()
    xp_copy.wait_send()
    pltpu.make_async_copy(dzt_out, dzt_out, dz_send).wait()
    for p, dev in group:
        remote(info, info_all.at[tp], sm_send, info_recv.at[p], dev).wait_send()
        remote(stat_v, stat_all.at[tp], sm_send, stat_recv.at[p], dev).wait_send()
        remote(gs_v, gsum_all.at[tp], g_send, g_recv.at[p], dev).wait()


def run_step(hidden, gain, bias, embed, info):
    any_spec = pl.BlockSpec(memory_space=pl.ANY)
    vmem_spec = pl.BlockSpec(memory_space=pltpu.VMEM)
    f32, bf16, i32 = jnp.float32, jnp.bfloat16, jnp.int32
    dma = pltpu.SemaphoreType.DMA
    small, ints = (4, 2, GROUPS, 128), (4, 3, GROUPS, 128)
    mat, square = ((TOK, DIM), bf16), ((ROWS, TOK), bf16)
    shapes = [((VOCAB, DIM), bf16), mat, ((TOK, VOCAB), f32), (small, f32), (ints, i32),
              mat, mat, mat, mat, square, square, square, ((2, ROWS, DEFER * XCH), bf16), ((ROWS, DIM), f32), ((4, 2, DIM), f32)]
    return pl.pallas_call(
        step_kernel,
        name="step",
        out_shape=[jax.ShapeDtypeStruct(s, d) for s, d in shapes],
        in_specs=[any_spec, vmem_spec, vmem_spec, any_spec, any_spec],
        out_specs=[any_spec] * len(shapes),
        scratch_shapes=[
            pltpu.VMEM((3, GROUPS, 128), i32), pltpu.VMEM((2, GROUPS, 128), f32), pltpu.VMEM(small, f32), pltpu.VMEM(ints, i32),
            pltpu.VMEM((2, 8, DIM), f32), pltpu.VMEM((2, DIM), f32), pltpu.VMEM((8, DIM), f32),
            dma((2,)), dma, dma((2,)), dma((2,)), dma((2,)), dma((2,)), dma((2,)), dma((2,)), dma((2,)), dma, dma,
            dma, dma, dma, dma, dma, dma, dma, dma, dma, dma,
            dma((CHUNKS,)), dma((CHUNKS,)), dma((TILES - NEAR,)), dma((ROWS // PE_ROWS,)), dma((4,)), dma((4,)),
            dma((XCHS,)), dma((XCHS,)), dma, dma((4,)), dma((4,)),
        ],
        compiler_params=pltpu.CompilerParams(collective_id=0, has_side_effects=True, vmem_limit_bytes=67043328),
        cost_estimate=pl.CostEstimate(flops=12 * TOK * VOCAB * DIM, bytes_accessed=700 * 2 ** 20, transcendentals=3 * TOK * VOCAB),
    )(hidden, gain, bias, embed, info)


def finish_kernel(*refs):
    nb = DEFER * XCH // KT
    de_in, dz0, dz1 = refs[:3]
    xs = refs[3:3 + 2 * nb]
    dh_in, stat_all, info_all, gsum_all, de_out, dh_out, loss, mean, d_gain, d_bias = refs[3 + 2 * nb:]
    for h in range(HBS):
        rows = slice(h * HB, (h + 1) * HB)
        prod = None
        for b in range(nb):
            for dz, x in ((dz0, xs[b]), (dz1, xs[nb + b])):
                part = jnp.dot(dz[0, rows, b * KT:(b + 1) * KT], x[...], preferred_element_type=jnp.float32)
                prod = part if prod is None else prod + part
        de_out[rows, :] = de_in[rows, :] + prod
    dh_out[...] = dh_in[...]

    @pl.when(pl.program_id(0) == 0)
    def _():
        weights = info_all[:, 1].astype(jnp.float32)
        all_loss = (stat_all[:, 0] - stat_all[:, 1]) * weights
        tp = lax.axis_index('tp')
        loss[...] = (stat_all[tp, 0] - stat_all[tp, 1]) * info_all[tp, 1].astype(jnp.float32)
        mean[...] = jnp.broadcast_to(jnp.sum(all_loss), (1, 1)) / jnp.broadcast_to(jnp.sum(weights), (1, 1))
        sums = ((gsum_all[0] + gsum_all[1]) + gsum_all[2]) + gsum_all[3]
        d_gain[...] = sums[0:1]
        d_bias[...] = sums[1:2]


def finish(de_part, dzt_last, x_xp, x_xq, dhid, stat_all, info_all, gsum_all):
    cols = 512
    steps = DIM // cols
    depth = DEFER * XCH
    rows = TOK // steps
    first = (TOK - depth) // KT
    once = pl.Buffered(1)
    x_specs = [pl.BlockSpec((KT, cols), lambda i, b=b: (b, i)) for b in range(first, TOK // KT)]

    def whole(shape):
        return pl.BlockSpec(shape, lambda i: (0,) * len(shape))
    nb = len(x_specs)
    outs = [((ROWS, DIM), jnp.float32), ((TOK, DIM), jnp.bfloat16), ((GROUPS, 128), jnp.float32), ((1, 1), jnp.float32), ((1, DIM), jnp.float32), ((1, DIM), jnp.float32)]
    return pl.pallas_call(
        finish_kernel,
        name="finish",
        grid=(steps,),
        out_shape=[jax.ShapeDtypeStruct(s, d) for s, d in outs],
        in_specs=[
            pl.BlockSpec((ROWS, cols), lambda i: (0, i)),
            pl.BlockSpec((1, ROWS, depth), lambda i: (0, 0, 0), pipeline_mode=once),
            pl.BlockSpec((1, ROWS, depth), lambda i: (1, 0, 0), pipeline_mode=once),
            *x_specs, *x_specs,
            pl.BlockSpec((rows, DIM), lambda i: (i, 0)),
            whole(stat_all.shape), whole(info_all.shape), whole(gsum_all.shape),
        ],
        out_specs=[pl.BlockSpec((ROWS, cols), lambda i: (0, i)), pl.BlockSpec((rows, DIM), lambda i: (i, 0)),
                   whole((GROUPS, 128)), whole((1, 1)), whole((1, DIM)), whole((1, DIM))],
        compiler_params=pltpu.CompilerParams(vmem_limit_bytes=60 * 1024 * 1024),
        cost_estimate=pl.CostEstimate(flops=4 * ROWS * DIM * depth, bytes_accessed=120 * 2 ** 20, transcendentals=0),
    )(de_part, dzt_last, dzt_last, *[x_xp] * nb, *[x_xq] * nb, dhid, stat_all, info_all, gsum_all)


def solution(mesh):
    def body(hidden, ln_gain, ln_bias, embed, targets, loss_mask):
        dp, rank = lax.axis_index('dp'), lax.axis_index('tp')
        shard = targets // ROWS
        block = jnp.bitwise_xor(shard, rank)
        row = targets % ROWS
        half = row // (ROWS // 2)
        sub = row % (ROWS // 2)
        piece = (block - 2) * 2 + jnp.bitwise_xor(half, dp)
        far = 2 * ROWS + (sub // PIECE_ROWS) * TILE + piece * PIECE_ROWS + sub % PIECE_ROWS
        tcol = jnp.where(block < 2, block * ROWS + row, far)
        info = jnp.stack([targets, loss_mask, tcol]).reshape(3, GROUPS, 128)
        outs = run_step(hidden, ln_gain.reshape(1, DIM), ln_bias.reshape(1, DIM), embed, info)
        stat_all, info_all, dhid, x_xp, x_xq, dzt_last, de_part, gsum_all = (outs[i] for i in (3, 4, 5, 7, 8, 12, 13, 14))
        d_embed, d_hidden, loss, mean, d_gain, d_bias = finish(de_part, dzt_last, x_xp, x_xq, dhid, stat_all, info_all, gsum_all)
        return loss.reshape(TOK), mean.reshape(1), d_hidden, d_embed, d_gain.reshape(DIM), d_bias.reshape(DIM)

    token_rows = P(('dp', 'tp'))
    token_mat = P(('dp', 'tp'), None)
    return jax.shard_map(body, mesh=mesh, in_specs=(token_mat, P(), P(), P('tp', None), token_rows, token_rows), out_specs=(token_rows, P('dp'), token_mat, token_mat, P('dp'), P('dp')), check_vma=False)
```

```python
import functools

import jax
import jax.numpy as jnp
from jax import lax
from jax.experimental import pallas as pl
from jax.experimental.pallas import tpu as pltpu
from jax.sharding import PartitionSpec as P

LN_EPS = 1e-5
LOWEST = float(jnp.finfo(jnp.float32).min)

TOK = 2048
ROWS = 2048
DIM = 4096
VOCAB = 8192
TILE = 256
TILES = VOCAB // TILE
HB = 1024
HBS = TOK // HB
CHUNK = 32
PIECE_ROWS = 2 * CHUNK
NEAR = 2 * ROWS // TILE
PE_ROWS = 512
CHUNKS = ROWS // 2 // CHUNK
LN_ROWS = 256
STAT_ROWS = 32
PIECE = 32
LN_UNROLL = 4
XCH = 256
XCHS = TOK // XCH
KT = 512
DEFER = 2
WAIT_STEP = {4: 0, 9: 1, 14: 2}
ZB = 512
NCOL = 512
KCOL = 1024
NB_UNROLL = 4
NB_ROWS = 128
GROUPS = TOK // 128
NT = (((1,), (1,)), ((), ()))


def peers():
    dp, tp = lax.axis_index('dp'), lax.axis_index('tp')
    core = lax.rem(tp, 2)
    pair = tp - core
    other = 2 - pair
    part = pair + 1 - core
    return dp, tp, (dp, part), (dp, other + core), (dp, other + 1 - core), (1 - dp, tp)


def remote(src, dst, ssem, rsem, dev):
    return pltpu.make_async_remote_copy(
        src_ref=src, dst_ref=dst, send_sem=ssem, recv_sem=rsem, device_id=dev, device_id_type=pl.DeviceIdType.MESH)


def spread(row, rows, dst):
    dst[rows, :] = jnp.transpose(jnp.broadcast_to(row, (128, 128)))


def step_kernel(hid, gain, bias, emb, info,
                e_all, x_out, z_out, stat_all, info_all,
                dhid, x_part, x_xp, x_xq, dzt_own, dzt_out, dzt_part, dzt_last, de_part, gsum_all,
                info_v, stat_v, stats, infos, gb_v, gs_v, g8,
                h_sem, xo_sem, e_sem, eo_sem, z_sem, zt_sem, et_sem, small_sem, dzo_sem, big_sem, g_sem,
                xs_send, ys_send, ds_send, pe_send, sm_send, xt_send, xd_send, xp_send, dz_send, g_send,
                x_recv, y_recv, d_recv, pe_recv, info_recv, stat_recv, xt_recv, xd_recv, xp_recv, dz_recv, g_recv):
    bf16, f32 = jnp.bfloat16, jnp.float32
    dp, tp, part, xp, xq, yp = peers()
    core = lax.rem(tp, 2)
    xp_rank = 2 - (tp - core) + core
    xq_rank = 2 - (tp - core) + 1 - core
    group = ((1, part), (2, xp), (3, xq))
    barrier = pltpu.get_barrier_semaphore()
    for dev in (part, xp, xq, yp):
        pl.semaphore_signal(barrier, inc=1, device_id=dev, device_id_type=pl.DeviceIdType.MESH)
    pl.semaphore_wait(barrier, 4)

    def xrows(ref, j):
        return ref.at[pl.ds(pl.multiple_of(j * XCH, XCH), XCH)]

    def xt_copy(j):
        return remote(xrows(x_out, j), xrows(x_xp, j), xt_send, xt_recv.at[j], xp)

    def xd_copy(j):
        return remote(xrows(x_xp, j), xrows(x_xq, j), xd_send, xd_recv.at[j], part)

    def xt_event(j):
        xt_copy(j).wait_recv()
        xd_copy(j).start()
    xp_copy = remote(x_out, x_part, xp_send, xp_recv, part)

    def forward(m_s, scale_v, tc_v, mr_v, zt, et, xs, hbuf, ebuf, z0, z1, s_s, t_s, gb8):
        def tile_row(j):
            return ROWS * 2 + (j // 2) * TILE + lax.rem(j, 2) * CHUNK

        def x_copy(j):
            src = emb.at[pl.ds(pl.multiple_of(dp * (ROWS // 2) + j * CHUNK, CHUNK), CHUNK)]
            return remote(src, e_all.at[pl.ds(pl.multiple_of(tile_row(j), CHUNK), CHUNK)], xs_send, x_recv.at[j], xp)

        def piece(j, p):
            return e_all.at[pl.ds(pl.multiple_of(tile_row(j) + p * PIECE_ROWS, CHUNK), CHUNK)]

        def y_copy(j):
            return remote(piece(j, 0), piece(j, 1), ys_send, y_recv.at[j], yp)

        def d_copy(j, p):
            return remote(piece(j, p), piece(j, p + 2), ds_send, d_recv.at[j // 2], part)

        def pe_copy(i):
            return remote(emb.at[pl.ds(pl.multiple_of(i * PE_ROWS, PE_ROWS), PE_ROWS)],
                          e_all.at[pl.ds(pl.multiple_of(ROWS + i * PE_ROWS, PE_ROWS), PE_ROWS)], pe_send, pe_recv.at[i], part)

        cp = pltpu.make_async_copy(info, info_v, small_sem.at[0])
        cp.start()

        def h_copy(i):
            return pltpu.make_async_copy(hid.at[pl.ds(pl.multiple_of(i * LN_ROWS, LN_ROWS), LN_ROWS)], hbuf.at[lax.rem(i, 2)], h_sem.at[lax.rem(i, 2)])
        h_copy(0).start()

        for p, dev in group:
            remote(info, info_all.at[tp], sm_send, info_recv.at[p], dev).start()

        def start_x(j, c):
            x_copy(j).start()
            return c
        lax.fori_loop(0, CHUNKS, start_x, 0)

        def start_pe(i, c):
            pe_copy(i).start()
            return c
        lax.fori_loop(0, ROWS // PE_ROWS, start_pe, 0)

        def e_load(t):
            slot = lax.rem(t, 2)
            return pltpu.make_async_copy(e_all.at[pl.ds(pl.multiple_of(t * TILE, TILE), TILE)], ebuf.at[slot], e_sem.at[slot])

        def e_load_own(t):
            slot = lax.rem(t, 2)
            return pltpu.make_async_copy(emb.at[pl.ds(pl.multiple_of(t * TILE, TILE), TILE)], ebuf.at[slot], e_sem.at[slot])
        e_load_own(0).start()

        def x_event(j):
            x_copy(j).wait_recv()
            y_copy(j).start()
            d_copy(j, 0).start()

        def y_event(j):
            y_copy(j).wait_recv()
            d_copy(j, 1).start()

        def p_event(k):
            rows = e_all.at[pl.ds(pl.multiple_of(2 * ROWS + k * TILE + TILE // 2, TILE // 2), TILE // 2)]
            pltpu.make_async_copy(rows, rows, d_recv.at[k]).wait()
            e_load(NEAR + k).start()

        cp.wait()
        pltpu.make_async_copy(info_v, info_all.at[tp], small_sem.at[0]).start()
        gb8[0] = jnp.broadcast_to(gain[...], (8, DIM))
        gb8[1] = jnp.broadcast_to(bias[...], (8, DIM))

        def ln_tile(i, c):
            slot = lax.rem(i, 2)

            @pl.when(i + 1 < TOK // LN_ROWS)
            def _():
                h_copy(i + 1).start()
            h_copy(i).wait()

            @pl.when(i == 6)
            def _():
                x_event(0)

            def ln_rows(r, c2):
                base = r * LN_UNROLL * 16

                def at(u):
                    return pl.ds(pl.multiple_of(base + u * 16, 16), 16)

                def part_of(u, k):
                    return hbuf[slot, at(u), k * 128:(k + 1) * 128].astype(jnp.float32)
                means, rstds = [], []
                for u in range(LN_UNROLL):
                    tot = part_of(u, 0)
                    for k in range(1, DIM // 128):
                        tot = tot + part_of(u, k)
                    means.append(jnp.broadcast_to(jnp.sum(tot, axis=-1, keepdims=True) * (1.0 / DIM), (16, 128)))
                for u in range(LN_UNROLL):
                    tot = jnp.zeros((16, 128), jnp.float32)
                    for k in range(DIM // 128):
                        diff = part_of(u, k) - means[u]
                        tot = tot + diff * diff
                    var = jnp.sum(tot, axis=-1, keepdims=True) * (1.0 / DIM)
                    rstds.append(jnp.broadcast_to(lax.rsqrt(var + LN_EPS), (16, 128)))
                for u in range(LN_UNROLL):
                    row = pl.ds(pl.multiple_of(i * LN_ROWS + base + u * 16, 16), 16)
                    mr_v[0, row, :] = means[u]
                    mr_v[1, row, :] = rstds[u]
                    for k in range(DIM // 128):
                        cols = slice(k * 128, (k + 1) * 128)
                        g2 = jnp.concatenate([gb8[0, :, cols]] * 2, axis=0)
                        b2 = jnp.concatenate([gb8[1, :, cols]] * 2, axis=0)
                        xs[row, cols] = ((part_of(u, k) - means[u]) * rstds[u] * g2 + b2).astype(jnp.bfloat16)
                return c2
            lax.fori_loop(0, LN_ROWS // (16 * LN_UNROLL), ln_rows, 0)
            rows = pl.ds(pl.multiple_of(i * LN_ROWS, LN_ROWS), LN_ROWS)
            pltpu.make_async_copy(xs.at[rows], x_out.at[rows], xo_sem).start()
            return c
        lax.fori_loop(0, TOK // LN_ROWS, ln_tile, 0)

        m_s[...] = jnp.full((TOK, 128), LOWEST, jnp.float32)
        s_s[...] = jnp.zeros((TOK, 128), jnp.float32)
        t_s[...] = jnp.zeros((TOK, 128), jnp.float32)
        for r in range(GROUPS):
            spread(info_v[2, r:r + 1, :], slice(r * 128, (r + 1) * 128), tc_v)
        z1[...] = jnp.full((HB, TILE), LOWEST, jnp.float32)

        zs = (z0, z1)

        def product(t, h):
            for r in range(0, HB, 512):
                zs[h][r:r + 512, :] = lax.dot_general(
                    xs[h * HB + r:h * HB + r + 512, :], ebuf[lax.rem(t, 2)], NT, preferred_element_type=jnp.float32)

        def statistics(t, h):
            z = zs[h]
            lane = lax.broadcasted_iota(jnp.int32, (STAT_ROWS, 128), 1)
            for r in range(0, HB, STAT_ROWS):
                rows = slice(h * HB + r, h * HB + r + STAT_ROWS)
                zk = [z[r:r + STAT_ROWS, k * 128:(k + 1) * 128] for k in range(TILE // 128)]
                old = m_s[rows, :]
                new = jnp.maximum(jnp.maximum(zk[0], zk[1]), old)
                tot = s_s[rows, :] * jnp.exp(old - new)
                tgt = t_s[rows, :]
                diff = tc_v[rows, :] - t * TILE
                for k in range(TILE // 128):
                    tot = tot + jnp.exp(zk[k] - new)
                    tgt = tgt + jnp.where(diff == lane + k * 128, zk[k], 0.0)
                m_s[rows, :] = new
                s_s[rows, :] = tot
                t_s[rows, :] = tgt

        def z_copy(t, h):
            return pltpu.make_async_copy(
                zs[h], z_out.at[pl.ds(h * HB, HB), pl.ds(pl.multiple_of(t * TILE, TILE), TILE)], z_sem.at[h])

        def start_events(t):
            @pl.when(t < TILES - 1)
            def _():
                x_event(t + 1)

            @pl.when(t == TILES - 2)
            def _():
                xt_copy(0).start()

            @pl.when(t == TILES - 1)
            def _():
                y_event(TILES - 1)
                p_event(TILES - 1 - NEAR)
            e_load(t).wait()

            @pl.when(t < ROWS // TILE)
            def _():
                slot = lax.rem(t, 2)
                pltpu.make_async_copy(ebuf.at[slot], e_all.at[pl.ds(pl.multiple_of(t * TILE, TILE), TILE)], eo_sem.at[slot]).start()

        def middle_events(t):
            @pl.when(t < TILES - 1)
            def _():
                y_event(t)

            @pl.when((t >= 1) & (t < ROWS // TILE + 1))
            def _():
                slot = lax.rem(t - 1, 2)
                pltpu.make_async_copy(ebuf.at[slot], e_all.at[pl.ds(0, TILE)], eo_sem.at[slot]).wait()

            @pl.when(t == NEAR)
            def _():
                pltpu.make_async_copy(xs, x_out, xo_sem).wait()

            @pl.when(t < ROWS // TILE - 1)
            def _():
                e_load_own(t + 1).start()

            @pl.when((t >= ROWS // TILE - 1) & (t < NEAR - 1))
            def _():
                @pl.when(lax.rem(t + 1, PE_ROWS // TILE) == 0)
                def _():
                    pe_copy((t + 1 - ROWS // TILE) // (PE_ROWS // TILE)).wait_recv()
                e_load(t + 1).start()

            @pl.when((t >= NEAR - 1) & (t < TILES - 2))
            def _():
                p_event(t - (NEAR - 1))

            @pl.when(t == NEAR + 1)
            def _():
                for p, dev in group:
                    remote(info, info_all.at[tp], sm_send, info_recv.at[p], dev).wait_recv()
                pltpu.make_async_copy(info_v, info_all.at[tp], small_sem.at[0]).wait()
                load = pltpu.make_async_copy(info_all, infos, small_sem.at[0])
                load.start()
                load.wait()
                count = jnp.broadcast_to(token_count(), (1, 128))
                for r in range(GROUPS):
                    spread(info_v[1, r:r + 1, :].astype(f32) / count, slice(r * 128, (r + 1) * 128), scale_v)

        def step(t, c):
            @pl.when(t > 0)
            def _():
                z_copy(t - 1, 1).start()
            start_events(t)

            @pl.when(t > 0)
            def _():
                z_copy(t - 1, 0).wait()
            statistics(t - 1, 1)
            product(t, 0)
            z_copy(t, 0).start()
            middle_events(t)

            @pl.when(t > 0)
            def _():
                z_copy(t - 1, 1).wait()
            statistics(t, 0)
            product(t, 1)
            return c
        last = TILES - 1
        lax.fori_loop(0, TILES, step, 0)
        z_copy(last, 1).start()
        statistics(last, 1)

        def finish(i, c):
            for u in range(4):
                r = i * 4 + u
                rows = pl.ds(pl.multiple_of(r * 128, 128), 128)
                m = m_s[rows, :]
                top = jnp.max(m, axis=-1, keepdims=True)
                tot = jnp.sum(s_s[rows, :] * jnp.exp(m - top), axis=-1, keepdims=True)
                lse = jnp.broadcast_to(top + jnp.log(tot), (128, 128))
                tgt = jnp.broadcast_to(jnp.sum(t_s[rows, :], axis=-1, keepdims=True), (128, 128))
                m_s[rows, :] = lse
                stat_v[0, pl.ds(r, 1), :] = jnp.transpose(lse)[0:1, :]
                stat_v[1, pl.ds(r, 1), :] = jnp.transpose(tgt)[0:1, :]
            return c
        lax.fori_loop(0, TOK // 512, finish, 0)
        for h in range(2):
            z_copy(last, h).wait()
        for k, h in ((0, 0), (1, 0), (0, 1)):
            z_load(zt, k, h).start()
        et_load(et, 0).start()
        half = e_all.at[pl.ds(0, ROWS // 2)]
        pltpu.make_async_copy(half, half, xs_send).wait()
        pltpu.make_async_copy(half, half, ys_send).wait()
        full = e_all.at[pl.ds(0, ROWS)]
        pltpu.make_async_copy(full, full, ds_send).wait()
        pltpu.make_async_copy(full, full, pe_send).wait()
        pltpu.make_async_copy(stat_v, stat_all.at[tp], small_sem.at[1]).start()
        for p, dev in group:
            remote(stat_v, stat_all.at[tp], sm_send, stat_recv.at[p], dev).start()

        def start_xt(j, c):
            xt_copy(j).start()
            return c
        lax.fori_loop(1, XCHS, start_xt, 0)
        xp_copy.start()

    def z_load(zt, k, h):
        slot = lax.rem(k, 2)
        rows = slice(h * HB, (h + 1) * HB)
        return pltpu.make_async_copy(
            z_out.at[rows, pl.ds(pl.multiple_of(k * KT, KT), KT)], zt.at[slot, rows], zt_sem.at[2 * h + slot])

    def et_load(et, k):
        slot = lax.rem(k, 2)
        return pltpu.make_async_copy(e_all.at[pl.ds(pl.multiple_of(k * KT, KT), KT)], et.at[slot], et_sem.at[slot])

    def dzt_copy(k):
        rows = pl.ds(pl.multiple_of(lax.rem(k, 4) * KT, KT), KT)
        return remote(dzt_out.at[rows], dzt_part.at[rows], dz_send, dz_recv.at[lax.rem(k, 4)], part)

    def token_count():
        return jnp.sum(infos[:, 1].astype(f32))

    def token_grads(lse_v, scale_v, tcol_v, mr, zt, et, acc):
        def d_phase(da, db, dzt):
            def dzt_store(k, ref):
                slot = lax.rem(k, 2)
                return pltpu.make_async_copy(dzt.at[slot], ref.at[pl.ds(pl.multiple_of(lax.rem(k, 4) * KT, KT), KT)], eo_sem.at[slot])
            lane = lax.broadcasted_iota(jnp.int32, (PIECE, 128), 1)

            def piece(dst, rows, low, k, tie):
                slot = lax.rem(k, 2)
                lse = lse_v[rows, :]
                if tie is not None:
                    floor = 0.0 - jnp.maximum(0.0 - tie, -LOWEST)
                    lse = jnp.maximum(lse, jnp.concatenate([floor] * (PIECE // 8), axis=0))
                scale = scale_v[rows, :]
                diff = tcol_v[rows, :] - k * KT
                for g in range(KT // 128):
                    cols = slice(g * 128, (g + 1) * 128)
                    hot = (diff == lane + g * 128).astype(f32)
                    val = (jnp.exp(zt[slot, rows, cols] - lse) - hot) * scale
                    dst[low, cols] = val.astype(bf16)

            def half_step(k, src, dst, base, dst_base, dst_k):
                slot = lax.rem(k, 2)
                per = HB // (DIM // NCOL)
                for n in range(DIM // NCOL):
                    cols = slice(n * NCOL, (n + 1) * NCOL)
                    prod = jnp.dot(src[...], et[slot, :, cols], preferred_element_type=f32)
                    acc[base:base + HB, cols] = jnp.where(k == 0, 0.0, acc[base:base + HB, cols]) + prod
                    for q in range(0, per, PIECE):
                        at = q * HB // per
                        low = n * per + q
                        piece(dst, slice(dst_base + low, dst_base + low + PIECE), slice(low, low + PIECE), dst_k, prod[at:at + 8, 0:128])
                    if n * per % 256 == 0:
                        low = n * per
                        dzt[slot, :, base + low:base + low + 256] = jnp.transpose(src[low:low + 256, :])

            z_load(zt, 0, 0).wait()

            def first(i, c):
                rows = pl.ds(pl.multiple_of(i * PIECE, PIECE), PIECE)
                piece(da, rows, rows, 0, None)
                return c
            lax.fori_loop(0, HB // PIECE, first, 0)

            def step(k, c):
                @pl.when(k + 2 < VOCAB // KT)
                def _():
                    z_load(zt, k + 2, 0).start()

                @pl.when(k + 1 < VOCAB // KT)
                def _():
                    z_load(zt, k + 1, 1).start()
                    et_load(et, k + 1).start()
                    z_load(zt, k + 1, 0).wait()
                for at, j in WAIT_STEP.items():
                    @pl.when(k == at)
                    def _(j=j):
                        xt_event(j)

                @pl.when((k >= 2) & (k < 10))
                def _():
                    dzt_store(k, dzt_own).wait()

                @pl.when((k >= 6) & (k < 10))
                def _():
                    dzt_copy(k - 2).start()
                et_load(et, k).wait()
                z_load(zt, k, 1).wait()
                half_step(k, da, db, 0, HB, k)
                half_step(k, db, da, HB, 0, k + 1)

                @pl.when(k < 4)
                def _():
                    dzt_store(k, dzt_own).start()

                @pl.when((k >= 4) & (k < 8))
                def _():
                    dzt_store(k, dzt_out).start()
                return c
            lax.fori_loop(0, VOCAB // KT, step, 0)
        half = pltpu.VMEM((HB, KT), bf16)
        pl.run_scoped(d_phase, half, half, pltpu.VMEM((2, KT, TOK), bf16))

        def n_phase(hb, ob):
            def h_load(i):
                slot = lax.rem(i, 2)
                return pltpu.make_async_copy(hid.at[pl.ds(pl.multiple_of(i * NB_ROWS, NB_ROWS), NB_ROWS)], hb.at[slot], z_sem.at[slot])

            def o_store(i):
                slot = lax.rem(i, 2)
                return pltpu.make_async_copy(ob.at[slot], dhid.at[pl.ds(pl.multiple_of(i * NB_ROWS, NB_ROWS), NB_ROWS)], e_sem.at[slot])
            h_load(0).start()
            gb_v[...] = jnp.zeros(gb_v.shape, jnp.float32)
            g8[...] = jnp.broadcast_to(gain[...], (8, DIM))

            def tile(i, c):
                slot = lax.rem(i, 2)

                @pl.when(i + 1 < TOK // NB_ROWS)
                def _():
                    h_load(i + 1).start()

                @pl.when(i >= 2)
                def _():
                    o_store(i - 2).wait()
                h_load(i).wait()

                def rows_body(r, c2):
                    units = range(NB_UNROLL)
                    base = r * 16 * NB_UNROLL
                    low = [pl.ds(pl.multiple_of(base + u * 16, 16), 16) for u in units]
                    row = [pl.ds(pl.multiple_of(i * NB_ROWS + base + u * 16, 16), 16) for u in units]
                    zero = jnp.zeros((16, 128), jnp.float32)
                    sum1, sum3 = [zero] * NB_UNROLL, [zero] * NB_UNROLL

                    def load(u, cols):
                        dx = acc[row[u], cols]
                        xhat = (hb[slot, low[u], cols].astype(jnp.float32) - mr[0, row[u], :]) * mr[1, row[u], :]
                        return dx, xhat, dx * jnp.concatenate([g8[:, cols]] * 2, axis=0)
                    for k in range(DIM // 128):
                        cols = slice(k * 128, (k + 1) * 128)
                        d_gain, d_bias = gb_v[0, :, cols], gb_v[1, :, cols]
                        for u in units:
                            dx, xhat, gx = load(u, cols)
                            sum1[u] = sum1[u] + gx
                            sum3[u] = sum3[u] + gx * xhat
                            dgx = dx * xhat
                            d_gain = d_gain + (dgx[0:8] + dgx[8:16])
                            d_bias = d_bias + (dx[0:8] + dx[8:16])
                        gb_v[0, :, cols] = d_gain
                        gb_v[1, :, cols] = d_bias
                    slope, shift = [], []
                    for u in units:
                        mean, rstd = mr[0, row[u], :], mr[1, row[u], :]
                        c1 = jnp.broadcast_to(jnp.sum(sum1[u], axis=-1, keepdims=True) * (1.0 / DIM), (16, 128))
                        c3 = jnp.broadcast_to(jnp.sum(sum3[u], axis=-1, keepdims=True) * (1.0 / DIM), (16, 128))
                        slope.append(c3 * rstd * rstd)
                        shift.append(slope[u] * mean - c1 * rstd)
                    for u in units:
                        rstd = mr[1, row[u], :]
                        for k in range(DIM // 128):
                            cols = slice(k * 128, (k + 1) * 128)
                            gx = acc[row[u], cols] * jnp.concatenate([g8[:, cols]] * 2, axis=0)
                            ob[slot, low[u], cols] = (gx * rstd - hb[slot, low[u], cols].astype(f32) * slope[u] + shift[u]).astype(bf16)
                    return c2
                lax.fori_loop(0, NB_ROWS // (16 * NB_UNROLL), rows_body, 0)
                o_store(i).start()
                return c
            lax.fori_loop(0, TOK // NB_ROWS, tile, 0)
            for i in range(2):
                o_store(TOK // NB_ROWS - 2 + i).wait()
            gs_v[0:1, :] = jnp.sum(gb_v[0], axis=0, keepdims=True)
            gs_v[1:2, :] = jnp.sum(gb_v[1], axis=0, keepdims=True)
        pl.run_scoped(n_phase, pltpu.VMEM((2, NB_ROWS, DIM), bf16), pltpu.VMEM((2, NB_ROWS, DIM), bf16))

    def weight_grads(acc):
        own = pltpu.make_async_copy(gs_v, gsum_all.at[tp], g_sem)

        def e_phase(eo, xt, dzb, zs, z1):
            eo_load = pltpu.make_async_copy(emb, eo, big_sem)

            def x_load(ref, row, slot):
                return pltpu.make_async_copy(ref.at[pl.ds(pl.multiple_of(row, KT), KT)], xt.at[slot], z_sem.at[slot])

            def dz_load(ref, col, slot):
                return pltpu.make_async_copy(ref.at[:, pl.ds(pl.multiple_of(col, KT), KT)], dzb.at[slot], e_sem.at[slot])

            def start_local(i):
                slot = lax.rem(i, 2)

                @pl.when(i < 4)
                def _():
                    x_load(x_out, i * KT, slot).start()
                    dz_load(dzt_own, i * KT, slot).start()

                @pl.when(i >= 4)
                def _():
                    x_load(x_part, (i - 4) * KT, slot).start()
                    dz_load(dzt_part, (i - 4) * KT, slot).start()

            def add(slot, first):
                for rows in (slice(0, HB), slice(HB, TOK)):
                    for n in range(0, DIM, NCOL):
                        prod = jnp.dot(dzb[slot, rows, :], xt[slot, :, n:n + NCOL], preferred_element_type=f32)
                        acc[rows, n:n + NCOL] = jnp.where(first, 0.0, acc[rows, n:n + NCOL]) + prod

            start_local(0)

            def rem_load(r):
                slot = lax.rem(r, 2)
                return [pltpu.make_async_copy(xrows(ref, r), xt.at[slot, pl.ds(i * XCH, XCH)], z_sem.at[slot])
                        for i, ref in enumerate((x_xp, x_xq))]

            def local(i, c):
                slot = lax.rem(i, 2)

                @pl.when(i == 0)
                def _():
                    eo_load.start()

                @pl.when(i == 2)
                def _():
                    xp_copy.wait_recv()

                    def wait_dz(q, c2):
                        dzt_copy(q).wait_recv()
                        return c2
                    lax.fori_loop(0, 4, wait_dz, 0)

                @pl.when(i == 1)
                def _():
                    own.start()
                    for p, dev in group:
                        remote(gs_v, gsum_all.at[tp], g_send, g_recv.at[p], dev).start()

                @pl.when(i == 1)
                def _():
                    xt_event(3)

                @pl.when(i == 6)
                def _():
                    xt_event(4)

                @pl.when(i < 7)
                def _():
                    start_local(i + 1)

                @pl.when(i == 7)
                def _():
                    xd_copy(0).wait_recv()
                    for cp in rem_load(0):
                        cp.start()
                x_load(x_out, 0, slot).wait()
                dz_load(dzt_own, 0, slot).wait()
                add(slot, i == 0)
                return c
            lax.fori_loop(0, 8, local, 0)
            eo_load.wait()
            for p, dev in group:
                remote(stat_v, stat_all.at[tp], sm_send, stat_recv.at[p], dev).wait_recv()
            pltpu.make_async_copy(stat_v, stat_all.at[tp], small_sem.at[1]).wait()
            stat_load = pltpu.make_async_copy(stat_all, stats, small_sem.at[1])
            stat_load.start()
            stat_load.wait()
            count = jnp.broadcast_to(token_count(), (1, 128))

            def far(r, c):
                slot = lax.rem(r, 2)

                @pl.when(r == 2)
                def _():
                    xt_event(5)

                @pl.when(r == 4)
                def _():
                    xt_event(6)

                def fetch():
                    xd_copy(r + 1).wait_recv()
                    for cp in rem_load(r + 1):
                        cp.start()
                pl.when(r < XCHS - 2)(fetch)
                x_load(x_out, 0, slot).wait()

                @pl.when(r == XCHS - DEFER)
                def _():
                    pltpu.make_async_copy(acc, de_part, big_sem).start()

                @pl.when(r > XCHS - DEFER + 1)
                def _():
                    dz_out(0, 0, slot).wait()
                    dz_out(0, 1, slot).wait()

                far_rows = []
                for g in range(4):
                    who = xp_rank if g < 2 else xq_rank
                    at = pl.ds(2 * r + g % 2, 1)
                    far_rows.append((stats[who, 0, at, :], infos[who, 1, at, :].astype(f32) / count, infos[who, 0, at, :] - tp * ROWS))

                def logits(h2, c2):
                    def multiply(h, z):
                        for k in range(0, DIM, KCOL):
                            prod = lax.dot_general(eo[pl.ds(pl.multiple_of(h * ZB, ZB), ZB), k:k + KCOL], xt[slot, :, k:k + KCOL], NT, preferred_element_type=jnp.float32)
                            z[...] = prod if k == 0 else z[...] + prod

                    def convert(h, z):
                        for q in range(ZB // 32):
                            row = h * ZB + q * 32
                            line = lax.broadcasted_iota(jnp.int32, (32, 128), 0)
                            for g, (lse, scale, trel) in enumerate(far_rows):
                                cols = slice(g * 128, (g + 1) * 128)
                                hot = ((trel - row) == line).astype(f32)
                                val = (jnp.exp(z[q * 32:(q + 1) * 32, cols] - lse) - hot) * scale
                                dzb[slot, pl.ds(pl.multiple_of(row, 32), 32), cols] = val.astype(bf16)
                    lo, hi = 2 * h2, 2 * h2 + 1
                    multiply(lo, zs)
                    multiply(hi, z1)
                    convert(lo, zs)
                    convert(hi, z1)
                    return c2
                lax.fori_loop(0, ROWS // (2 * ZB), logits, 0)

                @pl.when(r == XCHS - 2)
                def _():
                    xt_event(XCHS - 1)
                    fetch()

                @pl.when(r < XCHS - DEFER)
                def _():
                    def mul(h, c2):
                        rows = pl.ds(pl.multiple_of(h * HB, HB), HB)
                        for n in range(0, DIM, NCOL):
                            acc[rows, n:n + NCOL] += jnp.dot(dzb[slot, rows, :], xt[slot, :, n:n + NCOL], preferred_element_type=jnp.float32)
                        return c2
                    lax.fori_loop(0, HBS, mul, 0)

                @pl.when(r >= XCHS - DEFER)
                def _():
                    for i in range(2):
                        dz_out(r - (XCHS - DEFER), i, slot).start()
                return c

            def dz_out(q, i, slot):
                return pltpu.make_async_copy(
                    dzb.at[slot, :, pl.ds(i * XCH, XCH)], dzt_last.at[i, :, pl.ds(pl.multiple_of(q * XCH, XCH), XCH)], dzo_sem.at[slot])
            lax.fori_loop(0, XCHS, far, 0)
            for slot in range(2):
                dz_out(0, 0, slot).wait()
                dz_out(0, 1, slot).wait()
            pltpu.make_async_copy(acc, de_part, big_sem).wait()
        pl.run_scoped(e_phase, pltpu.VMEM((ROWS, DIM), jnp.bfloat16), pltpu.VMEM((2, KT, DIM), jnp.bfloat16),
                      pltpu.VMEM((2, ROWS, KT), jnp.bfloat16), pltpu.VMEM((ZB, KT), jnp.float32), pltpu.VMEM((ZB, KT), jnp.float32))

        own.wait()

    wide = pltpu.VMEM((TOK, 128), f32)
    big = pltpu.VMEM((TOK, DIM), f32)

    def tokens(m_s, scale_v, tc_v, mr_v, zt, et):
        kept = (m_s, scale_v, tc_v, mr_v, zt, et)
        pl.run_scoped(functools.partial(forward, *kept), pltpu.VMEM((TOK, DIM), bf16), pltpu.VMEM((2, LN_ROWS, DIM), bf16),
                      pltpu.VMEM((2, TILE, DIM), bf16), pltpu.VMEM((HB, TILE), f32), pltpu.VMEM((HB, TILE), f32), wide, wide,
                      pltpu.VMEM((2, 8, DIM), f32))
        pl.run_scoped(functools.partial(token_grads, *kept), big)
    pl.run_scoped(tokens, wide, wide, pltpu.VMEM((TOK, 128), jnp.int32), pltpu.VMEM((2, TOK, 128), f32),
                  pltpu.VMEM((2, TOK, KT), f32), pltpu.VMEM((2, KT, DIM), bf16))
    pl.run_scoped(weight_grads, big)

    pltpu.make_async_copy(x_out, x_out, xt_send).wait()
    pltpu.make_async_copy(x_out, x_out, xd_send).wait()
    xp_copy.wait_send()
    pltpu.make_async_copy(dzt_out, dzt_out, dz_send).wait()
    for p, dev in group:
        remote(info, info_all.at[tp], sm_send, info_recv.at[p], dev).wait_send()
        remote(stat_v, stat_all.at[tp], sm_send, stat_recv.at[p], dev).wait_send()
        remote(gs_v, gsum_all.at[tp], g_send, g_recv.at[p], dev).wait()


def run_step(hidden, gain, bias, embed, info):
    any_spec = pl.BlockSpec(memory_space=pl.ANY)
    vmem_spec = pl.BlockSpec(memory_space=pltpu.VMEM)
    f32, bf16, i32 = jnp.float32, jnp.bfloat16, jnp.int32
    dma = pltpu.SemaphoreType.DMA
    small, ints = (4, 2, GROUPS, 128), (4, 3, GROUPS, 128)
    mat, square = ((TOK, DIM), bf16), ((ROWS, TOK), bf16)
    shapes = [((VOCAB, DIM), bf16), mat, ((TOK, VOCAB), f32), (small, f32), (ints, i32),
              mat, mat, mat, mat, square, square, square, ((2, ROWS, DEFER * XCH), bf16), ((ROWS, DIM), f32), ((4, 2, DIM), f32)]
    return pl.pallas_call(
        step_kernel,
        name="step",
        out_shape=[jax.ShapeDtypeStruct(s, d) for s, d in shapes],
        in_specs=[any_spec, vmem_spec, vmem_spec, any_spec, any_spec],
        out_specs=[any_spec] * len(shapes),
        scratch_shapes=[
            pltpu.VMEM((3, GROUPS, 128), i32), pltpu.VMEM((2, GROUPS, 128), f32), pltpu.VMEM(small, f32), pltpu.VMEM(ints, i32),
            pltpu.VMEM((2, 8, DIM), f32), pltpu.VMEM((2, DIM), f32), pltpu.VMEM((8, DIM), f32),
            dma((2,)), dma, dma((2,)), dma((2,)), dma((2,)), dma((4,)), dma((2,)), dma((2,)), dma((2,)), dma, dma,
            dma, dma, dma, dma, dma, dma, dma, dma, dma, dma,
            dma((CHUNKS,)), dma((CHUNKS,)), dma((TILES - NEAR,)), dma((ROWS // PE_ROWS,)), dma((4,)), dma((4,)),
            dma((XCHS,)), dma((XCHS,)), dma, dma((4,)), dma((4,)),
        ],
        compiler_params=pltpu.CompilerParams(collective_id=0, has_side_effects=True, vmem_limit_bytes=67043328),
        cost_estimate=pl.CostEstimate(flops=12 * TOK * VOCAB * DIM, bytes_accessed=700 * 2 ** 20, transcendentals=3 * TOK * VOCAB),
    )(hidden, gain, bias, embed, info)


def finish_kernel(*refs):
    nb = DEFER * XCH // KT
    de_in, dz0, dz1 = refs[:3]
    xs = refs[3:3 + 2 * nb]
    dh_in, stat_all, info_all, gsum_all, de_out, dh_out, loss, mean, d_gain, d_bias = refs[3 + 2 * nb:]
    for h in range(HBS):
        rows = slice(h * HB, (h + 1) * HB)
        prod = None
        for b in range(nb):
            for dz, x in ((dz0, xs[b]), (dz1, xs[nb + b])):
                part = jnp.dot(dz[0, rows, b * KT:(b + 1) * KT], x[...], preferred_element_type=jnp.float32)
                prod = part if prod is None else prod + part
        de_out[rows, :] = de_in[rows, :] + prod
    dh_out[...] = dh_in[...]

    @pl.when(pl.program_id(0) == 0)
    def _():
        weights = info_all[:, 1].astype(jnp.float32)
        all_loss = (stat_all[:, 0] - stat_all[:, 1]) * weights
        tp = lax.axis_index('tp')
        loss[...] = (stat_all[tp, 0] - stat_all[tp, 1]) * info_all[tp, 1].astype(jnp.float32)
        mean[...] = jnp.broadcast_to(jnp.sum(all_loss), (1, 1)) / jnp.broadcast_to(jnp.sum(weights), (1, 1))
        sums = ((gsum_all[0] + gsum_all[1]) + gsum_all[2]) + gsum_all[3]
        d_gain[...] = sums[0:1]
        d_bias[...] = sums[1:2]


def finish(de_part, dzt_last, x_xp, x_xq, dhid, stat_all, info_all, gsum_all):
    cols = 512
    steps = DIM // cols
    depth = DEFER * XCH
    rows = TOK // steps
    first = (TOK - depth) // KT
    once = pl.Buffered(1)
    x_specs = [pl.BlockSpec((KT, cols), lambda i, b=b: (b, i)) for b in range(first, TOK // KT)]

    def whole(shape):
        return pl.BlockSpec(shape, lambda i: (0,) * len(shape))
    nb = len(x_specs)
    outs = [((ROWS, DIM), jnp.float32), ((TOK, DIM), jnp.bfloat16), ((GROUPS, 128), jnp.float32), ((1, 1), jnp.float32), ((1, DIM), jnp.float32), ((1, DIM), jnp.float32)]
    return pl.pallas_call(
        finish_kernel,
        name="finish",
        grid=(steps,),
        out_shape=[jax.ShapeDtypeStruct(s, d) for s, d in outs],
        in_specs=[
            pl.BlockSpec((ROWS, cols), lambda i: (0, i)),
            pl.BlockSpec((1, ROWS, depth), lambda i: (0, 0, 0), pipeline_mode=once),
            pl.BlockSpec((1, ROWS, depth), lambda i: (1, 0, 0), pipeline_mode=once),
            *x_specs, *x_specs,
            pl.BlockSpec((rows, DIM), lambda i: (i, 0)),
            whole(stat_all.shape), whole(info_all.shape), whole(gsum_all.shape),
        ],
        out_specs=[pl.BlockSpec((ROWS, cols), lambda i: (0, i)), pl.BlockSpec((rows, DIM), lambda i: (i, 0)),
                   whole((GROUPS, 128)), whole((1, 1)), whole((1, DIM)), whole((1, DIM))],
        compiler_params=pltpu.CompilerParams(vmem_limit_bytes=60 * 1024 * 1024),
        cost_estimate=pl.CostEstimate(flops=4 * ROWS * DIM * depth, bytes_accessed=120 * 2 ** 20, transcendentals=0),
    )(de_part, dzt_last, dzt_last, *[x_xp] * nb, *[x_xq] * nb, dhid, stat_all, info_all, gsum_all)


def solution(mesh):
    def body(hidden, ln_gain, ln_bias, embed, targets, loss_mask):
        dp, rank = lax.axis_index('dp'), lax.axis_index('tp')
        shard = targets // ROWS
        block = jnp.bitwise_xor(shard, rank)
        row = targets % ROWS
        half = row // (ROWS // 2)
        sub = row % (ROWS // 2)
        piece = (block - 2) * 2 + jnp.bitwise_xor(half, dp)
        far = 2 * ROWS + (sub // PIECE_ROWS) * TILE + piece * PIECE_ROWS + sub % PIECE_ROWS
        tcol = jnp.where(block < 2, block * ROWS + row, far)
        info = jnp.stack([targets, loss_mask, tcol]).reshape(3, GROUPS, 128)
        outs = run_step(hidden, ln_gain.reshape(1, DIM), ln_bias.reshape(1, DIM), embed, info)
        stat_all, info_all, dhid, x_xp, x_xq, dzt_last, de_part, gsum_all = (outs[i] for i in (3, 4, 5, 7, 8, 12, 13, 14))
        d_embed, d_hidden, loss, mean, d_gain, d_bias = finish(de_part, dzt_last, x_xp, x_xq, dhid, stat_all, info_all, gsum_all)
        return loss.reshape(TOK), mean.reshape(1), d_hidden, d_embed, d_gain.reshape(DIM), d_bias.reshape(DIM)

    token_rows = P(('dp', 'tp'))
    token_mat = P(('dp', 'tp'), None)
    return jax.shard_map(body, mesh=mesh, in_specs=(token_mat, P(), P(), P('tp', None), token_rows, token_rows), out_specs=(token_rows, P('dp'), token_mat, token_mat, P('dp'), P('dp')), check_vma=False)
```

```python
import functools

import jax
import jax.numpy as jnp
from jax import lax
from jax.experimental import pallas as pl
from jax.experimental.pallas import tpu as pltpu
from jax.sharding import PartitionSpec as P

LN_EPS = 1e-5
LOWEST = float(jnp.finfo(jnp.float32).min)

TOK = 2048
ROWS = 2048
DIM = 4096
VOCAB = 8192
TILE = 256
TILES = VOCAB // TILE
HB = 1024
HBS = TOK // HB
CHUNK = 32
PIECE_ROWS = 2 * CHUNK
NEAR = 2 * ROWS // TILE
PE_ROWS = 512
CHUNKS = ROWS // 2 // CHUNK
LN_ROWS = 256
STAT_ROWS = 32
PIECE = 32
LN_UNROLL = 4
XCH = 256
XCHS = TOK // XCH
KT = 512
DEFER = 4
WAIT_STEP = {4: 0, 9: 1, 14: 2}
ZB = 512
NCOL = 512
KCOL = 1024
NB_UNROLL = 4
NB_ROWS = 256
GROUPS = TOK // 128
NT = (((1,), (1,)), ((), ()))


def peers():
    dp, tp = lax.axis_index('dp'), lax.axis_index('tp')
    core = lax.rem(tp, 2)
    pair = tp - core
    other = 2 - pair
    part = pair + 1 - core
    return dp, tp, (dp, part), (dp, other + core), (dp, other + 1 - core), (1 - dp, tp)


def remote(src, dst, ssem, rsem, dev):
    return pltpu.make_async_remote_copy(
        src_ref=src, dst_ref=dst, send_sem=ssem, recv_sem=rsem, device_id=dev, device_id_type=pl.DeviceIdType.MESH)


def spread(row, rows, dst):
    dst[rows, :] = jnp.transpose(jnp.broadcast_to(row, (128, 128)))


def step_kernel(hid, gain, bias, emb, info,
                e_all, x_out, z_out, stat_all, info_all,
                dhid, x_part, x_xp, x_xq, dzt_own, dzt_out, dzt_part, dzt_last, de_part, gsum_all,
                info_v, stat_v, stats, infos, gb_v, gs_v, g8,
                h_sem, xo_sem, e_sem, eo_sem, z_sem, zt_sem, et_sem, small_sem, dzo_sem, big_sem, g_sem,
                xs_send, ys_send, ds_send, pe_send, sm_send, xt_send, xd_send, xp_send, dz_send, g_send,
                x_recv, y_recv, d_recv, pe_recv, info_recv, stat_recv, xt_recv, xd_recv, xp_recv, dz_recv, g_recv):
    bf16, f32 = jnp.bfloat16, jnp.float32
    dp, tp, part, xp, xq, yp = peers()
    core = lax.rem(tp, 2)
    xp_rank = 2 - (tp - core) + core
    xq_rank = 2 - (tp - core) + 1 - core
    group = ((1, part), (2, xp), (3, xq))
    barrier = pltpu.get_barrier_semaphore()
    for dev in (part, xp, xq, yp):
        pl.semaphore_signal(barrier, inc=1, device_id=dev, device_id_type=pl.DeviceIdType.MESH)
    pl.semaphore_wait(barrier, 4)

    def xrows(ref, j):
        return ref.at[pl.ds(pl.multiple_of(j * XCH, XCH), XCH)]

    def xt_copy(j):
        return remote(xrows(x_out, j), xrows(x_xp, j), xt_send, xt_recv.at[j], xp)

    def xd_copy(j):
        return remote(xrows(x_xp, j), xrows(x_xq, j), xd_send, xd_recv.at[j], part)

    def xt_event(j):
        xt_copy(j).wait_recv()
        xd_copy(j).start()
    xp_copy = remote(x_out, x_part, xp_send, xp_recv, part)

    def forward(m_s, scale_v, tc_v, mr_v, zt, et, xs, hbuf, ebuf, z0, z1, s_s, t_s, gb8):
        def tile_row(j):
            return ROWS * 2 + (j // 2) * TILE + lax.rem(j, 2) * CHUNK

        def x_copy(j):
            src = emb.at[pl.ds(pl.multiple_of(dp * (ROWS // 2) + j * CHUNK, CHUNK), CHUNK)]
            return remote(src, e_all.at[pl.ds(pl.multiple_of(tile_row(j), CHUNK), CHUNK)], xs_send, x_recv.at[j], xp)

        def piece(j, p):
            return e_all.at[pl.ds(pl.multiple_of(tile_row(j) + p * PIECE_ROWS, CHUNK), CHUNK)]

        def y_copy(j):
            return remote(piece(j, 0), piece(j, 1), ys_send, y_recv.at[j], yp)

        def d_copy(j, p):
            return remote(piece(j, p), piece(j, p + 2), ds_send, d_recv.at[j // 2], part)

        def pe_copy(i):
            return remote(emb.at[pl.ds(pl.multiple_of(i * PE_ROWS, PE_ROWS), PE_ROWS)],
                          e_all.at[pl.ds(pl.multiple_of(ROWS + i * PE_ROWS, PE_ROWS), PE_ROWS)], pe_send, pe_recv.at[i], part)

        cp = pltpu.make_async_copy(info, info_v, small_sem.at[0])
        cp.start()

        def h_copy(i):
            return pltpu.make_async_copy(hid.at[pl.ds(pl.multiple_of(i * LN_ROWS, LN_ROWS), LN_ROWS)], hbuf.at[lax.rem(i, 2)], h_sem.at[lax.rem(i, 2)])
        h_copy(0).start()

        for p, dev in group:
            remote(info, info_all.at[tp], sm_send, info_recv.at[p], dev).start()

        def start_x(j, c):
            x_copy(j).start()
            return c
        lax.fori_loop(0, CHUNKS, start_x, 0)

        def start_pe(i, c):
            pe_copy(i).start()
            return c
        lax.fori_loop(0, ROWS // PE_ROWS, start_pe, 0)

        def e_load(t):
            slot = lax.rem(t, 2)
            return pltpu.make_async_copy(e_all.at[pl.ds(pl.multiple_of(t * TILE, TILE), TILE)], ebuf.at[slot], e_sem.at[slot])

        def e_load_own(t):
            slot = lax.rem(t, 2)
            return pltpu.make_async_copy(emb.at[pl.ds(pl.multiple_of(t * TILE, TILE), TILE)], ebuf.at[slot], e_sem.at[slot])
        e_load_own(0).start()

        def x_event(j):
            x_copy(j).wait_recv()
            y_copy(j).start()
            d_copy(j, 0).start()

        def y_event(j):
            y_copy(j).wait_recv()
            d_copy(j, 1).start()

        def p_event(k):
            rows = e_all.at[pl.ds(pl.multiple_of(2 * ROWS + k * TILE + TILE // 2, TILE // 2), TILE // 2)]
            pltpu.make_async_copy(rows, rows, d_recv.at[k]).wait()
            e_load(NEAR + k).start()

        cp.wait()
        pltpu.make_async_copy(info_v, info_all.at[tp], small_sem.at[0]).start()
        gb8[0] = jnp.broadcast_to(gain[...], (8, DIM))
        gb8[1] = jnp.broadcast_to(bias[...], (8, DIM))

        def ln_tile(i, c):
            slot = lax.rem(i, 2)

            @pl.when(i + 1 < TOK // LN_ROWS)
            def _():
                h_copy(i + 1).start()
            h_copy(i).wait()

            @pl.when(i == 6)
            def _():
                x_event(0)

            def ln_rows(r, c2):
                base = r * LN_UNROLL * 16

                def at(u):
                    return pl.ds(pl.multiple_of(base + u * 16, 16), 16)

                def part_of(u, k):
                    return hbuf[slot, at(u), k * 128:(k + 1) * 128].astype(jnp.float32)
                means, rstds = [], []
                for u in range(LN_UNROLL):
                    tot = part_of(u, 0)
                    for k in range(1, DIM // 128):
                        tot = tot + part_of(u, k)
                    means.append(jnp.broadcast_to(jnp.sum(tot, axis=-1, keepdims=True) * (1.0 / DIM), (16, 128)))
                for u in range(LN_UNROLL):
                    tot = jnp.zeros((16, 128), jnp.float32)
                    for k in range(DIM // 128):
                        diff = part_of(u, k) - means[u]
                        tot = tot + diff * diff
                    var = jnp.sum(tot, axis=-1, keepdims=True) * (1.0 / DIM)
                    rstds.append(jnp.broadcast_to(lax.rsqrt(var + LN_EPS), (16, 128)))
                for u in range(LN_UNROLL):
                    row = pl.ds(pl.multiple_of(i * LN_ROWS + base + u * 16, 16), 16)
                    mr_v[0, row, :] = means[u]
                    mr_v[1, row, :] = rstds[u]
                    for k in range(DIM // 128):
                        cols = slice(k * 128, (k + 1) * 128)
                        g2 = jnp.concatenate([gb8[0, :, cols]] * 2, axis=0)
                        b2 = jnp.concatenate([gb8[1, :, cols]] * 2, axis=0)
                        xs[row, cols] = ((part_of(u, k) - means[u]) * rstds[u] * g2 + b2).astype(jnp.bfloat16)
                return c2
            lax.fori_loop(0, LN_ROWS // (16 * LN_UNROLL), ln_rows, 0)
            rows = pl.ds(pl.multiple_of(i * LN_ROWS, LN_ROWS), LN_ROWS)
            pltpu.make_async_copy(xs.at[rows], x_out.at[rows], xo_sem).start()
            return c
        lax.fori_loop(0, TOK // LN_ROWS, ln_tile, 0)

        m_s[...] = jnp.full((TOK, 128), LOWEST, jnp.float32)
        s_s[...] = jnp.zeros((TOK, 128), jnp.float32)
        t_s[...] = jnp.zeros((TOK, 128), jnp.float32)
        for r in range(GROUPS):
            spread(info_v[2, r:r + 1, :], slice(r * 128, (r + 1) * 128), tc_v)
        z1[...] = jnp.full((HB, TILE), LOWEST, jnp.float32)

        zs = (z0, z1)

        def product(t, h):
            for r in range(0, HB, 512):
                zs[h][r:r + 512, :] = lax.dot_general(
                    xs[h * HB + r:h * HB + r + 512, :], ebuf[lax.rem(t, 2)], NT, preferred_element_type=jnp.float32)

        def statistics(t, h):
            z = zs[h]
            lane = lax.broadcasted_iota(jnp.int32, (STAT_ROWS, 128), 1)
            for r in range(0, HB, STAT_ROWS):
                rows = slice(h * HB + r, h * HB + r + STAT_ROWS)
                zk = [z[r:r + STAT_ROWS, k * 128:(k + 1) * 128] for k in range(TILE // 128)]
                old = m_s[rows, :]
                new = jnp.maximum(jnp.maximum(zk[0], zk[1]), old)
                tot = s_s[rows, :] * jnp.exp(old - new)
                tgt = t_s[rows, :]
                diff = tc_v[rows, :] - t * TILE
                for k in range(TILE // 128):
                    tot = tot + jnp.exp(zk[k] - new)
                    tgt = tgt + jnp.where(diff == lane + k * 128, zk[k], 0.0)
                m_s[rows, :] = new
                s_s[rows, :] = tot
                t_s[rows, :] = tgt

        def z_copy(t, h):
            return pltpu.make_async_copy(
                zs[h], z_out.at[pl.ds(h * HB, HB), pl.ds(pl.multiple_of(t * TILE, TILE), TILE)], z_sem.at[h])

        def start_events(t):
            @pl.when(t < TILES - 1)
            def _():
                x_event(t + 1)

            @pl.when(t == TILES - 2)
            def _():
                xt_copy(0).start()

            @pl.when(t == TILES - 1)
            def _():
                y_event(TILES - 1)
                p_event(TILES - 1 - NEAR)
            e_load(t).wait()

            @pl.when(t < ROWS // TILE)
            def _():
                slot = lax.rem(t, 2)
                pltpu.make_async_copy(ebuf.at[slot], e_all.at[pl.ds(pl.multiple_of(t * TILE, TILE), TILE)], eo_sem.at[slot]).start()

        def middle_events(t):
            @pl.when(t < TILES - 1)
            def _():
                y_event(t)

            @pl.when((t >= 1) & (t < ROWS // TILE + 1))
            def _():
                slot = lax.rem(t - 1, 2)
                pltpu.make_async_copy(ebuf.at[slot], e_all.at[pl.ds(0, TILE)], eo_sem.at[slot]).wait()

            @pl.when(t == NEAR)
            def _():
                pltpu.make_async_copy(xs, x_out, xo_sem).wait()

            @pl.when(t < ROWS // TILE - 1)
            def _():
                e_load_own(t + 1).start()

            @pl.when((t >= ROWS // TILE - 1) & (t < NEAR - 1))
            def _():
                @pl.when(lax.rem(t + 1, PE_ROWS // TILE) == 0)
                def _():
                    pe_copy((t + 1 - ROWS // TILE) // (PE_ROWS // TILE)).wait_recv()
                e_load(t + 1).start()

            @pl.when((t >= NEAR - 1) & (t < TILES - 2))
            def _():
                p_event(t - (NEAR - 1))

            @pl.when(t == TILES - 2)
            def _():
                for k, h in ((0, 0), (1, 0), (0, 1)):
                    z_load(zt, k, h).start()
                et_load(et, 0).start()

            @pl.when(t == NEAR + 1)
            def _():
                for p, dev in group:
                    remote(info, info_all.at[tp], sm_send, info_recv.at[p], dev).wait_recv()
                pltpu.make_async_copy(info_v, info_all.at[tp], small_sem.at[0]).wait()
                load = pltpu.make_async_copy(info_all, infos, small_sem.at[0])
                load.start()
                load.wait()
                count = jnp.broadcast_to(token_count(), (1, 128))
                for r in range(GROUPS):
                    spread(info_v[1, r:r + 1, :].astype(f32) / count, slice(r * 128, (r + 1) * 128), scale_v)

        def step(t, c):
            @pl.when(t > 0)
            def _():
                z_copy(t - 1, 1).start()
            start_events(t)

            @pl.when(t > 0)
            def _():
                z_copy(t - 1, 0).wait()
            statistics(t - 1, 1)
            product(t, 0)
            z_copy(t, 0).start()
            middle_events(t)

            @pl.when(t > 0)
            def _():
                z_copy(t - 1, 1).wait()
            statistics(t, 0)
            product(t, 1)
            return c
        last = TILES - 1
        lax.fori_loop(0, TILES, step, 0)
        z_copy(last, 1).start()
        statistics(last, 1)

        def finish(i, c):
            for u in range(4):
                r = i * 4 + u
                rows = pl.ds(pl.multiple_of(r * 128, 128), 128)
                m = m_s[rows, :]
                top = jnp.max(m, axis=-1, keepdims=True)
                tot = jnp.sum(s_s[rows, :] * jnp.exp(m - top), axis=-1, keepdims=True)
                lse = jnp.broadcast_to(top + jnp.log(tot), (128, 128))
                tgt = jnp.broadcast_to(jnp.sum(t_s[rows, :], axis=-1, keepdims=True), (128, 128))
                m_s[rows, :] = lse
                stat_v[0, pl.ds(r, 1), :] = jnp.transpose(lse)[0:1, :]
                stat_v[1, pl.ds(r, 1), :] = jnp.transpose(tgt)[0:1, :]
            return c
        lax.fori_loop(0, TOK // 512, finish, 0)
        for h in range(2):
            z_copy(last, h).wait()
        half = e_all.at[pl.ds(0, ROWS // 2)]
        pltpu.make_async_copy(half, half, xs_send).wait()
        pltpu.make_async_copy(half, half, ys_send).wait()
        full = e_all.at[pl.ds(0, ROWS)]
        pltpu.make_async_copy(full, full, ds_send).wait()
        pltpu.make_async_copy(full, full, pe_send).wait()
        pltpu.make_async_copy(stat_v, stat_all.at[tp], small_sem.at[1]).start()
        for p, dev in group:
            remote(stat_v, stat_all.at[tp], sm_send, stat_recv.at[p], dev).start()

        def start_xt(j, c):
            xt_copy(j).start()
            return c
        lax.fori_loop(1, XCHS, start_xt, 0)
        xp_copy.start()

    def z_load(zt, k, h):
        slot = lax.rem(k, 2)
        rows = slice(h * HB, (h + 1) * HB)
        return pltpu.make_async_copy(
            z_out.at[rows, pl.ds(pl.multiple_of(k * KT, KT), KT)], zt.at[slot, rows], zt_sem.at[2 * h + slot])

    def et_load(et, k):
        slot = lax.rem(k, 2)
        return pltpu.make_async_copy(e_all.at[pl.ds(pl.multiple_of(k * KT, KT), KT)], et.at[slot], et_sem.at[slot])

    def dzt_copy(k):
        rows = pl.ds(pl.multiple_of(lax.rem(k, 4) * KT, KT), KT)
        return remote(dzt_out.at[rows], dzt_part.at[rows], dz_send, dz_recv.at[lax.rem(k, 4)], part)

    def token_count():
        return jnp.sum(infos[:, 1].astype(f32))

    def token_grads(lse_v, scale_v, tcol_v, mr, zt, et, acc):
        def d_phase(da, db, dzt):
            def dzt_store(k, ref):
                slot = lax.rem(k, 2)
                return pltpu.make_async_copy(dzt.at[slot], ref.at[pl.ds(pl.multiple_of(lax.rem(k, 4) * KT, KT), KT)], eo_sem.at[slot])
            lane = lax.broadcasted_iota(jnp.int32, (PIECE, 128), 1)

            def piece(dst, rows, low, k, tie):
                slot = lax.rem(k, 2)
                lse = lse_v[rows, :]
                if tie is not None:
                    floor = 0.0 - jnp.maximum(0.0 - tie, -LOWEST)
                    lse = jnp.maximum(lse, jnp.concatenate([floor] * (PIECE // 8), axis=0))
                scale = scale_v[rows, :]
                diff = tcol_v[rows, :] - k * KT
                for g in range(KT // 128):
                    cols = slice(g * 128, (g + 1) * 128)
                    hot = (diff == lane + g * 128).astype(f32)
                    val = (jnp.exp(zt[slot, rows, cols] - lse) - hot) * scale
                    dst[low, cols] = val.astype(bf16)

            def half_step(k, src, dst, base, dst_base, dst_k):
                slot = lax.rem(k, 2)
                per = HB // (DIM // NCOL)
                for n in range(DIM // NCOL):
                    cols = slice(n * NCOL, (n + 1) * NCOL)
                    prod = jnp.dot(src[...], et[slot, :, cols], preferred_element_type=f32)
                    acc[base:base + HB, cols] = jnp.where(k == 0, 0.0, acc[base:base + HB, cols]) + prod
                    for q in range(0, per, PIECE):
                        at = q * HB // per
                        low = n * per + q
                        piece(dst, slice(dst_base + low, dst_base + low + PIECE), slice(low, low + PIECE), dst_k, prod[at:at + 8, 0:128])
                    if n * per % 256 == 0:
                        low = n * per
                        dzt[slot, :, base + low:base + low + 256] = jnp.transpose(src[low:low + 256, :])

            z_load(zt, 0, 0).wait()

            def first(i, c):
                rows = pl.ds(pl.multiple_of(i * PIECE, PIECE), PIECE)
                piece(da, rows, rows, 0, None)
                return c
            lax.fori_loop(0, HB // PIECE, first, 0)

            def step(k, c):
                @pl.when(k + 2 < VOCAB // KT)
                def _():
                    z_load(zt, k + 2, 0).start()

                @pl.when(k + 1 < VOCAB // KT)
                def _():
                    z_load(zt, k + 1, 1).start()
                    et_load(et, k + 1).start()
                    z_load(zt, k + 1, 0).wait()
                for at, j in WAIT_STEP.items():
                    @pl.when(k == at)
                    def _(j=j):
                        xt_event(j)

                @pl.when((k >= 2) & (k < 10))
                def _():
                    dzt_store(k, dzt_own).wait()

                @pl.when((k >= 6) & (k < 10))
                def _():
                    dzt_copy(k - 2).start()
                et_load(et, k).wait()
                z_load(zt, k, 1).wait()
                half_step(k, da, db, 0, HB, k)
                half_step(k, db, da, HB, 0, k + 1)

                @pl.when(k < 4)
                def _():
                    dzt_store(k, dzt_own).start()

                @pl.when((k >= 4) & (k < 8))
                def _():
                    dzt_store(k, dzt_out).start()
                return c
            lax.fori_loop(0, VOCAB // KT, step, 0)
        half = pltpu.VMEM((HB, KT), bf16)
        pl.run_scoped(d_phase, half, half, pltpu.VMEM((2, KT, TOK), bf16))

        def n_phase(hb, ob):
            def h_load(i):
                slot = lax.rem(i, 2)
                return pltpu.make_async_copy(hid.at[pl.ds(pl.multiple_of(i * NB_ROWS, NB_ROWS), NB_ROWS)], hb.at[slot], z_sem.at[slot])

            def o_store(i):
                slot = lax.rem(i, 2)
                return pltpu.make_async_copy(ob.at[slot], dhid.at[pl.ds(pl.multiple_of(i * NB_ROWS, NB_ROWS), NB_ROWS)], e_sem.at[slot])
            h_load(0).start()
            gb_v[...] = jnp.zeros(gb_v.shape, jnp.float32)
            g8[...] = jnp.broadcast_to(gain[...], (8, DIM))

            def tile(i, c):
                slot = lax.rem(i, 2)

                @pl.when(i + 1 < TOK // NB_ROWS)
                def _():
                    h_load(i + 1).start()

                @pl.when(i >= 2)
                def _():
                    o_store(i - 2).wait()
                h_load(i).wait()

                def rows_body(r, c2):
                    units = range(NB_UNROLL)
                    base = r * 16 * NB_UNROLL
                    low = [pl.ds(pl.multiple_of(base + u * 16, 16), 16) for u in units]
                    row = [pl.ds(pl.multiple_of(i * NB_ROWS + base + u * 16, 16), 16) for u in units]
                    zero = jnp.zeros((16, 128), jnp.float32)
                    sum1, sum3 = [zero] * NB_UNROLL, [zero] * NB_UNROLL

                    def load(u, cols):
                        dx = acc[row[u], cols]
                        xhat = (hb[slot, low[u], cols].astype(jnp.float32) - mr[0, row[u], :]) * mr[1, row[u], :]
                        return dx, xhat, dx * jnp.concatenate([g8[:, cols]] * 2, axis=0)
                    for k in range(DIM // 128):
                        cols = slice(k * 128, (k + 1) * 128)
                        d_gain, d_bias = gb_v[0, :, cols], gb_v[1, :, cols]
                        for u in units:
                            dx, xhat, gx = load(u, cols)
                            sum1[u] = sum1[u] + gx
                            sum3[u] = sum3[u] + gx * xhat
                            dgx = dx * xhat
                            d_gain = d_gain + (dgx[0:8] + dgx[8:16])
                            d_bias = d_bias + (dx[0:8] + dx[8:16])
                        gb_v[0, :, cols] = d_gain
                        gb_v[1, :, cols] = d_bias
                    slope, shift = [], []
                    for u in units:
                        mean, rstd = mr[0, row[u], :], mr[1, row[u], :]
                        c1 = jnp.broadcast_to(jnp.sum(sum1[u], axis=-1, keepdims=True) * (1.0 / DIM), (16, 128))
                        c3 = jnp.broadcast_to(jnp.sum(sum3[u], axis=-1, keepdims=True) * (1.0 / DIM), (16, 128))
                        slope.append(c3 * rstd * rstd)
                        shift.append(slope[u] * mean - c1 * rstd)
                    for u in units:
                        rstd = mr[1, row[u], :]
                        for k in range(DIM // 128):
                            cols = slice(k * 128, (k + 1) * 128)
                            gx = acc[row[u], cols] * jnp.concatenate([g8[:, cols]] * 2, axis=0)
                            ob[slot, low[u], cols] = (gx * rstd - hb[slot, low[u], cols].astype(f32) * slope[u] + shift[u]).astype(bf16)
                    return c2
                lax.fori_loop(0, NB_ROWS // (16 * NB_UNROLL), rows_body, 0)
                o_store(i).start()
                return c
            lax.fori_loop(0, TOK // NB_ROWS, tile, 0)
            for i in range(2):
                o_store(TOK // NB_ROWS - 2 + i).wait()
            gs_v[0:1, :] = jnp.sum(gb_v[0], axis=0, keepdims=True)
            gs_v[1:2, :] = jnp.sum(gb_v[1], axis=0, keepdims=True)
        pl.run_scoped(n_phase, pltpu.VMEM((2, NB_ROWS, DIM), bf16), pltpu.VMEM((2, NB_ROWS, DIM), bf16))

    def weight_grads(acc):
        own = pltpu.make_async_copy(gs_v, gsum_all.at[tp], g_sem)
        xt_event(3)

        def e_phase(eo, xt, dzb, zs):
            eo_load = pltpu.make_async_copy(emb, eo, big_sem)

            def x_load(ref, row, slot):
                return pltpu.make_async_copy(ref.at[pl.ds(pl.multiple_of(row, KT), KT)], xt.at[slot], z_sem.at[slot])

            def dz_load(ref, col, slot):
                return pltpu.make_async_copy(ref.at[:, pl.ds(pl.multiple_of(col, KT), KT)], dzb.at[slot], e_sem.at[slot])

            def start_local(i):
                slot = lax.rem(i, 2)

                @pl.when(i < 4)
                def _():
                    x_load(x_out, i * KT, slot).start()
                    dz_load(dzt_own, i * KT, slot).start()

                @pl.when(i >= 4)
                def _():
                    x_load(x_part, (i - 4) * KT, slot).start()
                    dz_load(dzt_part, (i - 4) * KT, slot).start()

            def add(slot, first):
                def mul(h, c2):
                    rows = pl.ds(pl.multiple_of(h * HB, HB), HB)
                    for n in range(0, DIM, NCOL):
                        prod = jnp.dot(dzb[slot, rows, :], xt[slot, :, n:n + NCOL], preferred_element_type=f32)
                        acc[rows, n:n + NCOL] = jnp.where(first, 0.0, acc[rows, n:n + NCOL]) + prod
                    return c2
                lax.fori_loop(0, HBS, mul, 0)

            start_local(0)

            def rem_load(r):
                slot = lax.rem(r, 2)
                return [pltpu.make_async_copy(xrows(ref, r), xt.at[slot, pl.ds(i * XCH, XCH)], z_sem.at[slot])
                        for i, ref in enumerate((x_xp, x_xq))]

            def local(i, c):
                slot = lax.rem(i, 2)

                @pl.when(i == 0)
                def _():
                    eo_load.start()

                @pl.when(i == 2)
                def _():
                    xp_copy.wait_recv()

                    def wait_dz(q, c2):
                        dzt_copy(q).wait_recv()
                        return c2
                    lax.fori_loop(0, 4, wait_dz, 0)

                @pl.when(i == 1)
                def _():
                    own.start()
                    for p, dev in group:
                        remote(gs_v, gsum_all.at[tp], g_send, g_recv.at[p], dev).start()

                @pl.when(i == 6)
                def _():
                    xt_event(4)

                @pl.when(i < 7)
                def _():
                    start_local(i + 1)

                @pl.when(i == 7)
                def _():
                    xd_copy(0).wait_recv()
                    for cp in rem_load(0):
                        cp.start()
                x_load(x_out, 0, slot).wait()
                dz_load(dzt_own, 0, slot).wait()
                add(slot, i == 0)
                return c
            lax.fori_loop(0, 8, local, 0)
            eo_load.wait()
            for p, dev in group:
                remote(stat_v, stat_all.at[tp], sm_send, stat_recv.at[p], dev).wait_recv()
            pltpu.make_async_copy(stat_v, stat_all.at[tp], small_sem.at[1]).wait()
            stat_load = pltpu.make_async_copy(stat_all, stats, small_sem.at[1])
            stat_load.start()
            stat_load.wait()
            count = jnp.broadcast_to(token_count(), (1, 128))

            def far(r, c):
                slot = lax.rem(r, 2)

                @pl.when(r == 1)
                def _():
                    xt_event(5)

                @pl.when(r == 4)
                def _():
                    xt_event(6)

                def fetch():
                    xd_copy(r + 1).wait_recv()
                    for cp in rem_load(r + 1):
                        cp.start()
                pl.when(r < XCHS - 2)(fetch)
                x_load(x_out, 0, slot).wait()

                @pl.when(r == XCHS - DEFER)
                def _():
                    pltpu.make_async_copy(acc, de_part, big_sem).start()

                @pl.when(r > XCHS - DEFER + 1)
                def _():
                    dz_out(0, 0, slot).wait()
                    dz_out(0, 1, slot).wait()

                far_rows = []
                for g in range(4):
                    who = xp_rank if g < 2 else xq_rank
                    at = pl.ds(2 * r + g % 2, 1)
                    far_rows.append((stats[who, 0, at, :], infos[who, 1, at, :].astype(f32) / count, infos[who, 0, at, :] - tp * ROWS))

                def logits(h, c2):
                    for k in range(0, DIM, KCOL):
                        prod = lax.dot_general(eo[pl.ds(pl.multiple_of(h * ZB, ZB), ZB), k:k + KCOL], xt[slot, :, k:k + KCOL], NT, preferred_element_type=jnp.float32)
                        zs[...] = prod if k == 0 else zs[...] + prod
                    for q in range(ZB // 32):
                        row = h * ZB + q * 32
                        line = lax.broadcasted_iota(jnp.int32, (32, 128), 0)
                        for g, (lse, scale, trel) in enumerate(far_rows):
                            cols = slice(g * 128, (g + 1) * 128)
                            hot = ((trel - row) == line).astype(f32)
                            val = (jnp.exp(zs[q * 32:(q + 1) * 32, cols] - lse) - hot) * scale
                            dzb[slot, pl.ds(pl.multiple_of(row, 32), 32), cols] = val.astype(bf16)
                    return c2
                lax.fori_loop(0, ROWS // ZB, logits, 0)

                @pl.when(r == XCHS - 2)
                def _():
                    xt_event(XCHS - 1)
                    fetch()

                @pl.when(r < XCHS - DEFER)
                def _():
                    def mul(h, c2):
                        rows = pl.ds(pl.multiple_of(h * HB, HB), HB)
                        for n in range(0, DIM, NCOL):
                            acc[rows, n:n + NCOL] += jnp.dot(dzb[slot, rows, :], xt[slot, :, n:n + NCOL], preferred_element_type=jnp.float32)
                        return c2
                    lax.fori_loop(0, HBS, mul, 0)

                @pl.when(r >= XCHS - DEFER)
                def _():
                    for i in range(2):
                        dz_out(r - (XCHS - DEFER), i, slot).start()
                return c

            def dz_out(q, i, slot):
                return pltpu.make_async_copy(
                    dzb.at[slot, :, pl.ds(i * XCH, XCH)], dzt_last.at[i, :, pl.ds(pl.multiple_of(q * XCH, XCH), XCH)], dzo_sem.at[slot])
            lax.fori_loop(0, XCHS, far, 0)
            for slot in range(2):
                dz_out(0, 0, slot).wait()
                dz_out(0, 1, slot).wait()
            pltpu.make_async_copy(acc, de_part, big_sem).wait()
        pl.run_scoped(e_phase, pltpu.VMEM((ROWS, DIM), jnp.bfloat16), pltpu.VMEM((2, KT, DIM), jnp.bfloat16),
                      pltpu.VMEM((2, ROWS, KT), jnp.bfloat16), pltpu.VMEM((ZB, KT), jnp.float32))

        own.wait()

    wide = pltpu.VMEM((TOK, 128), f32)
    big = pltpu.VMEM((TOK, DIM), f32)

    def tokens(m_s, scale_v, tc_v, mr_v, zt, et):
        kept = (m_s, scale_v, tc_v, mr_v, zt, et)
        pl.run_scoped(functools.partial(forward, *kept), pltpu.VMEM((TOK, DIM), bf16), pltpu.VMEM((2, LN_ROWS, DIM), bf16),
                      pltpu.VMEM((2, TILE, DIM), bf16), pltpu.VMEM((HB, TILE), f32), pltpu.VMEM((HB, TILE), f32), wide, wide,
                      pltpu.VMEM((2, 8, DIM), f32))
        pl.run_scoped(functools.partial(token_grads, *kept), big)
    pl.run_scoped(tokens, wide, wide, pltpu.VMEM((TOK, 128), jnp.int32), pltpu.VMEM((2, TOK, 128), f32),
                  pltpu.VMEM((2, TOK, KT), f32), pltpu.VMEM((2, KT, DIM), bf16))
    pl.run_scoped(weight_grads, big)

    pltpu.make_async_copy(x_out, x_out, xt_send).wait()
    pltpu.make_async_copy(x_out, x_out, xd_send).wait()
    xp_copy.wait_send()
    pltpu.make_async_copy(dzt_out, dzt_out, dz_send).wait()
    for p, dev in group:
        remote(info, info_all.at[tp], sm_send, info_recv.at[p], dev).wait_send()
        remote(stat_v, stat_all.at[tp], sm_send, stat_recv.at[p], dev).wait_send()
        remote(gs_v, gsum_all.at[tp], g_send, g_recv.at[p], dev).wait()


def run_step(hidden, gain, bias, embed, info):
    any_spec = pl.BlockSpec(memory_space=pl.ANY)
    vmem_spec = pl.BlockSpec(memory_space=pltpu.VMEM)
    f32, bf16, i32 = jnp.float32, jnp.bfloat16, jnp.int32
    dma = pltpu.SemaphoreType.DMA
    small, ints = (4, 2, GROUPS, 128), (4, 3, GROUPS, 128)
    mat, square = ((TOK, DIM), bf16), ((ROWS, TOK), bf16)
    shapes = [((VOCAB, DIM), bf16), mat, ((TOK, VOCAB), f32), (small, f32), (ints, i32),
              mat, mat, mat, mat, square, square, square, ((2, ROWS, DEFER * XCH), bf16), ((ROWS, DIM), f32), ((4, 2, DIM), f32)]
    return pl.pallas_call(
        step_kernel,
        name="step",
        out_shape=[jax.ShapeDtypeStruct(s, d) for s, d in shapes],
        in_specs=[any_spec, vmem_spec, vmem_spec, any_spec, any_spec],
        out_specs=[any_spec] * len(shapes),
        scratch_shapes=[
            pltpu.VMEM((3, GROUPS, 128), i32), pltpu.VMEM((2, GROUPS, 128), f32), pltpu.VMEM(small, f32), pltpu.VMEM(ints, i32),
            pltpu.VMEM((2, 8, DIM), f32), pltpu.VMEM((2, DIM), f32), pltpu.VMEM((8, DIM), f32),
            dma((2,)), dma, dma((2,)), dma((2,)), dma((2,)), dma((4,)), dma((2,)), dma((2,)), dma((2,)), dma, dma,
            dma, dma, dma, dma, dma, dma, dma, dma, dma, dma,
            dma((CHUNKS,)), dma((CHUNKS,)), dma((TILES - NEAR,)), dma((ROWS // PE_ROWS,)), dma((4,)), dma((4,)),
            dma((XCHS,)), dma((XCHS,)), dma, dma((4,)), dma((4,)),
        ],
        compiler_params=pltpu.CompilerParams(collective_id=0, has_side_effects=True, vmem_limit_bytes=67043328),
        cost_estimate=pl.CostEstimate(flops=12 * TOK * VOCAB * DIM, bytes_accessed=700 * 2 ** 20, transcendentals=3 * TOK * VOCAB),
    )(hidden, gain, bias, embed, info)


def finish_kernel(*refs):
    nb = DEFER * XCH // KT
    de_in, dz0, dz1 = refs[:3]
    xs = refs[3:3 + 2 * nb]
    dh_in, stat_all, info_all, gsum_all, de_out, dh_out, loss, mean, d_gain, d_bias = refs[3 + 2 * nb:]
    for h in range(HBS):
        rows = slice(h * HB, (h + 1) * HB)
        prod = None
        for b in range(nb):
            for dz, x in ((dz0, xs[b]), (dz1, xs[nb + b])):
                part = jnp.dot(dz[0, rows, b * KT:(b + 1) * KT], x[...], preferred_element_type=jnp.float32)
                prod = part if prod is None else prod + part
        de_out[rows, :] = de_in[rows, :] + prod
    dh_out[...] = dh_in[...]

    @pl.when(pl.program_id(0) == 0)
    def _():
        weights = info_all[:, 1].astype(jnp.float32)
        all_loss = (stat_all[:, 0] - stat_all[:, 1]) * weights
        tp = lax.axis_index('tp')
        loss[...] = (stat_all[tp, 0] - stat_all[tp, 1]) * info_all[tp, 1].astype(jnp.float32)
        mean[...] = jnp.broadcast_to(jnp.sum(all_loss), (1, 1)) / jnp.broadcast_to(jnp.sum(weights), (1, 1))
        sums = ((gsum_all[0] + gsum_all[1]) + gsum_all[2]) + gsum_all[3]
        d_gain[...] = sums[0:1]
        d_bias[...] = sums[1:2]


def finish(de_part, dzt_last, x_xp, x_xq, dhid, stat_all, info_all, gsum_all):
    cols = 512
    steps = DIM // cols
    depth = DEFER * XCH
    rows = TOK // steps
    first = (TOK - depth) // KT
    once = pl.Buffered(1)
    x_specs = [pl.BlockSpec((KT, cols), lambda i, b=b: (b, i)) for b in range(first, TOK // KT)]

    def whole(shape):
        return pl.BlockSpec(shape, lambda i: (0,) * len(shape))
    nb = len(x_specs)
    outs = [((ROWS, DIM), jnp.float32), ((TOK, DIM), jnp.bfloat16), ((GROUPS, 128), jnp.float32), ((1, 1), jnp.float32), ((1, DIM), jnp.float32), ((1, DIM), jnp.float32)]
    return pl.pallas_call(
        finish_kernel,
        name="finish",
        grid=(steps,),
        out_shape=[jax.ShapeDtypeStruct(s, d) for s, d in outs],
        in_specs=[
            pl.BlockSpec((ROWS, cols), lambda i: (0, i)),
            pl.BlockSpec((1, ROWS, depth), lambda i: (0, 0, 0), pipeline_mode=once),
            pl.BlockSpec((1, ROWS, depth), lambda i: (1, 0, 0), pipeline_mode=once),
            *x_specs, *x_specs,
            pl.BlockSpec((rows, DIM), lambda i: (i, 0)),
            whole(stat_all.shape), whole(info_all.shape), whole(gsum_all.shape),
        ],
        out_specs=[pl.BlockSpec((ROWS, cols), lambda i: (0, i)), pl.BlockSpec((rows, DIM), lambda i: (i, 0)),
                   whole((GROUPS, 128)), whole((1, 1)), whole((1, DIM)), whole((1, DIM))],
        compiler_params=pltpu.CompilerParams(vmem_limit_bytes=60 * 1024 * 1024),
        cost_estimate=pl.CostEstimate(flops=4 * ROWS * DIM * depth, bytes_accessed=120 * 2 ** 20, transcendentals=0),
    )(de_part, dzt_last, dzt_last, *[x_xp] * nb, *[x_xq] * nb, dhid, stat_all, info_all, gsum_all)


def solution(mesh):
    def body(hidden, ln_gain, ln_bias, embed, targets, loss_mask):
        dp, rank = lax.axis_index('dp'), lax.axis_index('tp')
        shard = targets // ROWS
        block = jnp.bitwise_xor(shard, rank)
        row = targets % ROWS
        half = row // (ROWS // 2)
        sub = row % (ROWS // 2)
        piece = (block - 2) * 2 + jnp.bitwise_xor(half, dp)
        far = 2 * ROWS + (sub // PIECE_ROWS) * TILE + piece * PIECE_ROWS + sub % PIECE_ROWS
        tcol = jnp.where(block < 2, block * ROWS + row, far)
        info = jnp.stack([targets, loss_mask, tcol]).reshape(3, GROUPS, 128)
        outs = run_step(hidden, ln_gain.reshape(1, DIM), ln_bias.reshape(1, DIM), embed, info)
        stat_all, info_all, dhid, x_xp, x_xq, dzt_last, de_part, gsum_all = (outs[i] for i in (3, 4, 5, 7, 8, 12, 13, 14))
        d_embed, d_hidden, loss, mean, d_gain, d_bias = finish(de_part, dzt_last, x_xp, x_xq, dhid, stat_all, info_all, gsum_all)
        return loss.reshape(TOK), mean.reshape(1), d_hidden, d_embed, d_gain.reshape(DIM), d_bias.reshape(DIM)

    token_rows = P(('dp', 'tp'))
    token_mat = P(('dp', 'tp'), None)
    return jax.shard_map(body, mesh=mesh, in_specs=(token_mat, P(), P(), P('tp', None), token_rows, token_rows), out_specs=(token_rows, P('dp'), token_mat, token_mat, P('dp'), P('dp')), check_vma=False)
```

```python
import functools

import jax
import jax.numpy as jnp
from jax import lax
from jax.experimental import pallas as pl
from jax.experimental.pallas import tpu as pltpu
from jax.sharding import PartitionSpec as P

LN_EPS = 1e-5
LOWEST = float(jnp.finfo(jnp.float32).min)

TOK = 2048
ROWS = 2048
DIM = 4096
VOCAB = 8192
TILE = 256
TILES = VOCAB // TILE
HB = 1024
HBS = TOK // HB
CHUNK = 32
PIECE_ROWS = 2 * CHUNK
NEAR = 2 * ROWS // TILE
PE_ROWS = 512
CHUNKS = ROWS // 2 // CHUNK
LN_ROWS = 256
STAT_ROWS = 32
PIECE = 32
LN_UNROLL = 4
XCH = 256
XCHS = TOK // XCH
KT = 512
DEFER = 4
WAIT_STEP = {4: 0, 9: 1, 14: 2}
ZB = 512
NCOL = 512
KCOL = 1024
NB_UNROLL = 4
NB_ROWS = 256
GROUPS = TOK // 128
NT = (((1,), (1,)), ((), ()))


def peers():
    dp, tp = lax.axis_index('dp'), lax.axis_index('tp')
    core = lax.rem(tp, 2)
    pair = tp - core
    other = 2 - pair
    part = pair + 1 - core
    return dp, tp, (dp, part), (dp, other + core), (dp, other + 1 - core), (1 - dp, tp)


def remote(src, dst, ssem, rsem, dev):
    return pltpu.make_async_remote_copy(
        src_ref=src, dst_ref=dst, send_sem=ssem, recv_sem=rsem, device_id=dev, device_id_type=pl.DeviceIdType.MESH)


def spread(row, rows, dst):
    dst[rows, :] = jnp.transpose(jnp.broadcast_to(row, (128, 128)))


def step_kernel(hid, gain, bias, emb, info,
                e_all, x_out, z_out, stat_all, info_all,
                dhid, x_part, x_xp, x_xq, dzt_own, dzt_out, dzt_part, dzt_last, de_part, gsum_all,
                info_v, stat_v, stats, infos, gb_v, gs_v, g8,
                h_sem, xo_sem, e_sem, eo_sem, z_sem, zt_sem, et_sem, small_sem, dzo_sem, big_sem, g_sem,
                xs_send, ys_send, ds_send, pe_send, sm_send, xt_send, xd_send, xp_send, dz_send, g_send,
                x_recv, y_recv, d_recv, pe_recv, info_recv, stat_recv, xt_recv, xd_recv, xp_recv, dz_recv, g_recv):
    bf16, f32 = jnp.bfloat16, jnp.float32
    dp, tp, part, xp, xq, yp = peers()
    core = lax.rem(tp, 2)
    xp_rank = 2 - (tp - core) + core
    xq_rank = 2 - (tp - core) + 1 - core
    group = ((1, part), (2, xp), (3, xq))
    barrier = pltpu.get_barrier_semaphore()
    for dev in (part, xp, xq, yp):
        pl.semaphore_signal(barrier, inc=1, device_id=dev, device_id_type=pl.DeviceIdType.MESH)
    pl.semaphore_wait(barrier, 4)

    def xrows(ref, j):
        return ref.at[pl.ds(pl.multiple_of(j * XCH, XCH), XCH)]

    def xt_copy(j):
        return remote(xrows(x_out, j), xrows(x_xp, j), xt_send, xt_recv.at[j], xp)

    def xd_copy(j):
        return remote(xrows(x_xp, j), xrows(x_xq, j), xd_send, xd_recv.at[j], part)

    def xt_event(j):
        xt_copy(j).wait_recv()
        xd_copy(j).start()
    xp_copy = remote(x_out, x_part, xp_send, xp_recv, part)

    def forward(m_s, scale_v, tc_v, mr_v, zt, et, xs, hbuf, ebuf, z0, z1, s_s, t_s, gb8):
        def tile_row(j):
            return ROWS * 2 + (j // 2) * TILE + lax.rem(j, 2) * CHUNK

        def x_copy(j):
            src = emb.at[pl.ds(pl.multiple_of(dp * (ROWS // 2) + j * CHUNK, CHUNK), CHUNK)]
            return remote(src, e_all.at[pl.ds(pl.multiple_of(tile_row(j), CHUNK), CHUNK)], xs_send, x_recv.at[j], xp)

        def piece(j, p):
            return e_all.at[pl.ds(pl.multiple_of(tile_row(j) + p * PIECE_ROWS, CHUNK), CHUNK)]

        def y_copy(j):
            return remote(piece(j, 0), piece(j, 1), ys_send, y_recv.at[j], yp)

        def d_copy(j, p):
            return remote(piece(j, p), piece(j, p + 2), ds_send, d_recv.at[j // 2], part)

        def pe_copy(i):
            return remote(emb.at[pl.ds(pl.multiple_of(i * PE_ROWS, PE_ROWS), PE_ROWS)],
                          e_all.at[pl.ds(pl.multiple_of(ROWS + i * PE_ROWS, PE_ROWS), PE_ROWS)], pe_send, pe_recv.at[i], part)

        cp = pltpu.make_async_copy(info, info_v, small_sem.at[0])
        cp.start()

        def h_copy(i):
            return pltpu.make_async_copy(hid.at[pl.ds(pl.multiple_of(i * LN_ROWS, LN_ROWS), LN_ROWS)], hbuf.at[lax.rem(i, 2)], h_sem.at[lax.rem(i, 2)])
        h_copy(0).start()

        for p, dev in group:
            remote(info, info_all.at[tp], sm_send, info_recv.at[p], dev).start()

        def start_x(j, c):
            x_copy(j).start()
            return c
        lax.fori_loop(0, CHUNKS, start_x, 0)

        def start_pe(i, c):
            pe_copy(i).start()
            return c
        lax.fori_loop(0, ROWS // PE_ROWS, start_pe, 0)

        def e_load(t):
            slot = lax.rem(t, 2)
            return pltpu.make_async_copy(e_all.at[pl.ds(pl.multiple_of(t * TILE, TILE), TILE)], ebuf.at[slot], e_sem.at[slot])

        def e_load_own(t):
            slot = lax.rem(t, 2)
            return pltpu.make_async_copy(emb.at[pl.ds(pl.multiple_of(t * TILE, TILE), TILE)], ebuf.at[slot], e_sem.at[slot])
        e_load_own(0).start()

        def x_event(j):
            x_copy(j).wait_recv()
            y_copy(j).start()
            d_copy(j, 0).start()

        def y_event(j):
            y_copy(j).wait_recv()
            d_copy(j, 1).start()

        def p_event(k):
            rows = e_all.at[pl.ds(pl.multiple_of(2 * ROWS + k * TILE + TILE // 2, TILE // 2), TILE // 2)]
            pltpu.make_async_copy(rows, rows, d_recv.at[k]).wait()
            e_load(NEAR + k).start()

        cp.wait()
        pltpu.make_async_copy(info_v, info_all.at[tp], small_sem.at[0]).start()
        gb8[0] = jnp.broadcast_to(gain[...], (8, DIM))
        gb8[1] = jnp.broadcast_to(bias[...], (8, DIM))

        def ln_tile(i, c):
            slot = lax.rem(i, 2)

            @pl.when(i + 1 < TOK // LN_ROWS)
            def _():
                h_copy(i + 1).start()
            h_copy(i).wait()

            @pl.when(i == 6)
            def _():
                x_event(0)

            def ln_rows(r, c2):
                base = r * LN_UNROLL * 16

                def at(u):
                    return pl.ds(pl.multiple_of(base + u * 16, 16), 16)

                def part_of(u, k):
                    return hbuf[slot, at(u), k * 128:(k + 1) * 128].astype(jnp.float32)
                means, rstds = [], []
                for u in range(LN_UNROLL):
                    tot = part_of(u, 0)
                    for k in range(1, DIM // 128):
                        tot = tot + part_of(u, k)
                    means.append(jnp.broadcast_to(jnp.sum(tot, axis=-1, keepdims=True) * (1.0 / DIM), (16, 128)))
                for u in range(LN_UNROLL):
                    tot = jnp.zeros((16, 128), jnp.float32)
                    for k in range(DIM // 128):
                        diff = part_of(u, k) - means[u]
                        tot = tot + diff * diff
                    var = jnp.sum(tot, axis=-1, keepdims=True) * (1.0 / DIM)
                    rstds.append(jnp.broadcast_to(lax.rsqrt(var + LN_EPS), (16, 128)))
                for u in range(LN_UNROLL):
                    row = pl.ds(pl.multiple_of(i * LN_ROWS + base + u * 16, 16), 16)
                    mr_v[0, row, :] = means[u]
                    mr_v[1, row, :] = rstds[u]
                    for k in range(DIM // 128):
                        cols = slice(k * 128, (k + 1) * 128)
                        g2 = jnp.concatenate([gb8[0, :, cols]] * 2, axis=0)
                        b2 = jnp.concatenate([gb8[1, :, cols]] * 2, axis=0)
                        xs[row, cols] = ((part_of(u, k) - means[u]) * rstds[u] * g2 + b2).astype(jnp.bfloat16)
                return c2
            lax.fori_loop(0, LN_ROWS // (16 * LN_UNROLL), ln_rows, 0)
            rows = pl.ds(pl.multiple_of(i * LN_ROWS, LN_ROWS), LN_ROWS)
            pltpu.make_async_copy(xs.at[rows], x_out.at[rows], xo_sem).start()
            return c
        lax.fori_loop(0, TOK // LN_ROWS, ln_tile, 0)

        m_s[...] = jnp.full((TOK, 128), LOWEST, jnp.float32)
        s_s[...] = jnp.zeros((TOK, 128), jnp.float32)
        t_s[...] = jnp.zeros((TOK, 128), jnp.float32)
        for r in range(GROUPS):
            spread(info_v[2, r:r + 1, :], slice(r * 128, (r + 1) * 128), tc_v)
        z1[...] = jnp.full((HB, TILE), LOWEST, jnp.float32)

        zs = (z0, z1)

        def product(t, h):
            for r in range(0, HB, 512):
                zs[h][r:r + 512, :] = lax.dot_general(
                    xs[h * HB + r:h * HB + r + 512, :], ebuf[lax.rem(t, 2)], NT, preferred_element_type=jnp.float32)

        def statistics(t, h):
            z = zs[h]
            lane = lax.broadcasted_iota(jnp.int32, (STAT_ROWS, 128), 1)
            for r in range(0, HB, STAT_ROWS):
                rows = slice(h * HB + r, h * HB + r + STAT_ROWS)
                zk = [z[r:r + STAT_ROWS, k * 128:(k + 1) * 128] for k in range(TILE // 128)]
                old = m_s[rows, :]
                new = jnp.maximum(jnp.maximum(zk[0], zk[1]), old)
                tot = s_s[rows, :] * jnp.exp(old - new)
                tgt = t_s[rows, :]
                diff = tc_v[rows, :] - t * TILE
                for k in range(TILE // 128):
                    tot = tot + jnp.exp(zk[k] - new)
                    tgt = tgt + jnp.where(diff == lane + k * 128, zk[k], 0.0)
                m_s[rows, :] = new
                s_s[rows, :] = tot
                t_s[rows, :] = tgt

        def z_copy(t, h):
            return pltpu.make_async_copy(
                zs[h], z_out.at[pl.ds(h * HB, HB), pl.ds(pl.multiple_of(t * TILE, TILE), TILE)], z_sem.at[h])

        def start_events(t):
            @pl.when(t < TILES - 1)
            def _():
                x_event(t + 1)

            @pl.when(t == TILES - 2)
            def _():
                xt_copy(0).start()

            @pl.when(t == TILES - 1)
            def _():
                y_event(TILES - 1)
                p_event(TILES - 1 - NEAR)
            e_load(t).wait()

            @pl.when(t < ROWS // TILE)
            def _():
                slot = lax.rem(t, 2)
                pltpu.make_async_copy(ebuf.at[slot], e_all.at[pl.ds(pl.multiple_of(t * TILE, TILE), TILE)], eo_sem.at[slot]).start()

        def middle_events(t):
            @pl.when(t < TILES - 1)
            def _():
                y_event(t)

            @pl.when((t >= 1) & (t < ROWS // TILE + 1))
            def _():
                slot = lax.rem(t - 1, 2)
                pltpu.make_async_copy(ebuf.at[slot], e_all.at[pl.ds(0, TILE)], eo_sem.at[slot]).wait()

            @pl.when(t == NEAR)
            def _():
                pltpu.make_async_copy(xs, x_out, xo_sem).wait()

            @pl.when(t < ROWS // TILE - 1)
            def _():
                e_load_own(t + 1).start()

            @pl.when((t >= ROWS // TILE - 1) & (t < NEAR - 1))
            def _():
                @pl.when(lax.rem(t + 1, PE_ROWS // TILE) == 0)
                def _():
                    pe_copy((t + 1 - ROWS // TILE) // (PE_ROWS // TILE)).wait_recv()
                e_load(t + 1).start()

            @pl.when((t >= NEAR - 1) & (t < TILES - 2))
            def _():
                p_event(t - (NEAR - 1))

            @pl.when(t == TILES - 2)
            def _():
                for k, h in ((0, 0), (1, 0), (0, 1)):
                    z_load(zt, k, h).start()
                et_load(et, 0).start()

            @pl.when(t == NEAR + 1)
            def _():
                for p, dev in group:
                    remote(info, info_all.at[tp], sm_send, info_recv.at[p], dev).wait_recv()
                pltpu.make_async_copy(info_v, info_all.at[tp], small_sem.at[0]).wait()
                load = pltpu.make_async_copy(info_all, infos, small_sem.at[0])
                load.start()
                load.wait()
                count = jnp.broadcast_to(token_count(), (1, 128))
                for r in range(GROUPS):
                    spread(info_v[1, r:r + 1, :].astype(f32) / count, slice(r * 128, (r + 1) * 128), scale_v)

        def step(t, c):
            @pl.when(t > 0)
            def _():
                z_copy(t - 1, 1).start()
            start_events(t)

            @pl.when(t > 0)
            def _():
                z_copy(t - 1, 0).wait()
            statistics(t - 1, 1)
            product(t, 0)
            z_copy(t, 0).start()
            middle_events(t)

            @pl.when(t > 0)
            def _():
                z_copy(t - 1, 1).wait()
            statistics(t, 0)
            product(t, 1)
            return c
        last = TILES - 1
        lax.fori_loop(0, TILES, step, 0)
        z_copy(last, 1).start()
        statistics(last, 1)

        def finish(i, c):
            for u in range(4):
                r = i * 4 + u
                rows = pl.ds(pl.multiple_of(r * 128, 128), 128)
                m = m_s[rows, :]
                top = jnp.max(m, axis=-1, keepdims=True)
                tot = jnp.sum(s_s[rows, :] * jnp.exp(m - top), axis=-1, keepdims=True)
                lse = jnp.broadcast_to(top + jnp.log(tot), (128, 128))
                tgt = jnp.broadcast_to(jnp.sum(t_s[rows, :], axis=-1, keepdims=True), (128, 128))
                m_s[rows, :] = lse
                stat_v[0, pl.ds(r, 1), :] = jnp.transpose(lse)[0:1, :]
                stat_v[1, pl.ds(r, 1), :] = jnp.transpose(tgt)[0:1, :]
            return c
        lax.fori_loop(0, TOK // 512, finish, 0)
        for h in range(2):
            z_copy(last, h).wait()
        half = e_all.at[pl.ds(0, ROWS // 2)]
        pltpu.make_async_copy(half, half, xs_send).wait()
        pltpu.make_async_copy(half, half, ys_send).wait()
        full = e_all.at[pl.ds(0, ROWS)]
        pltpu.make_async_copy(full, full, ds_send).wait()
        pltpu.make_async_copy(full, full, pe_send).wait()
        pltpu.make_async_copy(stat_v, stat_all.at[tp], small_sem.at[1]).start()
        for p, dev in group:
            remote(stat_v, stat_all.at[tp], sm_send, stat_recv.at[p], dev).start()

        def start_xt(j, c):
            xt_copy(j).start()
            return c
        lax.fori_loop(1, XCHS, start_xt, 0)
        xp_copy.start()

    def z_load(zt, k, h):
        slot = lax.rem(k, 2)
        rows = slice(h * HB, (h + 1) * HB)
        return pltpu.make_async_copy(
            z_out.at[rows, pl.ds(pl.multiple_of(k * KT, KT), KT)], zt.at[slot, rows], zt_sem.at[2 * h + slot])

    def et_load(et, k):
        slot = lax.rem(k, 2)
        return pltpu.make_async_copy(e_all.at[pl.ds(pl.multiple_of(k * KT, KT), KT)], et.at[slot], et_sem.at[slot])

    def dzt_copy(k):
        rows = pl.ds(pl.multiple_of(lax.rem(k, 4) * KT, KT), KT)
        return remote(dzt_out.at[rows], dzt_part.at[rows], dz_send, dz_recv.at[lax.rem(k, 4)], part)

    def token_count():
        return jnp.sum(infos[:, 1].astype(f32))

    def token_grads(lse_v, scale_v, tcol_v, mr, zt, et, acc):
        def d_phase(da, db, dzt):
            def dzt_store(k, ref):
                slot = lax.rem(k, 2)
                return pltpu.make_async_copy(dzt.at[slot], ref.at[pl.ds(pl.multiple_of(lax.rem(k, 4) * KT, KT), KT)], eo_sem.at[slot])
            lane = lax.broadcasted_iota(jnp.int32, (PIECE, 128), 1)

            def piece(dst, rows, low, k, tie):
                slot = lax.rem(k, 2)
                lse = lse_v[rows, :]
                if tie is not None:
                    floor = 0.0 - jnp.maximum(0.0 - tie, -LOWEST)
                    lse = jnp.maximum(lse, jnp.concatenate([floor] * (PIECE // 8), axis=0))
                scale = scale_v[rows, :]
                diff = tcol_v[rows, :] - k * KT
                for g in range(KT // 128):
                    cols = slice(g * 128, (g + 1) * 128)
                    hot = (diff == lane + g * 128).astype(f32)
                    val = (jnp.exp(zt[slot, rows, cols] - lse) - hot) * scale
                    dst[low, cols] = val.astype(bf16)

            def half_step(k, src, dst, base, dst_base, dst_k):
                slot = lax.rem(k, 2)
                per = HB // (DIM // NCOL)
                for n in range(DIM // NCOL):
                    cols = slice(n * NCOL, (n + 1) * NCOL)
                    prod = jnp.dot(src[...], et[slot, :, cols], preferred_element_type=f32)
                    acc[base:base + HB, cols] = jnp.where(k == 0, 0.0, acc[base:base + HB, cols]) + prod
                    for q in range(0, per, PIECE):
                        at = q * HB // per
                        low = n * per + q
                        piece(dst, slice(dst_base + low, dst_base + low + PIECE), slice(low, low + PIECE), dst_k, prod[at:at + 8, 0:128])
                    if n * per % 256 == 0:
                        low = n * per
                        dzt[slot, :, base + low:base + low + 256] = jnp.transpose(src[low:low + 256, :])

            z_load(zt, 0, 0).wait()

            def first(i, c):
                rows = pl.ds(pl.multiple_of(i * PIECE, PIECE), PIECE)
                piece(da, rows, rows, 0, None)
                return c
            lax.fori_loop(0, HB // PIECE, first, 0)

            def step(k, c):
                @pl.when(k + 2 < VOCAB // KT)
                def _():
                    z_load(zt, k + 2, 0).start()

                @pl.when(k + 1 < VOCAB // KT)
                def _():
                    z_load(zt, k + 1, 1).start()
                    et_load(et, k + 1).start()
                    z_load(zt, k + 1, 0).wait()
                for at, j in WAIT_STEP.items():
                    @pl.when(k == at)
                    def _(j=j):
                        xt_event(j)

                @pl.when((k >= 2) & (k < 10))
                def _():
                    dzt_store(k, dzt_own).wait()

                @pl.when((k >= 6) & (k < 10))
                def _():
                    dzt_copy(k - 2).start()
                et_load(et, k).wait()
                z_load(zt, k, 1).wait()
                half_step(k, da, db, 0, HB, k)
                half_step(k, db, da, HB, 0, k + 1)

                @pl.when(k < 4)
                def _():
                    dzt_store(k, dzt_own).start()

                @pl.when((k >= 4) & (k < 8))
                def _():
                    dzt_store(k, dzt_out).start()
                return c
            lax.fori_loop(0, VOCAB // KT, step, 0)
        half = pltpu.VMEM((HB, KT), bf16)
        pl.run_scoped(d_phase, half, half, pltpu.VMEM((2, KT, TOK), bf16))

        def n_phase(hb, ob):
            def h_load(i):
                slot = lax.rem(i, 2)
                return pltpu.make_async_copy(hid.at[pl.ds(pl.multiple_of(i * NB_ROWS, NB_ROWS), NB_ROWS)], hb.at[slot], z_sem.at[slot])

            def o_store(i):
                slot = lax.rem(i, 2)
                return pltpu.make_async_copy(ob.at[slot], dhid.at[pl.ds(pl.multiple_of(i * NB_ROWS, NB_ROWS), NB_ROWS)], e_sem.at[slot])
            h_load(0).start()
            gb_v[...] = jnp.zeros(gb_v.shape, jnp.float32)
            g8[...] = jnp.broadcast_to(gain[...], (8, DIM))

            def tile(i, c):
                slot = lax.rem(i, 2)

                @pl.when(i + 1 < TOK // NB_ROWS)
                def _():
                    h_load(i + 1).start()

                @pl.when(i >= 2)
                def _():
                    o_store(i - 2).wait()
                h_load(i).wait()

                def rows_body(r, c2):
                    units = range(NB_UNROLL)
                    base = r * 16 * NB_UNROLL
                    low = [pl.ds(pl.multiple_of(base + u * 16, 16), 16) for u in units]
                    row = [pl.ds(pl.multiple_of(i * NB_ROWS + base + u * 16, 16), 16) for u in units]
                    zero = jnp.zeros((16, 128), jnp.float32)
                    sum1, sum3 = [zero] * NB_UNROLL, [zero] * NB_UNROLL

                    def load(u, cols):
                        dx = acc[row[u], cols]
                        xhat = (hb[slot, low[u], cols].astype(jnp.float32) - mr[0, row[u], :]) * mr[1, row[u], :]
                        return dx, xhat, dx * jnp.concatenate([g8[:, cols]] * 2, axis=0)
                    for k in range(DIM // 128):
                        cols = slice(k * 128, (k + 1) * 128)
                        d_gain, d_bias = gb_v[0, :, cols], gb_v[1, :, cols]
                        for u in units:
                            dx, xhat, gx = load(u, cols)
                            sum1[u] = sum1[u] + gx
                            sum3[u] = sum3[u] + gx * xhat
                            dgx = dx * xhat
                            d_gain = d_gain + (dgx[0:8] + dgx[8:16])
                            d_bias = d_bias + (dx[0:8] + dx[8:16])
                        gb_v[0, :, cols] = d_gain
                        gb_v[1, :, cols] = d_bias
                    slope, shift = [], []
                    for u in units:
                        mean, rstd = mr[0, row[u], :], mr[1, row[u], :]
                        c1 = jnp.broadcast_to(jnp.sum(sum1[u], axis=-1, keepdims=True) * (1.0 / DIM), (16, 128))
                        c3 = jnp.broadcast_to(jnp.sum(sum3[u], axis=-1, keepdims=True) * (1.0 / DIM), (16, 128))
                        slope.append(c3 * rstd * rstd)
                        shift.append(slope[u] * mean - c1 * rstd)
                    for u in units:
                        rstd = mr[1, row[u], :]
                        for k in range(DIM // 128):
                            cols = slice(k * 128, (k + 1) * 128)
                            gx = acc[row[u], cols] * jnp.concatenate([g8[:, cols]] * 2, axis=0)
                            ob[slot, low[u], cols] = (gx * rstd - hb[slot, low[u], cols].astype(f32) * slope[u] + shift[u]).astype(bf16)
                    return c2
                lax.fori_loop(0, NB_ROWS // (16 * NB_UNROLL), rows_body, 0)
                o_store(i).start()
                return c
            lax.fori_loop(0, TOK // NB_ROWS, tile, 0)
            for i in range(2):
                o_store(TOK // NB_ROWS - 2 + i).wait()
            gs_v[0:1, :] = jnp.sum(gb_v[0], axis=0, keepdims=True)
            gs_v[1:2, :] = jnp.sum(gb_v[1], axis=0, keepdims=True)
        pl.run_scoped(n_phase, pltpu.VMEM((2, NB_ROWS, DIM), bf16), pltpu.VMEM((2, NB_ROWS, DIM), bf16))

    def weight_grads(acc):
        own = pltpu.make_async_copy(gs_v, gsum_all.at[tp], g_sem)
        xt_event(3)

        def e_phase(eo, xt, dzb, zs):
            eo_load = pltpu.make_async_copy(emb, eo, big_sem)

            def x_load(ref, row, slot):
                return pltpu.make_async_copy(ref.at[pl.ds(pl.multiple_of(row, KT), KT)], xt.at[slot], z_sem.at[slot])

            def dz_load(ref, col, slot):
                return pltpu.make_async_copy(ref.at[:, pl.ds(pl.multiple_of(col, KT), KT)], dzb.at[slot], e_sem.at[slot])

            def start_local(i):
                slot = lax.rem(i, 2)

                @pl.when(i < 4)
                def _():
                    x_load(x_out, i * KT, slot).start()
                    dz_load(dzt_own, i * KT, slot).start()

                @pl.when(i >= 4)
                def _():
                    x_load(x_part, (i - 4) * KT, slot).start()
                    dz_load(dzt_part, (i - 4) * KT, slot).start()

            def add(slot, first):
                def mul(h, c2):
                    rows = pl.ds(pl.multiple_of(h * HB, HB), HB)
                    for n in range(0, DIM, NCOL):
                        prod = jnp.dot(dzb[slot, rows, :], xt[slot, :, n:n + NCOL], preferred_element_type=f32)
                        acc[rows, n:n + NCOL] = jnp.where(first, 0.0, acc[rows, n:n + NCOL]) + prod
                    return c2
                lax.fori_loop(0, HBS, mul, 0)

            start_local(0)

            def rem_load(r):
                slot = lax.rem(r, 2)
                return [pltpu.make_async_copy(xrows(ref, r), xt.at[slot, pl.ds(i * XCH, XCH)], z_sem.at[slot])
                        for i, ref in enumerate((x_xp, x_xq))]

            def local(i, c):
                slot = lax.rem(i, 2)

                @pl.when(i == 0)
                def _():
                    eo_load.start()

                @pl.when(i == 2)
                def _():
                    xp_copy.wait_recv()

                    def wait_dz(q, c2):
                        dzt_copy(q).wait_recv()
                        return c2
                    lax.fori_loop(0, 4, wait_dz, 0)

                @pl.when(i == 1)
                def _():
                    own.start()
                    for p, dev in group:
                        remote(gs_v, gsum_all.at[tp], g_send, g_recv.at[p], dev).start()

                @pl.when(i == 6)
                def _():
                    xt_event(4)

                @pl.when(i < 7)
                def _():
                    start_local(i + 1)

                @pl.when(i == 7)
                def _():
                    xd_copy(0).wait_recv()
                    for cp in rem_load(0):
                        cp.start()
                x_load(x_out, 0, slot).wait()
                dz_load(dzt_own, 0, slot).wait()
                add(slot, i == 0)
                return c
            lax.fori_loop(0, 8, local, 0)
            eo_load.wait()
            for p, dev in group:
                remote(stat_v, stat_all.at[tp], sm_send, stat_recv.at[p], dev).wait_recv()
            pltpu.make_async_copy(stat_v, stat_all.at[tp], small_sem.at[1]).wait()
            stat_load = pltpu.make_async_copy(stat_all, stats, small_sem.at[1])
            stat_load.start()
            stat_load.wait()
            count = jnp.broadcast_to(token_count(), (1, 128))

            def far(r, c):
                slot = lax.rem(r, 2)

                @pl.when(r == 1)
                def _():
                    xt_event(5)

                @pl.when(r == 4)
                def _():
                    xt_event(6)

                def fetch():
                    xd_copy(r + 1).wait_recv()
                    for cp in rem_load(r + 1):
                        cp.start()
                pl.when(r < XCHS - 2)(fetch)
                x_load(x_out, 0, slot).wait()

                @pl.when(r == XCHS - DEFER)
                def _():
                    pltpu.make_async_copy(acc, de_part, big_sem).start()

                @pl.when(r > XCHS - DEFER + 1)
                def _():
                    dz_out(0, slot).wait()

                far_rows = []
                for g in range(4):
                    who = xp_rank if g < 2 else xq_rank
                    at = pl.ds(2 * r + g % 2, 1)
                    far_rows.append((stats[who, 0, at, :], infos[who, 1, at, :].astype(f32) / count, infos[who, 0, at, :] - tp * ROWS))

                def logits(h, c2):
                    @pl.when((r == XCHS - 2) & (h == ROWS // ZB // 2))
                    def _():
                        xt_event(XCHS - 1)
                    for k in range(0, DIM, KCOL):
                        prod = lax.dot_general(eo[pl.ds(pl.multiple_of(h * ZB, ZB), ZB), k:k + KCOL], xt[slot, :, k:k + KCOL], NT, preferred_element_type=jnp.float32)
                        zs[...] = prod if k == 0 else zs[...] + prod
                    for q in range(ZB // 32):
                        row = h * ZB + q * 32
                        line = lax.broadcasted_iota(jnp.int32, (32, 128), 0)
                        for g, (lse, scale, trel) in enumerate(far_rows):
                            cols = slice(g * 128, (g + 1) * 128)
                            hot = ((trel - row) == line).astype(f32)
                            val = (jnp.exp(zs[q * 32:(q + 1) * 32, cols] - lse) - hot) * scale
                            dzb[slot, pl.ds(pl.multiple_of(row, 32), 32), cols] = val.astype(bf16)
                    return c2
                lax.fori_loop(0, ROWS // ZB, logits, 0)

                @pl.when(r < XCHS - DEFER)
                def _():
                    def mul(h, c2):
                        rows = pl.ds(pl.multiple_of(h * HB, HB), HB)
                        for n in range(0, DIM, NCOL):
                            acc[rows, n:n + NCOL] += jnp.dot(dzb[slot, rows, :], xt[slot, :, n:n + NCOL], preferred_element_type=jnp.float32)
                        return c2
                    lax.fori_loop(0, HBS, mul, 0)

                @pl.when(r >= XCHS - DEFER)
                def _():
                    dz_out(r - (XCHS - DEFER), slot).start()
                return c

            def dz_out(q, slot):
                return pltpu.make_async_copy(dzb.at[slot], dzt_last.at[q], dzo_sem.at[slot])
            lax.fori_loop(0, XCHS - 1, far, 0)
            for slot in range(2):
                dz_out(0, slot).wait()
            xd_copy(XCHS - 1).wait_recv()
            pltpu.make_async_copy(acc, de_part, big_sem).wait()
        pl.run_scoped(e_phase, pltpu.VMEM((ROWS, DIM), jnp.bfloat16), pltpu.VMEM((2, KT, DIM), jnp.bfloat16),
                      pltpu.VMEM((2, ROWS, KT), jnp.bfloat16), pltpu.VMEM((ZB, KT), jnp.float32))

        own.wait()

    wide = pltpu.VMEM((TOK, 128), f32)
    big = pltpu.VMEM((TOK, DIM), f32)

    def tokens(m_s, scale_v, tc_v, mr_v, zt, et):
        kept = (m_s, scale_v, tc_v, mr_v, zt, et)
        pl.run_scoped(functools.partial(forward, *kept), pltpu.VMEM((TOK, DIM), bf16), pltpu.VMEM((2, LN_ROWS, DIM), bf16),
                      pltpu.VMEM((2, TILE, DIM), bf16), pltpu.VMEM((HB, TILE), f32), pltpu.VMEM((HB, TILE), f32), wide, wide,
                      pltpu.VMEM((2, 8, DIM), f32))
        pl.run_scoped(functools.partial(token_grads, *kept), big)
    pl.run_scoped(tokens, wide, wide, pltpu.VMEM((TOK, 128), jnp.int32), pltpu.VMEM((2, TOK, 128), f32),
                  pltpu.VMEM((2, TOK, KT), f32), pltpu.VMEM((2, KT, DIM), bf16))
    pl.run_scoped(weight_grads, big)

    pltpu.make_async_copy(x_out, x_out, xt_send).wait()
    pltpu.make_async_copy(x_out, x_out, xd_send).wait()
    xp_copy.wait_send()
    pltpu.make_async_copy(dzt_out, dzt_out, dz_send).wait()
    for p, dev in group:
        remote(info, info_all.at[tp], sm_send, info_recv.at[p], dev).wait_send()
        remote(stat_v, stat_all.at[tp], sm_send, stat_recv.at[p], dev).wait_send()
        remote(gs_v, gsum_all.at[tp], g_send, g_recv.at[p], dev).wait()


def run_step(hidden, gain, bias, embed, info):
    any_spec = pl.BlockSpec(memory_space=pl.ANY)
    vmem_spec = pl.BlockSpec(memory_space=pltpu.VMEM)
    f32, bf16, i32 = jnp.float32, jnp.bfloat16, jnp.int32
    dma = pltpu.SemaphoreType.DMA
    small, ints = (4, 2, GROUPS, 128), (4, 3, GROUPS, 128)
    mat, square = ((TOK, DIM), bf16), ((ROWS, TOK), bf16)
    shapes = [((VOCAB, DIM), bf16), mat, ((TOK, VOCAB), f32), (small, f32), (ints, i32),
              mat, mat, mat, mat, square, square, square, ((DEFER - 1, ROWS, KT), bf16), ((ROWS, DIM), f32), ((4, 2, DIM), f32)]
    return pl.pallas_call(
        step_kernel,
        name="step",
        out_shape=[jax.ShapeDtypeStruct(s, d) for s, d in shapes],
        in_specs=[any_spec, vmem_spec, vmem_spec, any_spec, any_spec],
        out_specs=[any_spec] * len(shapes),
        scratch_shapes=[
            pltpu.VMEM((3, GROUPS, 128), i32), pltpu.VMEM((2, GROUPS, 128), f32), pltpu.VMEM(small, f32), pltpu.VMEM(ints, i32),
            pltpu.VMEM((2, 8, DIM), f32), pltpu.VMEM((2, DIM), f32), pltpu.VMEM((8, DIM), f32),
            dma((2,)), dma, dma((2,)), dma((2,)), dma((2,)), dma((4,)), dma((2,)), dma((2,)), dma((2,)), dma, dma,
            dma, dma, dma, dma, dma, dma, dma, dma, dma, dma,
            dma((CHUNKS,)), dma((CHUNKS,)), dma((TILES - NEAR,)), dma((ROWS // PE_ROWS,)), dma((4,)), dma((4,)),
            dma((XCHS,)), dma((XCHS,)), dma, dma((4,)), dma((4,)),
        ],
        compiler_params=pltpu.CompilerParams(collective_id=0, has_side_effects=True, vmem_limit_bytes=67043328),
        cost_estimate=pl.CostEstimate(flops=12 * TOK * VOCAB * DIM, bytes_accessed=700 * 2 ** 20, transcendentals=3 * TOK * VOCAB),
    )(hidden, gain, bias, embed, info)


def finish_kernel(de_in, dzt_last, x_xp, x_xq, emb, dh_in, stat_all, info_all, gsum_all,
                  de_out, dh_out, loss, mean, d_gain, d_bias,
                  xr, dz, eb, zs, din, dout, hb, x_sem, z_sem, e_sem, di_sem, do_sem, hi_sem, ho_sem):
    f32, bf16 = jnp.float32, jnp.bfloat16
    last = DEFER - 1

    def x_loads(q):
        rows = pl.ds((XCHS - DEFER + q) * XCH, XCH)
        return [pltpu.make_async_copy(ref.at[rows], xr.at[q, pl.ds(i * XCH, XCH)], x_sem.at[q]) for i, ref in enumerate((x_xp, x_xq))]

    def x_wait(q):
        pltpu.make_async_copy(xr.at[q], xr.at[q], x_sem.at[q]).wait()

    def e_load(h):
        slot = lax.rem(h, 2)
        return pltpu.make_async_copy(emb.at[pl.ds(pl.multiple_of(h * ZB, ZB), ZB)], eb.at[slot], e_sem.at[slot])

    def z_load(q):
        return pltpu.make_async_copy(dzt_last.at[q], dz.at[q], z_sem.at[q])

    def tile(ref, i):
        return ref.at[:, pl.ds(pl.multiple_of(i * KT, KT), KT)]

    def d_load(i):
        slot = lax.rem(i, 2)
        return pltpu.make_async_copy(tile(de_in, i), din.at[slot], di_sem.at[slot])

    def d_store(i):
        slot = lax.rem(i, 2)
        return pltpu.make_async_copy(dout.at[slot], tile(de_out, i), do_sem.at[slot])
    steps = DIM // KT
    per = TOK // steps

    def h_load(i):
        slot = lax.rem(i, 2)
        return pltpu.make_async_copy(dh_in.at[pl.ds(pl.multiple_of(i * per, per), per)], hb.at[slot], hi_sem.at[slot])

    def h_store(i):
        slot = lax.rem(i, 2)
        return pltpu.make_async_copy(hb.at[slot], dh_out.at[pl.ds(pl.multiple_of(i * per, per), per)], ho_sem.at[slot])
    for cp in x_loads(last):
        cp.start()
    e_load(0).start()
    e_load(1).start()
    for q in range(last):
        z_load(q).start()
        for cp in x_loads(q):
            cp.start()
    d_load(0).start()
    h_load(0).start()
    d_load(1).start()

    tp = lax.axis_index('tp')
    core = lax.rem(tp, 2)
    other = 2 - (tp - core)
    weights = info_all[:, 1].astype(f32)
    total = jnp.sum(weights)
    all_loss = (stat_all[:, 0] - stat_all[:, 1]) * weights
    loss[...] = (stat_all[tp, 0] - stat_all[tp, 1]) * info_all[tp, 1].astype(f32)
    mean[...] = jnp.broadcast_to(jnp.sum(all_loss), (1, 1)) / jnp.broadcast_to(total, (1, 1))
    sums = ((gsum_all[0] + gsum_all[1]) + gsum_all[2]) + gsum_all[3]
    d_gain[...] = sums[0:1]
    d_bias[...] = sums[1:2]
    count = jnp.broadcast_to(total, (1, 128))
    far_rows = []
    for g in range(4):
        who = other + core if g < 2 else other + 1 - core
        at = slice(GROUPS - 2 + g % 2, GROUPS - 1 + g % 2)
        far_rows.append((stat_all[who, 0, at, :], info_all[who, 1, at, :].astype(f32) / count, info_all[who, 0, at, :] - tp * ROWS))
    x_wait(last)

    def logits(h, c):
        slot = lax.rem(h, 2)
        e_load(h).wait()
        for k in range(0, DIM, KCOL):
            prod = lax.dot_general(eb[slot, :, k:k + KCOL], xr[last, :, k:k + KCOL], NT, preferred_element_type=f32)
            zs[...] = prod if k == 0 else zs[...] + prod

        @pl.when(h + 2 < ROWS // ZB)
        def _():
            e_load(h + 2).start()
        for q in range(ZB // 32):
            row = h * ZB + q * 32
            line = lax.broadcasted_iota(jnp.int32, (32, 128), 0)
            for g, (lse, scale, trel) in enumerate(far_rows):
                cols = slice(g * 128, (g + 1) * 128)
                hot = ((trel - row) == line).astype(f32)
                val = (jnp.exp(zs[q * 32:(q + 1) * 32, cols] - lse) - hot) * scale
                dz[last, pl.ds(pl.multiple_of(row, 32), 32), cols] = val.astype(bf16)
        return c
    lax.fori_loop(0, ROWS // ZB, logits, 0)
    for q in range(last):
        z_load(q).wait()
        x_wait(q)

    def step(i, c):
        slot = lax.rem(i, 2)
        cols = pl.ds(pl.multiple_of(i * KT, KT), KT)
        d_load(i).wait()
        h_load(i).wait()
        h_store(i).start()

        @pl.when(i >= 1)
        def _():
            h_store(i - 1).wait()

        @pl.when(i + 1 < steps)
        def _():
            h_load(i + 1).start()

        @pl.when(i >= 2)
        def _():
            d_store(i - 2).wait()
        for h in range(HBS):
            rows = slice(h * HB, (h + 1) * HB)
            prod = None
            for q in range(DEFER):
                part = jnp.dot(dz[q, rows, :], xr[q, :, cols], preferred_element_type=f32)
                prod = part if prod is None else prod + part
            dout[slot, rows, :] = din[slot, rows, :] + prod
        d_store(i).start()

        @pl.when(i + 2 < steps)
        def _():
            d_load(i + 2).start()
        return c
    lax.fori_loop(0, steps, step, 0)
    d_store(steps - 2).wait()
    d_store(steps - 1).wait()
    h_store(steps - 1).wait()


def finish(de_part, dzt_last, x_xp, x_xq, embed, dhid, stat_all, info_all, gsum_all):
    any_spec = pl.BlockSpec(memory_space=pl.ANY)
    vmem_spec = pl.BlockSpec(memory_space=pltpu.VMEM)
    f32, bf16 = jnp.float32, jnp.bfloat16
    dma = pltpu.SemaphoreType.DMA
    outs = [((ROWS, DIM), f32), ((TOK, DIM), bf16), ((GROUPS, 128), f32), ((1, 1), f32), ((1, DIM), f32), ((1, DIM), f32)]
    return pl.pallas_call(
        finish_kernel,
        name="finish",
        out_shape=[jax.ShapeDtypeStruct(s, d) for s, d in outs],
        in_specs=[any_spec] * 6 + [vmem_spec] * 3,
        out_specs=[any_spec] * 2 + [vmem_spec] * 4,
        scratch_shapes=[
            pltpu.VMEM((DEFER, KT, DIM), bf16), pltpu.VMEM((DEFER, ROWS, KT), bf16), pltpu.VMEM((2, ZB, DIM), bf16), pltpu.VMEM((ZB, KT), f32),
            pltpu.VMEM((2, ROWS, KT), f32), pltpu.VMEM((2, ROWS, KT), f32), pltpu.VMEM((2, TOK // (DIM // KT), DIM), bf16),
            dma((DEFER,)), dma((DEFER,)), dma((2,)), dma((2,)), dma((2,)), dma((2,)), dma((2,)),
        ],
        compiler_params=pltpu.CompilerParams(vmem_limit_bytes=67043328),
        cost_estimate=pl.CostEstimate(flops=2 * ROWS * DIM * KT * (DEFER + 1), bytes_accessed=130 * 2 ** 20, transcendentals=ROWS * KT),
    )(de_part, dzt_last, x_xp, x_xq, embed, dhid, stat_all, info_all, gsum_all)


def solution(mesh):
    def body(hidden, ln_gain, ln_bias, embed, targets, loss_mask):
        dp, rank = lax.axis_index('dp'), lax.axis_index('tp')
        shard = targets // ROWS
        block = jnp.bitwise_xor(shard, rank)
        row = targets % ROWS
        half = row // (ROWS // 2)
        sub = row % (ROWS // 2)
        piece = (block - 2) * 2 + jnp.bitwise_xor(half, dp)
        far = 2 * ROWS + (sub // PIECE_ROWS) * TILE + piece * PIECE_ROWS + sub % PIECE_ROWS
        tcol = jnp.where(block < 2, block * ROWS + row, far)
        info = jnp.stack([targets, loss_mask, tcol]).reshape(3, GROUPS, 128)
        outs = run_step(hidden, ln_gain.reshape(1, DIM), ln_bias.reshape(1, DIM), embed, info)
        stat_all, info_all, dhid, x_xp, x_xq, dzt_last, de_part, gsum_all = (outs[i] for i in (3, 4, 5, 7, 8, 12, 13, 14))
        d_embed, d_hidden, loss, mean, d_gain, d_bias = finish(de_part, dzt_last, x_xp, x_xq, embed, dhid, stat_all, info_all, gsum_all)
        return loss.reshape(TOK), mean.reshape(1), d_hidden, d_embed, d_gain.reshape(DIM), d_bias.reshape(DIM)

    token_rows = P(('dp', 'tp'))
    token_mat = P(('dp', 'tp'), None)
    return jax.shard_map(body, mesh=mesh, in_specs=(token_mat, P(), P(), P('tp', None), token_rows, token_rows), out_specs=(token_rows, P('dp'), token_mat, token_mat, P('dp'), P('dp')), check_vma=False)
```

```python
import functools

import jax
import jax.numpy as jnp
from jax import lax
from jax.experimental import pallas as pl
from jax.experimental.pallas import tpu as pltpu
from jax.sharding import PartitionSpec as P

LN_EPS = 1e-5
LOWEST = float(jnp.finfo(jnp.float32).min)

TOK = 2048
ROWS = 2048
DIM = 4096
VOCAB = 8192
TILE = 256
TILES = VOCAB // TILE
HB = 1024
HBS = TOK // HB
CHUNK = 32
PIECE_ROWS = 2 * CHUNK
NEAR = 2 * ROWS // TILE
PE_ROWS = 512
CHUNKS = ROWS // 2 // CHUNK
LN_ROWS = 256
STAT_ROWS = 32
PIECE = 32
LN_UNROLL = 4
XCH = 256
XCHS = TOK // XCH
KT = 512
DEFER = 4
WAIT_STEP = {4: 0, 9: 1, 14: 2}
ZB = 512
NCOL = 512
KCOL = 1024
NB_UNROLL = 4
NB_ROWS = 256
GROUPS = TOK // 128
NT = (((1,), (1,)), ((), ()))


def peers():
    dp, tp = lax.axis_index('dp'), lax.axis_index('tp')
    core = lax.rem(tp, 2)
    pair = tp - core
    other = 2 - pair
    part = pair + 1 - core
    return dp, tp, (dp, part), (dp, other + core), (dp, other + 1 - core), (1 - dp, tp)


def remote(src, dst, ssem, rsem, dev):
    return pltpu.make_async_remote_copy(
        src_ref=src, dst_ref=dst, send_sem=ssem, recv_sem=rsem, device_id=dev, device_id_type=pl.DeviceIdType.MESH)


def spread(row, rows, dst):
    dst[rows, :] = jnp.transpose(jnp.broadcast_to(row, (128, 128)))


def step_kernel(hid, gain, bias, emb, info,
                e_all, x_out, z_out, stat_all, info_all,
                dhid, x_part, x_xp, x_xq, dzt_own, dzt_out, dzt_part, dzt_last, de_part, gsum_all,
                info_v, stat_v, stats, infos, gb_v, gs_v, g8,
                h_sem, xo_sem, e_sem, eo_sem, z_sem, zt_sem, et_sem, small_sem, dzo_sem, big_sem, g_sem,
                xs_send, ys_send, ds_send, pe_send, sm_send, xt_send, xd_send, xp_send, dz_send, g_send,
                x_recv, y_recv, d_recv, pe_recv, info_recv, stat_recv, xt_recv, xd_recv, xp_recv, dz_recv, g_recv):
    bf16, f32 = jnp.bfloat16, jnp.float32
    dp, tp, part, xp, xq, yp = peers()
    core = lax.rem(tp, 2)
    xp_rank = 2 - (tp - core) + core
    xq_rank = 2 - (tp - core) + 1 - core
    group = ((1, part), (2, xp), (3, xq))
    barrier = pltpu.get_barrier_semaphore()
    for dev in (part, xp, xq, yp):
        pl.semaphore_signal(barrier, inc=1, device_id=dev, device_id_type=pl.DeviceIdType.MESH)
    pl.semaphore_wait(barrier, 4)

    def xrows(ref, j):
        return ref.at[pl.ds(pl.multiple_of(j * XCH, XCH), XCH)]

    def xt_copy(j):
        return remote(xrows(x_out, j), xrows(x_xp, j), xt_send, xt_recv.at[j], xp)

    def xd_copy(j):
        return remote(xrows(x_xp, j), xrows(x_xq, j), xd_send, xd_recv.at[j], part)

    def xt_event(j):
        xt_copy(j).wait_recv()
        xd_copy(j).start()
    xp_copy = remote(x_out, x_part, xp_send, xp_recv, part)

    def forward(m_s, scale_v, tc_v, mr_v, zt, et, xs, hbuf, ebuf, z0, z1, s_s, t_s, gb8):
        def tile_row(j):
            return ROWS * 2 + (j // 2) * TILE + lax.rem(j, 2) * CHUNK

        def x_copy(j):
            src = emb.at[pl.ds(pl.multiple_of(dp * (ROWS // 2) + j * CHUNK, CHUNK), CHUNK)]
            return remote(src, e_all.at[pl.ds(pl.multiple_of(tile_row(j), CHUNK), CHUNK)], xs_send, x_recv.at[j], xp)

        def piece(j, p):
            return e_all.at[pl.ds(pl.multiple_of(tile_row(j) + p * PIECE_ROWS, CHUNK), CHUNK)]

        def y_copy(j):
            return remote(piece(j, 0), piece(j, 1), ys_send, y_recv.at[j], yp)

        def d_copy(j, p):
            return remote(piece(j, p), piece(j, p + 2), ds_send, d_recv.at[j // 2], part)

        def pe_copy(i):
            return remote(emb.at[pl.ds(pl.multiple_of(i * PE_ROWS, PE_ROWS), PE_ROWS)],
                          e_all.at[pl.ds(pl.multiple_of(ROWS + i * PE_ROWS, PE_ROWS), PE_ROWS)], pe_send, pe_recv.at[i], part)

        cp = pltpu.make_async_copy(info, info_v, small_sem.at[0])
        cp.start()

        def h_copy(i):
            return pltpu.make_async_copy(hid.at[pl.ds(pl.multiple_of(i * LN_ROWS, LN_ROWS), LN_ROWS)], hbuf.at[lax.rem(i, 2)], h_sem.at[lax.rem(i, 2)])
        h_copy(0).start()

        for p, dev in group:
            remote(info, info_all.at[tp], sm_send, info_recv.at[p], dev).start()

        def start_x(j, c):
            x_copy(j).start()
            return c
        lax.fori_loop(0, CHUNKS, start_x, 0)

        def start_pe(i, c):
            pe_copy(i).start()
            return c
        lax.fori_loop(0, ROWS // PE_ROWS, start_pe, 0)

        def e_load(t):
            slot = lax.rem(t, 2)
            return pltpu.make_async_copy(e_all.at[pl.ds(pl.multiple_of(t * TILE, TILE), TILE)], ebuf.at[slot], e_sem.at[slot])

        def e_load_own(t):
            slot = lax.rem(t, 2)
            return pltpu.make_async_copy(emb.at[pl.ds(pl.multiple_of(t * TILE, TILE), TILE)], ebuf.at[slot], e_sem.at[slot])
        e_load_own(0).start()

        def x_event(j):
            x_copy(j).wait_recv()
            y_copy(j).start()
            d_copy(j, 0).start()

        def y_event(j):
            y_copy(j).wait_recv()
            d_copy(j, 1).start()

        def p_event(k):
            rows = e_all.at[pl.ds(pl.multiple_of(2 * ROWS + k * TILE + TILE // 2, TILE // 2), TILE // 2)]
            pltpu.make_async_copy(rows, rows, d_recv.at[k]).wait()
            e_load(NEAR + k).start()

        cp.wait()
        pltpu.make_async_copy(info_v, info_all.at[tp], small_sem.at[0]).start()
        gb8[0] = jnp.broadcast_to(gain[...], (8, DIM))
        gb8[1] = jnp.broadcast_to(bias[...], (8, DIM))

        def ln_tile(i, c):
            slot = lax.rem(i, 2)

            @pl.when(i + 1 < TOK // LN_ROWS)
            def _():
                h_copy(i + 1).start()
            h_copy(i).wait()

            @pl.when(i == 6)
            def _():
                x_event(0)

            def ln_rows(r, c2):
                base = r * LN_UNROLL * 16

                def at(u):
                    return pl.ds(pl.multiple_of(base + u * 16, 16), 16)

                def part_of(u, k):
                    return hbuf[slot, at(u), k * 128:(k + 1) * 128].astype(jnp.float32)
                means, rstds = [], []
                for u in range(LN_UNROLL):
                    tot = part_of(u, 0)
                    for k in range(1, DIM // 128):
                        tot = tot + part_of(u, k)
                    means.append(jnp.broadcast_to(jnp.sum(tot, axis=-1, keepdims=True) * (1.0 / DIM), (16, 128)))
                for u in range(LN_UNROLL):
                    tot = jnp.zeros((16, 128), jnp.float32)
                    for k in range(DIM // 128):
                        diff = part_of(u, k) - means[u]
                        tot = tot + diff * diff
                    var = jnp.sum(tot, axis=-1, keepdims=True) * (1.0 / DIM)
                    rstds.append(jnp.broadcast_to(lax.rsqrt(var + LN_EPS), (16, 128)))
                for u in range(LN_UNROLL):
                    row = pl.ds(pl.multiple_of(i * LN_ROWS + base + u * 16, 16), 16)
                    mr_v[0, row, :] = means[u]
                    mr_v[1, row, :] = rstds[u]
                    for k in range(DIM // 128):
                        cols = slice(k * 128, (k + 1) * 128)
                        g2 = jnp.concatenate([gb8[0, :, cols]] * 2, axis=0)
                        b2 = jnp.concatenate([gb8[1, :, cols]] * 2, axis=0)
                        xs[row, cols] = ((part_of(u, k) - means[u]) * rstds[u] * g2 + b2).astype(jnp.bfloat16)
                return c2
            lax.fori_loop(0, LN_ROWS // (16 * LN_UNROLL), ln_rows, 0)
            rows = pl.ds(pl.multiple_of(i * LN_ROWS, LN_ROWS), LN_ROWS)
            pltpu.make_async_copy(xs.at[rows], x_out.at[rows], xo_sem).start()
            return c
        lax.fori_loop(0, TOK // LN_ROWS, ln_tile, 0)

        m_s[...] = jnp.full((TOK, 128), LOWEST, jnp.float32)
        s_s[...] = jnp.zeros((TOK, 128), jnp.float32)
        t_s[...] = jnp.zeros((TOK, 128), jnp.float32)
        for r in range(GROUPS):
            spread(info_v[2, r:r + 1, :], slice(r * 128, (r + 1) * 128), tc_v)
        z1[...] = jnp.full((HB, TILE), LOWEST, jnp.float32)

        zs = (z0, z1)

        def product(t, h):
            for r in range(0, HB, 512):
                zs[h][r:r + 512, :] = lax.dot_general(
                    xs[h * HB + r:h * HB + r + 512, :], ebuf[lax.rem(t, 2)], NT, preferred_element_type=jnp.float32)

        def statistics(t, h):
            z = zs[h]
            lane = lax.broadcasted_iota(jnp.int32, (STAT_ROWS, 128), 1)
            for r in range(0, HB, STAT_ROWS):
                rows = slice(h * HB + r, h * HB + r + STAT_ROWS)
                zk = [z[r:r + STAT_ROWS, k * 128:(k + 1) * 128] for k in range(TILE // 128)]
                old = m_s[rows, :]
                new = jnp.maximum(jnp.maximum(zk[0], zk[1]), old)
                tot = s_s[rows, :] * jnp.exp(old - new)
                tgt = t_s[rows, :]
                diff = tc_v[rows, :] - t * TILE
                for k in range(TILE // 128):
                    tot = tot + jnp.exp(zk[k] - new)
                    tgt = tgt + jnp.where(diff == lane + k * 128, zk[k], 0.0)
                m_s[rows, :] = new
                s_s[rows, :] = tot
                t_s[rows, :] = tgt

        def z_copy(t, h):
            return pltpu.make_async_copy(
                zs[h], z_out.at[pl.ds(h * HB, HB), pl.ds(pl.multiple_of(t * TILE, TILE), TILE)], z_sem.at[h])

        def start_events(t):
            @pl.when(t < TILES - 1)
            def _():
                x_event(t + 1)

            @pl.when(t == TILES - 2)
            def _():
                xt_copy(0).start()

            @pl.when(t == TILES - 1)
            def _():
                y_event(TILES - 1)
                p_event(TILES - 1 - NEAR)
            e_load(t).wait()

            @pl.when(t < ROWS // TILE)
            def _():
                slot = lax.rem(t, 2)
                pltpu.make_async_copy(ebuf.at[slot], e_all.at[pl.ds(pl.multiple_of(t * TILE, TILE), TILE)], eo_sem.at[slot]).start()

        def middle_events(t):
            @pl.when(t < TILES - 1)
            def _():
                y_event(t)

            @pl.when((t >= 1) & (t < ROWS // TILE + 1))
            def _():
                slot = lax.rem(t - 1, 2)
                pltpu.make_async_copy(ebuf.at[slot], e_all.at[pl.ds(0, TILE)], eo_sem.at[slot]).wait()

            @pl.when(t == NEAR)
            def _():
                pltpu.make_async_copy(xs, x_out, xo_sem).wait()

            @pl.when(t < ROWS // TILE - 1)
            def _():
                e_load_own(t + 1).start()

            @pl.when((t >= ROWS // TILE - 1) & (t < NEAR - 1))
            def _():
                @pl.when(lax.rem(t + 1, PE_ROWS // TILE) == 0)
                def _():
                    pe_copy((t + 1 - ROWS // TILE) // (PE_ROWS // TILE)).wait_recv()
                e_load(t + 1).start()

            @pl.when((t >= NEAR - 1) & (t < TILES - 2))
            def _():
                p_event(t - (NEAR - 1))

            @pl.when(t == TILES - 2)
            def _():
                for k, h in ((0, 0), (1, 0), (0, 1)):
                    z_load(zt, k, h).start()
                et_load(et, 0).start()

            @pl.when(t == NEAR + 1)
            def _():
                for p, dev in group:
                    remote(info, info_all.at[tp], sm_send, info_recv.at[p], dev).wait_recv()
                pltpu.make_async_copy(info_v, info_all.at[tp], small_sem.at[0]).wait()
                load = pltpu.make_async_copy(info_all, infos, small_sem.at[0])
                load.start()
                load.wait()
                count = jnp.broadcast_to(token_count(), (1, 128))
                for r in range(GROUPS):
                    spread(info_v[1, r:r + 1, :].astype(f32) / count, slice(r * 128, (r + 1) * 128), scale_v)

        def step(t, c):
            @pl.when(t > 0)
            def _():
                z_copy(t - 1, 1).start()
            start_events(t)

            @pl.when(t > 0)
            def _():
                z_copy(t - 1, 0).wait()
            statistics(t - 1, 1)
            product(t, 0)
            z_copy(t, 0).start()
            middle_events(t)

            @pl.when(t > 0)
            def _():
                z_copy(t - 1, 1).wait()
            statistics(t, 0)
            product(t, 1)
            return c
        last = TILES - 1
        lax.fori_loop(0, TILES, step, 0)
        z_copy(last, 1).start()
        statistics(last, 1)

        def finish(i, c):
            for u in range(4):
                r = i * 4 + u
                rows = pl.ds(pl.multiple_of(r * 128, 128), 128)
                m = m_s[rows, :]
                top = jnp.max(m, axis=-1, keepdims=True)
                tot = jnp.sum(s_s[rows, :] * jnp.exp(m - top), axis=-1, keepdims=True)
                lse = jnp.broadcast_to(top + jnp.log(tot), (128, 128))
                tgt = jnp.broadcast_to(jnp.sum(t_s[rows, :], axis=-1, keepdims=True), (128, 128))
                m_s[rows, :] = lse
                stat_v[0, pl.ds(r, 1), :] = jnp.transpose(lse)[0:1, :]
                stat_v[1, pl.ds(r, 1), :] = jnp.transpose(tgt)[0:1, :]
            return c
        lax.fori_loop(0, TOK // 512, finish, 0)
        for h in range(2):
            z_copy(last, h).wait()
        half = e_all.at[pl.ds(0, ROWS // 2)]
        pltpu.make_async_copy(half, half, xs_send).wait()
        pltpu.make_async_copy(half, half, ys_send).wait()
        full = e_all.at[pl.ds(0, ROWS)]
        pltpu.make_async_copy(full, full, ds_send).wait()
        pltpu.make_async_copy(full, full, pe_send).wait()
        pltpu.make_async_copy(stat_v, stat_all.at[tp], small_sem.at[1]).start()
        for p, dev in group:
            remote(stat_v, stat_all.at[tp], sm_send, stat_recv.at[p], dev).start()

        def start_xt(j, c):
            xt_copy(j).start()
            return c
        lax.fori_loop(1, XCHS, start_xt, 0)
        xp_copy.start()

    def z_load(zt, k, h):
        slot = lax.rem(k, 2)
        rows = slice(h * HB, (h + 1) * HB)
        return pltpu.make_async_copy(
            z_out.at[rows, pl.ds(pl.multiple_of(k * KT, KT), KT)], zt.at[slot, rows], zt_sem.at[2 * h + slot])

    def et_load(et, k):
        slot = lax.rem(k, 2)
        return pltpu.make_async_copy(e_all.at[pl.ds(pl.multiple_of(k * KT, KT), KT)], et.at[slot], et_sem.at[slot])

    def dzt_copy(k):
        rows = pl.ds(pl.multiple_of(lax.rem(k, 4) * KT, KT), KT)
        return remote(dzt_out.at[rows], dzt_part.at[rows], dz_send, dz_recv.at[lax.rem(k, 4)], part)

    def token_count():
        return jnp.sum(infos[:, 1].astype(f32))

    def token_grads(lse_v, scale_v, tcol_v, mr, zt, et, acc):
        def d_phase(da, db, dzt):
            def dzt_store(k, ref):
                slot = lax.rem(k, 2)
                return pltpu.make_async_copy(dzt.at[slot], ref.at[pl.ds(pl.multiple_of(lax.rem(k, 4) * KT, KT), KT)], eo_sem.at[slot])
            lane = lax.broadcasted_iota(jnp.int32, (PIECE, 128), 1)

            def piece(dst, rows, low, k, tie):
                slot = lax.rem(k, 2)
                lse = lse_v[rows, :]
                if tie is not None:
                    floor = 0.0 - jnp.maximum(0.0 - tie, -LOWEST)
                    lse = jnp.maximum(lse, jnp.concatenate([floor] * (PIECE // 8), axis=0))
                scale = scale_v[rows, :]
                diff = tcol_v[rows, :] - k * KT
                for g in range(KT // 128):
                    cols = slice(g * 128, (g + 1) * 128)
                    hot = (diff == lane + g * 128).astype(f32)
                    val = (jnp.exp(zt[slot, rows, cols] - lse) - hot) * scale
                    dst[low, cols] = val.astype(bf16)

            def half_step(k, src, dst, base, dst_base, dst_k):
                slot = lax.rem(k, 2)
                per = HB // (DIM // NCOL)
                for n in range(DIM // NCOL):
                    cols = slice(n * NCOL, (n + 1) * NCOL)
                    prod = jnp.dot(src[...], et[slot, :, cols], preferred_element_type=f32)
                    acc[base:base + HB, cols] = jnp.where(k == 0, 0.0, acc[base:base + HB, cols]) + prod
                    for q in range(0, per, PIECE):
                        at = q * HB // per
                        low = n * per + q
                        piece(dst, slice(dst_base + low, dst_base + low + PIECE), slice(low, low + PIECE), dst_k, prod[at:at + 8, 0:128])
                    if n * per % 256 == 0:
                        low = n * per
                        dzt[slot, :, base + low:base + low + 256] = jnp.transpose(src[low:low + 256, :])

            z_load(zt, 0, 0).wait()

            def first(i, c):
                rows = pl.ds(pl.multiple_of(i * PIECE, PIECE), PIECE)
                piece(da, rows, rows, 0, None)
                return c
            lax.fori_loop(0, HB // PIECE, first, 0)

            def step(k, c):
                @pl.when(k + 2 < VOCAB // KT)
                def _():
                    z_load(zt, k + 2, 0).start()

                @pl.when(k + 1 < VOCAB // KT)
                def _():
                    z_load(zt, k + 1, 1).start()
                    et_load(et, k + 1).start()
                    z_load(zt, k + 1, 0).wait()
                for at, j in WAIT_STEP.items():
                    @pl.when(k == at)
                    def _(j=j):
                        xt_event(j)

                @pl.when((k >= 2) & (k < 10))
                def _():
                    dzt_store(k, dzt_own).wait()

                @pl.when((k >= 6) & (k < 10))
                def _():
                    dzt_copy(k - 2).start()
                et_load(et, k).wait()
                z_load(zt, k, 1).wait()
                half_step(k, da, db, 0, HB, k)
                half_step(k, db, da, HB, 0, k + 1)

                @pl.when(k < 4)
                def _():
                    dzt_store(k, dzt_own).start()

                @pl.when((k >= 4) & (k < 8))
                def _():
                    dzt_store(k, dzt_out).start()
                return c
            lax.fori_loop(0, VOCAB // KT, step, 0)
        half = pltpu.VMEM((HB, KT), bf16)
        pl.run_scoped(d_phase, half, half, pltpu.VMEM((2, KT, TOK), bf16))

        def n_phase(hb, ob):
            def h_load(i):
                slot = lax.rem(i, 2)
                return pltpu.make_async_copy(hid.at[pl.ds(pl.multiple_of(i * NB_ROWS, NB_ROWS), NB_ROWS)], hb.at[slot], z_sem.at[slot])

            def o_store(i):
                slot = lax.rem(i, 2)
                return pltpu.make_async_copy(ob.at[slot], dhid.at[pl.ds(pl.multiple_of(i * NB_ROWS, NB_ROWS), NB_ROWS)], e_sem.at[slot])
            h_load(0).start()
            gb_v[...] = jnp.zeros(gb_v.shape, jnp.float32)
            g8[...] = jnp.broadcast_to(gain[...], (8, DIM))

            def tile(i, c):
                slot = lax.rem(i, 2)

                @pl.when(i + 1 < TOK // NB_ROWS)
                def _():
                    h_load(i + 1).start()

                @pl.when(i >= 2)
                def _():
                    o_store(i - 2).wait()
                h_load(i).wait()

                def rows_body(r, c2):
                    units = range(NB_UNROLL)
                    base = r * 16 * NB_UNROLL
                    low = [pl.ds(pl.multiple_of(base + u * 16, 16), 16) for u in units]
                    row = [pl.ds(pl.multiple_of(i * NB_ROWS + base + u * 16, 16), 16) for u in units]
                    zero = jnp.zeros((16, 128), jnp.float32)
                    sum1, sum3 = [zero] * NB_UNROLL, [zero] * NB_UNROLL

                    def load(u, cols):
                        dx = acc[row[u], cols]
                        xhat = (hb[slot, low[u], cols].astype(jnp.float32) - mr[0, row[u], :]) * mr[1, row[u], :]
                        return dx, xhat, dx * jnp.concatenate([g8[:, cols]] * 2, axis=0)
                    for k in range(DIM // 128):
                        cols = slice(k * 128, (k + 1) * 128)
                        d_gain, d_bias = gb_v[0, :, cols], gb_v[1, :, cols]
                        for u in units:
                            dx, xhat, gx = load(u, cols)
                            sum1[u] = sum1[u] + gx
                            sum3[u] = sum3[u] + gx * xhat
                            dgx = dx * xhat
                            d_gain = d_gain + (dgx[0:8] + dgx[8:16])
                            d_bias = d_bias + (dx[0:8] + dx[8:16])
                        gb_v[0, :, cols] = d_gain
                        gb_v[1, :, cols] = d_bias
                    slope, shift = [], []
                    for u in units:
                        mean, rstd = mr[0, row[u], :], mr[1, row[u], :]
                        c1 = jnp.broadcast_to(jnp.sum(sum1[u], axis=-1, keepdims=True) * (1.0 / DIM), (16, 128))
                        c3 = jnp.broadcast_to(jnp.sum(sum3[u], axis=-1, keepdims=True) * (1.0 / DIM), (16, 128))
                        slope.append(c3 * rstd * rstd)
                        shift.append(slope[u] * mean - c1 * rstd)
                    for u in units:
                        rstd = mr[1, row[u], :]
                        for k in range(DIM // 128):
                            cols = slice(k * 128, (k + 1) * 128)
                            gx = acc[row[u], cols] * jnp.concatenate([g8[:, cols]] * 2, axis=0)
                            ob[slot, low[u], cols] = (gx * rstd - hb[slot, low[u], cols].astype(f32) * slope[u] + shift[u]).astype(bf16)
                    return c2
                lax.fori_loop(0, NB_ROWS // (16 * NB_UNROLL), rows_body, 0)
                o_store(i).start()
                return c
            lax.fori_loop(0, TOK // NB_ROWS, tile, 0)
            for i in range(2):
                o_store(TOK // NB_ROWS - 2 + i).wait()
            gs_v[0:1, :] = jnp.sum(gb_v[0], axis=0, keepdims=True)
            gs_v[1:2, :] = jnp.sum(gb_v[1], axis=0, keepdims=True)
        pl.run_scoped(n_phase, pltpu.VMEM((2, NB_ROWS, DIM), bf16), pltpu.VMEM((2, NB_ROWS, DIM), bf16))

    def weight_grads(acc):
        own = pltpu.make_async_copy(gs_v, gsum_all.at[tp], g_sem)
        xt_event(3)

        def e_phase(eo, xt, dzb, zs):
            eo_load = pltpu.make_async_copy(emb, eo, big_sem)

            def x_load(ref, row, slot):
                return pltpu.make_async_copy(ref.at[pl.ds(pl.multiple_of(row, KT), KT)], xt.at[slot], z_sem.at[slot])

            def dz_load(ref, col, slot):
                return pltpu.make_async_copy(ref.at[:, pl.ds(pl.multiple_of(col, KT), KT)], dzb.at[slot], e_sem.at[slot])

            def start_local(i):
                slot = lax.rem(i, 2)

                @pl.when(i < 4)
                def _():
                    x_load(x_out, i * KT, slot).start()
                    dz_load(dzt_own, i * KT, slot).start()

                @pl.when(i >= 4)
                def _():
                    x_load(x_part, (i - 4) * KT, slot).start()
                    dz_load(dzt_part, (i - 4) * KT, slot).start()

            def add(slot, first):
                def mul(h, c2):
                    rows = pl.ds(pl.multiple_of(h * HB, HB), HB)
                    for n in range(0, DIM, NCOL):
                        prod = jnp.dot(dzb[slot, rows, :], xt[slot, :, n:n + NCOL], preferred_element_type=f32)
                        acc[rows, n:n + NCOL] = jnp.where(first, 0.0, acc[rows, n:n + NCOL]) + prod
                    return c2
                lax.fori_loop(0, HBS, mul, 0)

            start_local(0)

            def rem_load(r):
                slot = lax.rem(r, 2)
                return [pltpu.make_async_copy(xrows(ref, r), xt.at[slot, pl.ds(i * XCH, XCH)], z_sem.at[slot])
                        for i, ref in enumerate((x_xp, x_xq))]

            def local(i, c):
                slot = lax.rem(i, 2)

                @pl.when(i == 0)
                def _():
                    eo_load.start()

                @pl.when(i == 2)
                def _():
                    xp_copy.wait_recv()

                    def wait_dz(q, c2):
                        dzt_copy(q).wait_recv()
                        return c2
                    lax.fori_loop(0, 4, wait_dz, 0)

                @pl.when(i == 1)
                def _():
                    own.start()
                    for p, dev in group:
                        remote(gs_v, gsum_all.at[tp], g_send, g_recv.at[p], dev).start()

                @pl.when(i == 6)
                def _():
                    xt_event(4)

                @pl.when(i < 7)
                def _():
                    start_local(i + 1)

                @pl.when(i == 7)
                def _():
                    xd_copy(0).wait_recv()
                    for cp in rem_load(0):
                        cp.start()
                x_load(x_out, 0, slot).wait()
                dz_load(dzt_own, 0, slot).wait()
                add(slot, i == 0)
                return c
            lax.fori_loop(0, 8, local, 0)
            eo_load.wait()
            for p, dev in group:
                remote(stat_v, stat_all.at[tp], sm_send, stat_recv.at[p], dev).wait_recv()
            pltpu.make_async_copy(stat_v, stat_all.at[tp], small_sem.at[1]).wait()
            stat_load = pltpu.make_async_copy(stat_all, stats, small_sem.at[1])
            stat_load.start()
            stat_load.wait()
            count = jnp.broadcast_to(token_count(), (1, 128))

            def far(r, c):
                slot = lax.rem(r, 2)

                @pl.when(r == 1)
                def _():
                    xt_event(5)

                @pl.when(r == 4)
                def _():
                    xt_event(6)

                def fetch():
                    xd_copy(r + 1).wait_recv()
                    for cp in rem_load(r + 1):
                        cp.start()
                pl.when(r < XCHS - 2)(fetch)
                x_load(x_out, 0, slot).wait()

                @pl.when(r == XCHS - DEFER)
                def _():
                    pltpu.make_async_copy(acc, de_part, big_sem).start()

                @pl.when(r > XCHS - DEFER + 1)
                def _():
                    dz_out(0, slot).wait()

                far_rows = []
                for g in range(4):
                    who = xp_rank if g < 2 else xq_rank
                    at = pl.ds(2 * r + g % 2, 1)
                    far_rows.append((stats[who, 0, at, :], infos[who, 1, at, :].astype(f32) / count, infos[who, 0, at, :] - tp * ROWS))

                def logits(h, c2):
                    @pl.when((r == XCHS - 2) & (h == ROWS // ZB // 2))
                    def _():
                        xt_event(XCHS - 1)
                    for k in range(0, DIM, KCOL):
                        prod = lax.dot_general(eo[pl.ds(pl.multiple_of(h * ZB, ZB), ZB), k:k + KCOL], xt[slot, :, k:k + KCOL], NT, preferred_element_type=jnp.float32)
                        zs[...] = prod if k == 0 else zs[...] + prod
                    for q in range(ZB // 32):
                        row = h * ZB + q * 32
                        line = lax.broadcasted_iota(jnp.int32, (32, 128), 0)
                        for g, (lse, scale, trel) in enumerate(far_rows):
                            cols = slice(g * 128, (g + 1) * 128)
                            hot = ((trel - row) == line).astype(f32)
                            val = (jnp.exp(zs[q * 32:(q + 1) * 32, cols] - lse) - hot) * scale
                            dzb[slot, pl.ds(pl.multiple_of(row, 32), 32), cols] = val.astype(bf16)
                    return c2
                lax.fori_loop(0, ROWS // ZB, logits, 0)

                @pl.when(r < XCHS - DEFER)
                def _():
                    def mul(h, c2):
                        rows = pl.ds(pl.multiple_of(h * HB, HB), HB)
                        for n in range(0, DIM, NCOL):
                            acc[rows, n:n + NCOL] += jnp.dot(dzb[slot, rows, :], xt[slot, :, n:n + NCOL], preferred_element_type=jnp.float32)
                        return c2
                    lax.fori_loop(0, HBS, mul, 0)

                @pl.when(r >= XCHS - DEFER)
                def _():
                    dz_out(r - (XCHS - DEFER), slot).start()
                return c

            def dz_out(q, slot):
                return pltpu.make_async_copy(dzb.at[slot], dzt_last.at[q], dzo_sem.at[slot])
            lax.fori_loop(0, XCHS - 1, far, 0)
            for slot in range(2):
                dz_out(0, slot).wait()
            xd_copy(XCHS - 1).wait_recv()
            pltpu.make_async_copy(acc, de_part, big_sem).wait()
        pl.run_scoped(e_phase, pltpu.VMEM((ROWS, DIM), jnp.bfloat16), pltpu.VMEM((2, KT, DIM), jnp.bfloat16),
                      pltpu.VMEM((2, ROWS, KT), jnp.bfloat16), pltpu.VMEM((ZB, KT), jnp.float32))

        own.wait()

    wide = pltpu.VMEM((TOK, 128), f32)
    big = pltpu.VMEM((TOK, DIM), f32)

    def tokens(m_s, scale_v, tc_v, mr_v, zt, et):
        kept = (m_s, scale_v, tc_v, mr_v, zt, et)
        pl.run_scoped(functools.partial(forward, *kept), pltpu.VMEM((TOK, DIM), bf16), pltpu.VMEM((2, LN_ROWS, DIM), bf16),
                      pltpu.VMEM((2, TILE, DIM), bf16), pltpu.VMEM((HB, TILE), f32), pltpu.VMEM((HB, TILE), f32), wide, wide,
                      pltpu.VMEM((2, 8, DIM), f32))
        pl.run_scoped(functools.partial(token_grads, *kept), big)
    pl.run_scoped(tokens, wide, wide, pltpu.VMEM((TOK, 128), jnp.int32), pltpu.VMEM((2, TOK, 128), f32),
                  pltpu.VMEM((2, TOK, KT), f32), pltpu.VMEM((2, KT, DIM), bf16))
    pl.run_scoped(weight_grads, big)

    pltpu.make_async_copy(x_out, x_out, xt_send).wait()
    pltpu.make_async_copy(x_out, x_out, xd_send).wait()
    xp_copy.wait_send()
    pltpu.make_async_copy(dzt_out, dzt_out, dz_send).wait()
    for p, dev in group:
        remote(info, info_all.at[tp], sm_send, info_recv.at[p], dev).wait_send()
        remote(stat_v, stat_all.at[tp], sm_send, stat_recv.at[p], dev).wait_send()
        remote(gs_v, gsum_all.at[tp], g_send, g_recv.at[p], dev).wait()


def run_step(hidden, gain, bias, embed, info):
    any_spec = pl.BlockSpec(memory_space=pl.ANY)
    vmem_spec = pl.BlockSpec(memory_space=pltpu.VMEM)
    f32, bf16, i32 = jnp.float32, jnp.bfloat16, jnp.int32
    dma = pltpu.SemaphoreType.DMA
    small, ints = (4, 2, GROUPS, 128), (4, 3, GROUPS, 128)
    mat, square = ((TOK, DIM), bf16), ((ROWS, TOK), bf16)
    shapes = [((VOCAB, DIM), bf16), mat, ((TOK, VOCAB), f32), (small, f32), (ints, i32),
              mat, mat, mat, mat, square, square, square, ((DEFER - 1, ROWS, KT), bf16), ((ROWS, DIM), f32), ((4, 2, DIM), f32)]
    return pl.pallas_call(
        step_kernel,
        name="step",
        out_shape=[jax.ShapeDtypeStruct(s, d) for s, d in shapes],
        in_specs=[any_spec, vmem_spec, vmem_spec, any_spec, any_spec],
        out_specs=[any_spec] * len(shapes),
        scratch_shapes=[
            pltpu.VMEM((3, GROUPS, 128), i32), pltpu.VMEM((2, GROUPS, 128), f32), pltpu.VMEM(small, f32), pltpu.VMEM(ints, i32),
            pltpu.VMEM((2, 8, DIM), f32), pltpu.VMEM((2, DIM), f32), pltpu.VMEM((8, DIM), f32),
            dma((2,)), dma, dma((2,)), dma((2,)), dma((2,)), dma((4,)), dma((2,)), dma((2,)), dma((2,)), dma, dma,
            dma, dma, dma, dma, dma, dma, dma, dma, dma, dma,
            dma((CHUNKS,)), dma((CHUNKS,)), dma((TILES - NEAR,)), dma((ROWS // PE_ROWS,)), dma((4,)), dma((4,)),
            dma((XCHS,)), dma((XCHS,)), dma, dma((4,)), dma((4,)),
        ],
        compiler_params=pltpu.CompilerParams(collective_id=0, has_side_effects=True, vmem_limit_bytes=67043328),
        cost_estimate=pl.CostEstimate(flops=12 * TOK * VOCAB * DIM, bytes_accessed=700 * 2 ** 20, transcendentals=3 * TOK * VOCAB),
    )(hidden, gain, bias, embed, info)


def finish_kernel(de_in, dzt_last, x_xp, x_xq, emb, dh_in, stat_all, info_all, gsum_all,
                  de_out, dh_out, loss, mean, d_gain, d_bias,
                  x7, xr, dz, eb, zs, din, dout, hb, x_sem, z_sem, e_sem, di_sem, do_sem, hi_sem, ho_sem):
    f32, bf16 = jnp.float32, jnp.bfloat16
    last = DEFER - 1

    def x_last():
        rows = pl.ds((XCHS - 1) * XCH, XCH)
        return [pltpu.make_async_copy(ref.at[rows], x7.at[pl.ds(i * XCH, XCH)], x_sem.at[3]) for i, ref in enumerate((x_xp, x_xq))]

    def x_tiles(i):
        slot = lax.rem(i, 3)
        cols = pl.ds(pl.multiple_of(i * KT, KT), KT)
        rows = pl.ds((XCHS - DEFER) * XCH, last * XCH)
        return [pltpu.make_async_copy(ref.at[rows, cols], xr.at[slot, j], x_sem.at[slot]) for j, ref in enumerate((x_xp, x_xq))]

    def e_load(h):
        slot = lax.rem(h, 2)
        return pltpu.make_async_copy(emb.at[pl.ds(pl.multiple_of(h * ZB, ZB), ZB)], eb.at[slot], e_sem.at[slot])

    def z_load(q):
        return pltpu.make_async_copy(dzt_last.at[q], dz.at[q], z_sem.at[q])

    def tile(ref, i):
        return ref.at[:, pl.ds(pl.multiple_of(i * KT, KT), KT)]

    def d_load(i):
        slot = lax.rem(i, 3)
        return pltpu.make_async_copy(tile(de_in, i), din.at[slot], di_sem.at[slot])

    def d_store(i):
        slot = lax.rem(i, 3)
        return pltpu.make_async_copy(dout.at[slot], tile(de_out, i), do_sem.at[slot])
    steps = DIM // KT
    per = TOK // steps

    def h_load(i):
        slot = lax.rem(i, 2)
        return pltpu.make_async_copy(dh_in.at[pl.ds(pl.multiple_of(i * per, per), per)], hb.at[slot], hi_sem.at[slot])

    def h_store(i):
        slot = lax.rem(i, 2)
        return pltpu.make_async_copy(hb.at[slot], dh_out.at[pl.ds(pl.multiple_of(i * per, per), per)], ho_sem.at[slot])
    for cp in x_last():
        cp.start()
    e_load(0).start()
    e_load(1).start()

    def tile_loads(i):
        for cp in (*x_tiles(i), d_load(i)):
            cp.start()

    tp = lax.axis_index('tp')
    core = lax.rem(tp, 2)
    other = 2 - (tp - core)
    weights = info_all[:, 1].astype(f32)
    total = jnp.sum(weights)
    all_loss = (stat_all[:, 0] - stat_all[:, 1]) * weights
    loss[...] = (stat_all[tp, 0] - stat_all[tp, 1]) * info_all[tp, 1].astype(f32)
    mean[...] = jnp.broadcast_to(jnp.sum(all_loss), (1, 1)) / jnp.broadcast_to(total, (1, 1))
    sums = ((gsum_all[0] + gsum_all[1]) + gsum_all[2]) + gsum_all[3]
    d_gain[...] = sums[0:1]
    d_bias[...] = sums[1:2]
    count = jnp.broadcast_to(total, (1, 128))
    far_rows = []
    for g in range(4):
        who = other + core if g < 2 else other + 1 - core
        at = slice(GROUPS - 2 + g % 2, GROUPS - 1 + g % 2)
        far_rows.append((stat_all[who, 0, at, :], info_all[who, 1, at, :].astype(f32) / count, info_all[who, 0, at, :] - tp * ROWS))
    pltpu.make_async_copy(x7, x7, x_sem.at[3]).wait()

    def logits(h, c):
        slot = lax.rem(h, 2)
        e_load(h).wait()
        for k in range(0, DIM, KCOL):
            prod = lax.dot_general(eb[slot, :, k:k + KCOL], x7[:, k:k + KCOL], NT, preferred_element_type=f32)
            zs[...] = prod if k == 0 else zs[...] + prod

        @pl.when(h == 0)
        def _():
            e_load(2).start()
            z_load(0).start()
            z_load(1).start()

        @pl.when(h == 1)
        def _():
            e_load(3).start()
            z_load(2).start()

        @pl.when(h == 2)
        def _():
            tile_loads(0)
            h_load(0).start()

        @pl.when(h == 3)
        def _():
            tile_loads(1)
        for q in range(ZB // 32):
            row = h * ZB + q * 32
            line = lax.broadcasted_iota(jnp.int32, (32, 128), 0)
            for g, (lse, scale, trel) in enumerate(far_rows):
                cols = slice(g * 128, (g + 1) * 128)
                hot = ((trel - row) == line).astype(f32)
                val = (jnp.exp(zs[q * 32:(q + 1) * 32, cols] - lse) - hot) * scale
                dz[last, pl.ds(pl.multiple_of(row, 32), 32), cols] = val.astype(bf16)
        return c
    lax.fori_loop(0, ROWS // ZB, logits, 0)
    for q in range(last):
        z_load(q).wait()

    def step(i, c):
        slot = lax.rem(i, 3)
        cols = pl.ds(pl.multiple_of(i * KT, KT), KT)

        @pl.when(i + 2 < steps)
        def _():
            tile_loads(i + 2)
        h_load(i).wait()
        h_store(i).start()

        @pl.when(i >= 1)
        def _():
            h_store(i - 1).wait()

        @pl.when(i + 1 < steps)
        def _():
            h_load(i + 1).start()

        @pl.when(i >= 3)
        def _():
            d_store(i - 3).wait()
        d_load(i).wait()
        for cp in x_tiles(i):
            cp.wait()
        for h in range(HBS):
            rows = slice(h * HB, (h + 1) * HB)
            prod = jnp.dot(dz[last, rows, :], x7[:, cols], preferred_element_type=f32)
            for q in range(last):
                for j in range(2):
                    prod = prod + jnp.dot(dz[q, rows, j * XCH:(j + 1) * XCH], xr[slot, j, q * XCH:(q + 1) * XCH, :], preferred_element_type=f32)
            dout[slot, rows, :] = din[slot, rows, :] + prod
        d_store(i).start()
        return c
    lax.fori_loop(0, steps, step, 0)
    for i in range(3):
        d_store(steps - 3 + i).wait()
    h_store(steps - 1).wait()


def finish(de_part, dzt_last, x_xp, x_xq, embed, dhid, stat_all, info_all, gsum_all):
    any_spec = pl.BlockSpec(memory_space=pl.ANY)
    vmem_spec = pl.BlockSpec(memory_space=pltpu.VMEM)
    f32, bf16 = jnp.float32, jnp.bfloat16
    dma = pltpu.SemaphoreType.DMA
    outs = [((ROWS, DIM), f32), ((TOK, DIM), bf16), ((GROUPS, 128), f32), ((1, 1), f32), ((1, DIM), f32), ((1, DIM), f32)]
    return pl.pallas_call(
        finish_kernel,
        name="finish",
        out_shape=[jax.ShapeDtypeStruct(s, d) for s, d in outs],
        in_specs=[any_spec] * 6 + [vmem_spec] * 3,
        out_specs=[any_spec] * 2 + [vmem_spec] * 4,
        scratch_shapes=[
            pltpu.VMEM((KT, DIM), bf16), pltpu.VMEM((3, 2, (DEFER - 1) * XCH, KT), bf16), pltpu.VMEM((DEFER, ROWS, KT), bf16), pltpu.VMEM((2, ZB, DIM), bf16), pltpu.VMEM((ZB, KT), f32),
            pltpu.VMEM((3, ROWS, KT), f32), pltpu.VMEM((3, ROWS, KT), f32), pltpu.VMEM((2, TOK // (DIM // KT), DIM), bf16),
            dma((4,)), dma((DEFER,)), dma((2,)), dma((3,)), dma((3,)), dma((2,)), dma((2,)),
        ],
        compiler_params=pltpu.CompilerParams(vmem_limit_bytes=67043328),
        cost_estimate=pl.CostEstimate(flops=2 * ROWS * DIM * KT * (DEFER + 1), bytes_accessed=130 * 2 ** 20, transcendentals=ROWS * KT),
    )(de_part, dzt_last, x_xp, x_xq, embed, dhid, stat_all, info_all, gsum_all)


def solution(mesh):
    def body(hidden, ln_gain, ln_bias, embed, targets, loss_mask):
        dp, rank = lax.axis_index('dp'), lax.axis_index('tp')
        shard = targets // ROWS
        block = jnp.bitwise_xor(shard, rank)
        row = targets % ROWS
        half = row // (ROWS // 2)
        sub = row % (ROWS // 2)
        piece = (block - 2) * 2 + jnp.bitwise_xor(half, dp)
        far = 2 * ROWS + (sub // PIECE_ROWS) * TILE + piece * PIECE_ROWS + sub % PIECE_ROWS
        tcol = jnp.where(block < 2, block * ROWS + row, far)
        info = jnp.stack([targets, loss_mask, tcol]).reshape(3, GROUPS, 128)
        outs = run_step(hidden, ln_gain.reshape(1, DIM), ln_bias.reshape(1, DIM), embed, info)
        stat_all, info_all, dhid, x_xp, x_xq, dzt_last, de_part, gsum_all = (outs[i] for i in (3, 4, 5, 7, 8, 12, 13, 14))
        d_embed, d_hidden, loss, mean, d_gain, d_bias = finish(de_part, dzt_last, x_xp, x_xq, embed, dhid, stat_all, info_all, gsum_all)
        return loss.reshape(TOK), mean.reshape(1), d_hidden, d_embed, d_gain.reshape(DIM), d_bias.reshape(DIM)

    token_rows = P(('dp', 'tp'))
    token_mat = P(('dp', 'tp'), None)
    return jax.shard_map(body, mesh=mesh, in_specs=(token_mat, P(), P(), P('tp', None), token_rows, token_rows), out_specs=(token_rows, P('dp'), token_mat, token_mat, P('dp'), P('dp')), check_vma=False)
```

```python
import functools

import jax
import jax.numpy as jnp
from jax import lax
from jax.experimental import pallas as pl
from jax.experimental.pallas import tpu as pltpu
from jax.sharding import PartitionSpec as P

LN_EPS = 1e-5
LOWEST = float(jnp.finfo(jnp.float32).min)

TOK = 2048
ROWS = 2048
DIM = 4096
VOCAB = 8192
TILE = 256
TILES = VOCAB // TILE
HB = 1024
HBS = TOK // HB
CHUNK = 32
PIECE_ROWS = 2 * CHUNK
NEAR = 2 * ROWS // TILE
PE_ROWS = 512
CHUNKS = ROWS // 2 // CHUNK
LN_ROWS = 256
STAT_ROWS = 32
PIECE = 32
LN_UNROLL = 4
XCH = 256
XCHS = TOK // XCH
KT = 512
DEFER = 4
WAIT_STEP = {4: 0, 9: 1, 14: 2}
ZB = 512
NCOL = 512
KCOL = 1024
NB_UNROLL = 4
NB_ROWS = 256
GROUPS = TOK // 128
NT = (((1,), (1,)), ((), ()))


def peers():
    dp, tp = lax.axis_index('dp'), lax.axis_index('tp')
    core = lax.rem(tp, 2)
    pair = tp - core
    other = 2 - pair
    part = pair + 1 - core
    return dp, tp, (dp, part), (dp, other + core), (dp, other + 1 - core), (1 - dp, tp)


def remote(src, dst, ssem, rsem, dev):
    return pltpu.make_async_remote_copy(
        src_ref=src, dst_ref=dst, send_sem=ssem, recv_sem=rsem, device_id=dev, device_id_type=pl.DeviceIdType.MESH)


def spread(row, rows, dst):
    dst[rows, :] = jnp.transpose(jnp.broadcast_to(row, (128, 128)))


def step_kernel(hid, gain, bias, emb, targets, mask,
                e_all, x_out, z_out, stat_all, info_all,
                dhid, x_part, x_xp, x_xq, dzt_own, dzt_out, dzt_part, dzt_last, de_part, gsum_all,
                tcol, stat_v, stats, infos, gb_v, gs_v, g8,
                h_sem, xo_sem, e_sem, eo_sem, z_sem, zt_sem, et_sem, small_sem, dzo_sem, big_sem, g_sem,
                xs_send, ys_send, ds_send, pe_send, sm_send, xt_send, xd_send, xp_send, dz_send, g_send,
                x_recv, y_recv, d_recv, pe_recv, info_recv, stat_recv, xt_recv, xd_recv, xp_recv, dz_recv, g_recv):
    bf16, f32 = jnp.bfloat16, jnp.float32
    dp, tp, part, xp, xq, yp = peers()
    core = lax.rem(tp, 2)
    xp_rank = 2 - (tp - core) + core
    xq_rank = 2 - (tp - core) + 1 - core
    group = ((1, part), (2, xp), (3, xq))
    barrier = pltpu.get_barrier_semaphore()
    for dev in (part, xp, xq, yp):
        pl.semaphore_signal(barrier, inc=1, device_id=dev, device_id_type=pl.DeviceIdType.MESH)
    pl.semaphore_wait(barrier, 4)

    def info_copies():
        return [remote(ref, info_all.at[tp, i], sm_send, info_recv.at[2 * p + i], dev)
                for p, dev in group for i, ref in enumerate((targets, mask))]

    def columns():
        for s in range(4):
            pair, odd = s - s % 2, s % 2
            near = ((tp - core) == pair).astype(jnp.int32)
            same = (core == odd).astype(jnp.int32)
            row = targets[...] - s * ROWS
            low = (row < ROWS // 2).astype(jnp.int32)
            sub = row - (1 - low) * (ROWS // 2)
            crossed = low * dp + (1 - low) * (1 - dp)
            piece = (1 - same) * 2 + crossed
            tile = (sub.astype(f32) * (1.0 / PIECE_ROWS)).astype(jnp.int32)
            far = 2 * ROWS + tile * (TILE - PIECE_ROWS) + sub + piece * PIECE_ROWS
            col = near * ((1 - same) * ROWS + row) + (1 - near) * far
            inside = (row >= 0) & (row < ROWS)
            tcol[...] = jnp.where(inside, col, 0 if s == 0 else tcol[...])

    def xrows(ref, j):
        return ref.at[pl.ds(pl.multiple_of(j * XCH, XCH), XCH)]

    def xt_copy(j):
        return remote(xrows(x_out, j), xrows(x_xp, j), xt_send, xt_recv.at[j], xp)

    def xd_copy(j):
        return remote(xrows(x_xp, j), xrows(x_xq, j), xd_send, xd_recv.at[j], part)

    def xt_event(j):
        xt_copy(j).wait_recv()
        xd_copy(j).start()
    xp_copy = remote(x_out, x_part, xp_send, xp_recv, part)

    def forward(m_s, scale_v, tc_v, mr_v, zt, et, xs, hbuf, ebuf, z0, z1, s_s, t_s, gb8):
        def tile_row(j):
            return ROWS * 2 + (j // 2) * TILE + lax.rem(j, 2) * CHUNK

        def x_copy(j):
            src = emb.at[pl.ds(pl.multiple_of(dp * (ROWS // 2) + j * CHUNK, CHUNK), CHUNK)]
            return remote(src, e_all.at[pl.ds(pl.multiple_of(tile_row(j), CHUNK), CHUNK)], xs_send, x_recv.at[j], xp)

        def piece(j, p):
            return e_all.at[pl.ds(pl.multiple_of(tile_row(j) + p * PIECE_ROWS, CHUNK), CHUNK)]

        def y_copy(j):
            return remote(piece(j, 0), piece(j, 1), ys_send, y_recv.at[j], yp)

        def d_copy(j, p):
            return remote(piece(j, p), piece(j, p + 2), ds_send, d_recv.at[j // 2], part)

        def pe_copy(i):
            return remote(emb.at[pl.ds(pl.multiple_of(i * PE_ROWS, PE_ROWS), PE_ROWS)],
                          e_all.at[pl.ds(pl.multiple_of(ROWS + i * PE_ROWS, PE_ROWS), PE_ROWS)], pe_send, pe_recv.at[i], part)


        def h_copy(i):
            return pltpu.make_async_copy(hid.at[pl.ds(pl.multiple_of(i * LN_ROWS, LN_ROWS), LN_ROWS)], hbuf.at[lax.rem(i, 2)], h_sem.at[lax.rem(i, 2)])
        h_copy(0).start()

        for cp in info_copies():
            cp.start()

        def start_x(j, c):
            x_copy(j).start()
            return c
        lax.fori_loop(0, CHUNKS, start_x, 0)

        def start_pe(i, c):
            pe_copy(i).start()
            return c
        lax.fori_loop(0, ROWS // PE_ROWS, start_pe, 0)

        def e_load(t):
            slot = lax.rem(t, 2)
            return pltpu.make_async_copy(e_all.at[pl.ds(pl.multiple_of(t * TILE, TILE), TILE)], ebuf.at[slot], e_sem.at[slot])

        def e_load_own(t):
            slot = lax.rem(t, 2)
            return pltpu.make_async_copy(emb.at[pl.ds(pl.multiple_of(t * TILE, TILE), TILE)], ebuf.at[slot], e_sem.at[slot])
        e_load_own(0).start()

        def x_event(j):
            x_copy(j).wait_recv()
            y_copy(j).start()
            d_copy(j, 0).start()

        def y_event(j):
            y_copy(j).wait_recv()
            d_copy(j, 1).start()

        def p_event(k):
            rows = e_all.at[pl.ds(pl.multiple_of(2 * ROWS + k * TILE + TILE // 2, TILE // 2), TILE // 2)]
            pltpu.make_async_copy(rows, rows, d_recv.at[k]).wait()
            e_load(NEAR + k).start()

        own_info = [pltpu.make_async_copy(ref, info_all.at[tp, i], small_sem.at[0]) for i, ref in enumerate((targets, mask))]
        for cp in own_info:
            cp.start()
        columns()
        gb8[0] = jnp.broadcast_to(gain[...], (8, DIM))
        gb8[1] = jnp.broadcast_to(bias[...], (8, DIM))

        def ln_tile(i, c):
            slot = lax.rem(i, 2)

            @pl.when(i + 1 < TOK // LN_ROWS)
            def _():
                h_copy(i + 1).start()
            h_copy(i).wait()

            @pl.when(i == 6)
            def _():
                x_event(0)

            def ln_rows(r, c2):
                base = r * LN_UNROLL * 16

                def at(u):
                    return pl.ds(pl.multiple_of(base + u * 16, 16), 16)

                def part_of(u, k):
                    return hbuf[slot, at(u), k * 128:(k + 1) * 128].astype(jnp.float32)
                means, rstds = [], []
                for u in range(LN_UNROLL):
                    tot = part_of(u, 0)
                    for k in range(1, DIM // 128):
                        tot = tot + part_of(u, k)
                    means.append(jnp.broadcast_to(jnp.sum(tot, axis=-1, keepdims=True) * (1.0 / DIM), (16, 128)))
                for u in range(LN_UNROLL):
                    tot = jnp.zeros((16, 128), jnp.float32)
                    for k in range(DIM // 128):
                        diff = part_of(u, k) - means[u]
                        tot = tot + diff * diff
                    var = jnp.sum(tot, axis=-1, keepdims=True) * (1.0 / DIM)
                    rstds.append(jnp.broadcast_to(lax.rsqrt(var + LN_EPS), (16, 128)))
                for u in range(LN_UNROLL):
                    row = pl.ds(pl.multiple_of(i * LN_ROWS + base + u * 16, 16), 16)
                    mr_v[0, row, :] = means[u]
                    mr_v[1, row, :] = rstds[u]
                    for k in range(DIM // 128):
                        cols = slice(k * 128, (k + 1) * 128)
                        g2 = jnp.concatenate([gb8[0, :, cols]] * 2, axis=0)
                        b2 = jnp.concatenate([gb8[1, :, cols]] * 2, axis=0)
                        xs[row, cols] = ((part_of(u, k) - means[u]) * rstds[u] * g2 + b2).astype(jnp.bfloat16)
                return c2
            lax.fori_loop(0, LN_ROWS // (16 * LN_UNROLL), ln_rows, 0)
            rows = pl.ds(pl.multiple_of(i * LN_ROWS, LN_ROWS), LN_ROWS)
            pltpu.make_async_copy(xs.at[rows], x_out.at[rows], xo_sem).start()
            return c
        lax.fori_loop(0, TOK // LN_ROWS, ln_tile, 0)

        m_s[...] = jnp.full((TOK, 128), LOWEST, jnp.float32)
        s_s[...] = jnp.zeros((TOK, 128), jnp.float32)
        t_s[...] = jnp.zeros((TOK, 128), jnp.float32)
        for r in range(GROUPS):
            spread(tcol[r:r + 1, :], slice(r * 128, (r + 1) * 128), tc_v)
        z1[...] = jnp.full((HB, TILE), LOWEST, jnp.float32)

        zs = (z0, z1)

        def product(t, h):
            for r in range(0, HB, 512):
                zs[h][r:r + 512, :] = lax.dot_general(
                    xs[h * HB + r:h * HB + r + 512, :], ebuf[lax.rem(t, 2)], NT, preferred_element_type=jnp.float32)

        def statistics(t, h):
            z = zs[h]
            lane = lax.broadcasted_iota(jnp.int32, (STAT_ROWS, 128), 1)
            for r in range(0, HB, STAT_ROWS):
                rows = slice(h * HB + r, h * HB + r + STAT_ROWS)
                zk = [z[r:r + STAT_ROWS, k * 128:(k + 1) * 128] for k in range(TILE // 128)]
                old = m_s[rows, :]
                new = jnp.maximum(jnp.maximum(zk[0], zk[1]), old)
                tot = s_s[rows, :] * jnp.exp(old - new)
                tgt = t_s[rows, :]
                diff = tc_v[rows, :] - t * TILE
                for k in range(TILE // 128):
                    tot = tot + jnp.exp(zk[k] - new)
                    tgt = tgt + jnp.where(diff == lane + k * 128, zk[k], 0.0)
                m_s[rows, :] = new
                s_s[rows, :] = tot
                t_s[rows, :] = tgt

        def z_copy(t, h):
            return pltpu.make_async_copy(
                zs[h], z_out.at[pl.ds(h * HB, HB), pl.ds(pl.multiple_of(t * TILE, TILE), TILE)], z_sem.at[h])

        def start_events(t):
            @pl.when(t < TILES - 1)
            def _():
                x_event(t + 1)

            @pl.when(t == TILES - 2)
            def _():
                xt_copy(0).start()

            @pl.when(t == TILES - 1)
            def _():
                y_event(TILES - 1)
                p_event(TILES - 1 - NEAR)
            e_load(t).wait()

            @pl.when(t < ROWS // TILE)
            def _():
                slot = lax.rem(t, 2)
                pltpu.make_async_copy(ebuf.at[slot], e_all.at[pl.ds(pl.multiple_of(t * TILE, TILE), TILE)], eo_sem.at[slot]).start()

        def middle_events(t):
            @pl.when(t < TILES - 1)
            def _():
                y_event(t)

            @pl.when((t >= 1) & (t < ROWS // TILE + 1))
            def _():
                slot = lax.rem(t - 1, 2)
                pltpu.make_async_copy(ebuf.at[slot], e_all.at[pl.ds(0, TILE)], eo_sem.at[slot]).wait()

            @pl.when(t == NEAR)
            def _():
                pltpu.make_async_copy(xs, x_out, xo_sem).wait()

            @pl.when(t < ROWS // TILE - 1)
            def _():
                e_load_own(t + 1).start()

            @pl.when((t >= ROWS // TILE - 1) & (t < NEAR - 1))
            def _():
                @pl.when(lax.rem(t + 1, PE_ROWS // TILE) == 0)
                def _():
                    pe_copy((t + 1 - ROWS // TILE) // (PE_ROWS // TILE)).wait_recv()
                e_load(t + 1).start()

            @pl.when((t >= NEAR - 1) & (t < TILES - 2))
            def _():
                p_event(t - (NEAR - 1))

            @pl.when(t == TILES - 2)
            def _():
                for k, h in ((0, 0), (1, 0), (0, 1)):
                    z_load(zt, k, h).start()
                et_load(et, 0).start()

            @pl.when(t == NEAR + 1)
            def _():
                for cp in info_copies():
                    cp.wait_recv()
                for cp in own_info:
                    cp.wait()
                load = pltpu.make_async_copy(info_all, infos, small_sem.at[0])
                load.start()
                load.wait()
                count = jnp.broadcast_to(token_count(), (1, 128))
                for r in range(GROUPS):
                    spread(mask[r:r + 1, :].astype(f32) / count, slice(r * 128, (r + 1) * 128), scale_v)

        def step(t, c):
            @pl.when(t > 0)
            def _():
                z_copy(t - 1, 1).start()
            start_events(t)

            @pl.when(t > 0)
            def _():
                z_copy(t - 1, 0).wait()
            statistics(t - 1, 1)
            product(t, 0)
            z_copy(t, 0).start()
            middle_events(t)

            @pl.when(t > 0)
            def _():
                z_copy(t - 1, 1).wait()
            statistics(t, 0)
            product(t, 1)
            return c
        last = TILES - 1
        lax.fori_loop(0, TILES, step, 0)
        z_copy(last, 1).start()
        statistics(last, 1)

        def finish(i, c):
            for u in range(8):
                r = i * 8 + u
                rows = pl.ds(pl.multiple_of(r * 128, 128), 128)
                m = m_s[rows, :]
                top = jnp.max(m, axis=-1, keepdims=True)
                tot = jnp.sum(s_s[rows, :] * jnp.exp(m - top), axis=-1, keepdims=True)
                lse = jnp.broadcast_to(top + jnp.log(tot), (128, 128))
                tgt = jnp.broadcast_to(jnp.sum(t_s[rows, :], axis=-1, keepdims=True), (128, 128))
                m_s[rows, :] = lse
                stat_v[0, pl.ds(r, 1), :] = jnp.transpose(lse)[0:1, :]
                stat_v[1, pl.ds(r, 1), :] = jnp.transpose(tgt)[0:1, :]
            return c
        lax.fori_loop(0, TOK // 1024, finish, 0)
        for h in range(2):
            z_copy(last, h).wait()
        half = e_all.at[pl.ds(0, ROWS // 2)]
        pltpu.make_async_copy(half, half, xs_send).wait()
        pltpu.make_async_copy(half, half, ys_send).wait()
        full = e_all.at[pl.ds(0, ROWS)]
        pltpu.make_async_copy(full, full, ds_send).wait()
        pltpu.make_async_copy(full, full, pe_send).wait()
        pltpu.make_async_copy(stat_v, stat_all.at[tp], small_sem.at[1]).start()
        for p, dev in group:
            remote(stat_v, stat_all.at[tp], sm_send, stat_recv.at[p], dev).start()

        def start_xt(j, c):
            xt_copy(j).start()
            return c
        lax.fori_loop(1, XCHS, start_xt, 0)
        xp_copy.start()

    def z_load(zt, k, h):
        slot = lax.rem(k, 2)
        rows = slice(h * HB, (h + 1) * HB)
        return pltpu.make_async_copy(
            z_out.at[rows, pl.ds(pl.multiple_of(k * KT, KT), KT)], zt.at[slot, rows], zt_sem.at[2 * h + slot])

    def et_load(et, k):
        slot = lax.rem(k, 2)
        return pltpu.make_async_copy(e_all.at[pl.ds(pl.multiple_of(k * KT, KT), KT)], et.at[slot], et_sem.at[slot])

    def dzt_copy(k):
        rows = pl.ds(pl.multiple_of(lax.rem(k, 4) * KT, KT), KT)
        return remote(dzt_out.at[rows], dzt_part.at[rows], dz_send, dz_recv.at[lax.rem(k, 4)], part)

    def token_count():
        return jnp.sum(infos[:, 1].astype(f32))

    def token_grads(lse_v, scale_v, tcol_v, mr, zt, et, acc):
        def d_phase(da, db, dzt):
            def dzt_store(k, ref):
                slot = lax.rem(k, 2)
                return pltpu.make_async_copy(dzt.at[slot], ref.at[pl.ds(pl.multiple_of(lax.rem(k, 4) * KT, KT), KT)], eo_sem.at[slot])
            lane = lax.broadcasted_iota(jnp.int32, (PIECE, 128), 1)

            def piece(dst, rows, low, k, tie):
                slot = lax.rem(k, 2)
                lse = lse_v[rows, :]
                if tie is not None:
                    floor = 0.0 - jnp.maximum(0.0 - tie, -LOWEST)
                    lse = jnp.maximum(lse, jnp.concatenate([floor] * (PIECE // 8), axis=0))
                scale = scale_v[rows, :]
                diff = tcol_v[rows, :] - k * KT
                for g in range(KT // 128):
                    cols = slice(g * 128, (g + 1) * 128)
                    hot = (diff == lane + g * 128).astype(f32)
                    val = (jnp.exp(zt[slot, rows, cols] - lse) - hot) * scale
                    dst[low, cols] = val.astype(bf16)

            def half_step(k, src, dst, base, dst_base, dst_k):
                slot = lax.rem(k, 2)
                per = HB // (DIM // NCOL)
                for n in range(DIM // NCOL):
                    cols = slice(n * NCOL, (n + 1) * NCOL)
                    prod = jnp.dot(src[...], et[slot, :, cols], preferred_element_type=f32)
                    acc[base:base + HB, cols] = jnp.where(k == 0, 0.0, acc[base:base + HB, cols]) + prod
                    for q in range(0, per, PIECE):
                        at = q * HB // per
                        low = n * per + q
                        piece(dst, slice(dst_base + low, dst_base + low + PIECE), slice(low, low + PIECE), dst_k, prod[at:at + 8, 0:128])
                    if n * per % 256 == 0:
                        low = n * per
                        dzt[slot, :, base + low:base + low + 256] = jnp.transpose(src[low:low + 256, :])

            z_load(zt, 0, 0).wait()

            def first(i, c):
                rows = pl.ds(pl.multiple_of(i * PIECE, PIECE), PIECE)
                piece(da, rows, rows, 0, None)
                return c
            lax.fori_loop(0, HB // PIECE, first, 0)

            def step(k, c):
                @pl.when(k + 2 < VOCAB // KT)
                def _():
                    z_load(zt, k + 2, 0).start()

                @pl.when(k + 1 < VOCAB // KT)
                def _():
                    z_load(zt, k + 1, 1).start()
                    et_load(et, k + 1).start()
                    z_load(zt, k + 1, 0).wait()
                for at, j in WAIT_STEP.items():
                    @pl.when(k == at)
                    def _(j=j):
                        xt_event(j)

                @pl.when((k >= 2) & (k < 10))
                def _():
                    dzt_store(k, dzt_own).wait()

                @pl.when((k >= 6) & (k < 10))
                def _():
                    dzt_copy(k - 2).start()
                et_load(et, k).wait()
                z_load(zt, k, 1).wait()
                half_step(k, da, db, 0, HB, k)
                half_step(k, db, da, HB, 0, k + 1)

                @pl.when(k < 4)
                def _():
                    dzt_store(k, dzt_own).start()

                @pl.when((k >= 4) & (k < 8))
                def _():
                    dzt_store(k, dzt_out).start()
                return c
            lax.fori_loop(0, VOCAB // KT, step, 0)
        half = pltpu.VMEM((HB, KT), bf16)
        pl.run_scoped(d_phase, half, half, pltpu.VMEM((2, KT, TOK), bf16))

        def n_phase(hb, ob):
            def h_load(i):
                slot = lax.rem(i, 2)
                return pltpu.make_async_copy(hid.at[pl.ds(pl.multiple_of(i * NB_ROWS, NB_ROWS), NB_ROWS)], hb.at[slot], z_sem.at[slot])

            def o_store(i):
                slot = lax.rem(i, 2)
                return pltpu.make_async_copy(ob.at[slot], dhid.at[pl.ds(pl.multiple_of(i * NB_ROWS, NB_ROWS), NB_ROWS)], e_sem.at[slot])
            h_load(0).start()
            gb_v[...] = jnp.zeros(gb_v.shape, jnp.float32)
            g8[...] = jnp.broadcast_to(gain[...], (8, DIM))

            def tile(i, c):
                slot = lax.rem(i, 2)

                @pl.when(i + 1 < TOK // NB_ROWS)
                def _():
                    h_load(i + 1).start()

                @pl.when(i >= 2)
                def _():
                    o_store(i - 2).wait()
                h_load(i).wait()

                def rows_body(r, c2):
                    units = range(NB_UNROLL)
                    base = r * 16 * NB_UNROLL
                    low = [pl.ds(pl.multiple_of(base + u * 16, 16), 16) for u in units]
                    row = [pl.ds(pl.multiple_of(i * NB_ROWS + base + u * 16, 16), 16) for u in units]
                    zero = jnp.zeros((16, 128), jnp.float32)
                    sum1, sum3 = [zero] * NB_UNROLL, [zero] * NB_UNROLL

                    def load(u, cols):
                        dx = acc[row[u], cols]
                        xhat = (hb[slot, low[u], cols].astype(jnp.float32) - mr[0, row[u], :]) * mr[1, row[u], :]
                        return dx, xhat, dx * jnp.concatenate([g8[:, cols]] * 2, axis=0)
                    for k in range(DIM // 128):
                        cols = slice(k * 128, (k + 1) * 128)
                        d_gain, d_bias = gb_v[0, :, cols], gb_v[1, :, cols]
                        for u in units:
                            dx, xhat, gx = load(u, cols)
                            sum1[u] = sum1[u] + gx
                            sum3[u] = sum3[u] + gx * xhat
                            dgx = dx * xhat
                            d_gain = d_gain + (dgx[0:8] + dgx[8:16])
                            d_bias = d_bias + (dx[0:8] + dx[8:16])
                        gb_v[0, :, cols] = d_gain
                        gb_v[1, :, cols] = d_bias
                    slope, shift = [], []
                    for u in units:
                        mean, rstd = mr[0, row[u], :], mr[1, row[u], :]
                        c1 = jnp.broadcast_to(jnp.sum(sum1[u], axis=-1, keepdims=True) * (1.0 / DIM), (16, 128))
                        c3 = jnp.broadcast_to(jnp.sum(sum3[u], axis=-1, keepdims=True) * (1.0 / DIM), (16, 128))
                        slope.append(c3 * rstd * rstd)
                        shift.append(slope[u] * mean - c1 * rstd)
                    for u in units:
                        rstd = mr[1, row[u], :]
                        for k in range(DIM // 128):
                            cols = slice(k * 128, (k + 1) * 128)
                            gx = acc[row[u], cols] * jnp.concatenate([g8[:, cols]] * 2, axis=0)
                            ob[slot, low[u], cols] = (gx * rstd - hb[slot, low[u], cols].astype(f32) * slope[u] + shift[u]).astype(bf16)
                    return c2
                lax.fori_loop(0, NB_ROWS // (16 * NB_UNROLL), rows_body, 0)
                o_store(i).start()
                return c
            lax.fori_loop(0, TOK // NB_ROWS, tile, 0)
            for i in range(2):
                o_store(TOK // NB_ROWS - 2 + i).wait()
            gs_v[0:1, :] = jnp.sum(gb_v[0], axis=0, keepdims=True)
            gs_v[1:2, :] = jnp.sum(gb_v[1], axis=0, keepdims=True)
        pl.run_scoped(n_phase, pltpu.VMEM((2, NB_ROWS, DIM), bf16), pltpu.VMEM((2, NB_ROWS, DIM), bf16))

    def weight_grads(acc):
        own = pltpu.make_async_copy(gs_v, gsum_all.at[tp], g_sem)
        xt_event(3)

        def e_phase(eo, xt, dzb, zs, z1):
            eo_load = pltpu.make_async_copy(emb, eo, big_sem)

            def x_load(ref, row, slot):
                return pltpu.make_async_copy(ref.at[pl.ds(pl.multiple_of(row, KT), KT)], xt.at[slot], z_sem.at[slot])

            def dz_load(ref, col, slot):
                return pltpu.make_async_copy(ref.at[:, pl.ds(pl.multiple_of(col, KT), KT)], dzb.at[slot], e_sem.at[slot])

            def start_local(i):
                slot = lax.rem(i, 2)

                @pl.when(i < 4)
                def _():
                    x_load(x_out, i * KT, slot).start()
                    dz_load(dzt_own, i * KT, slot).start()

                @pl.when(i >= 4)
                def _():
                    x_load(x_part, (i - 4) * KT, slot).start()
                    dz_load(dzt_part, (i - 4) * KT, slot).start()

            def add(slot, first):
                def mul(h, c2):
                    rows = pl.ds(pl.multiple_of(h * HB, HB), HB)
                    for n in range(0, DIM, NCOL):
                        prod = jnp.dot(dzb[slot, rows, :], xt[slot, :, n:n + NCOL], preferred_element_type=f32)
                        acc[rows, n:n + NCOL] = jnp.where(first, 0.0, acc[rows, n:n + NCOL]) + prod
                    return c2
                lax.fori_loop(0, HBS, mul, 0)

            start_local(0)

            def rem_load(r):
                slot = lax.rem(r, 2)
                return [pltpu.make_async_copy(xrows(ref, r), xt.at[slot, pl.ds(i * XCH, XCH)], z_sem.at[slot])
                        for i, ref in enumerate((x_xp, x_xq))]

            def local(i, c):
                slot = lax.rem(i, 2)

                @pl.when(i == 0)
                def _():
                    eo_load.start()

                @pl.when(i == 2)
                def _():
                    xp_copy.wait_recv()

                    def wait_dz(q, c2):
                        dzt_copy(q).wait_recv()
                        return c2
                    lax.fori_loop(0, 4, wait_dz, 0)

                @pl.when(i == 1)
                def _():
                    own.start()
                    for p, dev in group:
                        remote(gs_v, gsum_all.at[tp], g_send, g_recv.at[p], dev).start()

                @pl.when(i == 6)
                def _():
                    xt_event(4)

                @pl.when(i < 7)
                def _():
                    start_local(i + 1)

                @pl.when(i == 7)
                def _():
                    xd_copy(0).wait_recv()
                    for cp in rem_load(0):
                        cp.start()
                x_load(x_out, 0, slot).wait()
                dz_load(dzt_own, 0, slot).wait()
                add(slot, i == 0)
                return c
            lax.fori_loop(0, 8, local, 0)
            eo_load.wait()
            for p, dev in group:
                remote(stat_v, stat_all.at[tp], sm_send, stat_recv.at[p], dev).wait_recv()
            pltpu.make_async_copy(stat_v, stat_all.at[tp], small_sem.at[1]).wait()
            stat_load = pltpu.make_async_copy(stat_all, stats, small_sem.at[1])
            stat_load.start()
            stat_load.wait()
            count = jnp.broadcast_to(token_count(), (1, 128))

            def far(r, c):
                slot = lax.rem(r, 2)

                @pl.when(r == 1)
                def _():
                    xt_event(5)

                @pl.when(r == 4)
                def _():
                    xt_event(6)

                def fetch():
                    xd_copy(r + 1).wait_recv()
                    for cp in rem_load(r + 1):
                        cp.start()
                pl.when(r < XCHS - 2)(fetch)
                x_load(x_out, 0, slot).wait()

                @pl.when(r == XCHS - DEFER)
                def _():
                    pltpu.make_async_copy(acc, de_part, big_sem).start()

                @pl.when(r > XCHS - DEFER + 1)
                def _():
                    dz_out(0, slot).wait()

                far_rows = []
                for g in range(4):
                    who = xp_rank if g < 2 else xq_rank
                    at = pl.ds(2 * r + g % 2, 1)
                    far_rows.append((stats[who, 0, at, :], infos[who, 1, at, :].astype(f32) / count, infos[who, 0, at, :] - tp * ROWS))

                def logits(h2, c2):
                    @pl.when((r == XCHS - 2) & (h2 == 1))
                    def _():
                        xt_event(XCHS - 1)

                    def multiply(h, z):
                        for k in range(0, DIM, KCOL):
                            prod = lax.dot_general(eo[pl.ds(pl.multiple_of(h * ZB, ZB), ZB), k:k + KCOL], xt[slot, :, k:k + KCOL], NT, preferred_element_type=f32)
                            z[...] = prod if k == 0 else z[...] + prod

                    def convert(h, z):
                        for q in range(ZB // 32):
                            row = h * ZB + q * 32
                            line = lax.broadcasted_iota(jnp.int32, (32, 128), 0)
                            for g, (lse, scale, trel) in enumerate(far_rows):
                                cols = slice(g * 128, (g + 1) * 128)
                                hot = ((trel - row) == line).astype(f32)
                                val = (jnp.exp(z[q * 32:(q + 1) * 32, cols] - lse) - hot) * scale
                                dzb[slot, pl.ds(pl.multiple_of(row, 32), 32), cols] = val.astype(bf16)
                    multiply(2 * h2, zs)
                    multiply(2 * h2 + 1, z1)
                    convert(2 * h2, zs)
                    convert(2 * h2 + 1, z1)
                    return c2
                lax.fori_loop(0, ROWS // (2 * ZB), logits, 0)

                @pl.when(r < XCHS - DEFER)
                def _():
                    def mul(h, c2):
                        rows = pl.ds(pl.multiple_of(h * HB, HB), HB)
                        for n in range(0, DIM, NCOL):
                            acc[rows, n:n + NCOL] += jnp.dot(dzb[slot, rows, :], xt[slot, :, n:n + NCOL], preferred_element_type=jnp.float32)
                        return c2
                    lax.fori_loop(0, HBS, mul, 0)

                @pl.when(r >= XCHS - DEFER)
                def _():
                    dz_out(r - (XCHS - DEFER), slot).start()
                return c

            def dz_out(q, slot):
                return pltpu.make_async_copy(dzb.at[slot], dzt_last.at[q], dzo_sem.at[slot])
            lax.fori_loop(0, XCHS - 1, far, 0)
            for slot in range(2):
                dz_out(0, slot).wait()
            xd_copy(XCHS - 1).wait_recv()
            pltpu.make_async_copy(acc, de_part, big_sem).wait()
        pl.run_scoped(e_phase, pltpu.VMEM((ROWS, DIM), jnp.bfloat16), pltpu.VMEM((2, KT, DIM), jnp.bfloat16),
                      pltpu.VMEM((2, ROWS, KT), jnp.bfloat16), pltpu.VMEM((ZB, KT), f32), pltpu.VMEM((ZB, KT), f32))

        own.wait()

    wide = pltpu.VMEM((TOK, 128), f32)
    big = pltpu.VMEM((TOK, DIM), f32)

    def tokens(m_s, scale_v, tc_v, mr_v, zt, et):
        kept = (m_s, scale_v, tc_v, mr_v, zt, et)
        pl.run_scoped(functools.partial(forward, *kept), pltpu.VMEM((TOK, DIM), bf16), pltpu.VMEM((2, LN_ROWS, DIM), bf16),
                      pltpu.VMEM((2, TILE, DIM), bf16), pltpu.VMEM((HB, TILE), f32), pltpu.VMEM((HB, TILE), f32), wide, wide,
                      pltpu.VMEM((2, 8, DIM), f32))
        pl.run_scoped(functools.partial(token_grads, *kept), big)
    pl.run_scoped(tokens, wide, wide, pltpu.VMEM((TOK, 128), jnp.int32), pltpu.VMEM((2, TOK, 128), f32),
                  pltpu.VMEM((2, TOK, KT), f32), pltpu.VMEM((2, KT, DIM), bf16))
    pl.run_scoped(weight_grads, big)

    pltpu.make_async_copy(x_out, x_out, xt_send).wait()
    pltpu.make_async_copy(x_out, x_out, xd_send).wait()
    xp_copy.wait_send()
    pltpu.make_async_copy(dzt_out, dzt_out, dz_send).wait()
    for cp in info_copies():
        cp.wait_send()
    for p, dev in group:
        remote(stat_v, stat_all.at[tp], sm_send, stat_recv.at[p], dev).wait_send()
        remote(gs_v, gsum_all.at[tp], g_send, g_recv.at[p], dev).wait()


def run_step(hidden, gain, bias, embed, targets, mask):
    any_spec = pl.BlockSpec(memory_space=pl.ANY)
    vmem_spec = pl.BlockSpec(memory_space=pltpu.VMEM)
    f32, bf16, i32 = jnp.float32, jnp.bfloat16, jnp.int32
    dma = pltpu.SemaphoreType.DMA
    small, ints = (4, 2, GROUPS, 128), (4, 2, GROUPS, 128)
    mat, square = ((TOK, DIM), bf16), ((ROWS, TOK), bf16)
    shapes = [((VOCAB, DIM), bf16), mat, ((TOK, VOCAB), f32), (small, f32), (ints, i32),
              mat, mat, mat, mat, square, square, square, ((DEFER - 1, ROWS, KT), bf16), ((ROWS, DIM), f32), ((4, 2, DIM), f32)]
    return pl.pallas_call(
        step_kernel,
        name="step",
        out_shape=[jax.ShapeDtypeStruct(s, d) for s, d in shapes],
        in_specs=[any_spec, vmem_spec, vmem_spec, any_spec, vmem_spec, vmem_spec],
        out_specs=[any_spec] * len(shapes),
        scratch_shapes=[
            pltpu.VMEM((GROUPS, 128), i32), pltpu.VMEM((2, GROUPS, 128), f32), pltpu.VMEM(small, f32), pltpu.VMEM(ints, i32),
            pltpu.VMEM((2, 8, DIM), f32), pltpu.VMEM((2, DIM), f32), pltpu.VMEM((8, DIM), f32),
            dma((2,)), dma, dma((2,)), dma((2,)), dma((2,)), dma((4,)), dma((2,)), dma((2,)), dma((2,)), dma, dma,
            dma, dma, dma, dma, dma, dma, dma, dma, dma, dma,
            dma((CHUNKS,)), dma((CHUNKS,)), dma((TILES - NEAR,)), dma((ROWS // PE_ROWS,)), dma((8,)), dma((4,)),
            dma((XCHS,)), dma((XCHS,)), dma, dma((4,)), dma((4,)),
        ],
        compiler_params=pltpu.CompilerParams(collective_id=0, has_side_effects=True, vmem_limit_bytes=67043328),
        cost_estimate=pl.CostEstimate(flops=12 * TOK * VOCAB * DIM, bytes_accessed=700 * 2 ** 20, transcendentals=3 * TOK * VOCAB),
    )(hidden, gain, bias, embed, targets, mask)


def finish_kernel(de_in, dzt_last, x_xp, x_xq, emb, dh_in, stat_all, info_all, gsum_all,
                  de_out, dh_out, loss, mean, d_gain, d_bias,
                  x7, xr, dz, eb, zs, din, dout, hb, x_sem, z_sem, e_sem, di_sem, do_sem, hi_sem, ho_sem):
    f32, bf16 = jnp.float32, jnp.bfloat16
    last = DEFER - 1

    def x_last():
        rows = pl.ds((XCHS - 1) * XCH, XCH)
        return [pltpu.make_async_copy(ref.at[rows], x7.at[pl.ds(i * XCH, XCH)], x_sem.at[3]) for i, ref in enumerate((x_xp, x_xq))]

    def x_tiles(i):
        slot = lax.rem(i, 3)
        cols = pl.ds(pl.multiple_of(i * KT, KT), KT)
        rows = pl.ds((XCHS - DEFER) * XCH, last * XCH)
        return [pltpu.make_async_copy(ref.at[rows, cols], xr.at[slot, j], x_sem.at[slot]) for j, ref in enumerate((x_xp, x_xq))]

    def e_load(h):
        slot = lax.rem(h, 2)
        return pltpu.make_async_copy(emb.at[pl.ds(pl.multiple_of(h * ZB, ZB), ZB)], eb.at[slot], e_sem.at[slot])

    def z_load(q):
        return pltpu.make_async_copy(dzt_last.at[q], dz.at[q], z_sem.at[q])

    def tile(ref, i):
        return ref.at[:, pl.ds(pl.multiple_of(i * KT, KT), KT)]

    def d_load(i):
        slot = lax.rem(i, 3)
        return pltpu.make_async_copy(tile(de_in, i), din.at[slot], di_sem.at[slot])

    def d_store(i):
        slot = lax.rem(i, 3)
        return pltpu.make_async_copy(dout.at[slot], tile(de_out, i), do_sem.at[slot])
    steps = DIM // KT
    per = TOK // steps

    def h_load(i):
        slot = lax.rem(i, 2)
        return pltpu.make_async_copy(dh_in.at[pl.ds(pl.multiple_of(i * per, per), per)], hb.at[slot], hi_sem.at[slot])

    def h_store(i):
        slot = lax.rem(i, 2)
        return pltpu.make_async_copy(hb.at[slot], dh_out.at[pl.ds(pl.multiple_of(i * per, per), per)], ho_sem.at[slot])
    for cp in x_last():
        cp.start()
    e_load(0).start()
    e_load(1).start()

    def tile_loads(i):
        for cp in (*x_tiles(i), d_load(i)):
            cp.start()

    tp = lax.axis_index('tp')
    core = lax.rem(tp, 2)
    other = 2 - (tp - core)
    weights = info_all[:, 1].astype(f32)
    total = jnp.sum(weights)
    all_loss = (stat_all[:, 0] - stat_all[:, 1]) * weights
    loss[...] = (stat_all[tp, 0] - stat_all[tp, 1]) * info_all[tp, 1].astype(f32)
    mean[...] = jnp.broadcast_to(jnp.sum(all_loss), (1, 1)) / jnp.broadcast_to(total, (1, 1))
    sums = ((gsum_all[0] + gsum_all[1]) + gsum_all[2]) + gsum_all[3]
    d_gain[...] = sums[0:1]
    d_bias[...] = sums[1:2]
    count = jnp.broadcast_to(total, (1, 128))
    far_rows = []
    for g in range(4):
        who = other + core if g < 2 else other + 1 - core
        at = slice(GROUPS - 2 + g % 2, GROUPS - 1 + g % 2)
        far_rows.append((stat_all[who, 0, at, :], info_all[who, 1, at, :].astype(f32) / count, info_all[who, 0, at, :] - tp * ROWS))
    pltpu.make_async_copy(x7, x7, x_sem.at[3]).wait()

    def logits(h, c):
        slot = lax.rem(h, 2)
        e_load(h).wait()
        for k in range(0, DIM, KCOL):
            prod = lax.dot_general(eb[slot, :, k:k + KCOL], x7[:, k:k + KCOL], NT, preferred_element_type=f32)
            zs[...] = prod if k == 0 else zs[...] + prod

        @pl.when(h == 0)
        def _():
            e_load(2).start()
            z_load(0).start()
            z_load(1).start()

        @pl.when(h == 1)
        def _():
            e_load(3).start()
            z_load(2).start()

        @pl.when(h == 2)
        def _():
            tile_loads(0)
            h_load(0).start()

        @pl.when(h == 3)
        def _():
            tile_loads(1)
        for q in range(ZB // 32):
            row = h * ZB + q * 32
            line = lax.broadcasted_iota(jnp.int32, (32, 128), 0)
            for g, (lse, scale, trel) in enumerate(far_rows):
                cols = slice(g * 128, (g + 1) * 128)
                hot = ((trel - row) == line).astype(f32)
                val = (jnp.exp(zs[q * 32:(q + 1) * 32, cols] - lse) - hot) * scale
                dz[last, pl.ds(pl.multiple_of(row, 32), 32), cols] = val.astype(bf16)
        return c
    lax.fori_loop(0, ROWS // ZB, logits, 0)
    for q in range(last):
        z_load(q).wait()

    def step(i, c):
        slot = lax.rem(i, 3)
        cols = pl.ds(pl.multiple_of(i * KT, KT), KT)

        @pl.when(i + 2 < steps)
        def _():
            tile_loads(i + 2)
        h_load(i).wait()
        h_store(i).start()

        @pl.when(i >= 1)
        def _():
            h_store(i - 1).wait()

        @pl.when(i + 1 < steps)
        def _():
            h_load(i + 1).start()

        @pl.when(i >= 3)
        def _():
            d_store(i - 3).wait()
        d_load(i).wait()
        for cp in x_tiles(i):
            cp.wait()
        for h in range(HBS):
            rows = slice(h * HB, (h + 1) * HB)
            prod = jnp.dot(dz[last, rows, :], x7[:, cols], preferred_element_type=f32)
            for q in range(last):
                for j in range(2):
                    prod = prod + jnp.dot(dz[q, rows, j * XCH:(j + 1) * XCH], xr[slot, j, q * XCH:(q + 1) * XCH, :], preferred_element_type=f32)
            dout[slot, rows, :] = din[slot, rows, :] + prod
        d_store(i).start()
        return c
    lax.fori_loop(0, steps, step, 0)
    for i in range(3):
        d_store(steps - 3 + i).wait()
    h_store(steps - 1).wait()


def finish(de_part, dzt_last, x_xp, x_xq, embed, dhid, stat_all, info_all, gsum_all):
    any_spec = pl.BlockSpec(memory_space=pl.ANY)
    vmem_spec = pl.BlockSpec(memory_space=pltpu.VMEM)
    f32, bf16 = jnp.float32, jnp.bfloat16
    dma = pltpu.SemaphoreType.DMA
    outs = [((ROWS, DIM), f32), ((TOK, DIM), bf16), ((GROUPS, 128), f32), ((1, 1), f32), ((1, DIM), f32), ((1, DIM), f32)]
    return pl.pallas_call(
        finish_kernel,
        name="finish",
        out_shape=[jax.ShapeDtypeStruct(s, d) for s, d in outs],
        in_specs=[any_spec] * 6 + [vmem_spec] * 3,
        out_specs=[any_spec] * 2 + [vmem_spec] * 4,
        scratch_shapes=[
            pltpu.VMEM((KT, DIM), bf16), pltpu.VMEM((3, 2, (DEFER - 1) * XCH, KT), bf16), pltpu.VMEM((DEFER, ROWS, KT), bf16), pltpu.VMEM((2, ZB, DIM), bf16), pltpu.VMEM((ZB, KT), f32),
            pltpu.VMEM((3, ROWS, KT), f32), pltpu.VMEM((3, ROWS, KT), f32), pltpu.VMEM((2, TOK // (DIM // KT), DIM), bf16),
            dma((4,)), dma((DEFER,)), dma((2,)), dma((3,)), dma((3,)), dma((2,)), dma((2,)),
        ],
        compiler_params=pltpu.CompilerParams(vmem_limit_bytes=67043328),
        cost_estimate=pl.CostEstimate(flops=2 * ROWS * DIM * KT * (DEFER + 1), bytes_accessed=130 * 2 ** 20, transcendentals=ROWS * KT),
    )(de_part, dzt_last, x_xp, x_xq, embed, dhid, stat_all, info_all, gsum_all)


def solution(mesh):
    def body(hidden, ln_gain, ln_bias, embed, targets, loss_mask):
        outs = run_step(hidden, ln_gain.reshape(1, DIM), ln_bias.reshape(1, DIM), embed, targets.reshape(GROUPS, 128), loss_mask.reshape(GROUPS, 128))
        stat_all, info_all, dhid, x_xp, x_xq, dzt_last, de_part, gsum_all = (outs[i] for i in (3, 4, 5, 7, 8, 12, 13, 14))
        d_embed, d_hidden, loss, mean, d_gain, d_bias = finish(de_part, dzt_last, x_xp, x_xq, embed, dhid, stat_all, info_all, gsum_all)
        return loss.reshape(TOK), mean.reshape(1), d_hidden, d_embed, d_gain.reshape(DIM), d_bias.reshape(DIM)

    token_rows = P(('dp', 'tp'))
    token_mat = P(('dp', 'tp'), None)
    return jax.shard_map(body, mesh=mesh, in_specs=(token_mat, P(), P(), P('tp', None), token_rows, token_rows), out_specs=(token_rows, P('dp'), token_mat, token_mat, P('dp'), P('dp')), check_vma=False)
```

```python
import functools

import jax
import jax.numpy as jnp
from jax import lax
from jax.experimental import pallas as pl
from jax.experimental.pallas import tpu as pltpu
from jax.sharding import PartitionSpec as P

LN_EPS = 1e-5
LOWEST = float(jnp.finfo(jnp.float32).min)

TOK = 2048
ROWS = 2048
DIM = 4096
VOCAB = 8192
TILE = 256
TILES = VOCAB // TILE
HB = 1024
HBS = TOK // HB
CHUNK = 32
PIECE_ROWS = 2 * CHUNK
NEAR = 2 * ROWS // TILE
PE_ROWS = 512
CHUNKS = ROWS // 2 // CHUNK
LN_ROWS = 256
STAT_ROWS = 32
PIECE = 32
LN_UNROLL = 4
XCH = 256
XCHS = TOK // XCH
KT = 512
DEFER = 4
WAIT_STEP = {4: 0, 9: 1, 14: 2}
ZB = 512
NCOL = 512
KCOL = 1024
NB_UNROLL = 4
NB_ROWS = 256
GROUPS = TOK // 128
NT = (((1,), (1,)), ((), ()))


def peers():
    dp, tp = lax.axis_index('dp'), lax.axis_index('tp')
    core = lax.rem(tp, 2)
    pair = tp - core
    other = 2 - pair
    part = pair + 1 - core
    return dp, tp, (dp, part), (dp, other + core), (dp, other + 1 - core), (1 - dp, tp)


def remote(src, dst, ssem, rsem, dev):
    return pltpu.make_async_remote_copy(
        src_ref=src, dst_ref=dst, send_sem=ssem, recv_sem=rsem, device_id=dev, device_id_type=pl.DeviceIdType.MESH)


def spread(row, rows, dst):
    dst[rows, :] = jnp.transpose(jnp.broadcast_to(row, (128, 128)))


def step_kernel(hid, gain, bias, emb, targets, mask,
                e_all, x_out, z_out, stat_all, info_all,
                dhid, x_part, x_xp, x_xq, dzt_own, dzt_out, dzt_part, dzt_last, de_part, gsum_all,
                tcol, stat_v, stats, infos, gb_v, gs_v, g8,
                h_sem, xo_sem, e_sem, eo_sem, z_sem, zt_sem, et_sem, small_sem, dzo_sem, big_sem, g_sem,
                xs_send, ys_send, ds_send, pe_send, sm_send, xt_send, xd_send, xp_send, dz_send, g_send,
                x_recv, y_recv, d_recv, pe_recv, info_recv, stat_recv, xt_recv, xd_recv, xp_recv, dz_recv, g_recv):
    bf16, f32 = jnp.bfloat16, jnp.float32
    dp, tp, part, xp, xq, yp = peers()
    core = lax.rem(tp, 2)
    xp_rank = 2 - (tp - core) + core
    xq_rank = 2 - (tp - core) + 1 - core
    group = ((1, part), (2, xp), (3, xq))
    barrier = pltpu.get_barrier_semaphore()
    for dev in (part, xp, xq, yp):
        pl.semaphore_signal(barrier, inc=1, device_id=dev, device_id_type=pl.DeviceIdType.MESH)
    pl.semaphore_wait(barrier, 4)

    def info_copies(i):
        ref = (targets, mask)[i]
        return [remote(ref, info_all.at[tp, i], sm_send, info_recv.at[2 * p + i], dev) for p, dev in group]

    def columns():
        for s in range(4):
            pair, odd = s - s % 2, s % 2
            near = ((tp - core) == pair).astype(jnp.int32)
            same = (core == odd).astype(jnp.int32)
            row = targets[...] - s * ROWS
            low = (row < ROWS // 2).astype(jnp.int32)
            sub = row - (1 - low) * (ROWS // 2)
            crossed = low * dp + (1 - low) * (1 - dp)
            piece = (1 - same) * 2 + crossed
            tile = (sub.astype(f32) * (1.0 / PIECE_ROWS)).astype(jnp.int32)
            far = 2 * ROWS + tile * (TILE - PIECE_ROWS) + sub + piece * PIECE_ROWS
            col = near * ((1 - same) * ROWS + row) + (1 - near) * far
            inside = (row >= 0) & (row < ROWS)
            tcol[...] = jnp.where(inside, col, 0 if s == 0 else tcol[...])

    def xrows(ref, j):
        return ref.at[pl.ds(pl.multiple_of(j * XCH, XCH), XCH)]

    def xt_copy(j):
        return remote(xrows(x_out, j), xrows(x_xp, j), xt_send, xt_recv.at[j], xp)

    def xd_copy(j):
        return remote(xrows(x_xp, j), xrows(x_xq, j), xd_send, xd_recv.at[j], part)

    def xt_event(j):
        xt_copy(j).wait_recv()
        xd_copy(j).start()
    xp_copy = remote(x_out, x_part, xp_send, xp_recv, part)

    def forward(m_s, scale_v, tc_v, mr_v, zt, et, xs, hbuf, ebuf, z0, z1, s_s, t_s, gb8):
        def tile_row(j):
            return ROWS * 2 + (j // 2) * TILE + lax.rem(j, 2) * CHUNK

        def x_copy(j):
            src = emb.at[pl.ds(pl.multiple_of(dp * (ROWS // 2) + j * CHUNK, CHUNK), CHUNK)]
            return remote(src, e_all.at[pl.ds(pl.multiple_of(tile_row(j), CHUNK), CHUNK)], xs_send, x_recv.at[j], xp)

        def piece(j, p):
            return e_all.at[pl.ds(pl.multiple_of(tile_row(j) + p * PIECE_ROWS, CHUNK), CHUNK)]

        def y_copy(j):
            return remote(piece(j, 0), piece(j, 1), ys_send, y_recv.at[j], yp)

        def d_copy(j, p):
            return remote(piece(j, p), piece(j, p + 2), ds_send, d_recv.at[j // 2], part)

        def pe_copy(i):
            return remote(emb.at[pl.ds(pl.multiple_of(i * PE_ROWS, PE_ROWS), PE_ROWS)],
                          e_all.at[pl.ds(pl.multiple_of(ROWS + i * PE_ROWS, PE_ROWS), PE_ROWS)], pe_send, pe_recv.at[i], part)


        def h_copy(i):
            return pltpu.make_async_copy(hid.at[pl.ds(pl.multiple_of(i * LN_ROWS, LN_ROWS), LN_ROWS)], hbuf.at[lax.rem(i, 2)], h_sem.at[lax.rem(i, 2)])
        h_copy(0).start()

        for j in range(2):
            x_copy(j).start()
        for cp in info_copies(1):
            cp.start()

        def start_x(j, c):
            x_copy(j).start()
            return c
        lax.fori_loop(2, CHUNKS, start_x, 0)
        for cp in info_copies(0):
            cp.start()

        def start_pe(i, c):
            pe_copy(i).start()
            return c
        lax.fori_loop(0, ROWS // PE_ROWS, start_pe, 0)

        def e_load(t):
            slot = lax.rem(t, 2)
            return pltpu.make_async_copy(e_all.at[pl.ds(pl.multiple_of(t * TILE, TILE), TILE)], ebuf.at[slot], e_sem.at[slot])

        def e_load_own(t):
            slot = lax.rem(t, 2)
            return pltpu.make_async_copy(emb.at[pl.ds(pl.multiple_of(t * TILE, TILE), TILE)], ebuf.at[slot], e_sem.at[slot])
        e_load_own(0).start()

        def x_event(j):
            x_copy(j).wait_recv()
            y_copy(j).start()
            d_copy(j, 0).start()

        def y_event(j):
            y_copy(j).wait_recv()
            d_copy(j, 1).start()

        def p_event(k):
            rows = e_all.at[pl.ds(pl.multiple_of(2 * ROWS + k * TILE + TILE // 2, TILE // 2), TILE // 2)]
            pltpu.make_async_copy(rows, rows, d_recv.at[k]).wait()
            e_load(NEAR + k).start()

        own_info = [pltpu.make_async_copy(ref, info_all.at[tp, i], small_sem.at[0]) for i, ref in enumerate((targets, mask))]
        for cp in own_info:
            cp.start()
        columns()
        gb8[0] = jnp.broadcast_to(gain[...], (8, DIM))
        gb8[1] = jnp.broadcast_to(bias[...], (8, DIM))

        def ln_tile(i, c):
            slot = lax.rem(i, 2)

            @pl.when(i + 1 < TOK // LN_ROWS)
            def _():
                h_copy(i + 1).start()
            h_copy(i).wait()

            for at, j in ((4, 0), (7, 1)):
                @pl.when(i == at)
                def _(j=j):
                    x_event(j)

            def ln_rows(r, c2):
                base = r * LN_UNROLL * 16

                def at(u):
                    return pl.ds(pl.multiple_of(base + u * 16, 16), 16)

                def part_of(u, k):
                    return hbuf[slot, at(u), k * 128:(k + 1) * 128].astype(jnp.float32)
                means, rstds = [], []
                for u in range(LN_UNROLL):
                    tot = part_of(u, 0)
                    for k in range(1, DIM // 128):
                        tot = tot + part_of(u, k)
                    means.append(jnp.broadcast_to(jnp.sum(tot, axis=-1, keepdims=True) * (1.0 / DIM), (16, 128)))
                for u in range(LN_UNROLL):
                    tot = jnp.zeros((16, 128), jnp.float32)
                    for k in range(DIM // 128):
                        diff = part_of(u, k) - means[u]
                        tot = tot + diff * diff
                    var = jnp.sum(tot, axis=-1, keepdims=True) * (1.0 / DIM)
                    rstds.append(jnp.broadcast_to(lax.rsqrt(var + LN_EPS), (16, 128)))
                for u in range(LN_UNROLL):
                    row = pl.ds(pl.multiple_of(i * LN_ROWS + base + u * 16, 16), 16)
                    mr_v[0, row, :] = means[u]
                    mr_v[1, row, :] = rstds[u]
                    for k in range(DIM // 128):
                        cols = slice(k * 128, (k + 1) * 128)
                        g2 = jnp.concatenate([gb8[0, :, cols]] * 2, axis=0)
                        b2 = jnp.concatenate([gb8[1, :, cols]] * 2, axis=0)
                        xs[row, cols] = ((part_of(u, k) - means[u]) * rstds[u] * g2 + b2).astype(jnp.bfloat16)
                return c2
            lax.fori_loop(0, LN_ROWS // (16 * LN_UNROLL), ln_rows, 0)
            rows = pl.ds(pl.multiple_of(i * LN_ROWS, LN_ROWS), LN_ROWS)
            pltpu.make_async_copy(xs.at[rows], x_out.at[rows], xo_sem).start()
            return c
        lax.fori_loop(0, TOK // LN_ROWS, ln_tile, 0)

        m_s[...] = jnp.full((TOK, 128), LOWEST, jnp.float32)
        s_s[...] = jnp.zeros((TOK, 128), jnp.float32)
        t_s[...] = jnp.zeros((TOK, 128), jnp.float32)
        for r in range(GROUPS):
            spread(tcol[r:r + 1, :], slice(r * 128, (r + 1) * 128), tc_v)
        z1[...] = jnp.full((HB, TILE), LOWEST, jnp.float32)

        zs = (z0, z1)

        def product(t, h):
            for r in range(0, HB, 512):
                zs[h][r:r + 512, :] = lax.dot_general(
                    xs[h * HB + r:h * HB + r + 512, :], ebuf[lax.rem(t, 2)], NT, preferred_element_type=jnp.float32)

        def statistics(t, h):
            z = zs[h]
            lane = lax.broadcasted_iota(jnp.int32, (STAT_ROWS, 128), 1)
            for r in range(0, HB, STAT_ROWS):
                rows = slice(h * HB + r, h * HB + r + STAT_ROWS)
                zk = [z[r:r + STAT_ROWS, k * 128:(k + 1) * 128] for k in range(TILE // 128)]
                old = m_s[rows, :]
                new = jnp.maximum(jnp.maximum(zk[0], zk[1]), old)
                tot = s_s[rows, :] * jnp.exp(old - new)
                tgt = t_s[rows, :]
                diff = tc_v[rows, :] - t * TILE
                for k in range(TILE // 128):
                    tot = tot + jnp.exp(zk[k] - new)
                    tgt = tgt + jnp.where(diff == lane + k * 128, zk[k], 0.0)
                m_s[rows, :] = new
                s_s[rows, :] = tot
                t_s[rows, :] = tgt

        def z_copy(t, h):
            return pltpu.make_async_copy(
                zs[h], z_out.at[pl.ds(h * HB, HB), pl.ds(pl.multiple_of(t * TILE, TILE), TILE)], z_sem.at[h])

        def start_events(t):
            @pl.when(t < TILES - 2)
            def _():
                x_event(t + 2)

            @pl.when(t == 0)
            def _():
                y_event(0)

            @pl.when(t == TILES - 3)
            def _():
                xt_copy(0).start()

            @pl.when(t == TILES - 1)
            def _():
                p_event(TILES - 1 - NEAR)
            e_load(t).wait()

            @pl.when(t < ROWS // TILE)
            def _():
                slot = lax.rem(t, 2)
                pltpu.make_async_copy(ebuf.at[slot], e_all.at[pl.ds(pl.multiple_of(t * TILE, TILE), TILE)], eo_sem.at[slot]).start()

        def middle_events(t):
            @pl.when(t < TILES - 1)
            def _():
                y_event(t + 1)

            @pl.when((t >= 1) & (t < ROWS // TILE + 1))
            def _():
                slot = lax.rem(t - 1, 2)
                pltpu.make_async_copy(ebuf.at[slot], e_all.at[pl.ds(0, TILE)], eo_sem.at[slot]).wait()

            @pl.when(t == NEAR)
            def _():
                pltpu.make_async_copy(xs, x_out, xo_sem).wait()

            @pl.when(t < ROWS // TILE - 1)
            def _():
                e_load_own(t + 1).start()

            @pl.when((t >= ROWS // TILE - 1) & (t < NEAR - 1))
            def _():
                @pl.when(lax.rem(t + 1, PE_ROWS // TILE) == 0)
                def _():
                    pe_copy((t + 1 - ROWS // TILE) // (PE_ROWS // TILE)).wait_recv()
                e_load(t + 1).start()

            @pl.when((t >= NEAR - 1) & (t < TILES - 2))
            def _():
                p_event(t - (NEAR - 1))

            @pl.when(t == TILES - 2)
            def _():
                for k, h in ((0, 0), (1, 0), (0, 1)):
                    z_load(zt, k, h).start()
                et_load(et, 0).start()

            @pl.when(t == NEAR + 1)
            def _():
                for cp in info_copies(1):
                    cp.wait_recv()
                for cp in own_info:
                    cp.wait()
                loads = [pltpu.make_async_copy(info_all.at[q, 1], infos.at[q, 1], small_sem.at[0]) for q in range(4)]
                for load in loads:
                    load.start()
                for load in loads:
                    load.wait()
                count = jnp.broadcast_to(token_count(), (1, 128))
                for r in range(GROUPS):
                    spread(mask[r:r + 1, :].astype(f32) / count, slice(r * 128, (r + 1) * 128), scale_v)

        def step(t, c):
            @pl.when(t > 0)
            def _():
                z_copy(t - 1, 1).start()
            start_events(t)

            @pl.when(t > 0)
            def _():
                z_copy(t - 1, 0).wait()
            statistics(t - 1, 1)
            product(t, 0)
            z_copy(t, 0).start()
            middle_events(t)

            @pl.when(t > 0)
            def _():
                z_copy(t - 1, 1).wait()
            statistics(t, 0)
            product(t, 1)
            return c
        last = TILES - 1
        lax.fori_loop(0, TILES, step, 0)
        z_copy(last, 1).start()
        statistics(last, 1)

        def finish(i, c):
            for u in range(8):
                r = i * 8 + u
                rows = pl.ds(pl.multiple_of(r * 128, 128), 128)
                m = m_s[rows, :]
                top = jnp.max(m, axis=-1, keepdims=True)
                tot = jnp.sum(s_s[rows, :] * jnp.exp(m - top), axis=-1, keepdims=True)
                lse = jnp.broadcast_to(top + jnp.log(tot), (128, 128))
                tgt = jnp.broadcast_to(jnp.sum(t_s[rows, :], axis=-1, keepdims=True), (128, 128))
                m_s[rows, :] = lse
                stat_v[0, pl.ds(r, 1), :] = jnp.transpose(lse)[0:1, :]
                stat_v[1, pl.ds(r, 1), :] = jnp.transpose(tgt)[0:1, :]
            return c
        lax.fori_loop(0, TOK // 1024, finish, 0)
        for h in range(2):
            z_copy(last, h).wait()
        half = e_all.at[pl.ds(0, ROWS // 2)]
        pltpu.make_async_copy(half, half, xs_send).wait()
        pltpu.make_async_copy(half, half, ys_send).wait()
        full = e_all.at[pl.ds(0, ROWS)]
        pltpu.make_async_copy(full, full, ds_send).wait()
        pltpu.make_async_copy(full, full, pe_send).wait()
        pltpu.make_async_copy(stat_v, stat_all.at[tp], small_sem.at[1]).start()
        for p, dev in group:
            remote(stat_v, stat_all.at[tp], sm_send, stat_recv.at[p], dev).start()

        def start_xt(j, c):
            xt_copy(j).start()
            return c
        lax.fori_loop(1, XCHS, start_xt, 0)
        xp_copy.start()

    def z_load(zt, k, h):
        slot = lax.rem(k, 2)
        rows = slice(h * HB, (h + 1) * HB)
        return pltpu.make_async_copy(
            z_out.at[rows, pl.ds(pl.multiple_of(k * KT, KT), KT)], zt.at[slot, rows], zt_sem.at[2 * h + slot])

    def et_load(et, k):
        slot = lax.rem(k, 2)
        return pltpu.make_async_copy(e_all.at[pl.ds(pl.multiple_of(k * KT, KT), KT)], et.at[slot], et_sem.at[slot])

    def dzt_copy(k):
        rows = pl.ds(pl.multiple_of(lax.rem(k, 4) * KT, KT), KT)
        return remote(dzt_out.at[rows], dzt_part.at[rows], dz_send, dz_recv.at[lax.rem(k, 4)], part)

    def token_count():
        return jnp.sum(infos[:, 1].astype(f32))

    def token_grads(lse_v, scale_v, tcol_v, mr, zt, et, acc):
        def d_phase(da, db, dzt):
            def dzt_store(k, ref):
                slot = lax.rem(k, 2)
                return pltpu.make_async_copy(dzt.at[slot], ref.at[pl.ds(pl.multiple_of(lax.rem(k, 4) * KT, KT), KT)], eo_sem.at[slot])
            lane = lax.broadcasted_iota(jnp.int32, (PIECE, 128), 1)

            def piece(dst, rows, low, k, tie):
                slot = lax.rem(k, 2)
                lse = lse_v[rows, :]
                if tie is not None:
                    floor = 0.0 - jnp.maximum(0.0 - tie, -LOWEST)
                    lse = jnp.maximum(lse, jnp.concatenate([floor] * (PIECE // 8), axis=0))
                scale = scale_v[rows, :]
                diff = tcol_v[rows, :] - k * KT
                for g in range(KT // 128):
                    cols = slice(g * 128, (g + 1) * 128)
                    hot = (diff == lane + g * 128).astype(f32)
                    val = (jnp.exp(zt[slot, rows, cols] - lse) - hot) * scale
                    dst[low, cols] = val.astype(bf16)

            def half_step(k, src, dst, base, dst_base, dst_k):
                slot = lax.rem(k, 2)
                per = HB // (DIM // NCOL)
                for n in range(DIM // NCOL):
                    cols = slice(n * NCOL, (n + 1) * NCOL)
                    prod = jnp.dot(src[...], et[slot, :, cols], preferred_element_type=f32)
                    acc[base:base + HB, cols] = jnp.where(k == 0, 0.0, acc[base:base + HB, cols]) + prod
                    for q in range(0, per, PIECE):
                        at = q * HB // per
                        low = n * per + q
                        piece(dst, slice(dst_base + low, dst_base + low + PIECE), slice(low, low + PIECE), dst_k, prod[at:at + 8, 0:128])
                    if n * per % 256 == 0:
                        low = n * per
                        dzt[slot, :, base + low:base + low + 256] = jnp.transpose(src[low:low + 256, :])

            z_load(zt, 0, 0).wait()

            def first(i, c):
                rows = pl.ds(pl.multiple_of(i * PIECE, PIECE), PIECE)
                piece(da, rows, rows, 0, None)
                return c
            lax.fori_loop(0, HB // PIECE, first, 0)

            def step(k, c):
                @pl.when(k + 2 < VOCAB // KT)
                def _():
                    z_load(zt, k + 2, 0).start()

                @pl.when(k + 1 < VOCAB // KT)
                def _():
                    z_load(zt, k + 1, 1).start()
                    et_load(et, k + 1).start()
                    z_load(zt, k + 1, 0).wait()
                for at, j in WAIT_STEP.items():
                    @pl.when(k == at)
                    def _(j=j):
                        xt_event(j)

                @pl.when((k >= 2) & (k < 10))
                def _():
                    dzt_store(k, dzt_own).wait()

                @pl.when((k >= 6) & (k < 10))
                def _():
                    dzt_copy(k - 2).start()
                et_load(et, k).wait()
                z_load(zt, k, 1).wait()
                half_step(k, da, db, 0, HB, k)
                half_step(k, db, da, HB, 0, k + 1)

                @pl.when(k < 4)
                def _():
                    dzt_store(k, dzt_own).start()

                @pl.when((k >= 4) & (k < 8))
                def _():
                    dzt_store(k, dzt_out).start()
                return c
            lax.fori_loop(0, VOCAB // KT, step, 0)
        half = pltpu.VMEM((HB, KT), bf16)
        pl.run_scoped(d_phase, half, half, pltpu.VMEM((2, KT, TOK), bf16))

        def n_phase(hb, ob):
            def h_load(i):
                slot = lax.rem(i, 2)
                return pltpu.make_async_copy(hid.at[pl.ds(pl.multiple_of(i * NB_ROWS, NB_ROWS), NB_ROWS)], hb.at[slot], z_sem.at[slot])

            def o_store(i):
                slot = lax.rem(i, 2)
                return pltpu.make_async_copy(ob.at[slot], dhid.at[pl.ds(pl.multiple_of(i * NB_ROWS, NB_ROWS), NB_ROWS)], e_sem.at[slot])
            h_load(0).start()
            gb_v[...] = jnp.zeros(gb_v.shape, jnp.float32)
            g8[...] = jnp.broadcast_to(gain[...], (8, DIM))

            def tile(i, c):
                slot = lax.rem(i, 2)

                @pl.when(i + 1 < TOK // NB_ROWS)
                def _():
                    h_load(i + 1).start()

                @pl.when(i >= 2)
                def _():
                    o_store(i - 2).wait()
                h_load(i).wait()

                def rows_body(r, c2):
                    units = range(NB_UNROLL)
                    base = r * 16 * NB_UNROLL
                    low = [pl.ds(pl.multiple_of(base + u * 16, 16), 16) for u in units]
                    row = [pl.ds(pl.multiple_of(i * NB_ROWS + base + u * 16, 16), 16) for u in units]
                    zero = jnp.zeros((16, 128), jnp.float32)
                    sum1, sum3 = [zero] * NB_UNROLL, [zero] * NB_UNROLL

                    def load(u, cols):
                        dx = acc[row[u], cols]
                        xhat = (hb[slot, low[u], cols].astype(jnp.float32) - mr[0, row[u], :]) * mr[1, row[u], :]
                        return dx, xhat, dx * jnp.concatenate([g8[:, cols]] * 2, axis=0)
                    for k in range(DIM // 128):
                        cols = slice(k * 128, (k + 1) * 128)
                        d_gain, d_bias = gb_v[0, :, cols], gb_v[1, :, cols]
                        for u in units:
                            dx, xhat, gx = load(u, cols)
                            sum1[u] = sum1[u] + gx
                            sum3[u] = sum3[u] + gx * xhat
                            dgx = dx * xhat
                            d_gain = d_gain + (dgx[0:8] + dgx[8:16])
                            d_bias = d_bias + (dx[0:8] + dx[8:16])
                        gb_v[0, :, cols] = d_gain
                        gb_v[1, :, cols] = d_bias
                    slope, shift = [], []
                    for u in units:
                        mean, rstd = mr[0, row[u], :], mr[1, row[u], :]
                        c1 = jnp.broadcast_to(jnp.sum(sum1[u], axis=-1, keepdims=True) * (1.0 / DIM), (16, 128))
                        c3 = jnp.broadcast_to(jnp.sum(sum3[u], axis=-1, keepdims=True) * (1.0 / DIM), (16, 128))
                        slope.append(c3 * rstd * rstd)
                        shift.append(slope[u] * mean - c1 * rstd)
                    for u in units:
                        rstd = mr[1, row[u], :]
                        for k in range(DIM // 128):
                            cols = slice(k * 128, (k + 1) * 128)
                            gx = acc[row[u], cols] * jnp.concatenate([g8[:, cols]] * 2, axis=0)
                            ob[slot, low[u], cols] = (gx * rstd - hb[slot, low[u], cols].astype(f32) * slope[u] + shift[u]).astype(bf16)
                    return c2
                lax.fori_loop(0, NB_ROWS // (16 * NB_UNROLL), rows_body, 0)
                o_store(i).start()
                return c
            lax.fori_loop(0, TOK // NB_ROWS, tile, 0)
            for i in range(2):
                o_store(TOK // NB_ROWS - 2 + i).wait()
            gs_v[0:1, :] = jnp.sum(gb_v[0], axis=0, keepdims=True)
            gs_v[1:2, :] = jnp.sum(gb_v[1], axis=0, keepdims=True)
        pl.run_scoped(n_phase, pltpu.VMEM((2, NB_ROWS, DIM), bf16), pltpu.VMEM((2, NB_ROWS, DIM), bf16))

    def weight_grads(acc):
        own = pltpu.make_async_copy(gs_v, gsum_all.at[tp], g_sem)
        xt_event(3)

        def e_phase(eo, xt, dzb, zs, z1):
            eo_load = pltpu.make_async_copy(emb, eo, big_sem)

            def x_load(ref, row, slot):
                return pltpu.make_async_copy(ref.at[pl.ds(pl.multiple_of(row, KT), KT)], xt.at[slot], z_sem.at[slot])

            def dz_load(ref, col, slot):
                return pltpu.make_async_copy(ref.at[:, pl.ds(pl.multiple_of(col, KT), KT)], dzb.at[slot], e_sem.at[slot])

            def start_local(i):
                slot = lax.rem(i, 2)

                @pl.when(i < 4)
                def _():
                    x_load(x_out, i * KT, slot).start()
                    dz_load(dzt_own, i * KT, slot).start()

                @pl.when(i >= 4)
                def _():
                    x_load(x_part, (i - 4) * KT, slot).start()
                    dz_load(dzt_part, (i - 4) * KT, slot).start()

            def add(slot, first):
                def mul(h, c2):
                    rows = pl.ds(pl.multiple_of(h * HB, HB), HB)
                    for n in range(0, DIM, NCOL):
                        prod = jnp.dot(dzb[slot, rows, :], xt[slot, :, n:n + NCOL], preferred_element_type=f32)
                        acc[rows, n:n + NCOL] = jnp.where(first, 0.0, acc[rows, n:n + NCOL]) + prod
                    return c2
                lax.fori_loop(0, HBS, mul, 0)

            start_local(0)

            def rem_load(r):
                slot = lax.rem(r, 2)
                return [pltpu.make_async_copy(xrows(ref, r), xt.at[slot, pl.ds(i * XCH, XCH)], z_sem.at[slot])
                        for i, ref in enumerate((x_xp, x_xq))]

            def local(i, c):
                slot = lax.rem(i, 2)

                @pl.when(i == 0)
                def _():
                    eo_load.start()

                @pl.when(i == 2)
                def _():
                    xp_copy.wait_recv()

                    def wait_dz(q, c2):
                        dzt_copy(q).wait_recv()
                        return c2
                    lax.fori_loop(0, 4, wait_dz, 0)

                @pl.when(i == 1)
                def _():
                    own.start()
                    for p, dev in group:
                        remote(gs_v, gsum_all.at[tp], g_send, g_recv.at[p], dev).start()

                @pl.when(i == 6)
                def _():
                    xt_event(4)

                @pl.when(i < 7)
                def _():
                    start_local(i + 1)

                @pl.when(i == 7)
                def _():
                    xd_copy(0).wait_recv()
                    for cp in rem_load(0):
                        cp.start()
                x_load(x_out, 0, slot).wait()
                dz_load(dzt_own, 0, slot).wait()
                add(slot, i == 0)
                return c
            lax.fori_loop(0, 8, local, 0)
            eo_load.wait()
            for p, dev in group:
                remote(stat_v, stat_all.at[tp], sm_send, stat_recv.at[p], dev).wait_recv()
            pltpu.make_async_copy(stat_v, stat_all.at[tp], small_sem.at[1]).wait()
            for cp in info_copies(0):
                cp.wait_recv()
            loads = [pltpu.make_async_copy(stat_all, stats, small_sem.at[1])]
            loads += [pltpu.make_async_copy(info_all.at[q, 0], infos.at[q, 0], small_sem.at[0]) for q in range(4)]
            for load in loads:
                load.start()
            for load in loads:
                load.wait()
            count = jnp.broadcast_to(token_count(), (1, 128))

            def far(r, c):
                slot = lax.rem(r, 2)

                @pl.when(r == 1)
                def _():
                    xt_event(5)

                @pl.when(r == 4)
                def _():
                    xt_event(6)

                def fetch():
                    xd_copy(r + 1).wait_recv()
                    for cp in rem_load(r + 1):
                        cp.start()
                pl.when(r < XCHS - 2)(fetch)
                x_load(x_out, 0, slot).wait()

                @pl.when(r == XCHS - DEFER)
                def _():
                    pltpu.make_async_copy(acc, de_part, big_sem).start()

                @pl.when(r > XCHS - DEFER + 1)
                def _():
                    dz_out(0, slot).wait()

                far_rows = []
                for g in range(4):
                    who = xp_rank if g < 2 else xq_rank
                    at = pl.ds(2 * r + g % 2, 1)
                    far_rows.append((stats[who, 0, at, :], infos[who, 1, at, :].astype(f32) / count, infos[who, 0, at, :] - tp * ROWS))

                def logits(h2, c2):
                    @pl.when((r == XCHS - 2) & (h2 == 1))
                    def _():
                        xt_event(XCHS - 1)

                    def multiply(h, z):
                        for k in range(0, DIM, KCOL):
                            prod = lax.dot_general(eo[pl.ds(pl.multiple_of(h * ZB, ZB), ZB), k:k + KCOL], xt[slot, :, k:k + KCOL], NT, preferred_element_type=f32)
                            z[...] = prod if k == 0 else z[...] + prod

                    def convert(h, z):
                        for q in range(ZB // 32):
                            row = h * ZB + q * 32
                            line = lax.broadcasted_iota(jnp.int32, (32, 128), 0)
                            for g, (lse, scale, trel) in enumerate(far_rows):
                                cols = slice(g * 128, (g + 1) * 128)
                                hot = ((trel - row) == line).astype(f32)
                                val = (jnp.exp(z[q * 32:(q + 1) * 32, cols] - lse) - hot) * scale
                                dzb[slot, pl.ds(pl.multiple_of(row, 32), 32), cols] = val.astype(bf16)
                    multiply(2 * h2, zs)
                    multiply(2 * h2 + 1, z1)
                    convert(2 * h2, zs)
                    convert(2 * h2 + 1, z1)
                    return c2
                lax.fori_loop(0, ROWS // (2 * ZB), logits, 0)

                @pl.when(r < XCHS - DEFER)
                def _():
                    def mul(h, c2):
                        rows = pl.ds(pl.multiple_of(h * HB, HB), HB)
                        for n in range(0, DIM, NCOL):
                            acc[rows, n:n + NCOL] += jnp.dot(dzb[slot, rows, :], xt[slot, :, n:n + NCOL], preferred_element_type=jnp.float32)
                        return c2
                    lax.fori_loop(0, HBS, mul, 0)

                @pl.when(r >= XCHS - DEFER)
                def _():
                    dz_out(r - (XCHS - DEFER), slot).start()
                return c

            def dz_out(q, slot):
                return pltpu.make_async_copy(dzb.at[slot], dzt_last.at[q], dzo_sem.at[slot])
            lax.fori_loop(0, XCHS - 1, far, 0)
            for slot in range(2):
                dz_out(0, slot).wait()
            xd_copy(XCHS - 1).wait_recv()
            pltpu.make_async_copy(acc, de_part, big_sem).wait()
        pl.run_scoped(e_phase, pltpu.VMEM((ROWS, DIM), jnp.bfloat16), pltpu.VMEM((2, KT, DIM), jnp.bfloat16),
                      pltpu.VMEM((2, ROWS, KT), jnp.bfloat16), pltpu.VMEM((ZB, KT), f32), pltpu.VMEM((ZB, KT), f32))

        own.wait()

    wide = pltpu.VMEM((TOK, 128), f32)
    big = pltpu.VMEM((TOK, DIM), f32)

    def tokens(m_s, scale_v, tc_v, mr_v, zt, et):
        kept = (m_s, scale_v, tc_v, mr_v, zt, et)
        pl.run_scoped(functools.partial(forward, *kept), pltpu.VMEM((TOK, DIM), bf16), pltpu.VMEM((2, LN_ROWS, DIM), bf16),
                      pltpu.VMEM((2, TILE, DIM), bf16), pltpu.VMEM((HB, TILE), f32), pltpu.VMEM((HB, TILE), f32), wide, wide,
                      pltpu.VMEM((2, 8, DIM), f32))
        pl.run_scoped(functools.partial(token_grads, *kept), big)
    pl.run_scoped(tokens, wide, wide, pltpu.VMEM((TOK, 128), jnp.int32), pltpu.VMEM((2, TOK, 128), f32),
                  pltpu.VMEM((2, TOK, KT), f32), pltpu.VMEM((2, KT, DIM), bf16))
    pl.run_scoped(weight_grads, big)

    pltpu.make_async_copy(x_out, x_out, xt_send).wait()
    pltpu.make_async_copy(x_out, x_out, xd_send).wait()
    xp_copy.wait_send()
    pltpu.make_async_copy(dzt_out, dzt_out, dz_send).wait()
    for cp in (*info_copies(0), *info_copies(1)):
        cp.wait_send()
    for p, dev in group:
        remote(stat_v, stat_all.at[tp], sm_send, stat_recv.at[p], dev).wait_send()
        remote(gs_v, gsum_all.at[tp], g_send, g_recv.at[p], dev).wait()


def run_step(hidden, gain, bias, embed, targets, mask):
    any_spec = pl.BlockSpec(memory_space=pl.ANY)
    vmem_spec = pl.BlockSpec(memory_space=pltpu.VMEM)
    f32, bf16, i32 = jnp.float32, jnp.bfloat16, jnp.int32
    dma = pltpu.SemaphoreType.DMA
    small, ints = (4, 2, GROUPS, 128), (4, 2, GROUPS, 128)
    mat, square = ((TOK, DIM), bf16), ((ROWS, TOK), bf16)
    shapes = [((VOCAB, DIM), bf16), mat, ((TOK, VOCAB), f32), (small, f32), (ints, i32),
              mat, mat, mat, mat, square, square, square, ((DEFER - 1, ROWS, KT), bf16), ((ROWS, DIM), f32), ((4, 2, DIM), f32)]
    return pl.pallas_call(
        step_kernel,
        name="step",
        out_shape=[jax.ShapeDtypeStruct(s, d) for s, d in shapes],
        in_specs=[any_spec, vmem_spec, vmem_spec, any_spec, vmem_spec, vmem_spec],
        out_specs=[any_spec] * len(shapes),
        scratch_shapes=[
            pltpu.VMEM((GROUPS, 128), i32), pltpu.VMEM((2, GROUPS, 128), f32), pltpu.VMEM(small, f32), pltpu.VMEM(ints, i32),
            pltpu.VMEM((2, 8, DIM), f32), pltpu.VMEM((2, DIM), f32), pltpu.VMEM((8, DIM), f32),
            dma((2,)), dma, dma((2,)), dma((2,)), dma((2,)), dma((4,)), dma((2,)), dma((2,)), dma((2,)), dma, dma,
            dma, dma, dma, dma, dma, dma, dma, dma, dma, dma,
            dma((CHUNKS,)), dma((CHUNKS,)), dma((TILES - NEAR,)), dma((ROWS // PE_ROWS,)), dma((8,)), dma((4,)),
            dma((XCHS,)), dma((XCHS,)), dma, dma((4,)), dma((4,)),
        ],
        compiler_params=pltpu.CompilerParams(collective_id=0, has_side_effects=True, vmem_limit_bytes=67043328),
        cost_estimate=pl.CostEstimate(flops=12 * TOK * VOCAB * DIM, bytes_accessed=700 * 2 ** 20, transcendentals=3 * TOK * VOCAB),
    )(hidden, gain, bias, embed, targets, mask)


def finish_kernel(de_in, dzt_last, x_xp, x_xq, emb, dh_in, stat_all, info_all, gsum_all,
                  de_out, dh_out, loss, mean, d_gain, d_bias,
                  x7, xr, dz, eb, zs, din, dout, hb, x_sem, z_sem, e_sem, di_sem, do_sem, hi_sem, ho_sem):
    f32, bf16 = jnp.float32, jnp.bfloat16
    last = DEFER - 1

    def x_last():
        rows = pl.ds((XCHS - 1) * XCH, XCH)
        return [pltpu.make_async_copy(ref.at[rows], x7.at[pl.ds(i * XCH, XCH)], x_sem.at[3]) for i, ref in enumerate((x_xp, x_xq))]

    def x_tiles(i):
        slot = lax.rem(i, 3)
        cols = pl.ds(pl.multiple_of(i * KT, KT), KT)
        rows = pl.ds((XCHS - DEFER) * XCH, last * XCH)
        return [pltpu.make_async_copy(ref.at[rows, cols], xr.at[slot, j], x_sem.at[slot]) for j, ref in enumerate((x_xp, x_xq))]

    def e_load(h):
        slot = lax.rem(h, 2)
        return pltpu.make_async_copy(emb.at[pl.ds(pl.multiple_of(h * ZB, ZB), ZB)], eb.at[slot], e_sem.at[slot])

    def z_load(q):
        return pltpu.make_async_copy(dzt_last.at[q], dz.at[q], z_sem.at[q])

    def tile(ref, i):
        return ref.at[:, pl.ds(pl.multiple_of(i * KT, KT), KT)]

    def d_load(i):
        slot = lax.rem(i, 3)
        return pltpu.make_async_copy(tile(de_in, i), din.at[slot], di_sem.at[slot])

    def d_store(i):
        slot = lax.rem(i, 3)
        return pltpu.make_async_copy(dout.at[slot], tile(de_out, i), do_sem.at[slot])
    steps = DIM // KT
    per = TOK // steps

    def h_load(i):
        slot = lax.rem(i, 2)
        return pltpu.make_async_copy(dh_in.at[pl.ds(pl.multiple_of(i * per, per), per)], hb.at[slot], hi_sem.at[slot])

    def h_store(i):
        slot = lax.rem(i, 2)
        return pltpu.make_async_copy(hb.at[slot], dh_out.at[pl.ds(pl.multiple_of(i * per, per), per)], ho_sem.at[slot])
    for cp in x_last():
        cp.start()
    e_load(0).start()
    e_load(1).start()

    def tile_loads(i):
        for cp in (*x_tiles(i), d_load(i)):
            cp.start()

    tp = lax.axis_index('tp')
    core = lax.rem(tp, 2)
    other = 2 - (tp - core)
    weights = info_all[:, 1].astype(f32)
    total = jnp.sum(weights)
    all_loss = (stat_all[:, 0] - stat_all[:, 1]) * weights
    loss[...] = (stat_all[tp, 0] - stat_all[tp, 1]) * info_all[tp, 1].astype(f32)
    mean[...] = jnp.broadcast_to(jnp.sum(all_loss), (1, 1)) / jnp.broadcast_to(total, (1, 1))
    sums = ((gsum_all[0] + gsum_all[1]) + gsum_all[2]) + gsum_all[3]
    d_gain[...] = sums[0:1]
    d_bias[...] = sums[1:2]
    count = jnp.broadcast_to(total, (1, 128))
    far_rows = []
    for g in range(4):
        who = other + core if g < 2 else other + 1 - core
        at = slice(GROUPS - 2 + g % 2, GROUPS - 1 + g % 2)
        far_rows.append((stat_all[who, 0, at, :], info_all[who, 1, at, :].astype(f32) / count, info_all[who, 0, at, :] - tp * ROWS))
    pltpu.make_async_copy(x7, x7, x_sem.at[3]).wait()

    def logits(h, c):
        slot = lax.rem(h, 2)
        e_load(h).wait()
        for k in range(0, DIM, KCOL):
            prod = lax.dot_general(eb[slot, :, k:k + KCOL], x7[:, k:k + KCOL], NT, preferred_element_type=f32)
            zs[...] = prod if k == 0 else zs[...] + prod

        @pl.when(h == 0)
        def _():
            e_load(2).start()
            z_load(0).start()
            z_load(1).start()

        @pl.when(h == 1)
        def _():
            e_load(3).start()
            z_load(2).start()

        @pl.when(h == 2)
        def _():
            tile_loads(0)
            h_load(0).start()

        @pl.when(h == 3)
        def _():
            tile_loads(1)
        for q in range(ZB // 32):
            row = h * ZB + q * 32
            line = lax.broadcasted_iota(jnp.int32, (32, 128), 0)
            for g, (lse, scale, trel) in enumerate(far_rows):
                cols = slice(g * 128, (g + 1) * 128)
                hot = ((trel - row) == line).astype(f32)
                val = (jnp.exp(zs[q * 32:(q + 1) * 32, cols] - lse) - hot) * scale
                dz[last, pl.ds(pl.multiple_of(row, 32), 32), cols] = val.astype(bf16)
        return c
    lax.fori_loop(0, ROWS // ZB, logits, 0)
    for q in range(last):
        z_load(q).wait()

    def step(i, c):
        slot = lax.rem(i, 3)
        cols = pl.ds(pl.multiple_of(i * KT, KT), KT)

        @pl.when(i + 2 < steps)
        def _():
            tile_loads(i + 2)
        h_load(i).wait()
        h_store(i).start()

        @pl.when(i >= 1)
        def _():
            h_store(i - 1).wait()

        @pl.when(i + 1 < steps)
        def _():
            h_load(i + 1).start()

        @pl.when(i >= 3)
        def _():
            d_store(i - 3).wait()
        d_load(i).wait()
        for cp in x_tiles(i):
            cp.wait()
        for h in range(HBS):
            rows = slice(h * HB, (h + 1) * HB)
            prod = jnp.dot(dz[last, rows, :], x7[:, cols], preferred_element_type=f32)
            for q in range(last):
                for j in range(2):
                    prod = prod + jnp.dot(dz[q, rows, j * XCH:(j + 1) * XCH], xr[slot, j, q * XCH:(q + 1) * XCH, :], preferred_element_type=f32)
            dout[slot, rows, :] = din[slot, rows, :] + prod
        d_store(i).start()
        return c
    lax.fori_loop(0, steps, step, 0)
    for i in range(3):
        d_store(steps - 3 + i).wait()
    h_store(steps - 1).wait()


def finish(de_part, dzt_last, x_xp, x_xq, embed, dhid, stat_all, info_all, gsum_all):
    any_spec = pl.BlockSpec(memory_space=pl.ANY)
    vmem_spec = pl.BlockSpec(memory_space=pltpu.VMEM)
    f32, bf16 = jnp.float32, jnp.bfloat16
    dma = pltpu.SemaphoreType.DMA
    outs = [((ROWS, DIM), f32), ((TOK, DIM), bf16), ((GROUPS, 128), f32), ((1, 1), f32), ((1, DIM), f32), ((1, DIM), f32)]
    return pl.pallas_call(
        finish_kernel,
        name="finish",
        out_shape=[jax.ShapeDtypeStruct(s, d) for s, d in outs],
        in_specs=[any_spec] * 6 + [vmem_spec] * 3,
        out_specs=[any_spec] * 2 + [vmem_spec] * 4,
        scratch_shapes=[
            pltpu.VMEM((KT, DIM), bf16), pltpu.VMEM((3, 2, (DEFER - 1) * XCH, KT), bf16), pltpu.VMEM((DEFER, ROWS, KT), bf16), pltpu.VMEM((2, ZB, DIM), bf16), pltpu.VMEM((ZB, KT), f32),
            pltpu.VMEM((3, ROWS, KT), f32), pltpu.VMEM((3, ROWS, KT), f32), pltpu.VMEM((2, TOK // (DIM // KT), DIM), bf16),
            dma((4,)), dma((DEFER,)), dma((2,)), dma((3,)), dma((3,)), dma((2,)), dma((2,)),
        ],
        compiler_params=pltpu.CompilerParams(vmem_limit_bytes=67043328),
        cost_estimate=pl.CostEstimate(flops=2 * ROWS * DIM * KT * (DEFER + 1), bytes_accessed=130 * 2 ** 20, transcendentals=ROWS * KT),
    )(de_part, dzt_last, x_xp, x_xq, embed, dhid, stat_all, info_all, gsum_all)


def solution(mesh):
    def body(hidden, ln_gain, ln_bias, embed, targets, loss_mask):
        outs = run_step(hidden, ln_gain.reshape(1, DIM), ln_bias.reshape(1, DIM), embed, targets.reshape(GROUPS, 128), loss_mask.reshape(GROUPS, 128))
        stat_all, info_all, dhid, x_xp, x_xq, dzt_last, de_part, gsum_all = (outs[i] for i in (3, 4, 5, 7, 8, 12, 13, 14))
        d_embed, d_hidden, loss, mean, d_gain, d_bias = finish(de_part, dzt_last, x_xp, x_xq, embed, dhid, stat_all, info_all, gsum_all)
        return loss.reshape(TOK), mean.reshape(1), d_hidden, d_embed, d_gain.reshape(DIM), d_bias.reshape(DIM)

    token_rows = P(('dp', 'tp'))
    token_mat = P(('dp', 'tp'), None)
    return jax.shard_map(body, mesh=mesh, in_specs=(token_mat, P(), P(), P('tp', None), token_rows, token_rows), out_specs=(token_rows, P('dp'), token_mat, token_mat, P('dp'), P('dp')), check_vma=False)
```

```python
import functools

import jax
import jax.numpy as jnp
from jax import lax
from jax.experimental import pallas as pl
from jax.experimental.pallas import tpu as pltpu
from jax.sharding import PartitionSpec as P

LN_EPS = 1e-5
LOWEST = float(jnp.finfo(jnp.float32).min)

TOK = 2048
ROWS = 2048
DIM = 4096
VOCAB = 8192
TILE = 256
TILES = VOCAB // TILE
HB = 1024
HBS = TOK // HB
CHUNK = 32
PIECE_ROWS = 2 * CHUNK
NEAR = 2 * ROWS // TILE
PE_ROWS = 512
CHUNKS = ROWS // 2 // CHUNK
LN_ROWS = 256
STAT_ROWS = 32
PIECE = 32
LN_UNROLL = 4
XCH = 256
XCHS = TOK // XCH
KT = 512
DEFER = 4
WAIT_STEP = {4: 0, 9: 1, 14: 2}
ZB = 512
NCOL = 512
KCOL = 1024
NB_UNROLL = 4
NB_ROWS = 256
GROUPS = TOK // 128
NT = (((1,), (1,)), ((), ()))


def peers():
    dp, tp = lax.axis_index('dp'), lax.axis_index('tp')
    core = lax.rem(tp, 2)
    pair = tp - core
    other = 2 - pair
    part = pair + 1 - core
    return dp, tp, (dp, part), (dp, other + core), (dp, other + 1 - core), (1 - dp, tp)


def remote(src, dst, ssem, rsem, dev):
    return pltpu.make_async_remote_copy(
        src_ref=src, dst_ref=dst, send_sem=ssem, recv_sem=rsem, device_id=dev, device_id_type=pl.DeviceIdType.MESH)


def spread(row, rows, dst):
    dst[rows, :] = jnp.transpose(jnp.broadcast_to(row, (128, 128)))


def step_kernel(hid, gain, bias, emb, targets, mask,
                e_all, x_out, z_out, stat_all, info_all,
                dhid, x_part, x_xp, x_xq, dzt_own, dzt_out, dzt_part, dzt_last, de_part, gsum_all,
                tcol, stat_v, stats, infos, gb_v, gs_v, g8,
                h_sem, xo_sem, e_sem, eo_sem, z_sem, zt_sem, et_sem, small_sem, dzo_sem, big_sem, g_sem,
                xs_send, ys_send, ds_send, pe_send, sm_send, xt_send, xd_send, xp_send, dz_send, g_send,
                x_recv, y_recv, d_recv, pe_recv, info_recv, stat_recv, xt_recv, xd_recv, xp_recv, dz_recv, g_recv):
    bf16, f32 = jnp.bfloat16, jnp.float32
    dp, tp, part, xp, xq, yp = peers()
    core = lax.rem(tp, 2)
    xp_rank = 2 - (tp - core) + core
    xq_rank = 2 - (tp - core) + 1 - core
    group = ((1, part), (2, xp), (3, xq))
    barrier = pltpu.get_barrier_semaphore()
    for dev in (part, xp, xq, yp):
        pl.semaphore_signal(barrier, inc=1, device_id=dev, device_id_type=pl.DeviceIdType.MESH)
    pl.semaphore_wait(barrier, 4)

    def info_copies(i):
        ref = (targets, mask)[i]
        return [remote(ref, info_all.at[tp, i], sm_send, info_recv.at[2 * p + i], dev) for p, dev in group]

    def columns():
        for s in range(4):
            pair, odd = s - s % 2, s % 2
            near = ((tp - core) == pair).astype(jnp.int32)
            same = (core == odd).astype(jnp.int32)
            row = targets[...] - s * ROWS
            low = (row < ROWS // 2).astype(jnp.int32)
            sub = row - (1 - low) * (ROWS // 2)
            crossed = low * dp + (1 - low) * (1 - dp)
            piece = (1 - same) * 2 + crossed
            tile = (sub.astype(f32) * (1.0 / PIECE_ROWS)).astype(jnp.int32)
            far = 2 * ROWS + tile * (TILE - PIECE_ROWS) + sub + piece * PIECE_ROWS
            col = near * ((1 - same) * ROWS + row) + (1 - near) * far
            inside = (row >= 0) & (row < ROWS)
            tcol[...] = jnp.where(inside, col, 0 if s == 0 else tcol[...])

    def xrows(ref, j):
        return ref.at[pl.ds(pl.multiple_of(j * XCH, XCH), XCH)]

    def xt_copy(j):
        return remote(xrows(x_out, j), xrows(x_xp, j), xt_send, xt_recv.at[j], xp)

    def xd_copy(j):
        return remote(xrows(x_xp, j), xrows(x_xq, j), xd_send, xd_recv.at[j], part)

    def last_part(q):
        rows = pl.ds((XCHS - 1) * XCH + q * (XCH // 4), XCH // 4)
        return (remote(x_out.at[rows], x_xp.at[rows], xt_send, xt_recv.at[XCHS - 1 + q], xp),
                remote(x_xp.at[rows], x_xq.at[rows], xd_send, xd_recv.at[XCHS - 1], part))

    def last_event(q):
        arrive, hand_on = last_part(q)
        arrive.wait_recv()
        hand_on.start()

    def xt_event(j):
        xt_copy(j).wait_recv()
        xd_copy(j).start()
    xp_copy = remote(x_out, x_part, xp_send, xp_recv, part)

    def forward(m_s, scale_v, tc_v, mr_v, zt, et, xs, hbuf, ebuf, z0, z1, s_s, t_s, gb8):
        def tile_row(j):
            return ROWS * 2 + (j // 2) * TILE + lax.rem(j, 2) * CHUNK

        def x_copy(j):
            src = emb.at[pl.ds(pl.multiple_of(dp * (ROWS // 2) + j * CHUNK, CHUNK), CHUNK)]
            return remote(src, e_all.at[pl.ds(pl.multiple_of(tile_row(j), CHUNK), CHUNK)], xs_send, x_recv.at[j], xp)

        def piece(j, p):
            return e_all.at[pl.ds(pl.multiple_of(tile_row(j) + p * PIECE_ROWS, CHUNK), CHUNK)]

        def y_copy(j):
            return remote(piece(j, 0), piece(j, 1), ys_send, y_recv.at[j], yp)

        def d_copy(j, p):
            return remote(piece(j, p), piece(j, p + 2), ds_send, d_recv.at[j // 2], part)

        def pe_copy(i):
            return remote(emb.at[pl.ds(pl.multiple_of(i * PE_ROWS, PE_ROWS), PE_ROWS)],
                          e_all.at[pl.ds(pl.multiple_of(ROWS + i * PE_ROWS, PE_ROWS), PE_ROWS)], pe_send, pe_recv.at[i], part)


        def h_copy(i):
            return pltpu.make_async_copy(hid.at[pl.ds(pl.multiple_of(i * LN_ROWS, LN_ROWS), LN_ROWS)], hbuf.at[lax.rem(i, 2)], h_sem.at[lax.rem(i, 2)])
        h_copy(0).start()

        for j in range(2):
            x_copy(j).start()
        for cp in info_copies(1):
            cp.start()

        def start_x(j, c):
            x_copy(j).start()
            return c
        lax.fori_loop(2, CHUNKS, start_x, 0)
        for cp in info_copies(0):
            cp.start()

        def start_pe(i, c):
            pe_copy(i).start()
            return c
        lax.fori_loop(0, ROWS // PE_ROWS, start_pe, 0)

        def e_load(t):
            slot = lax.rem(t, 2)
            return pltpu.make_async_copy(e_all.at[pl.ds(pl.multiple_of(t * TILE, TILE), TILE)], ebuf.at[slot], e_sem.at[slot])

        def e_load_own(t):
            slot = lax.rem(t, 2)
            return pltpu.make_async_copy(emb.at[pl.ds(pl.multiple_of(t * TILE, TILE), TILE)], ebuf.at[slot], e_sem.at[slot])
        e_load_own(0).start()

        def x_event(j):
            x_copy(j).wait_recv()
            y_copy(j).start()
            d_copy(j, 0).start()

        def y_event(j):
            y_copy(j).wait_recv()
            d_copy(j, 1).start()

        def p_event(k):
            rows = e_all.at[pl.ds(pl.multiple_of(2 * ROWS + k * TILE + TILE // 2, TILE // 2), TILE // 2)]
            pltpu.make_async_copy(rows, rows, d_recv.at[k]).wait()
            e_load(NEAR + k).start()

        own_info = [pltpu.make_async_copy(ref, info_all.at[tp, i], small_sem.at[0]) for i, ref in enumerate((targets, mask))]
        for cp in own_info:
            cp.start()
        columns()
        gb8[0] = jnp.broadcast_to(gain[...], (8, DIM))
        gb8[1] = jnp.broadcast_to(bias[...], (8, DIM))

        def ln_tile(i, c):
            slot = lax.rem(i, 2)

            @pl.when(i + 1 < TOK // LN_ROWS)
            def _():
                h_copy(i + 1).start()
            h_copy(i).wait()

            for at, j in ((4, 0), (7, 1)):
                @pl.when(i == at)
                def _(j=j):
                    x_event(j)

            def ln_rows(r, c2):
                base = r * LN_UNROLL * 16

                def at(u):
                    return pl.ds(pl.multiple_of(base + u * 16, 16), 16)

                def part_of(u, k):
                    return hbuf[slot, at(u), k * 128:(k + 1) * 128].astype(jnp.float32)
                means, rstds = [], []
                for u in range(LN_UNROLL):
                    tot = part_of(u, 0)
                    for k in range(1, DIM // 128):
                        tot = tot + part_of(u, k)
                    means.append(jnp.broadcast_to(jnp.sum(tot, axis=-1, keepdims=True) * (1.0 / DIM), (16, 128)))
                for u in range(LN_UNROLL):
                    tot = jnp.zeros((16, 128), jnp.float32)
                    for k in range(DIM // 128):
                        diff = part_of(u, k) - means[u]
                        tot = tot + diff * diff
                    var = jnp.sum(tot, axis=-1, keepdims=True) * (1.0 / DIM)
                    rstds.append(jnp.broadcast_to(lax.rsqrt(var + LN_EPS), (16, 128)))
                for u in range(LN_UNROLL):
                    row = pl.ds(pl.multiple_of(i * LN_ROWS + base + u * 16, 16), 16)
                    mr_v[0, row, :] = means[u]
                    mr_v[1, row, :] = rstds[u]
                    for k in range(DIM // 128):
                        cols = slice(k * 128, (k + 1) * 128)
                        g2 = jnp.concatenate([gb8[0, :, cols]] * 2, axis=0)
                        b2 = jnp.concatenate([gb8[1, :, cols]] * 2, axis=0)
                        xs[row, cols] = ((part_of(u, k) - means[u]) * rstds[u] * g2 + b2).astype(jnp.bfloat16)
                return c2
            lax.fori_loop(0, LN_ROWS // (16 * LN_UNROLL), ln_rows, 0)
            rows = pl.ds(pl.multiple_of(i * LN_ROWS, LN_ROWS), LN_ROWS)
            pltpu.make_async_copy(xs.at[rows], x_out.at[rows], xo_sem).start()
            return c
        lax.fori_loop(0, TOK // LN_ROWS, ln_tile, 0)

        m_s[...] = jnp.full((TOK, 128), LOWEST, jnp.float32)
        s_s[...] = jnp.zeros((TOK, 128), jnp.float32)
        t_s[...] = jnp.zeros((TOK, 128), jnp.float32)
        for r in range(GROUPS):
            spread(tcol[r:r + 1, :], slice(r * 128, (r + 1) * 128), tc_v)
        z1[...] = jnp.full((HB, TILE), LOWEST, jnp.float32)

        zs = (z0, z1)

        def product(t, h):
            for r in range(0, HB, 512):
                zs[h][r:r + 512, :] = lax.dot_general(
                    xs[h * HB + r:h * HB + r + 512, :], ebuf[lax.rem(t, 2)], NT, preferred_element_type=jnp.float32)

        def statistics(t, h):
            z = zs[h]
            lane = lax.broadcasted_iota(jnp.int32, (STAT_ROWS, 128), 1)
            for r in range(0, HB, STAT_ROWS):
                rows = slice(h * HB + r, h * HB + r + STAT_ROWS)
                zk = [z[r:r + STAT_ROWS, k * 128:(k + 1) * 128] for k in range(TILE // 128)]
                old = m_s[rows, :]
                new = jnp.maximum(jnp.maximum(zk[0], zk[1]), old)
                tot = s_s[rows, :] * jnp.exp(old - new)
                tgt = t_s[rows, :]
                diff = tc_v[rows, :] - t * TILE
                for k in range(TILE // 128):
                    tot = tot + jnp.exp(zk[k] - new)
                    tgt = tgt + jnp.where(diff == lane + k * 128, zk[k], 0.0)
                m_s[rows, :] = new
                s_s[rows, :] = tot
                t_s[rows, :] = tgt

        def z_copy(t, h):
            return pltpu.make_async_copy(
                zs[h], z_out.at[pl.ds(h * HB, HB), pl.ds(pl.multiple_of(t * TILE, TILE), TILE)], z_sem.at[h])

        def start_events(t):
            @pl.when(t < TILES - 2)
            def _():
                x_event(t + 2)

            @pl.when(t == 0)
            def _():
                y_event(0)

            @pl.when(t == TILES - 3)
            def _():
                xt_copy(0).start()

            @pl.when(t == TILES - 1)
            def _():
                p_event(TILES - 1 - NEAR)
            e_load(t).wait()

            @pl.when(t < ROWS // TILE)
            def _():
                slot = lax.rem(t, 2)
                pltpu.make_async_copy(ebuf.at[slot], e_all.at[pl.ds(pl.multiple_of(t * TILE, TILE), TILE)], eo_sem.at[slot]).start()

        def middle_events(t):
            @pl.when(t < TILES - 1)
            def _():
                y_event(t + 1)

            @pl.when((t >= 1) & (t < ROWS // TILE + 1))
            def _():
                slot = lax.rem(t - 1, 2)
                pltpu.make_async_copy(ebuf.at[slot], e_all.at[pl.ds(0, TILE)], eo_sem.at[slot]).wait()

            @pl.when(t == NEAR)
            def _():
                pltpu.make_async_copy(xs, x_out, xo_sem).wait()

            @pl.when(t < ROWS // TILE - 1)
            def _():
                e_load_own(t + 1).start()

            @pl.when((t >= ROWS // TILE - 1) & (t < NEAR - 1))
            def _():
                @pl.when(lax.rem(t + 1, PE_ROWS // TILE) == 0)
                def _():
                    pe_copy((t + 1 - ROWS // TILE) // (PE_ROWS // TILE)).wait_recv()
                e_load(t + 1).start()

            @pl.when((t >= NEAR - 1) & (t < TILES - 2))
            def _():
                p_event(t - (NEAR - 1))

            @pl.when(t == TILES - 2)
            def _():
                for k, h in ((0, 0), (1, 0), (0, 1)):
                    z_load(zt, k, h).start()
                et_load(et, 0).start()

            @pl.when(t == NEAR + 1)
            def _():
                for cp in info_copies(1):
                    cp.wait_recv()
                for cp in own_info:
                    cp.wait()
                loads = [pltpu.make_async_copy(info_all.at[q, 1], infos.at[q, 1], small_sem.at[0]) for q in range(4)]
                for load in loads:
                    load.start()
                for load in loads:
                    load.wait()
                count = jnp.broadcast_to(token_count(), (1, 128))
                for r in range(GROUPS):
                    spread(mask[r:r + 1, :].astype(f32) / count, slice(r * 128, (r + 1) * 128), scale_v)

        def step(t, c):
            @pl.when(t > 0)
            def _():
                z_copy(t - 1, 1).start()
            start_events(t)

            @pl.when(t > 0)
            def _():
                z_copy(t - 1, 0).wait()
            statistics(t - 1, 1)
            product(t, 0)
            z_copy(t, 0).start()
            middle_events(t)

            @pl.when(t > 0)
            def _():
                z_copy(t - 1, 1).wait()
            statistics(t, 0)
            product(t, 1)
            return c
        last = TILES - 1
        lax.fori_loop(0, TILES, step, 0)
        z_copy(last, 1).start()
        statistics(last, 1)

        def finish(i, c):
            for u in range(8):
                r = i * 8 + u
                rows = pl.ds(pl.multiple_of(r * 128, 128), 128)
                m = m_s[rows, :]
                top = jnp.max(m, axis=-1, keepdims=True)
                tot = jnp.sum(s_s[rows, :] * jnp.exp(m - top), axis=-1, keepdims=True)
                lse = jnp.broadcast_to(top + jnp.log(tot), (128, 128))
                tgt = jnp.broadcast_to(jnp.sum(t_s[rows, :], axis=-1, keepdims=True), (128, 128))
                m_s[rows, :] = lse
                stat_v[0, pl.ds(r, 1), :] = jnp.transpose(lse)[0:1, :]
                stat_v[1, pl.ds(r, 1), :] = jnp.transpose(tgt)[0:1, :]
            return c
        lax.fori_loop(0, TOK // 1024, finish, 0)
        for h in range(2):
            z_copy(last, h).wait()
        half = e_all.at[pl.ds(0, ROWS // 2)]
        pltpu.make_async_copy(half, half, xs_send).wait()
        pltpu.make_async_copy(half, half, ys_send).wait()
        full = e_all.at[pl.ds(0, ROWS)]
        pltpu.make_async_copy(full, full, ds_send).wait()
        pltpu.make_async_copy(full, full, pe_send).wait()
        pltpu.make_async_copy(stat_v, stat_all.at[tp], small_sem.at[1]).start()
        for p, dev in group:
            remote(stat_v, stat_all.at[tp], sm_send, stat_recv.at[p], dev).start()

        def start_xt(j, c):
            xt_copy(j).start()
            return c
        lax.fori_loop(1, XCHS - 1, start_xt, 0)
        for q in range(4):
            last_part(q)[0].start()
        xp_copy.start()

    def z_load(zt, k, h):
        slot = lax.rem(k, 2)
        rows = slice(h * HB, (h + 1) * HB)
        return pltpu.make_async_copy(
            z_out.at[rows, pl.ds(pl.multiple_of(k * KT, KT), KT)], zt.at[slot, rows], zt_sem.at[2 * h + slot])

    def et_load(et, k):
        slot = lax.rem(k, 2)
        return pltpu.make_async_copy(e_all.at[pl.ds(pl.multiple_of(k * KT, KT), KT)], et.at[slot], et_sem.at[slot])

    def dzt_copy(k):
        rows = pl.ds(pl.multiple_of(lax.rem(k, 4) * KT, KT), KT)
        return remote(dzt_out.at[rows], dzt_part.at[rows], dz_send, dz_recv.at[lax.rem(k, 4)], part)

    def token_count():
        return jnp.sum(infos[:, 1].astype(f32))

    def token_grads(lse_v, scale_v, tcol_v, mr, zt, et, acc):
        def d_phase(da, db, dzt):
            def dzt_store(k, ref):
                slot = lax.rem(k, 2)
                return pltpu.make_async_copy(dzt.at[slot], ref.at[pl.ds(pl.multiple_of(lax.rem(k, 4) * KT, KT), KT)], eo_sem.at[slot])
            lane = lax.broadcasted_iota(jnp.int32, (PIECE, 128), 1)

            def piece(dst, rows, low, k, tie):
                slot = lax.rem(k, 2)
                lse = lse_v[rows, :]
                if tie is not None:
                    floor = 0.0 - jnp.maximum(0.0 - tie, -LOWEST)
                    lse = jnp.maximum(lse, jnp.concatenate([floor] * (PIECE // 8), axis=0))
                scale = scale_v[rows, :]
                diff = tcol_v[rows, :] - k * KT
                for g in range(KT // 128):
                    cols = slice(g * 128, (g + 1) * 128)
                    hot = (diff == lane + g * 128).astype(f32)
                    val = (jnp.exp(zt[slot, rows, cols] - lse) - hot) * scale
                    dst[low, cols] = val.astype(bf16)

            def half_step(k, src, dst, base, dst_base, dst_k):
                slot = lax.rem(k, 2)
                per = HB // (DIM // NCOL)
                for n in range(DIM // NCOL):
                    cols = slice(n * NCOL, (n + 1) * NCOL)
                    prod = jnp.dot(src[...], et[slot, :, cols], preferred_element_type=f32)
                    acc[base:base + HB, cols] = jnp.where(k == 0, 0.0, acc[base:base + HB, cols]) + prod
                    for q in range(0, per, PIECE):
                        at = q * HB // per
                        low = n * per + q
                        piece(dst, slice(dst_base + low, dst_base + low + PIECE), slice(low, low + PIECE), dst_k, prod[at:at + 8, 0:128])
                    if n * per % 256 == 0:
                        low = n * per
                        dzt[slot, :, base + low:base + low + 256] = jnp.transpose(src[low:low + 256, :])

            z_load(zt, 0, 0).wait()

            def first(i, c):
                rows = pl.ds(pl.multiple_of(i * PIECE, PIECE), PIECE)
                piece(da, rows, rows, 0, None)
                return c
            lax.fori_loop(0, HB // PIECE, first, 0)

            def step(k, c):
                @pl.when(k + 2 < VOCAB // KT)
                def _():
                    z_load(zt, k + 2, 0).start()

                @pl.when(k + 1 < VOCAB // KT)
                def _():
                    z_load(zt, k + 1, 1).start()
                    et_load(et, k + 1).start()
                    z_load(zt, k + 1, 0).wait()
                for at, j in WAIT_STEP.items():
                    @pl.when(k == at)
                    def _(j=j):
                        xt_event(j)

                @pl.when((k >= 2) & (k < 10))
                def _():
                    dzt_store(k, dzt_own).wait()

                @pl.when((k >= 6) & (k < 10))
                def _():
                    dzt_copy(k - 2).start()
                et_load(et, k).wait()
                z_load(zt, k, 1).wait()
                half_step(k, da, db, 0, HB, k)
                half_step(k, db, da, HB, 0, k + 1)

                @pl.when(k < 4)
                def _():
                    dzt_store(k, dzt_own).start()

                @pl.when((k >= 4) & (k < 8))
                def _():
                    dzt_store(k, dzt_out).start()
                return c
            lax.fori_loop(0, VOCAB // KT, step, 0)
        half = pltpu.VMEM((HB, KT), bf16)
        pl.run_scoped(d_phase, half, half, pltpu.VMEM((2, KT, TOK), bf16))

        def n_phase(hb, ob):
            def h_load(i):
                slot = lax.rem(i, 2)
                return pltpu.make_async_copy(hid.at[pl.ds(pl.multiple_of(i * NB_ROWS, NB_ROWS), NB_ROWS)], hb.at[slot], z_sem.at[slot])

            def o_store(i):
                slot = lax.rem(i, 2)
                return pltpu.make_async_copy(ob.at[slot], dhid.at[pl.ds(pl.multiple_of(i * NB_ROWS, NB_ROWS), NB_ROWS)], e_sem.at[slot])
            h_load(0).start()
            gb_v[...] = jnp.zeros(gb_v.shape, jnp.float32)
            g8[...] = jnp.broadcast_to(gain[...], (8, DIM))

            def tile(i, c):
                slot = lax.rem(i, 2)

                @pl.when(i + 1 < TOK // NB_ROWS)
                def _():
                    h_load(i + 1).start()

                @pl.when(i >= 2)
                def _():
                    o_store(i - 2).wait()
                h_load(i).wait()

                def rows_body(r, c2):
                    units = range(NB_UNROLL)
                    base = r * 16 * NB_UNROLL
                    low = [pl.ds(pl.multiple_of(base + u * 16, 16), 16) for u in units]
                    row = [pl.ds(pl.multiple_of(i * NB_ROWS + base + u * 16, 16), 16) for u in units]
                    zero = jnp.zeros((16, 128), jnp.float32)
                    sum1, sum3 = [zero] * NB_UNROLL, [zero] * NB_UNROLL

                    def load(u, cols):
                        dx = acc[row[u], cols]
                        xhat = (hb[slot, low[u], cols].astype(jnp.float32) - mr[0, row[u], :]) * mr[1, row[u], :]
                        return dx, xhat, dx * jnp.concatenate([g8[:, cols]] * 2, axis=0)
                    for k in range(DIM // 128):
                        cols = slice(k * 128, (k + 1) * 128)
                        d_gain, d_bias = gb_v[0, :, cols], gb_v[1, :, cols]
                        for u in units:
                            dx, xhat, gx = load(u, cols)
                            sum1[u] = sum1[u] + gx
                            sum3[u] = sum3[u] + gx * xhat
                            dgx = dx * xhat
                            d_gain = d_gain + (dgx[0:8] + dgx[8:16])
                            d_bias = d_bias + (dx[0:8] + dx[8:16])
                        gb_v[0, :, cols] = d_gain
                        gb_v[1, :, cols] = d_bias
                    slope, shift = [], []
                    for u in units:
                        mean, rstd = mr[0, row[u], :], mr[1, row[u], :]
                        c1 = jnp.broadcast_to(jnp.sum(sum1[u], axis=-1, keepdims=True) * (1.0 / DIM), (16, 128))
                        c3 = jnp.broadcast_to(jnp.sum(sum3[u], axis=-1, keepdims=True) * (1.0 / DIM), (16, 128))
                        slope.append(c3 * rstd * rstd)
                        shift.append(slope[u] * mean - c1 * rstd)
                    for u in units:
                        rstd = mr[1, row[u], :]
                        for k in range(DIM // 128):
                            cols = slice(k * 128, (k + 1) * 128)
                            gx = acc[row[u], cols] * jnp.concatenate([g8[:, cols]] * 2, axis=0)
                            ob[slot, low[u], cols] = (gx * rstd - hb[slot, low[u], cols].astype(f32) * slope[u] + shift[u]).astype(bf16)
                    return c2
                lax.fori_loop(0, NB_ROWS // (16 * NB_UNROLL), rows_body, 0)
                o_store(i).start()
                return c
            lax.fori_loop(0, TOK // NB_ROWS, tile, 0)
            for i in range(2):
                o_store(TOK // NB_ROWS - 2 + i).wait()
            gs_v[0:1, :] = jnp.sum(gb_v[0], axis=0, keepdims=True)
            gs_v[1:2, :] = jnp.sum(gb_v[1], axis=0, keepdims=True)
        pl.run_scoped(n_phase, pltpu.VMEM((2, NB_ROWS, DIM), bf16), pltpu.VMEM((2, NB_ROWS, DIM), bf16))

    def weight_grads(acc):
        own = pltpu.make_async_copy(gs_v, gsum_all.at[tp], g_sem)
        xt_event(3)

        def e_phase(eo, xt, dzb, zs, z1):
            eo_load = pltpu.make_async_copy(emb, eo, big_sem)

            def x_load(ref, row, slot):
                return pltpu.make_async_copy(ref.at[pl.ds(pl.multiple_of(row, KT), KT)], xt.at[slot], z_sem.at[slot])

            def dz_load(ref, col, slot):
                return pltpu.make_async_copy(ref.at[:, pl.ds(pl.multiple_of(col, KT), KT)], dzb.at[slot], e_sem.at[slot])

            def start_local(i):
                slot = lax.rem(i, 2)

                @pl.when(i < 4)
                def _():
                    x_load(x_out, i * KT, slot).start()
                    dz_load(dzt_own, i * KT, slot).start()

                @pl.when(i >= 4)
                def _():
                    x_load(x_part, (i - 4) * KT, slot).start()
                    dz_load(dzt_part, (i - 4) * KT, slot).start()

            def add(slot, first):
                def mul(h, c2):
                    rows = pl.ds(pl.multiple_of(h * HB, HB), HB)
                    for n in range(0, DIM, NCOL):
                        prod = jnp.dot(dzb[slot, rows, :], xt[slot, :, n:n + NCOL], preferred_element_type=f32)
                        acc[rows, n:n + NCOL] = jnp.where(first, 0.0, acc[rows, n:n + NCOL]) + prod
                    return c2
                lax.fori_loop(0, HBS, mul, 0)

            start_local(0)

            def rem_load(r):
                slot = lax.rem(r, 2)
                return [pltpu.make_async_copy(xrows(ref, r), xt.at[slot, pl.ds(i * XCH, XCH)], z_sem.at[slot])
                        for i, ref in enumerate((x_xp, x_xq))]

            def local(i, c):
                slot = lax.rem(i, 2)

                @pl.when(i == 0)
                def _():
                    eo_load.start()

                @pl.when(i == 2)
                def _():
                    xp_copy.wait_recv()

                    def wait_dz(q, c2):
                        dzt_copy(q).wait_recv()
                        return c2
                    lax.fori_loop(0, 4, wait_dz, 0)

                @pl.when(i == 1)
                def _():
                    own.start()
                    for p, dev in group:
                        remote(gs_v, gsum_all.at[tp], g_send, g_recv.at[p], dev).start()

                @pl.when(i == 6)
                def _():
                    xt_event(4)

                @pl.when(i < 7)
                def _():
                    start_local(i + 1)

                @pl.when(i == 7)
                def _():
                    xd_copy(0).wait_recv()
                    for cp in rem_load(0):
                        cp.start()
                x_load(x_out, 0, slot).wait()
                dz_load(dzt_own, 0, slot).wait()
                add(slot, i == 0)
                return c
            lax.fori_loop(0, 8, local, 0)
            eo_load.wait()
            for p, dev in group:
                remote(stat_v, stat_all.at[tp], sm_send, stat_recv.at[p], dev).wait_recv()
            pltpu.make_async_copy(stat_v, stat_all.at[tp], small_sem.at[1]).wait()
            for cp in info_copies(0):
                cp.wait_recv()
            loads = [pltpu.make_async_copy(stat_all, stats, small_sem.at[1])]
            loads += [pltpu.make_async_copy(info_all.at[q, 0], infos.at[q, 0], small_sem.at[0]) for q in range(4)]
            for load in loads:
                load.start()
            for load in loads:
                load.wait()
            count = jnp.broadcast_to(token_count(), (1, 128))

            def far(r, c):
                slot = lax.rem(r, 2)

                @pl.when(r == 1)
                def _():
                    xt_event(5)

                @pl.when(r == 4)
                def _():
                    xt_event(6)

                def fetch():
                    xd_copy(r + 1).wait_recv()
                    for cp in rem_load(r + 1):
                        cp.start()
                pl.when(r < XCHS - 2)(fetch)
                x_load(x_out, 0, slot).wait()

                @pl.when(r == XCHS - DEFER)
                def _():
                    pltpu.make_async_copy(acc, de_part, big_sem).start()

                @pl.when(r > XCHS - DEFER + 1)
                def _():
                    dz_out(0, slot).wait()

                far_rows = []
                for g in range(4):
                    who = xp_rank if g < 2 else xq_rank
                    at = pl.ds(2 * r + g % 2, 1)
                    far_rows.append((stats[who, 0, at, :], infos[who, 1, at, :].astype(f32) / count, infos[who, 0, at, :] - tp * ROWS))

                def logits(h2, c2):
                    @pl.when((r == XCHS - 2) & (h2 == 1))
                    def _():
                        for q in range(3):
                            last_event(q)

                    def multiply(h, z):
                        for k in range(0, DIM, KCOL):
                            prod = lax.dot_general(eo[pl.ds(pl.multiple_of(h * ZB, ZB), ZB), k:k + KCOL], xt[slot, :, k:k + KCOL], NT, preferred_element_type=f32)
                            z[...] = prod if k == 0 else z[...] + prod

                    def convert(h, z):
                        for q in range(ZB // 32):
                            row = h * ZB + q * 32
                            line = lax.broadcasted_iota(jnp.int32, (32, 128), 0)
                            for g, (lse, scale, trel) in enumerate(far_rows):
                                cols = slice(g * 128, (g + 1) * 128)
                                hot = ((trel - row) == line).astype(f32)
                                val = (jnp.exp(z[q * 32:(q + 1) * 32, cols] - lse) - hot) * scale
                                dzb[slot, pl.ds(pl.multiple_of(row, 32), 32), cols] = val.astype(bf16)
                    multiply(2 * h2, zs)
                    multiply(2 * h2 + 1, z1)
                    convert(2 * h2, zs)
                    convert(2 * h2 + 1, z1)
                    return c2
                lax.fori_loop(0, ROWS // (2 * ZB), logits, 0)

                @pl.when(r == XCHS - 2)
                def _():
                    last_event(3)

                @pl.when(r < XCHS - DEFER)
                def _():
                    def mul(h, c2):
                        rows = pl.ds(pl.multiple_of(h * HB, HB), HB)
                        for n in range(0, DIM, NCOL):
                            acc[rows, n:n + NCOL] += jnp.dot(dzb[slot, rows, :], xt[slot, :, n:n + NCOL], preferred_element_type=jnp.float32)
                        return c2
                    lax.fori_loop(0, HBS, mul, 0)

                @pl.when(r >= XCHS - DEFER)
                def _():
                    dz_out(r - (XCHS - DEFER), slot).start()
                return c

            def dz_out(q, slot):
                return pltpu.make_async_copy(dzb.at[slot], dzt_last.at[q], dzo_sem.at[slot])
            lax.fori_loop(0, XCHS - 1, far, 0)
            for slot in range(2):
                dz_out(0, slot).wait()
            xd_copy(XCHS - 1).wait_recv()
            pltpu.make_async_copy(acc, de_part, big_sem).wait()
        pl.run_scoped(e_phase, pltpu.VMEM((ROWS, DIM), jnp.bfloat16), pltpu.VMEM((2, KT, DIM), jnp.bfloat16),
                      pltpu.VMEM((2, ROWS, KT), jnp.bfloat16), pltpu.VMEM((ZB, KT), f32), pltpu.VMEM((ZB, KT), f32))

        own.wait()

    wide = pltpu.VMEM((TOK, 128), f32)
    big = pltpu.VMEM((TOK, DIM), f32)

    def tokens(m_s, scale_v, tc_v, mr_v, zt, et):
        kept = (m_s, scale_v, tc_v, mr_v, zt, et)
        pl.run_scoped(functools.partial(forward, *kept), pltpu.VMEM((TOK, DIM), bf16), pltpu.VMEM((2, LN_ROWS, DIM), bf16),
                      pltpu.VMEM((2, TILE, DIM), bf16), pltpu.VMEM((HB, TILE), f32), pltpu.VMEM((HB, TILE), f32), wide, wide,
                      pltpu.VMEM((2, 8, DIM), f32))
        pl.run_scoped(functools.partial(token_grads, *kept), big)
    pl.run_scoped(tokens, wide, wide, pltpu.VMEM((TOK, 128), jnp.int32), pltpu.VMEM((2, TOK, 128), f32),
                  pltpu.VMEM((2, TOK, KT), f32), pltpu.VMEM((2, KT, DIM), bf16))
    pl.run_scoped(weight_grads, big)

    pltpu.make_async_copy(x_out, x_out, xt_send).wait()
    pltpu.make_async_copy(x_out, x_out, xd_send).wait()
    xp_copy.wait_send()
    pltpu.make_async_copy(dzt_out, dzt_out, dz_send).wait()
    for cp in (*info_copies(0), *info_copies(1)):
        cp.wait_send()
    for p, dev in group:
        remote(stat_v, stat_all.at[tp], sm_send, stat_recv.at[p], dev).wait_send()
        remote(gs_v, gsum_all.at[tp], g_send, g_recv.at[p], dev).wait()


def run_step(hidden, gain, bias, embed, targets, mask):
    any_spec = pl.BlockSpec(memory_space=pl.ANY)
    vmem_spec = pl.BlockSpec(memory_space=pltpu.VMEM)
    f32, bf16, i32 = jnp.float32, jnp.bfloat16, jnp.int32
    dma = pltpu.SemaphoreType.DMA
    small, ints = (4, 2, GROUPS, 128), (4, 2, GROUPS, 128)
    mat, square = ((TOK, DIM), bf16), ((ROWS, TOK), bf16)
    shapes = [((VOCAB, DIM), bf16), mat, ((TOK, VOCAB), f32), (small, f32), (ints, i32),
              mat, mat, mat, mat, square, square, square, ((DEFER - 1, ROWS, KT), bf16), ((ROWS, DIM), f32), ((4, 2, DIM), f32)]
    return pl.pallas_call(
        step_kernel,
        name="step",
        out_shape=[jax.ShapeDtypeStruct(s, d) for s, d in shapes],
        in_specs=[any_spec, vmem_spec, vmem_spec, any_spec, vmem_spec, vmem_spec],
        out_specs=[any_spec] * len(shapes),
        scratch_shapes=[
            pltpu.VMEM((GROUPS, 128), i32), pltpu.VMEM((2, GROUPS, 128), f32), pltpu.VMEM(small, f32), pltpu.VMEM(ints, i32),
            pltpu.VMEM((2, 8, DIM), f32), pltpu.VMEM((2, DIM), f32), pltpu.VMEM((8, DIM), f32),
            dma((2,)), dma, dma((2,)), dma((2,)), dma((2,)), dma((4,)), dma((2,)), dma((2,)), dma((2,)), dma, dma,
            dma, dma, dma, dma, dma, dma, dma, dma, dma, dma,
            dma((CHUNKS,)), dma((CHUNKS,)), dma((TILES - NEAR,)), dma((ROWS // PE_ROWS,)), dma((8,)), dma((4,)),
            dma((XCHS + 3,)), dma((XCHS,)), dma, dma((4,)), dma((4,)),
        ],
        compiler_params=pltpu.CompilerParams(collective_id=0, has_side_effects=True, vmem_limit_bytes=67043328),
        cost_estimate=pl.CostEstimate(flops=12 * TOK * VOCAB * DIM, bytes_accessed=700 * 2 ** 20, transcendentals=3 * TOK * VOCAB),
    )(hidden, gain, bias, embed, targets, mask)


def finish_kernel(de_in, dzt_last, x_xp, x_xq, emb, dh_in, stat_all, info_all, gsum_all,
                  de_out, dh_out, loss, mean, d_gain, d_bias,
                  x7, xr, dz, eb, zs, din, dout, hb, x_sem, z_sem, e_sem, di_sem, do_sem, hi_sem, ho_sem):
    f32, bf16 = jnp.float32, jnp.bfloat16
    last = DEFER - 1

    def x_last():
        rows = pl.ds((XCHS - 1) * XCH, XCH)
        return [pltpu.make_async_copy(ref.at[rows], x7.at[pl.ds(i * XCH, XCH)], x_sem.at[3]) for i, ref in enumerate((x_xp, x_xq))]

    def x_tiles(i):
        slot = lax.rem(i, 3)
        cols = pl.ds(pl.multiple_of(i * KT, KT), KT)
        rows = pl.ds((XCHS - DEFER) * XCH, last * XCH)
        return [pltpu.make_async_copy(ref.at[rows, cols], xr.at[slot, j], x_sem.at[slot]) for j, ref in enumerate((x_xp, x_xq))]

    def e_load(h):
        slot = lax.rem(h, 2)
        return pltpu.make_async_copy(emb.at[pl.ds(pl.multiple_of(h * ZB, ZB), ZB)], eb.at[slot], e_sem.at[slot])

    def z_load(q):
        return pltpu.make_async_copy(dzt_last.at[q], dz.at[q], z_sem.at[q])

    def tile(ref, i):
        return ref.at[:, pl.ds(pl.multiple_of(i * KT, KT), KT)]

    def d_load(i):
        slot = lax.rem(i, 3)
        return pltpu.make_async_copy(tile(de_in, i), din.at[slot], di_sem.at[slot])

    def d_store(i):
        slot = lax.rem(i, 3)
        return pltpu.make_async_copy(dout.at[slot], tile(de_out, i), do_sem.at[slot])
    steps = DIM // KT
    per = TOK // steps

    def h_load(i):
        slot = lax.rem(i, 2)
        return pltpu.make_async_copy(dh_in.at[pl.ds(pl.multiple_of(i * per, per), per)], hb.at[slot], hi_sem.at[slot])

    def h_store(i):
        slot = lax.rem(i, 2)
        return pltpu.make_async_copy(hb.at[slot], dh_out.at[pl.ds(pl.multiple_of(i * per, per), per)], ho_sem.at[slot])
    for cp in x_last():
        cp.start()
    e_load(0).start()
    e_load(1).start()

    def tile_loads(i):
        for cp in (*x_tiles(i), d_load(i)):
            cp.start()

    tp = lax.axis_index('tp')
    core = lax.rem(tp, 2)
    other = 2 - (tp - core)
    weights = info_all[:, 1].astype(f32)
    total = jnp.sum(weights)
    all_loss = (stat_all[:, 0] - stat_all[:, 1]) * weights
    loss[...] = (stat_all[tp, 0] - stat_all[tp, 1]) * info_all[tp, 1].astype(f32)
    mean[...] = jnp.broadcast_to(jnp.sum(all_loss), (1, 1)) / jnp.broadcast_to(total, (1, 1))
    sums = ((gsum_all[0] + gsum_all[1]) + gsum_all[2]) + gsum_all[3]
    d_gain[...] = sums[0:1]
    d_bias[...] = sums[1:2]
    count = jnp.broadcast_to(total, (1, 128))
    far_rows = []
    for g in range(4):
        who = other + core if g < 2 else other + 1 - core
        at = slice(GROUPS - 2 + g % 2, GROUPS - 1 + g % 2)
        far_rows.append((stat_all[who, 0, at, :], info_all[who, 1, at, :].astype(f32) / count, info_all[who, 0, at, :] - tp * ROWS))
    pltpu.make_async_copy(x7, x7, x_sem.at[3]).wait()

    def logits(h, c):
        slot = lax.rem(h, 2)
        e_load(h).wait()
        for k in range(0, DIM, KCOL):
            prod = lax.dot_general(eb[slot, :, k:k + KCOL], x7[:, k:k + KCOL], NT, preferred_element_type=f32)
            zs[...] = prod if k == 0 else zs[...] + prod

        @pl.when(h == 0)
        def _():
            e_load(2).start()
            z_load(0).start()
            z_load(1).start()

        @pl.when(h == 1)
        def _():
            e_load(3).start()
            z_load(2).start()

        @pl.when(h == 2)
        def _():
            tile_loads(0)
            h_load(0).start()

        @pl.when(h == 3)
        def _():
            tile_loads(1)
        for q in range(ZB // 32):
            row = h * ZB + q * 32
            line = lax.broadcasted_iota(jnp.int32, (32, 128), 0)
            for g, (lse, scale, trel) in enumerate(far_rows):
                cols = slice(g * 128, (g + 1) * 128)
                hot = ((trel - row) == line).astype(f32)
                val = (jnp.exp(zs[q * 32:(q + 1) * 32, cols] - lse) - hot) * scale
                dz[last, pl.ds(pl.multiple_of(row, 32), 32), cols] = val.astype(bf16)
        return c
    lax.fori_loop(0, ROWS // ZB, logits, 0)
    for q in range(last):
        z_load(q).wait()

    def step(i, c):
        slot = lax.rem(i, 3)
        cols = pl.ds(pl.multiple_of(i * KT, KT), KT)

        @pl.when(i + 2 < steps)
        def _():
            tile_loads(i + 2)
        h_load(i).wait()
        h_store(i).start()

        @pl.when(i >= 1)
        def _():
            h_store(i - 1).wait()

        @pl.when(i + 1 < steps)
        def _():
            h_load(i + 1).start()

        @pl.when(i >= 3)
        def _():
            d_store(i - 3).wait()
        d_load(i).wait()
        for cp in x_tiles(i):
            cp.wait()
        for h in range(HBS):
            rows = slice(h * HB, (h + 1) * HB)
            prod = jnp.dot(dz[last, rows, :], x7[:, cols], preferred_element_type=f32)
            for q in range(last):
                for j in range(2):
                    prod = prod + jnp.dot(dz[q, rows, j * XCH:(j + 1) * XCH], xr[slot, j, q * XCH:(q + 1) * XCH, :], preferred_element_type=f32)
            dout[slot, rows, :] = din[slot, rows, :] + prod
        d_store(i).start()
        return c
    lax.fori_loop(0, steps, step, 0)
    for i in range(3):
        d_store(steps - 3 + i).wait()
    h_store(steps - 1).wait()


def finish(de_part, dzt_last, x_xp, x_xq, embed, dhid, stat_all, info_all, gsum_all):
    any_spec = pl.BlockSpec(memory_space=pl.ANY)
    vmem_spec = pl.BlockSpec(memory_space=pltpu.VMEM)
    f32, bf16 = jnp.float32, jnp.bfloat16
    dma = pltpu.SemaphoreType.DMA
    outs = [((ROWS, DIM), f32), ((TOK, DIM), bf16), ((GROUPS, 128), f32), ((1, 1), f32), ((1, DIM), f32), ((1, DIM), f32)]
    return pl.pallas_call(
        finish_kernel,
        name="finish",
        out_shape=[jax.ShapeDtypeStruct(s, d) for s, d in outs],
        in_specs=[any_spec] * 6 + [vmem_spec] * 3,
        out_specs=[any_spec] * 2 + [vmem_spec] * 4,
        scratch_shapes=[
            pltpu.VMEM((KT, DIM), bf16), pltpu.VMEM((3, 2, (DEFER - 1) * XCH, KT), bf16), pltpu.VMEM((DEFER, ROWS, KT), bf16), pltpu.VMEM((2, ZB, DIM), bf16), pltpu.VMEM((ZB, KT), f32),
            pltpu.VMEM((3, ROWS, KT), f32), pltpu.VMEM((3, ROWS, KT), f32), pltpu.VMEM((2, TOK // (DIM // KT), DIM), bf16),
            dma((4,)), dma((DEFER,)), dma((2,)), dma((3,)), dma((3,)), dma((2,)), dma((2,)),
        ],
        compiler_params=pltpu.CompilerParams(vmem_limit_bytes=67043328),
        cost_estimate=pl.CostEstimate(flops=2 * ROWS * DIM * KT * (DEFER + 1), bytes_accessed=130 * 2 ** 20, transcendentals=ROWS * KT),
    )(de_part, dzt_last, x_xp, x_xq, embed, dhid, stat_all, info_all, gsum_all)


def solution(mesh):
    def body(hidden, ln_gain, ln_bias, embed, targets, loss_mask):
        outs = run_step(hidden, ln_gain.reshape(1, DIM), ln_bias.reshape(1, DIM), embed, targets.reshape(GROUPS, 128), loss_mask.reshape(GROUPS, 128))
        stat_all, info_all, dhid, x_xp, x_xq, dzt_last, de_part, gsum_all = (outs[i] for i in (3, 4, 5, 7, 8, 12, 13, 14))
        d_embed, d_hidden, loss, mean, d_gain, d_bias = finish(de_part, dzt_last, x_xp, x_xq, embed, dhid, stat_all, info_all, gsum_all)
        return loss.reshape(TOK), mean.reshape(1), d_hidden, d_embed, d_gain.reshape(DIM), d_bias.reshape(DIM)

    token_rows = P(('dp', 'tp'))
    token_mat = P(('dp', 'tp'), None)
    return jax.shard_map(body, mesh=mesh, in_specs=(token_mat, P(), P(), P('tp', None), token_rows, token_rows), out_specs=(token_rows, P('dp'), token_mat, token_mat, P('dp'), P('dp')), check_vma=False)
```

```python
import functools

import jax
import jax.numpy as jnp
from jax import lax
from jax.experimental import pallas as pl
from jax.experimental.pallas import tpu as pltpu
from jax.sharding import PartitionSpec as P

LN_EPS = 1e-5
LOWEST = float(jnp.finfo(jnp.float32).min)

TOK = 2048
ROWS = 2048
DIM = 4096
VOCAB = 8192
TILE = 256
TILES = VOCAB // TILE
HB = 1024
HBS = TOK // HB
CHUNK = 32
PIECE_ROWS = 2 * CHUNK
NEAR = 2 * ROWS // TILE
PE_ROWS = 512
CHUNKS = ROWS // 2 // CHUNK
LN_ROWS = 256
STAT_ROWS = 32
PIECE = 32
LN_UNROLL = 4
XCH = 256
XCHS = TOK // XCH
KT = 512
DEFER = 3
WAIT_STEP = {4: 0, 9: 1, 14: 2}
ZB = 512
NCOL = 512
KCOL = 1024
NB_UNROLL = 4
NB_ROWS = 256
GROUPS = TOK // 128
NT = (((1,), (1,)), ((), ()))


def peers():
    dp, tp = lax.axis_index('dp'), lax.axis_index('tp')
    core = lax.rem(tp, 2)
    pair = tp - core
    other = 2 - pair
    part = pair + 1 - core
    return dp, tp, (dp, part), (dp, other + core), (dp, other + 1 - core), (1 - dp, tp)


def remote(src, dst, ssem, rsem, dev):
    return pltpu.make_async_remote_copy(
        src_ref=src, dst_ref=dst, send_sem=ssem, recv_sem=rsem, device_id=dev, device_id_type=pl.DeviceIdType.MESH)


def spread(row, rows, dst):
    dst[rows, :] = jnp.transpose(jnp.broadcast_to(row, (128, 128)))


def step_kernel(hid, gain, bias, emb, targets, mask,
                e_all, x_out, z_out, stat_all, info_all,
                dhid, x_part, x_xp, x_xq, dzt_own, dzt_out, dzt_part, dzt_last, de_part, gsum_all,
                tcol, stat_v, stats, infos, gb_v, gs_v, g8,
                h_sem, xo_sem, e_sem, eo_sem, z_sem, zt_sem, et_sem, small_sem, dzo_sem, big_sem, g_sem,
                xs_send, ys_send, ds_send, pe_send, sm_send, xt_send, xd_send, xp_send, dz_send, g_send,
                x_recv, y_recv, d_recv, pe_recv, info_recv, stat_recv, xt_recv, xd_recv, xp_recv, dz_recv, g_recv):
    bf16, f32 = jnp.bfloat16, jnp.float32
    dp, tp, part, xp, xq, yp = peers()
    core = lax.rem(tp, 2)
    xp_rank = 2 - (tp - core) + core
    xq_rank = 2 - (tp - core) + 1 - core
    group = ((1, part), (2, xp), (3, xq))
    barrier = pltpu.get_barrier_semaphore()
    for dev in (part, xp, xq, yp):
        pl.semaphore_signal(barrier, inc=1, device_id=dev, device_id_type=pl.DeviceIdType.MESH)
    pl.semaphore_wait(barrier, 4)

    def info_copies(i):
        ref = (targets, mask)[i]
        return [remote(ref, info_all.at[tp, i], sm_send, info_recv.at[2 * p + i], dev) for p, dev in group]

    def columns():
        for s in range(4):
            pair, odd = s - s % 2, s % 2
            near = ((tp - core) == pair).astype(jnp.int32)
            same = (core == odd).astype(jnp.int32)
            row = targets[...] - s * ROWS
            low = (row < ROWS // 2).astype(jnp.int32)
            sub = row - (1 - low) * (ROWS // 2)
            crossed = low * dp + (1 - low) * (1 - dp)
            piece = (1 - same) * 2 + crossed
            tile = (sub.astype(f32) * (1.0 / PIECE_ROWS)).astype(jnp.int32)
            far = 2 * ROWS + tile * (TILE - PIECE_ROWS) + sub + piece * PIECE_ROWS
            col = near * ((1 - same) * ROWS + row) + (1 - near) * far
            inside = (row >= 0) & (row < ROWS)
            tcol[...] = jnp.where(inside, col, 0 if s == 0 else tcol[...])

    def xrows(ref, j):
        return ref.at[pl.ds(pl.multiple_of(j * XCH, XCH), XCH)]

    def xt_copy(j):
        return remote(xrows(x_out, j), xrows(x_xp, j), xt_send, xt_recv.at[j], xp)

    def xd_copy(j):
        return remote(xrows(x_xp, j), xrows(x_xq, j), xd_send, xd_recv.at[j], part)

    def last_part(q):
        rows = pl.ds((XCHS - 1) * XCH + q * (XCH // 4), XCH // 4)
        return (remote(x_out.at[rows], x_xp.at[rows], xt_send, xt_recv.at[XCHS - 1 + q], xp),
                remote(x_xp.at[rows], x_xq.at[rows], xd_send, xd_recv.at[XCHS - 1], part))

    def last_event(q):
        arrive, hand_on = last_part(q)
        arrive.wait_recv()
        hand_on.start()

    def xt_event(j):
        xt_copy(j).wait_recv()
        xd_copy(j).start()
    xp_copy = remote(x_out, x_part, xp_send, xp_recv, part)

    def forward(m_s, scale_v, tc_v, mr_v, zt, et, xs, hbuf, ebuf, z0, z1, s_s, t_s, gb8):
        def tile_row(j):
            return ROWS * 2 + (j // 2) * TILE + lax.rem(j, 2) * CHUNK

        def x_copy(j):
            src = emb.at[pl.ds(pl.multiple_of(dp * (ROWS // 2) + j * CHUNK, CHUNK), CHUNK)]
            return remote(src, e_all.at[pl.ds(pl.multiple_of(tile_row(j), CHUNK), CHUNK)], xs_send, x_recv.at[j], xp)

        def piece(j, p):
            return e_all.at[pl.ds(pl.multiple_of(tile_row(j) + p * PIECE_ROWS, CHUNK), CHUNK)]

        def y_copy(j):
            return remote(piece(j, 0), piece(j, 1), ys_send, y_recv.at[j], yp)

        def d_copy(j, p):
            return remote(piece(j, p), piece(j, p + 2), ds_send, d_recv.at[j // 2], part)

        def pe_copy(i):
            return remote(emb.at[pl.ds(pl.multiple_of(i * PE_ROWS, PE_ROWS), PE_ROWS)],
                          e_all.at[pl.ds(pl.multiple_of(ROWS + i * PE_ROWS, PE_ROWS), PE_ROWS)], pe_send, pe_recv.at[i], part)


        def h_copy(i):
            return pltpu.make_async_copy(hid.at[pl.ds(pl.multiple_of(i * LN_ROWS, LN_ROWS), LN_ROWS)], hbuf.at[lax.rem(i, 2)], h_sem.at[lax.rem(i, 2)])
        h_copy(0).start()

        for j in range(2):
            x_copy(j).start()
        for cp in info_copies(1):
            cp.start()

        def start_x(j, c):
            x_copy(j).start()
            return c
        lax.fori_loop(2, CHUNKS, start_x, 0)
        for cp in info_copies(0):
            cp.start()

        def start_pe(i, c):
            pe_copy(i).start()
            return c
        lax.fori_loop(0, ROWS // PE_ROWS, start_pe, 0)

        def e_load(t):
            slot = lax.rem(t, 2)
            return pltpu.make_async_copy(e_all.at[pl.ds(pl.multiple_of(t * TILE, TILE), TILE)], ebuf.at[slot], e_sem.at[slot])

        def e_load_own(t):
            slot = lax.rem(t, 2)
            return pltpu.make_async_copy(emb.at[pl.ds(pl.multiple_of(t * TILE, TILE), TILE)], ebuf.at[slot], e_sem.at[slot])
        e_load_own(0).start()

        def x_event(j):
            x_copy(j).wait_recv()
            y_copy(j).start()
            d_copy(j, 0).start()

        def y_event(j):
            y_copy(j).wait_recv()
            d_copy(j, 1).start()

        def p_event(k):
            rows = e_all.at[pl.ds(pl.multiple_of(2 * ROWS + k * TILE + TILE // 2, TILE // 2), TILE // 2)]
            pltpu.make_async_copy(rows, rows, d_recv.at[k]).wait()
            e_load(NEAR + k).start()

        own_info = [pltpu.make_async_copy(ref, info_all.at[tp, i], small_sem.at[0]) for i, ref in enumerate((targets, mask))]
        for cp in own_info:
            cp.start()
        columns()
        gb8[0] = jnp.broadcast_to(gain[...], (8, DIM))
        gb8[1] = jnp.broadcast_to(bias[...], (8, DIM))

        def ln_tile(i, c):
            slot = lax.rem(i, 2)

            @pl.when(i + 1 < TOK // LN_ROWS)
            def _():
                h_copy(i + 1).start()
            h_copy(i).wait()

            for at, j in ((4, 0), (7, 1)):
                @pl.when(i == at)
                def _(j=j):
                    x_event(j)

            def ln_rows(r, c2):
                base = r * LN_UNROLL * 16

                def at(u):
                    return pl.ds(pl.multiple_of(base + u * 16, 16), 16)

                def part_of(u, k):
                    return hbuf[slot, at(u), k * 128:(k + 1) * 128].astype(jnp.float32)
                means, rstds = [], []
                for u in range(LN_UNROLL):
                    tot = part_of(u, 0)
                    for k in range(1, DIM // 128):
                        tot = tot + part_of(u, k)
                    means.append(jnp.broadcast_to(jnp.sum(tot, axis=-1, keepdims=True) * (1.0 / DIM), (16, 128)))
                for u in range(LN_UNROLL):
                    tot = jnp.zeros((16, 128), jnp.float32)
                    for k in range(DIM // 128):
                        diff = part_of(u, k) - means[u]
                        tot = tot + diff * diff
                    var = jnp.sum(tot, axis=-1, keepdims=True) * (1.0 / DIM)
                    rstds.append(jnp.broadcast_to(lax.rsqrt(var + LN_EPS), (16, 128)))
                for u in range(LN_UNROLL):
                    row = pl.ds(pl.multiple_of(i * LN_ROWS + base + u * 16, 16), 16)
                    mr_v[0, row, :] = means[u]
                    mr_v[1, row, :] = rstds[u]
                    for k in range(DIM // 128):
                        cols = slice(k * 128, (k + 1) * 128)
                        g2 = jnp.concatenate([gb8[0, :, cols]] * 2, axis=0)
                        b2 = jnp.concatenate([gb8[1, :, cols]] * 2, axis=0)
                        xs[row, cols] = ((part_of(u, k) - means[u]) * rstds[u] * g2 + b2).astype(jnp.bfloat16)
                return c2
            lax.fori_loop(0, LN_ROWS // (16 * LN_UNROLL), ln_rows, 0)
            rows = pl.ds(pl.multiple_of(i * LN_ROWS, LN_ROWS), LN_ROWS)
            pltpu.make_async_copy(xs.at[rows], x_out.at[rows], xo_sem).start()
            return c
        lax.fori_loop(0, TOK // LN_ROWS, ln_tile, 0)

        m_s[...] = jnp.full((TOK, 128), LOWEST, jnp.float32)
        s_s[...] = jnp.zeros((TOK, 128), jnp.float32)
        t_s[...] = jnp.zeros((TOK, 128), jnp.float32)
        for r in range(GROUPS):
            spread(tcol[r:r + 1, :], slice(r * 128, (r + 1) * 128), tc_v)
        z1[...] = jnp.full((HB, TILE), LOWEST, jnp.float32)

        zs = (z0, z1)

        def product(t, h):
            for r in range(0, HB, 512):
                zs[h][r:r + 512, :] = lax.dot_general(
                    xs[h * HB + r:h * HB + r + 512, :], ebuf[lax.rem(t, 2)], NT, preferred_element_type=jnp.float32)

        def statistics(t, h):
            z = zs[h]
            lane = lax.broadcasted_iota(jnp.int32, (STAT_ROWS, 128), 1)
            for r in range(0, HB, STAT_ROWS):
                rows = slice(h * HB + r, h * HB + r + STAT_ROWS)
                zk = [z[r:r + STAT_ROWS, k * 128:(k + 1) * 128] for k in range(TILE // 128)]
                old = m_s[rows, :]
                new = jnp.maximum(jnp.maximum(zk[0], zk[1]), old)
                tot = s_s[rows, :] * jnp.exp(old - new)
                tgt = t_s[rows, :]
                diff = tc_v[rows, :] - t * TILE
                for k in range(TILE // 128):
                    tot = tot + jnp.exp(zk[k] - new)
                    tgt = tgt + jnp.where(diff == lane + k * 128, zk[k], 0.0)
                m_s[rows, :] = new
                s_s[rows, :] = tot
                t_s[rows, :] = tgt

        def z_copy(t, h):
            return pltpu.make_async_copy(
                zs[h], z_out.at[pl.ds(h * HB, HB), pl.ds(pl.multiple_of(t * TILE, TILE), TILE)], z_sem.at[h])

        def start_events(t):
            @pl.when(t < TILES - 2)
            def _():
                x_event(t + 2)

            @pl.when(t == 0)
            def _():
                y_event(0)

            @pl.when(t == TILES - 3)
            def _():
                xt_copy(0).start()

            @pl.when(t == TILES - 1)
            def _():
                p_event(TILES - 1 - NEAR)
            e_load(t).wait()

            @pl.when(t < ROWS // TILE)
            def _():
                slot = lax.rem(t, 2)
                pltpu.make_async_copy(ebuf.at[slot], e_all.at[pl.ds(pl.multiple_of(t * TILE, TILE), TILE)], eo_sem.at[slot]).start()

        def middle_events(t):
            @pl.when(t < TILES - 1)
            def _():
                y_event(t + 1)

            @pl.when((t >= 1) & (t < ROWS // TILE + 1))
            def _():
                slot = lax.rem(t - 1, 2)
                pltpu.make_async_copy(ebuf.at[slot], e_all.at[pl.ds(0, TILE)], eo_sem.at[slot]).wait()

            @pl.when(t == NEAR)
            def _():
                pltpu.make_async_copy(xs, x_out, xo_sem).wait()

            @pl.when(t < ROWS // TILE - 1)
            def _():
                e_load_own(t + 1).start()

            @pl.when((t >= ROWS // TILE - 1) & (t < NEAR - 1))
            def _():
                @pl.when(lax.rem(t + 1, PE_ROWS // TILE) == 0)
                def _():
                    pe_copy((t + 1 - ROWS // TILE) // (PE_ROWS // TILE)).wait_recv()
                e_load(t + 1).start()

            @pl.when((t >= NEAR - 1) & (t < TILES - 2))
            def _():
                p_event(t - (NEAR - 1))

            @pl.when(t == TILES - 2)
            def _():
                for k, h in ((0, 0), (1, 0), (0, 1)):
                    z_load(zt, k, h).start()
                et_load(et, 0).start()

            @pl.when(t == NEAR + 1)
            def _():
                for cp in info_copies(1):
                    cp.wait_recv()
                for cp in own_info:
                    cp.wait()
                loads = [pltpu.make_async_copy(info_all.at[q, 1], infos.at[q, 1], small_sem.at[0]) for q in range(4)]
                for load in loads:
                    load.start()
                for load in loads:
                    load.wait()
                count = jnp.broadcast_to(token_count(), (1, 128))
                for r in range(GROUPS):
                    spread(mask[r:r + 1, :].astype(f32) / count, slice(r * 128, (r + 1) * 128), scale_v)

        def step(t, c):
            @pl.when(t > 0)
            def _():
                z_copy(t - 1, 1).start()
            start_events(t)

            @pl.when(t > 0)
            def _():
                z_copy(t - 1, 0).wait()
            statistics(t - 1, 1)
            product(t, 0)
            z_copy(t, 0).start()
            middle_events(t)

            @pl.when(t > 0)
            def _():
                z_copy(t - 1, 1).wait()
            statistics(t, 0)
            product(t, 1)
            return c
        last = TILES - 1
        lax.fori_loop(0, TILES, step, 0)
        z_copy(last, 1).start()
        statistics(last, 1)

        def finish(i, c):
            for u in range(8):
                r = i * 8 + u
                rows = pl.ds(pl.multiple_of(r * 128, 128), 128)
                m = m_s[rows, :]
                top = jnp.max(m, axis=-1, keepdims=True)
                tot = jnp.sum(s_s[rows, :] * jnp.exp(m - top), axis=-1, keepdims=True)
                lse = jnp.broadcast_to(top + jnp.log(tot), (128, 128))
                tgt = jnp.broadcast_to(jnp.sum(t_s[rows, :], axis=-1, keepdims=True), (128, 128))
                m_s[rows, :] = lse
                stat_v[0, pl.ds(r, 1), :] = jnp.transpose(lse)[0:1, :]
                stat_v[1, pl.ds(r, 1), :] = jnp.transpose(tgt)[0:1, :]
            return c
        lax.fori_loop(0, TOK // 1024, finish, 0)
        for h in range(2):
            z_copy(last, h).wait()
        half = e_all.at[pl.ds(0, ROWS // 2)]
        pltpu.make_async_copy(half, half, xs_send).wait()
        pltpu.make_async_copy(half, half, ys_send).wait()
        full = e_all.at[pl.ds(0, ROWS)]
        pltpu.make_async_copy(full, full, ds_send).wait()
        pltpu.make_async_copy(full, full, pe_send).wait()
        pltpu.make_async_copy(stat_v, stat_all.at[tp], small_sem.at[1]).start()
        for p, dev in group:
            remote(stat_v, stat_all.at[tp], sm_send, stat_recv.at[p], dev).start()

        def start_xt(j, c):
            xt_copy(j).start()
            return c
        lax.fori_loop(1, XCHS - 1, start_xt, 0)
        for q in range(4):
            last_part(q)[0].start()
        xp_copy.start()

    def z_load(zt, k, h):
        slot = lax.rem(k, 2)
        rows = slice(h * HB, (h + 1) * HB)
        return pltpu.make_async_copy(
            z_out.at[rows, pl.ds(pl.multiple_of(k * KT, KT), KT)], zt.at[slot, rows], zt_sem.at[2 * h + slot])

    def et_load(et, k):
        slot = lax.rem(k, 2)
        return pltpu.make_async_copy(e_all.at[pl.ds(pl.multiple_of(k * KT, KT), KT)], et.at[slot], et_sem.at[slot])

    def dzt_copy(k):
        rows = pl.ds(pl.multiple_of(lax.rem(k, 4) * KT, KT), KT)
        return remote(dzt_out.at[rows], dzt_part.at[rows], dz_send, dz_recv.at[lax.rem(k, 4)], part)

    def token_count():
        return jnp.sum(infos[:, 1].astype(f32))

    def token_grads(lse_v, scale_v, tcol_v, mr, zt, et, acc):
        def d_phase(da, db, dzt):
            def dzt_store(k, ref):
                slot = lax.rem(k, 2)
                return pltpu.make_async_copy(dzt.at[slot], ref.at[pl.ds(pl.multiple_of(lax.rem(k, 4) * KT, KT), KT)], eo_sem.at[slot])
            lane = lax.broadcasted_iota(jnp.int32, (PIECE, 128), 1)

            def piece(dst, rows, low, k, tie):
                slot = lax.rem(k, 2)
                lse = lse_v[rows, :]
                if tie is not None:
                    floor = 0.0 - jnp.maximum(0.0 - tie, -LOWEST)
                    lse = jnp.maximum(lse, jnp.concatenate([floor] * (PIECE // 8), axis=0))
                scale = scale_v[rows, :]
                diff = tcol_v[rows, :] - k * KT
                for g in range(KT // 128):
                    cols = slice(g * 128, (g + 1) * 128)
                    hot = (diff == lane + g * 128).astype(f32)
                    val = (jnp.exp(zt[slot, rows, cols] - lse) - hot) * scale
                    dst[low, cols] = val.astype(bf16)

            def half_step(k, src, dst, base, dst_base, dst_k):
                slot = lax.rem(k, 2)
                per = HB // (DIM // NCOL)
                for n in range(DIM // NCOL):
                    cols = slice(n * NCOL, (n + 1) * NCOL)
                    prod = jnp.dot(src[...], et[slot, :, cols], preferred_element_type=f32)
                    acc[base:base + HB, cols] = jnp.where(k == 0, 0.0, acc[base:base + HB, cols]) + prod
                    for q in range(0, per, PIECE):
                        at = q * HB // per
                        low = n * per + q
                        piece(dst, slice(dst_base + low, dst_base + low + PIECE), slice(low, low + PIECE), dst_k, prod[at:at + 8, 0:128])
                    if n * per % 256 == 0:
                        low = n * per
                        dzt[slot, :, base + low:base + low + 256] = jnp.transpose(src[low:low + 256, :])

            z_load(zt, 0, 0).wait()

            def first(i, c):
                rows = pl.ds(pl.multiple_of(i * PIECE, PIECE), PIECE)
                piece(da, rows, rows, 0, None)
                return c
            lax.fori_loop(0, HB // PIECE, first, 0)

            def step(k, c):
                @pl.when(k + 2 < VOCAB // KT)
                def _():
                    z_load(zt, k + 2, 0).start()

                @pl.when(k + 1 < VOCAB // KT)
                def _():
                    z_load(zt, k + 1, 1).start()
                    et_load(et, k + 1).start()
                    z_load(zt, k + 1, 0).wait()
                for at, j in WAIT_STEP.items():
                    @pl.when(k == at)
                    def _(j=j):
                        xt_event(j)

                @pl.when((k >= 2) & (k < 10))
                def _():
                    dzt_store(k, dzt_own).wait()

                @pl.when((k >= 6) & (k < 10))
                def _():
                    dzt_copy(k - 2).start()
                et_load(et, k).wait()
                z_load(zt, k, 1).wait()
                half_step(k, da, db, 0, HB, k)
                half_step(k, db, da, HB, 0, k + 1)

                @pl.when(k < 4)
                def _():
                    dzt_store(k, dzt_own).start()

                @pl.when((k >= 4) & (k < 8))
                def _():
                    dzt_store(k, dzt_out).start()
                return c
            lax.fori_loop(0, VOCAB // KT, step, 0)
        half = pltpu.VMEM((HB, KT), bf16)
        pl.run_scoped(d_phase, half, half, pltpu.VMEM((2, KT, TOK), bf16))

        def n_phase(hb, ob):
            def h_load(i):
                slot = lax.rem(i, 2)
                return pltpu.make_async_copy(hid.at[pl.ds(pl.multiple_of(i * NB_ROWS, NB_ROWS), NB_ROWS)], hb.at[slot], z_sem.at[slot])

            def o_store(i):
                slot = lax.rem(i, 2)
                return pltpu.make_async_copy(ob.at[slot], dhid.at[pl.ds(pl.multiple_of(i * NB_ROWS, NB_ROWS), NB_ROWS)], e_sem.at[slot])
            h_load(0).start()
            gb_v[...] = jnp.zeros(gb_v.shape, jnp.float32)
            g8[...] = jnp.broadcast_to(gain[...], (8, DIM))

            def tile(i, c):
                slot = lax.rem(i, 2)

                @pl.when(i + 1 < TOK // NB_ROWS)
                def _():
                    h_load(i + 1).start()

                @pl.when(i >= 2)
                def _():
                    o_store(i - 2).wait()
                h_load(i).wait()

                def rows_body(r, c2):
                    units = range(NB_UNROLL)
                    base = r * 16 * NB_UNROLL
                    low = [pl.ds(pl.multiple_of(base + u * 16, 16), 16) for u in units]
                    row = [pl.ds(pl.multiple_of(i * NB_ROWS + base + u * 16, 16), 16) for u in units]
                    zero = jnp.zeros((16, 128), jnp.float32)
                    sum1, sum3 = [zero] * NB_UNROLL, [zero] * NB_UNROLL

                    def load(u, cols):
                        dx = acc[row[u], cols]
                        xhat = (hb[slot, low[u], cols].astype(jnp.float32) - mr[0, row[u], :]) * mr[1, row[u], :]
                        return dx, xhat, dx * jnp.concatenate([g8[:, cols]] * 2, axis=0)
                    for k in range(DIM // 128):
                        cols = slice(k * 128, (k + 1) * 128)
                        d_gain, d_bias = gb_v[0, :, cols], gb_v[1, :, cols]
                        for u in units:
                            dx, xhat, gx = load(u, cols)
                            sum1[u] = sum1[u] + gx
                            sum3[u] = sum3[u] + gx * xhat
                            dgx = dx * xhat
                            d_gain = d_gain + (dgx[0:8] + dgx[8:16])
                            d_bias = d_bias + (dx[0:8] + dx[8:16])
                        gb_v[0, :, cols] = d_gain
                        gb_v[1, :, cols] = d_bias
                    slope, shift = [], []
                    for u in units:
                        mean, rstd = mr[0, row[u], :], mr[1, row[u], :]
                        c1 = jnp.broadcast_to(jnp.sum(sum1[u], axis=-1, keepdims=True) * (1.0 / DIM), (16, 128))
                        c3 = jnp.broadcast_to(jnp.sum(sum3[u], axis=-1, keepdims=True) * (1.0 / DIM), (16, 128))
                        slope.append(c3 * rstd * rstd)
                        shift.append(slope[u] * mean - c1 * rstd)
                    for u in units:
                        rstd = mr[1, row[u], :]
                        for k in range(DIM // 128):
                            cols = slice(k * 128, (k + 1) * 128)
                            gx = acc[row[u], cols] * jnp.concatenate([g8[:, cols]] * 2, axis=0)
                            ob[slot, low[u], cols] = (gx * rstd - hb[slot, low[u], cols].astype(f32) * slope[u] + shift[u]).astype(bf16)
                    return c2
                lax.fori_loop(0, NB_ROWS // (16 * NB_UNROLL), rows_body, 0)
                o_store(i).start()
                return c
            lax.fori_loop(0, TOK // NB_ROWS, tile, 0)
            for i in range(2):
                o_store(TOK // NB_ROWS - 2 + i).wait()
            gs_v[0:1, :] = jnp.sum(gb_v[0], axis=0, keepdims=True)
            gs_v[1:2, :] = jnp.sum(gb_v[1], axis=0, keepdims=True)
        pl.run_scoped(n_phase, pltpu.VMEM((2, NB_ROWS, DIM), bf16), pltpu.VMEM((2, NB_ROWS, DIM), bf16))

    def weight_grads(acc):
        own = pltpu.make_async_copy(gs_v, gsum_all.at[tp], g_sem)

        def e_phase(eo, xt, dzb, zs, z1):
            eo_load = pltpu.make_async_copy(emb, eo, big_sem)

            def x_load(ref, row, slot):
                return pltpu.make_async_copy(ref.at[pl.ds(pl.multiple_of(row, KT), KT)], xt.at[slot], z_sem.at[slot])

            def dz_load(ref, col, slot):
                return pltpu.make_async_copy(ref.at[:, pl.ds(pl.multiple_of(col, KT), KT)], dzb.at[slot], e_sem.at[slot])

            def start_local(i):
                slot = lax.rem(i, 2)

                @pl.when(i < 4)
                def _():
                    x_load(x_out, i * KT, slot).start()
                    dz_load(dzt_own, i * KT, slot).start()

                @pl.when(i >= 4)
                def _():
                    x_load(x_part, (i - 4) * KT, slot).start()
                    dz_load(dzt_part, (i - 4) * KT, slot).start()

            def add(slot, first):
                def mul(h, c2):
                    rows = pl.ds(pl.multiple_of(h * HB, HB), HB)
                    for n in range(0, DIM, NCOL):
                        prod = jnp.dot(dzb[slot, rows, :], xt[slot, :, n:n + NCOL], preferred_element_type=f32)
                        acc[rows, n:n + NCOL] = jnp.where(first, 0.0, acc[rows, n:n + NCOL]) + prod
                    return c2
                lax.fori_loop(0, HBS, mul, 0)

            start_local(0)

            def rem_load(r):
                slot = lax.rem(r, 2)
                return [pltpu.make_async_copy(xrows(ref, r), xt.at[slot, pl.ds(i * XCH, XCH)], z_sem.at[slot])
                        for i, ref in enumerate((x_xp, x_xq))]

            def local(i, c):
                slot = lax.rem(i, 2)

                @pl.when(i == 0)
                def _():
                    eo_load.start()

                @pl.when(i == 2)
                def _():
                    xp_copy.wait_recv()

                    def wait_dz(q, c2):
                        dzt_copy(q).wait_recv()
                        return c2
                    lax.fori_loop(0, 4, wait_dz, 0)

                @pl.when(i == 1)
                def _():
                    own.start()
                    for p, dev in group:
                        remote(gs_v, gsum_all.at[tp], g_send, g_recv.at[p], dev).start()

                @pl.when(i == 1)
                def _():
                    xt_event(3)

                @pl.when(i == 6)
                def _():
                    xt_event(4)

                @pl.when(i < 7)
                def _():
                    start_local(i + 1)

                @pl.when(i == 7)
                def _():
                    xd_copy(0).wait_recv()
                    for cp in rem_load(0):
                        cp.start()
                x_load(x_out, 0, slot).wait()
                dz_load(dzt_own, 0, slot).wait()
                add(slot, i == 0)
                return c
            lax.fori_loop(0, 8, local, 0)
            eo_load.wait()
            for p, dev in group:
                remote(stat_v, stat_all.at[tp], sm_send, stat_recv.at[p], dev).wait_recv()
            pltpu.make_async_copy(stat_v, stat_all.at[tp], small_sem.at[1]).wait()
            for cp in info_copies(0):
                cp.wait_recv()
            loads = [pltpu.make_async_copy(stat_all, stats, small_sem.at[1])]
            loads += [pltpu.make_async_copy(info_all.at[q, 0], infos.at[q, 0], small_sem.at[0]) for q in range(4)]
            for load in loads:
                load.start()
            for load in loads:
                load.wait()
            count = jnp.broadcast_to(token_count(), (1, 128))

            def far(r, c):
                slot = lax.rem(r, 2)

                @pl.when(r == 2)
                def _():
                    xt_event(5)

                @pl.when(r == 4)
                def _():
                    xt_event(6)

                def fetch():
                    xd_copy(r + 1).wait_recv()
                    for cp in rem_load(r + 1):
                        cp.start()
                pl.when(r < XCHS - 2)(fetch)
                x_load(x_out, 0, slot).wait()

                @pl.when(r == XCHS - DEFER)
                def _():
                    pltpu.make_async_copy(acc, de_part, big_sem).start()

                @pl.when(r > XCHS - DEFER + 1)
                def _():
                    dz_out(0, slot).wait()

                far_rows = []
                for g in range(4):
                    who = xp_rank if g < 2 else xq_rank
                    at = pl.ds(2 * r + g % 2, 1)
                    far_rows.append((stats[who, 0, at, :], infos[who, 1, at, :].astype(f32) / count, infos[who, 0, at, :] - tp * ROWS))

                def logits(h2, c2):
                    @pl.when((r == XCHS - 2) & (h2 == 1))
                    def _():
                        for q in range(3):
                            last_event(q)

                    def multiply(h, z):
                        for k in range(0, DIM, KCOL):
                            prod = lax.dot_general(eo[pl.ds(pl.multiple_of(h * ZB, ZB), ZB), k:k + KCOL], xt[slot, :, k:k + KCOL], NT, preferred_element_type=f32)
                            z[...] = prod if k == 0 else z[...] + prod

                    def convert(h, z):
                        for q in range(ZB // 32):
                            row = h * ZB + q * 32
                            line = lax.broadcasted_iota(jnp.int32, (32, 128), 0)
                            for g, (lse, scale, trel) in enumerate(far_rows):
                                cols = slice(g * 128, (g + 1) * 128)
                                hot = ((trel - row) == line).astype(f32)
                                val = (jnp.exp(z[q * 32:(q + 1) * 32, cols] - lse) - hot) * scale
                                dzb[slot, pl.ds(pl.multiple_of(row, 32), 32), cols] = val.astype(bf16)
                    multiply(2 * h2, zs)
                    multiply(2 * h2 + 1, z1)
                    convert(2 * h2, zs)
                    convert(2 * h2 + 1, z1)
                    return c2
                lax.fori_loop(0, ROWS // (2 * ZB), logits, 0)

                @pl.when(r == XCHS - 2)
                def _():
                    last_event(3)

                @pl.when(r < XCHS - DEFER)
                def _():
                    def mul(h, c2):
                        rows = pl.ds(pl.multiple_of(h * HB, HB), HB)
                        for n in range(0, DIM, NCOL):
                            acc[rows, n:n + NCOL] += jnp.dot(dzb[slot, rows, :], xt[slot, :, n:n + NCOL], preferred_element_type=jnp.float32)
                        return c2
                    lax.fori_loop(0, HBS, mul, 0)

                @pl.when(r >= XCHS - DEFER)
                def _():
                    dz_out(r - (XCHS - DEFER), slot).start()
                return c

            def dz_out(q, slot):
                return pltpu.make_async_copy(dzb.at[slot], dzt_last.at[q], dzo_sem.at[slot])
            lax.fori_loop(0, XCHS - 1, far, 0)
            for slot in range(2):
                dz_out(0, slot).wait()
            xd_copy(XCHS - 1).wait_recv()
            pltpu.make_async_copy(acc, de_part, big_sem).wait()
        pl.run_scoped(e_phase, pltpu.VMEM((ROWS, DIM), jnp.bfloat16), pltpu.VMEM((2, KT, DIM), jnp.bfloat16),
                      pltpu.VMEM((2, ROWS, KT), jnp.bfloat16), pltpu.VMEM((ZB, KT), f32), pltpu.VMEM((ZB, KT), f32))

        own.wait()

    wide = pltpu.VMEM((TOK, 128), f32)
    big = pltpu.VMEM((TOK, DIM), f32)

    def tokens(m_s, scale_v, tc_v, mr_v, zt, et):
        kept = (m_s, scale_v, tc_v, mr_v, zt, et)
        pl.run_scoped(functools.partial(forward, *kept), pltpu.VMEM((TOK, DIM), bf16), pltpu.VMEM((2, LN_ROWS, DIM), bf16),
                      pltpu.VMEM((2, TILE, DIM), bf16), pltpu.VMEM((HB, TILE), f32), pltpu.VMEM((HB, TILE), f32), wide, wide,
                      pltpu.VMEM((2, 8, DIM), f32))
        pl.run_scoped(functools.partial(token_grads, *kept), big)
    pl.run_scoped(tokens, wide, wide, pltpu.VMEM((TOK, 128), jnp.int32), pltpu.VMEM((2, TOK, 128), f32),
                  pltpu.VMEM((2, TOK, KT), f32), pltpu.VMEM((2, KT, DIM), bf16))
    pl.run_scoped(weight_grads, big)

    pltpu.make_async_copy(x_out, x_out, xt_send).wait()
    pltpu.make_async_copy(x_out, x_out, xd_send).wait()
    xp_copy.wait_send()
    pltpu.make_async_copy(dzt_out, dzt_out, dz_send).wait()
    for cp in (*info_copies(0), *info_copies(1)):
        cp.wait_send()
    for p, dev in group:
        remote(stat_v, stat_all.at[tp], sm_send, stat_recv.at[p], dev).wait_send()
        remote(gs_v, gsum_all.at[tp], g_send, g_recv.at[p], dev).wait()


def run_step(hidden, gain, bias, embed, targets, mask):
    any_spec = pl.BlockSpec(memory_space=pl.ANY)
    vmem_spec = pl.BlockSpec(memory_space=pltpu.VMEM)
    f32, bf16, i32 = jnp.float32, jnp.bfloat16, jnp.int32
    dma = pltpu.SemaphoreType.DMA
    small, ints = (4, 2, GROUPS, 128), (4, 2, GROUPS, 128)
    mat, square = ((TOK, DIM), bf16), ((ROWS, TOK), bf16)
    shapes = [((VOCAB, DIM), bf16), mat, ((TOK, VOCAB), f32), (small, f32), (ints, i32),
              mat, mat, mat, mat, square, square, square, ((DEFER - 1, ROWS, KT), bf16), ((ROWS, DIM), f32), ((4, 2, DIM), f32)]
    return pl.pallas_call(
        step_kernel,
        name="step",
        out_shape=[jax.ShapeDtypeStruct(s, d) for s, d in shapes],
        in_specs=[any_spec, vmem_spec, vmem_spec, any_spec, vmem_spec, vmem_spec],
        out_specs=[any_spec] * len(shapes),
        scratch_shapes=[
            pltpu.VMEM((GROUPS, 128), i32), pltpu.VMEM((2, GROUPS, 128), f32), pltpu.VMEM(small, f32), pltpu.VMEM(ints, i32),
            pltpu.VMEM((2, 8, DIM), f32), pltpu.VMEM((2, DIM), f32), pltpu.VMEM((8, DIM), f32),
            dma((2,)), dma, dma((2,)), dma((2,)), dma((2,)), dma((4,)), dma((2,)), dma((2,)), dma((2,)), dma, dma,
            dma, dma, dma, dma, dma, dma, dma, dma, dma, dma,
            dma((CHUNKS,)), dma((CHUNKS,)), dma((TILES - NEAR,)), dma((ROWS // PE_ROWS,)), dma((8,)), dma((4,)),
            dma((XCHS + 3,)), dma((XCHS,)), dma, dma((4,)), dma((4,)),
        ],
        compiler_params=pltpu.CompilerParams(collective_id=0, has_side_effects=True, vmem_limit_bytes=67043328),
        cost_estimate=pl.CostEstimate(flops=12 * TOK * VOCAB * DIM, bytes_accessed=700 * 2 ** 20, transcendentals=3 * TOK * VOCAB),
    )(hidden, gain, bias, embed, targets, mask)


def finish_kernel(de_in, dzt_last, x_xp, x_xq, emb, dh_in, stat_all, info_all, gsum_all,
                  de_out, dh_out, loss, mean, d_gain, d_bias,
                  x7, xr, dz, eb, zs, din, dout, hb, x_sem, z_sem, e_sem, di_sem, do_sem, hi_sem, ho_sem):
    f32, bf16 = jnp.float32, jnp.bfloat16
    last = DEFER - 1

    def x_last():
        rows = pl.ds((XCHS - 1) * XCH, XCH)
        return [pltpu.make_async_copy(ref.at[rows], x7.at[pl.ds(i * XCH, XCH)], x_sem.at[3]) for i, ref in enumerate((x_xp, x_xq))]

    def x_tiles(i):
        slot = lax.rem(i, 3)
        cols = pl.ds(pl.multiple_of(i * KT, KT), KT)
        rows = pl.ds((XCHS - DEFER) * XCH, last * XCH)
        return [pltpu.make_async_copy(ref.at[rows, cols], xr.at[slot, j], x_sem.at[slot]) for j, ref in enumerate((x_xp, x_xq))]

    def e_load(h):
        slot = lax.rem(h, 2)
        return pltpu.make_async_copy(emb.at[pl.ds(pl.multiple_of(h * ZB, ZB), ZB)], eb.at[slot], e_sem.at[slot])

    def z_load(q):
        return pltpu.make_async_copy(dzt_last.at[q], dz.at[q], z_sem.at[q])

    def tile(ref, i):
        return ref.at[:, pl.ds(pl.multiple_of(i * KT, KT), KT)]

    def d_load(i):
        slot = lax.rem(i, 3)
        return pltpu.make_async_copy(tile(de_in, i), din.at[slot], di_sem.at[slot])

    def d_store(i):
        slot = lax.rem(i, 3)
        return pltpu.make_async_copy(dout.at[slot], tile(de_out, i), do_sem.at[slot])
    steps = DIM // KT
    per = TOK // steps

    def h_load(i):
        slot = lax.rem(i, 2)
        return pltpu.make_async_copy(dh_in.at[pl.ds(pl.multiple_of(i * per, per), per)], hb.at[slot], hi_sem.at[slot])

    def h_store(i):
        slot = lax.rem(i, 2)
        return pltpu.make_async_copy(hb.at[slot], dh_out.at[pl.ds(pl.multiple_of(i * per, per), per)], ho_sem.at[slot])
    for cp in x_last():
        cp.start()
    e_load(0).start()
    e_load(1).start()

    def tile_loads(i):
        for cp in (*x_tiles(i), d_load(i)):
            cp.start()

    tp = lax.axis_index('tp')
    core = lax.rem(tp, 2)
    other = 2 - (tp - core)
    weights = info_all[:, 1].astype(f32)
    total = jnp.sum(weights)
    all_loss = (stat_all[:, 0] - stat_all[:, 1]) * weights
    loss[...] = (stat_all[tp, 0] - stat_all[tp, 1]) * info_all[tp, 1].astype(f32)
    mean[...] = jnp.broadcast_to(jnp.sum(all_loss), (1, 1)) / jnp.broadcast_to(total, (1, 1))
    sums = ((gsum_all[0] + gsum_all[1]) + gsum_all[2]) + gsum_all[3]
    d_gain[...] = sums[0:1]
    d_bias[...] = sums[1:2]
    count = jnp.broadcast_to(total, (1, 128))
    far_rows = []
    for g in range(4):
        who = other + core if g < 2 else other + 1 - core
        at = slice(GROUPS - 2 + g % 2, GROUPS - 1 + g % 2)
        far_rows.append((stat_all[who, 0, at, :], info_all[who, 1, at, :].astype(f32) / count, info_all[who, 0, at, :] - tp * ROWS))
    pltpu.make_async_copy(x7, x7, x_sem.at[3]).wait()

    def logits(h, c):
        slot = lax.rem(h, 2)
        e_load(h).wait()
        for k in range(0, DIM, KCOL):
            prod = lax.dot_general(eb[slot, :, k:k + KCOL], x7[:, k:k + KCOL], NT, preferred_element_type=f32)
            zs[...] = prod if k == 0 else zs[...] + prod

        @pl.when(h == 0)
        def _():
            e_load(2).start()
            z_load(0).start()
            z_load(1).start()

        @pl.when(h == 1)
        def _():
            e_load(3).start()
            for q in range(2, last):
                z_load(q).start()

        @pl.when(h == 2)
        def _():
            tile_loads(0)
            h_load(0).start()

        @pl.when(h == 3)
        def _():
            tile_loads(1)
        for q in range(ZB // 32):
            row = h * ZB + q * 32
            line = lax.broadcasted_iota(jnp.int32, (32, 128), 0)
            for g, (lse, scale, trel) in enumerate(far_rows):
                cols = slice(g * 128, (g + 1) * 128)
                hot = ((trel - row) == line).astype(f32)
                val = (jnp.exp(zs[q * 32:(q + 1) * 32, cols] - lse) - hot) * scale
                dz[last, pl.ds(pl.multiple_of(row, 32), 32), cols] = val.astype(bf16)
        return c
    lax.fori_loop(0, ROWS // ZB, logits, 0)
    for q in range(last):
        z_load(q).wait()

    def step(i, c):
        slot = lax.rem(i, 3)
        cols = pl.ds(pl.multiple_of(i * KT, KT), KT)

        @pl.when(i + 2 < steps)
        def _():
            tile_loads(i + 2)
        h_load(i).wait()
        h_store(i).start()

        @pl.when(i >= 1)
        def _():
            h_store(i - 1).wait()

        @pl.when(i + 1 < steps)
        def _():
            h_load(i + 1).start()

        @pl.when(i >= 3)
        def _():
            d_store(i - 3).wait()
        d_load(i).wait()
        for cp in x_tiles(i):
            cp.wait()
        for h in range(HBS):
            rows = slice(h * HB, (h + 1) * HB)
            prod = jnp.dot(dz[last, rows, :], x7[:, cols], preferred_element_type=f32)
            for q in range(last):
                for j in range(2):
                    prod = prod + jnp.dot(dz[q, rows, j * XCH:(j + 1) * XCH], xr[slot, j, q * XCH:(q + 1) * XCH, :], preferred_element_type=f32)
            dout[slot, rows, :] = din[slot, rows, :] + prod
        d_store(i).start()
        return c
    lax.fori_loop(0, steps, step, 0)
    for i in range(3):
        d_store(steps - 3 + i).wait()
    h_store(steps - 1).wait()


def finish(de_part, dzt_last, x_xp, x_xq, embed, dhid, stat_all, info_all, gsum_all):
    any_spec = pl.BlockSpec(memory_space=pl.ANY)
    vmem_spec = pl.BlockSpec(memory_space=pltpu.VMEM)
    f32, bf16 = jnp.float32, jnp.bfloat16
    dma = pltpu.SemaphoreType.DMA
    outs = [((ROWS, DIM), f32), ((TOK, DIM), bf16), ((GROUPS, 128), f32), ((1, 1), f32), ((1, DIM), f32), ((1, DIM), f32)]
    return pl.pallas_call(
        finish_kernel,
        name="finish",
        out_shape=[jax.ShapeDtypeStruct(s, d) for s, d in outs],
        in_specs=[any_spec] * 6 + [vmem_spec] * 3,
        out_specs=[any_spec] * 2 + [vmem_spec] * 4,
        scratch_shapes=[
            pltpu.VMEM((KT, DIM), bf16), pltpu.VMEM((3, 2, (DEFER - 1) * XCH, KT), bf16), pltpu.VMEM((DEFER, ROWS, KT), bf16), pltpu.VMEM((2, ZB, DIM), bf16), pltpu.VMEM((ZB, KT), f32),
            pltpu.VMEM((3, ROWS, KT), f32), pltpu.VMEM((3, ROWS, KT), f32), pltpu.VMEM((2, TOK // (DIM // KT), DIM), bf16),
            dma((4,)), dma((DEFER,)), dma((2,)), dma((3,)), dma((3,)), dma((2,)), dma((2,)),
        ],
        compiler_params=pltpu.CompilerParams(vmem_limit_bytes=67043328),
        cost_estimate=pl.CostEstimate(flops=2 * ROWS * DIM * KT * (DEFER + 1), bytes_accessed=130 * 2 ** 20, transcendentals=ROWS * KT),
    )(de_part, dzt_last, x_xp, x_xq, embed, dhid, stat_all, info_all, gsum_all)


def solution(mesh):
    def body(hidden, ln_gain, ln_bias, embed, targets, loss_mask):
        outs = run_step(hidden, ln_gain.reshape(1, DIM), ln_bias.reshape(1, DIM), embed, targets.reshape(GROUPS, 128), loss_mask.reshape(GROUPS, 128))
        stat_all, info_all, dhid, x_xp, x_xq, dzt_last, de_part, gsum_all = (outs[i] for i in (3, 4, 5, 7, 8, 12, 13, 14))
        d_embed, d_hidden, loss, mean, d_gain, d_bias = finish(de_part, dzt_last, x_xp, x_xq, embed, dhid, stat_all, info_all, gsum_all)
        return loss.reshape(TOK), mean.reshape(1), d_hidden, d_embed, d_gain.reshape(DIM), d_bias.reshape(DIM)

    token_rows = P(('dp', 'tp'))
    token_mat = P(('dp', 'tp'), None)
    return jax.shard_map(body, mesh=mesh, in_specs=(token_mat, P(), P(), P('tp', None), token_rows, token_rows), out_specs=(token_rows, P('dp'), token_mat, token_mat, P('dp'), P('dp')), check_vma=False)
```
